256 devices in a mesh: tm: 8 (over x, core), space: 32 (over z, y).
Axes of the slice: x: 4, y: 4, z: 8, core: 2. Of those that a mesh axis runs over, the one named last changes fastest.
Arguments:
- span_opening: float32 [8, 128, 64, 128], P('tm', 'space'), may hold values from -8 to 8
- source_power: float32 [8, 2, 128, 64, 128], P('tm', None, 'space'), may hold values from -24 to 24
- warmth_retention: float32 [128, 64, 128], P('space'), may hold values from 0.02 to 0.4
Outputs:
- fpoint: float32 [8, 128, 64, 128], P('tm', 'space')
- updated: float32 [8, 128, 64, 128], P('tm', 'space')
The draws below stay inside these ranges and needn't reach their ends.
All inputs are finite; a program needn't handle non-finite values.
Results may differ from the reference program's by a relative error of at most 0.0001.
Values sent between devices are 32-bit elements; how exact they have to be, the bound alone decides.
A program may use at most 64 MiB of HBM per device.

```python
import math
import jax
import jax.numpy as jnp

NY = 64
NX = 128
STEPS = 2
COARSE_SWEEPS = 24
GROUPS = 8
NZ = 128


def draw_source_power(key, part):
    rough = 4.0 * jax.random.normal(key, (GROUPS, STEPS, NZ, NY, NX), jnp.float32)
    return jnp.clip(rough, -24.0, 24.0)


def shard_levels(rng, extent, pieces, smallest, largest):
    level, own = 1.0, jax.random.fold_in(rng, 6)
    for axis_at, blocks in pieces:
        steps = jnp.exp(jax.random.uniform(jax.random.fold_in(own, axis_at), (blocks,), jnp.float32, smallest / len(pieces), largest / len(pieces)))
        level = level * jnp.repeat(steps, extent[axis_at] // blocks).reshape([-1 if axis == axis_at else 1 for axis in range(len(extent))])
    return level


def scatter_about(own_key, shape, scale, reach, cuts=(), held_as=jnp.bfloat16):
    loudness = shard_levels(own_key, shape, cuts, -0.22, 0.18) if cuts else 1.0
    result = jax.random.normal(own_key, shape, jnp.float32) * scale * loudness
    return jnp.minimum(jnp.maximum(result, -reach), reach).astype(held_as)


def setup_inputs(seed: int = 0) -> dict:
    arg_keys = jax.random.split(jax.random.key(seed), 4)
    span_opening = scatter_about(arg_keys[0], (GROUPS, NZ, NY, NX), 2.0, 8.0, ((0, 8), (1, 32)), jnp.float32)
    source_power = draw_source_power(jax.random.fold_in(arg_keys[3], 71), 0)
    warmth_retention = jnp.clip(jnp.exp(math.log(0.4) - 2.9957323 * jax.random.uniform(arg_keys[2], (NZ, NY, NX), jnp.float32) ** shard_levels(arg_keys[2], (NZ, NY, NX), ((0, 32),), -0.2, 0.2)), 0.02, 0.4)
    return {"span_opening": span_opening, "source_power": source_power, "warmth_retention": warmth_retention}


relax_weight = 0.8


def mean_to_rougher(field):
    extent_layout = field.shape
    blocks = field.reshape(extent_layout[0] // 2, 2, extent_layout[1] // 2, 2, extent_layout[2] // 2, 2)
    return blocks.mean(axis=(1, 3, 5))


def lift_to_finer(field):
    extent_layout = field.shape
    grown = jnp.broadcast_to(field[:, None, :, None, :, None], (extent_layout[0], 2, extent_layout[1], 2, extent_layout[2], 2))
    return grown.reshape(2 * extent_layout[0], 2 * extent_layout[1], 2 * extent_layout[2])


def neighbour_sum(field, padded):
    flat = jnp.pad(field, ((0, 0), (1, 1), (1, 1)))
    total = padded[2:] + padded[:-2]
    total = total + flat[:, 2:, 1:-1] + flat[:, :-2, 1:-1]
    return total + flat[:, 1:-1, 2:] + flat[:, 1:-1, :-2]


def apply_nearby_part(field, retention_quantities, conductance):
    padded = jnp.pad(field, ((1, 1), (0, 0), (0, 0)))
    return (retention_quantities + 6.0 * conductance) * field - conductance * neighbour_sum(field, padded)


def bottom_grid_inversion(load_components, retention_quantities):
    conductance = 0.125
    diagonal = retention_quantities + 6.0 * conductance
    first_approximation = relax_weight * load_components / diagonal
    for sweep_index in range(COARSE_SWEEPS - 1):
        first_approximation = first_approximation + relax_weight * (load_components - apply_nearby_part(first_approximation, retention_quantities, conductance)) / diagonal
    return first_approximation


def personal_hierarchy_cycle(load_components, volume_holdings, hierarchy_layers):
    if hierarchy_layers == 3:
        return bottom_grid_inversion(load_components, volume_holdings[3])
    conductance = 0.5 ** hierarchy_layers
    retention_quantities = volume_holdings[hierarchy_layers]
    diagonal = retention_quantities + 6.0 * conductance
    first_approximation = relax_weight * load_components / diagonal
    first_approximation = first_approximation + relax_weight * (load_components - apply_nearby_part(first_approximation, retention_quantities, conductance)) / diagonal
    further_moments = load_components - apply_nearby_part(first_approximation, retention_quantities, conductance)
    first_approximation = first_approximation + lift_to_finer(personal_hierarchy_cycle(mean_to_rougher(further_moments), volume_holdings, hierarchy_layers + 1))
    for sweep_index in range(2):
        first_approximation = first_approximation + relax_weight * (load_components - apply_nearby_part(first_approximation, retention_quantities, conductance)) / diagonal
    return first_approximation


def reference(span_opening, source_power, warmth_retention):
    volume_holdings = [warmth_retention]
    for level_index in range(3):
        volume_holdings.append(mean_to_rougher(volume_holdings[-1]))
    fpoints = []
    closing_results = []
    for moment_packet in range(GROUPS):
        warmth_distribution = span_opening[moment_packet]
        opening_condition = warmth_distribution
        for moment_count in range(STEPS):
            warmth_distribution = personal_hierarchy_cycle(warmth_retention * warmth_distribution + source_power[moment_packet, moment_count], volume_holdings, 0)
            if moment_count == 0:
                opening_condition = warmth_distribution
        fpoints.append(opening_condition)
        closing_results.append(warmth_distribution)
    updated = jnp.stack([span_opening[0]] + closing_results[:-1])
    return jnp.stack(fpoints), updated
```

```python
import functools

import jax
import jax.numpy as jnp
from jax import lax
from jax.experimental import pallas as pl
from jax.experimental.pallas import tpu as pltpu
from jax.sharding import PartitionSpec as P

COARSE_SWEEPS = 24
W = 0.8
GROUP = 32
NEAR = (1, 2, 3, 4, 8, 12)
F32 = jnp.float32
MESH = pl.DeviceIdType.MESH


def iota(shape, dim):
    return lax.broadcasted_iota(jnp.int32, shape, dim)


def dot(a, b):
    total = None
    for _ in range(3):
        part = a.astype(jnp.bfloat16)
        a = a - part.astype(F32)
        term = jnp.dot(part, b, preferred_element_type=F32)
        total = term if total is None else total + term
    return total


def picks(lanes, pick, scale):
    src, dst = iota((lanes, lanes), 0), iota((lanes, lanes), 1)
    return jnp.where(pick(src, dst), scale, 0.0).astype(jnp.bfloat16)


def in_plane(x, width):
    rows, lanes = x.shape[1], x.shape[2]
    lane, row = iota(x.shape, 2), iota(x.shape, 1)
    left, right = pltpu.roll(x, 1, 2), pltpu.roll(x, lanes - 1, 2)
    left = jnp.where(lane % width == 0, 0.0, left)
    right = jnp.where(lane % width == width - 1, 0.0, right)
    up = jnp.where(row == 0, 0.0, pltpu.roll(x, 1, 1))
    down = jnp.where(row == rows - 1, 0.0, pltpu.roll(x, rows - 1, 1))
    return (left + right) + (up + down)


def shifted(x):
    zero = jnp.zeros((1,) + x.shape[1:], F32)
    return jnp.concatenate([zero, x[:-1]], 0), jnp.concatenate([x[1:], zero], 0)


def earlier(x, by=1, shift=0):
    lanes = x.shape[2]
    moved = pltpu.roll(x[-by:], (GROUP + shift) % lanes, 2)
    return jnp.where(iota(moved.shape, 2) < GROUP, 0.0, moved)


def later(x, by=1, shift=0):
    lanes = x.shape[2]
    moved = pltpu.roll(x[:by], (lanes - GROUP + shift) % lanes, 2)
    return jnp.where(iota(moved.shape, 2) >= lanes - GROUP, 0.0, moved)


def before(x):
    return jnp.concatenate([earlier(x), x[:-1]], 0)


def after(x):
    return jnp.concatenate([x[1:], later(x)], 0)


def sum_grouped(x):
    return in_plane(x, GROUP) + (before(x) + after(x))


def sum_packed(x, width):
    half = pltpu.roll(x, width, 2)
    before, after = shifted(half)
    return in_plane(x, width) + (half + jnp.where(iota(x.shape, 2) < width, before, after))


def sum_inner(x, width):
    return in_plane(x[1:-1], width) + (x[:-2] + x[2:])


def column_sum(x):
    rows = x.shape[1]
    mid = x[1:-1]
    row = iota(mid.shape, 1)
    up = jnp.where(row == 0, 0.0, pltpu.roll(mid, 1, 1))
    down = jnp.where(row == rows - 1, 0.0, pltpu.roll(mid, rows - 1, 1))
    return (x[:-2] + x[2:]) + (up + down)


def coarse_solve(c, a):
    n, lanes = c.shape[0], c.shape[2]

    def turned(x, by):
        return x if by == 0 else pltpu.roll(x, by % lanes, 2)

    def longer(x, by, reach=1):
        return jnp.concatenate([earlier(x, reach, by), turned(x, by), later(x, reach, by)], 0)

    c_at, a_at = [[longer(x, 0) if by == 0 else turned(x, by) for by in (1, 0, -1)] for x in (c, a)]

    def sweep(y, side, c, a):
        return (0.2 * y[1:-1] + c) + a * (side + column_sum(y))

    def two_sweeps(_, y):
        left, mid, right = longer(y, 1), longer(y, 0, 2), longer(y, -1)
        once_left = sweep(left, turned(y, 2) + y, c_at[0], a_at[0])
        once_mid = sweep(mid, left + right, c_at[1], a_at[1])
        once_right = sweep(right, y + turned(y, -2), c_at[2], a_at[2])
        return sweep(once_mid, once_left + once_right, c, a)

    left = COARSE_SWEEPS - 1
    y = c
    if left % 2:
        y = 1.2 * c + a * sum_grouped(c)
    return lax.fori_loop(0, left // 2, two_sweeps, y, unroll=True)


def flat(x):
    return x.reshape(x.shape[0] * x.shape[1], x.shape[2])


def kernel(
    parts, spans, steps,
    open_ref, src_ref, cap_in,
    fp_ref, up_ref,
    u0, src0, src1, cap, c0, c1x, cw, vw, gr, y2s, own, tmp, fin,
    far_sem, in_sem, hs, hr, ks, kr, fs, fr, gs, gv, ws, wr, ts,
):
    me, span = lax.axis_index("space"), lax.axis_index("tm")
    depth, rows, lanes = open_ref.shape
    half = lanes // 2
    groups = lanes // GROUP
    stack = parts // groups
    assert parts % groups == 0 and lanes == 128 and rows == 64
    close = sorted({k % parts for k in NEAR} | {-k % parts for k in NEAR})
    assert {(a + b) % parts for a in close + [0] for b in close + [0]} == set(range(parts))

    cw[...] = jnp.zeros(cw.shape, F32)
    vw[...] = jnp.zeros(vw.shape, F32)

    barrier = pltpu.get_barrier_semaphore()
    for k in close:
        pl.semaphore_signal(barrier, inc=1, device_id={"space": (me + k) % parts}, device_id_type=MESH)
    for k in range(1, spans):
        pl.semaphore_signal(barrier, inc=1, device_id={"tm": (span + k) % spans}, device_id_type=MESH)

    loads = [
        pltpu.make_async_copy(cap_in, cap.at[pl.ds(depth, depth)], in_sem.at[0]),
        pltpu.make_async_copy(open_ref, u0, in_sem.at[1]),
        pltpu.make_async_copy(src_ref.at[0], src0, in_sem.at[2]),
        pltpu.make_async_copy(src_ref.at[1], src1.at[pl.ds(2, depth)], in_sem.at[3]),
    ]
    for load in loads:
        load.start()

    group = me // stack
    down_lo = picks(lanes, lambda s, d: (s // 2 == d) & (d < half), 0.125)
    down_hi = picks(lanes, lambda s, d: s // 2 + half == d, 0.125)
    down_2 = [
        picks(lanes, lambda s, d: (s % half) // 2 + GROUP * ((group + q) % groups) == d, 0.125)
        for q in range(groups)
    ]
    down_3 = picks(lanes, lambda s, d: s // GROUP * GROUP + s % GROUP // 2 == d, 0.125)
    up_lo = picks(lanes, lambda s, d: d // 2 == s, 1.0)
    up_hi = picks(lanes, lambda s, d: d // 2 + half == s, 1.0)
    up_2 = picks(lanes, lambda s, d: (d % half) // 2 == s, 1.0)
    up_3 = picks(lanes, lambda s, d: d // GROUP * GROUP + d % GROUP // 2 == s, 1.0)

    def pair_rows(x):
        n, r, w = x.shape
        tmp[pl.ds(0, n * r), :] = flat(x)
        return tmp[pl.ds(0, n * r // 2, 2), :] + tmp[pl.ds(1, n * r // 2, 2), :]

    def twice_rows(x, planes):
        r = x.shape[0]
        tmp[pl.ds(0, r, 2), :] = x
        tmp[pl.ds(1, r, 2), :] = x
        return tmp[pl.ds(0, 2 * r), :].reshape(planes, 2 * r // planes, lanes)

    def pack(x):
        s = pair_rows(x.reshape(depth // 2, 2, rows, lanes).sum(1))
        n = rows // 2
        return dot(s[:n], down_lo) + dot(s[n:], down_hi)

    def to_2(x, q):
        return dot(pair_rows(x), down_2[q])

    def to_3(x):
        s = x.reshape(stack // 2, 2, rows // 4, lanes).sum(1)
        return dot(pair_rows(s), down_3).reshape(stack // 2, rows // 8, lanes)

    def unpack(x, q):
        at = (iota((stack,) + x.shape[1:], 2) // GROUP + groups - q) % groups
        out = x[:stack]
        for g in range(1, groups):
            out = jnp.where(at == g, x[g * stack:(g + 1) * stack], out)
        return pltpu.roll(out, lanes - GROUP * q, 2) if q else out

    def within(k):
        return (me + k >= 0) & (me + k < parts)

    def window(buf, sends, recvs, reach):
        middle = buf.shape[0] // 2
        return [
            (k, pltpu.make_async_remote_copy(
                buf.at[middle], buf.at[middle - k], sends.at[middle + k], recvs.at[middle + k],
                device_id={"space": (me + k + parts) % parts}, device_id_type=MESH))
            for far in range(1, reach + 1) for k in (far, -far)
        ]

    def where_within(copies, sign, act):
        for k, copy in copies:
            @pl.when(within(sign * k))
            def _(copy=copy):
                act(copy)

    def window_start(copies):
        where_within(copies, 1, lambda copy: copy.start())

    def window_arrive(copies):
        where_within(copies, -1, lambda copy: copy.wait_recv())

    def window_sent(copies):
        where_within(copies, 1, lambda copy: copy.wait_send())

    def halo(buf, sends, recvs, at, count, up, down, reach=1, rows_at=None):
        def cut(start):
            return buf.at[pl.ds(start, count)] if rows_at is None else buf.at[pl.ds(start, count), rows_at]

        ways = ((up, reach, at), (down, parts - reach, at + 1))
        pair = [
            pltpu.make_async_remote_copy(
                cut(way[0]), cut(way[1]), sends.at[sem], recvs.at[sem],
                device_id={"space": (me + by) % parts}, device_id_type=MESH)
            for way, by, sem in ways
        ]
        return pair + [reach]

    def begin(pair):
        @pl.when(me < parts - pair[2])
        def _():
            pair[0].start()

        @pl.when(me >= pair[2])
        def _():
            pair[1].start()

    def arrive(pair):
        @pl.when(me >= pair[2])
        def _():
            pair[0].wait_recv()

        @pl.when(me < parts - pair[2])
        def _():
            pair[1].wait_recv()

    def sent(pair):
        @pl.when(me < parts - pair[2])
        def _():
            pair[0].wait_send()

        @pl.when(me >= pair[2])
        def _():
            pair[1].wait_send()

    share = rows // spans
    my_rows = pl.ds(pl.multiple_of(span * share, share), share)

    def hand_on(at, count, below, above):
        def copies(start, sem):
            return [
                pltpu.make_async_remote_copy(
                    cap.at[pl.ds(start, count), my_rows], cap.at[pl.ds(start, count), my_rows],
                    fs.at[sem, k], fr.at[sem, k],
                    device_id={"tm": (span + k) % spans}, device_id_type=MESH)
                for k in range(1, spans)
            ]

        return copies(below, at), copies(above, at + 1)

    def each(pair, act):
        @pl.when(me > 0)
        def _():
            for copy in pair[0]:
                act(copy)

        @pl.when(me < parts - 1)
        def _():
            for copy in pair[1]:
                act(copy)

    def hops(k):
        z, y = k // 4, k % 4
        return min(z, parts // 4 - z) + min(y, 4 - y)

    def gather(buf, sends, recvs):
        return [
            pltpu.make_async_remote_copy(
                buf.at[me], buf.at[me], sends.at[k], recvs.at[k],
                device_id={"space": (me + k) % parts}, device_id_type=MESH)
            for k in sorted(range(1, parts), key=lambda k: -hops(k))
        ]

    d = depth
    near = halo(c0, hs, hr, 0, 2, (2 * d - 1, d - 1), (d + 1, 2 * d + 1))
    far = halo(c0, hs, hr, 2, d - 2, (d + 1, 1), (d + 3, 2 * d + 3))
    beyond = halo(c0, hs, hr, 4, 1, (2 * d, 0), (d + 1, 3 * d + 1), reach=2)
    source = halo(src1, hs, hr, 6, 2, (d, 0), (2, d + 2))
    third = halo(c1x, hs, hr, 8, 1, (d, 0), (5, d + 5))
    cap_near = halo(cap, ks, kr, 0, 1, (2 * d - 1, d - 1), (d, 2 * d))
    cap_far = halo(cap, ks, kr, 2, d - 1, (d, 0), (d + 1, 2 * d + 1), rows_at=my_rows)
    pass_far = hand_on(0, d - 1, 0, 2 * d + 1)
    gather_r = [gather(gr.at[t], gs.at[t], gv.at[t]) for t in range(steps)]
    cap_window = window(cw, ws.at[0], wr.at[0], 2)
    c_window = [window(vw.at[t], ws.at[1 + t], wr.at[1 + t], 3 - t) for t in range(steps)]

    def clear(ref, start, stop):
        ref[start:stop] = jnp.zeros((stop - start, rows, lanes), F32)

    @pl.when(me == 0)
    def _():
        clear(cap, 0, d)
        clear(c0, 0, d + 1)
        clear(c1x, 0, 3)
        clear(src1, 0, 2)

    @pl.when(me == 1)
    def _():
        clear(c0, 0, 1)

    @pl.when(me == parts - 2)
    def _():
        clear(c0, 3 * d + 1, 3 * d + 2)

    @pl.when(me == parts - 1)
    def _():
        clear(cap, 2 * d, 3 * d)
        clear(c0, 2 * d + 1, 3 * d + 2)
        clear(c1x, d + 3, d + 6)
        clear(src1, d + 2, d + 4)

    loads[0].wait()
    mine = cap[d:2 * d]
    loads[1].wait()
    loads[2].wait()
    b = mine * u0[...] + src0[...]
    own[...] = b
    c0[d + 1:2 * d + 1] = b * (W / (mine + 6.0))
    cap1 = pack(mine)
    cw[2] = cap1
    loads[3].wait()

    pl.semaphore_wait(barrier, len(close) + spans - 1)
    begin(near)
    begin(cap_near)
    window_start(cap_window)
    for k in close:
        pl.semaphore_signal(far_sem, inc=1, device_id={"space": (me + k) % parts}, device_id_type=MESH)
    begin(far)
    begin(beyond)
    begin(cap_far)
    cap2_sent = to_2(cap1[None], groups - 1)

    def weights(start, count):
        plane = (me - 1) * depth + start + iota((count, 1, 1), 0)
        inside = (plane >= 0) & (plane < parts * depth)
        return jnp.where(inside, W / (cap[start:start + count] + 6.0), 0.0)

    arrive(cap_near)
    a = weights(d - 1, d + 2)

    for t in range(steps):
        if t == 0:
            arrive(near)
            c = c0[d - 1:2 * d + 3]
        else:
            c = c1x[1:d + 5]
        x = 1.2 * c[1:-1] + a * sum_inner(c, lanes)
        inner = x[1:-1]
        d0 = cap[d:2 * d] + 6.0
        r = own[...] - d0 * inner + sum_inner(x, lanes)
        b1 = pack(r)
        if t == 0:
            window_arrive(cap_window)
            block = me - 2 + iota((5, 1, 1), 0)
            d1 = cw[...] + 3.0
            i1 = jnp.where((block >= 0) & (block < parts), W / d1, 0.0)
            a1 = 0.5 * i1
        c1 = b1 * i1[2]
        vw[t, 3] = c1
        none = jnp.zeros((1,) + b1.shape, F32)
        c1 = jnp.concatenate([none, c1[None], none], 0)
        y1 = 1.2 * c1 + a1[1:4] * sum_packed(c1, half)
        r1 = jnp.concatenate([none, b1[None], none], 0) - d1[1:4] * y1 + 0.5 * sum_packed(y1, half)
        parts_2 = to_2(r1[1:2], 0) + to_2(r1[0:1], 1) + to_2(r1[2:3], 2)
        if t == 0:
            parts_2 = parts_2 + cap2_sent
            pl.semaphore_wait(far_sem, len(close))
        gr[t, me] = parts_2
        for copy in gather_r[t]:
            copy.start()
        window_start(c_window[t])
        if t == 1:
            begin(third)
        else:
            begin(source)
            arrive(cap_far)
            each(pass_far, lambda copy: copy.start())

        for copy in gather_r[t]:
            copy.wait_recv()
        got = gr[t]
        if t == 0:
            cap2 = unpack(got, 3)
            i2 = W / (cap2 + 1.5)
            cap3 = to_3(cap2)
            i3 = jnp.where(iota(cap3.shape, 2) % GROUP < GROUP // 2, W / (cap3 + 0.75), 0.0)
            a2, a3 = 0.25 * i2, 0.125 * i3
        b2 = unpack(got, 0) + after(unpack(got, 1)) + before(unpack(got, 2))
        c2 = b2 * i2
        y2 = 1.2 * c2 + a2 * sum_grouped(c2)
        r2 = b2 - (cap2 + 1.5) * y2 + 0.25 * sum_grouped(y2)
        c3 = to_3(r2) * i3
        y3 = coarse_solve(c3, a3)
        lift = twice_rows(dot(flat(y3), up_3), stack // 2)
        lift = jnp.broadcast_to(lift[:, None], (stack // 2, 2) + lift.shape[1:]).reshape(y2.shape)
        y2 = y2 + lift
        for _ in range(2):
            y2 = (0.2 * y2 + c2) + a2 * sum_grouped(y2)
        y2s[...] = y2
        window_arrive(c_window[t])

        lifts = []
        for k in range(-2, 3):
            at = (me + k + parts) % parts
            plane = pltpu.roll(y2s[at % stack], (lanes - GROUP * (at // stack)) % lanes, 1)
            lifts.append(jnp.where(within(k), plane, 0.0))
        lift = twice_rows(dot(jnp.concatenate(lifts, 0), up_2), 5)
        if t == 0:
            c1 = vw[t]
            y1 = 1.2 * c1[1:-1] + a1 * sum_packed(c1, half)[1:-1] + lift
            c1 = c1[1:-1]
            y1 = (0.2 * y1 + c1) + a1 * sum_packed(y1, half)
            y1 = ((0.2 * y1 + c1) + a1 * sum_packed(y1, half))[1:-1]
        else:
            c1 = vw[t, 1:6]
            y1 = 1.2 * c1 + a1 * sum_packed(c1, half) + lift
            y1 = ((0.2 * y1 + c1) + a1 * sum_packed(y1, half))[1:-1]
            y1 = (0.2 * y1 + c1[1:-1]) + a1[1:-1] * sum_packed(y1, half)

        n = rows // 2
        around = flat(y1)
        even, odd = dot(around, up_lo), dot(around, up_hi)
        halves = [part[n * k:n * k + n] for k in range(3) for part in (even, odd)]
        if t == 1:
            halves = halves[1:-1]
        planes = len(halves)
        lift = twice_rows(jnp.concatenate(halves, 0), planes)
        lift = jnp.broadcast_to(lift[:, None], (planes, 2) + lift.shape[1:]).reshape(2 * planes, rows, lanes)
        if t == 0:
            each(pass_far, lambda copy: copy.wait_recv())
            arrive(far)
            arrive(beyond)
            a_lo, a_hi = weights(0, d - 1), weights(2 * d + 1, d - 1)
            first = 1.2 * c0[1:d] + a_lo * sum_inner(c0[0:d + 1], lanes)
            final = 1.2 * c0[2 * d + 2:3 * d + 1] + a_hi * sum_inner(c0[2 * d + 1:3 * d + 2], lanes)
            wide = jnp.concatenate([a_lo, a, a_hi], 0)
            x = jnp.concatenate([first, x, final], 0) + lift
            x = (0.2 * x[1:-1] + c0[2:3 * d]) + wide[1:-1] * sum_inner(x, lanes)
            x = (0.2 * x[1:-1] + c0[3:3 * d - 1]) + wide[2:-2] * sum_inner(x, lanes)
            fp_ref[...] = x[2:-2]
            arrive(source)
            b = cap[2:3 * d - 2] * x + src1[...]
            own[...] = b[2:-2]
            c1x[1:d + 5] = b * wide[2:-2]
        else:
            arrive(third)
            first = 1.2 * c1x[1:2] + wide[2:3] * sum_inner(c1x[0:3], lanes)
            final = 1.2 * c1x[d + 4:d + 5] + wide[-3:-2] * sum_inner(c1x[d + 3:d + 6], lanes)
            x = jnp.concatenate([first, x, final], 0) + lift
            x = (0.2 * x[1:-1] + c1x[2:d + 4]) + a * sum_inner(x, lanes)
            fin[...] = (0.2 * x[1:-1] + c1x[3:d + 3]) + a[1:-1] * sum_inner(x, lanes)

    onward = pltpu.make_async_remote_copy(
        fin, up_ref, ts.at[0], ts.at[1],
        device_id={"tm": (span + 1) % spans}, device_id_type=MESH)

    @pl.when(span < spans - 1)
    def _():
        onward.start()

    @pl.when(span == 0)
    def _():
        up_ref[...] = u0[...]

    for pair in (near, far, beyond, source, third, cap_near, cap_far):
        sent(pair)
    each(pass_far, lambda copy: copy.wait_send())
    for copies in [cap_window] + c_window:
        window_sent(copies)
    for copies in gather_r:
        for copy in copies:
            copy.wait_send()

    @pl.when(span < spans - 1)
    def _():
        onward.wait_send()

    @pl.when(span > 0)
    def _():
        onward.wait_recv()


def shards(span_opening, source_power, warmth_retention):
    parts, spans = lax.axis_size("space"), lax.axis_size("tm")
    steps = source_power.shape[1]
    depth, rows, lanes = warmth_retention.shape
    assert steps == 2 and depth == 4
    slab = jax.ShapeDtypeStruct((depth, rows, lanes), F32)
    vmem = pl.BlockSpec(memory_space=pltpu.VMEM)
    dma = pltpu.SemaphoreType.DMA
    fpoint, updated = pl.pallas_call(
        functools.partial(kernel, parts, spans, steps),
        out_shape=(pltpu.VMEM(slab.shape, F32),) * 2,
        in_specs=[pl.BlockSpec(memory_space=pl.ANY)] * 3,
        out_specs=(vmem, vmem),
        scratch_shapes=[
            pltpu.VMEM((depth, rows, lanes), F32),
            pltpu.VMEM((depth, rows, lanes), F32),
            pltpu.VMEM((depth + 4, rows, lanes), F32),
            pltpu.VMEM((3 * depth, rows, lanes), F32),
            pltpu.VMEM((3 * depth + 2, rows, lanes), F32),
            pltpu.VMEM((depth + 6, rows, lanes), F32),
            pltpu.VMEM((5, rows // 2, lanes), F32),
            pltpu.VMEM((steps, 7, rows // 2, lanes), F32),
            pltpu.VMEM((steps, parts, rows // 4, lanes), F32),
            pltpu.VMEM((parts * GROUP // lanes, rows // 4, lanes), F32),
            pltpu.VMEM((depth, rows, lanes), F32),
            pltpu.VMEM((6 * rows, lanes), F32),
            pltpu.VMEM((depth, rows, lanes), F32),
            pltpu.SemaphoreType.REGULAR,
            dma((4,)), dma((10,)), dma((10,)), dma((4,)), dma((4,)), dma((2, spans)), dma((2, spans)),
            dma((steps, parts)), dma((steps, parts)), dma((1 + steps, 7)), dma((1 + steps, 7)), dma((2,)),
        ],
        compiler_params=pltpu.CompilerParams(
            collective_id=0, has_side_effects=True, vmem_limit_bytes=67043328 - 2 * 4 * slab.size
        ),
    )(span_opening[0], source_power[0], warmth_retention)
    return fpoint[None], updated[None]


def solution(mesh):
    in_specs = (
        P("tm", "space", None, None),
        P("tm", None, "space", None, None),
        P("space", None, None),
    )
    out_specs = (P("tm", "space", None, None), P("tm", "space", None, None))
    return jax.shard_map(shards, mesh=mesh, in_specs=in_specs, out_specs=out_specs, check_vma=False)
```

```python
import functools

import jax
import jax.numpy as jnp
from jax import lax
from jax.experimental import pallas as pl
from jax.experimental.pallas import tpu as pltpu
from jax.sharding import PartitionSpec as P

COARSE_SWEEPS = 24
W = 0.8
GROUP = 32
NEAR = (1, 2, 3, 4, 8, 12)
F32 = jnp.float32
MESH = pl.DeviceIdType.MESH


def iota(shape, dim):
    return lax.broadcasted_iota(jnp.int32, shape, dim)


def dot(a, b):
    total = None
    for _ in range(3):
        part = a.astype(jnp.bfloat16)
        a = a - part.astype(F32)
        term = jnp.dot(part, b, preferred_element_type=F32)
        total = term if total is None else total + term
    return total


def picks(lanes, pick, scale):
    src, dst = iota((lanes, lanes), 0), iota((lanes, lanes), 1)
    return jnp.where(pick(src, dst), scale, 0.0).astype(jnp.bfloat16)


def in_plane(x, width):
    rows, lanes = x.shape[1], x.shape[2]
    lane, row = iota(x.shape, 2), iota(x.shape, 1)
    left, right = pltpu.roll(x, 1, 2), pltpu.roll(x, lanes - 1, 2)
    left = jnp.where(lane % width == 0, 0.0, left)
    right = jnp.where(lane % width == width - 1, 0.0, right)
    up = jnp.where(row == 0, 0.0, pltpu.roll(x, 1, 1))
    down = jnp.where(row == rows - 1, 0.0, pltpu.roll(x, rows - 1, 1))
    return (left + right) + (up + down)


def shifted(x):
    zero = jnp.zeros((1,) + x.shape[1:], F32)
    return jnp.concatenate([zero, x[:-1]], 0), jnp.concatenate([x[1:], zero], 0)


def earlier(x, by=1, shift=0):
    lanes = x.shape[2]
    moved = pltpu.roll(x[-by:], (GROUP + shift) % lanes, 2)
    return jnp.where(iota(moved.shape, 2) < GROUP, 0.0, moved)


def later(x, by=1, shift=0):
    lanes = x.shape[2]
    moved = pltpu.roll(x[:by], (lanes - GROUP + shift) % lanes, 2)
    return jnp.where(iota(moved.shape, 2) >= lanes - GROUP, 0.0, moved)


def before(x):
    return jnp.concatenate([earlier(x), x[:-1]], 0)


def after(x):
    return jnp.concatenate([x[1:], later(x)], 0)


def sum_grouped(x):
    return in_plane(x, GROUP) + (before(x) + after(x))


def sum_packed(x, width):
    half = pltpu.roll(x, width, 2)
    before, after = shifted(half)
    return in_plane(x, width) + (half + jnp.where(iota(x.shape, 2) < width, before, after))


def sum_inner(x, width):
    return in_plane(x[1:-1], width) + (x[:-2] + x[2:])


def column_sum(x):
    rows = x.shape[1]
    mid = x[1:-1]
    row = iota(mid.shape, 1)
    up = jnp.where(row == 0, 0.0, pltpu.roll(mid, 1, 1))
    down = jnp.where(row == rows - 1, 0.0, pltpu.roll(mid, rows - 1, 1))
    return (x[:-2] + x[2:]) + (up + down)


def coarse_solve(c, a):
    n, lanes = c.shape[0], c.shape[2]

    def turned(x, by):
        return x if by == 0 else pltpu.roll(x, by % lanes, 2)

    def longer(x, by, reach=1):
        return jnp.concatenate([earlier(x, reach, by), turned(x, by), later(x, reach, by)], 0)

    c_at, a_at = [[longer(x, 0) if by == 0 else turned(x, by) for by in (1, 0, -1)] for x in (c, a)]

    def sweep(y, side, c, a):
        return (0.2 * y[1:-1] + c) + a * (side + column_sum(y))

    def two_sweeps(_, y):
        left, mid, right = longer(y, 1), longer(y, 0, 2), longer(y, -1)
        once_left = sweep(left, turned(y, 2) + y, c_at[0], a_at[0])
        once_mid = sweep(mid, left + right, c_at[1], a_at[1])
        once_right = sweep(right, y + turned(y, -2), c_at[2], a_at[2])
        return sweep(once_mid, once_left + once_right, c, a)

    left = COARSE_SWEEPS - 1
    y = c
    if left % 2:
        y = 1.2 * c + a * sum_grouped(c)
    return lax.fori_loop(0, left // 2, two_sweeps, y, unroll=True)


def flat(x):
    return x.reshape(x.shape[0] * x.shape[1], x.shape[2])


def kernel(
    parts, spans, steps,
    open_ref, src_ref, cap_in,
    fp_ref, up_ref,
    u0, src0, src1, cap, c0, c1x, cw, vw, c_sent, gr, r_sent, y2s, own, tmp, fin,
    far_sem, in_sem, hs, hr, ks, kr, fs, fr, gs, gv, ws, wr, ts,
):
    me, span = lax.axis_index("space"), lax.axis_index("tm")
    depth, rows, lanes = open_ref.shape
    half = lanes // 2
    groups = lanes // GROUP
    stack = parts // groups
    assert parts % groups == 0 and lanes == 128 and rows == 64
    close = sorted({k % parts for k in NEAR} | {-k % parts for k in NEAR})
    assert {(a + b) % parts for a in close + [0] for b in close + [0]} == set(range(parts))

    cw[...] = jnp.zeros(cw.shape, F32)
    vw[...] = jnp.zeros(vw.shape, F32)

    barrier = pltpu.get_barrier_semaphore()
    for k in close:
        pl.semaphore_signal(barrier, inc=1, device_id={"space": (me + k) % parts}, device_id_type=MESH)
    for k in range(1, spans):
        pl.semaphore_signal(barrier, inc=1, device_id={"tm": (span + k) % spans}, device_id_type=MESH)

    loads = [
        pltpu.make_async_copy(cap_in, cap.at[pl.ds(depth, depth)], in_sem.at[0]),
        pltpu.make_async_copy(open_ref, u0, in_sem.at[1]),
        pltpu.make_async_copy(src_ref.at[0], src0, in_sem.at[2]),
        pltpu.make_async_copy(src_ref.at[1], src1.at[pl.ds(2, depth)], in_sem.at[3]),
    ]
    for load in loads:
        load.start()

    group = me // stack
    down_lo = picks(lanes, lambda s, d: (s // 2 == d) & (d < half), 0.125)
    down_hi = picks(lanes, lambda s, d: s // 2 + half == d, 0.125)
    down_2 = [
        picks(lanes, lambda s, d: (s % half) // 2 + GROUP * ((group + q) % groups) == d, 0.125)
        for q in range(groups)
    ]
    down_3 = picks(lanes, lambda s, d: s // GROUP * GROUP + s % GROUP // 2 == d, 0.125)
    up_lo = picks(lanes, lambda s, d: d // 2 == s, 1.0)
    up_hi = picks(lanes, lambda s, d: d // 2 + half == s, 1.0)
    up_2 = picks(lanes, lambda s, d: (d % half) // 2 == s, 1.0)
    up_3 = picks(lanes, lambda s, d: d // GROUP * GROUP + d % GROUP // 2 == s, 1.0)

    def pair_rows(x):
        n, r, w = x.shape
        tmp[pl.ds(0, n * r), :] = flat(x)
        return tmp[pl.ds(0, n * r // 2, 2), :] + tmp[pl.ds(1, n * r // 2, 2), :]

    def twice_rows(x, planes):
        r = x.shape[0]
        tmp[pl.ds(0, r, 2), :] = x
        tmp[pl.ds(1, r, 2), :] = x
        return tmp[pl.ds(0, 2 * r), :].reshape(planes, 2 * r // planes, lanes)

    def pack(x):
        s = pair_rows(x.reshape(depth // 2, 2, rows, lanes).sum(1))
        n = rows // 2
        return dot(s[:n], down_lo) + dot(s[n:], down_hi)

    def to_2(x, q):
        return dot(pair_rows(x), down_2[q])

    def to_3(x):
        s = x.reshape(stack // 2, 2, rows // 4, lanes).sum(1)
        return dot(pair_rows(s), down_3).reshape(stack // 2, rows // 8, lanes)

    def unpack(x, q):
        at = (iota((stack,) + x.shape[1:], 2) // GROUP + groups - q) % groups
        out = x[:stack]
        for g in range(1, groups):
            out = jnp.where(at == g, x[g * stack:(g + 1) * stack], out)
        return pltpu.roll(out, lanes - GROUP * q, 2) if q else out

    def within(k):
        return (me + k >= 0) & (me + k < parts)

    def window(buf, source, sends, recvs, nearest, reach, to={}):
        middle = buf.shape[0] // 2
        return [
            (k, pltpu.make_async_remote_copy(
                source, buf.at[middle - k], sends.at[middle + k], recvs.at[middle + k],
                device_id={"space": (me + k + parts) % parts, **to}, device_id_type=MESH))
            for far in range(nearest, reach + 1) for k in ((far, -far) if far else (0,))
        ]

    def where_within(copies, sign, act):
        for k, copy in copies:
            @pl.when(within(sign * k))
            def _(copy=copy):
                act(copy)

    def window_start(copies):
        where_within(copies, 1, lambda copy: copy.start())

    def window_arrive(copies):
        where_within(copies, -1, lambda copy: copy.wait_recv())

    def window_sent(copies):
        where_within(copies, 1, lambda copy: copy.wait_send())

    def halo(buf, sends, recvs, at, count, up, down, reach=1, rows_at=None):
        def cut(start):
            return buf.at[pl.ds(start, count)] if rows_at is None else buf.at[pl.ds(start, count), rows_at]

        ways = ((up, reach, at), (down, parts - reach, at + 1))
        pair = [
            pltpu.make_async_remote_copy(
                cut(way[0]), cut(way[1]), sends.at[sem], recvs.at[sem],
                device_id={"space": (me + by) % parts}, device_id_type=MESH)
            for way, by, sem in ways
        ]
        return pair + [reach]

    def begin(pair):
        @pl.when(me < parts - pair[2])
        def _():
            pair[0].start()

        @pl.when(me >= pair[2])
        def _():
            pair[1].start()

    def arrive(pair):
        @pl.when(me >= pair[2])
        def _():
            pair[0].wait_recv()

        @pl.when(me < parts - pair[2])
        def _():
            pair[1].wait_recv()

    def sent(pair):
        @pl.when(me < parts - pair[2])
        def _():
            pair[0].wait_send()

        @pl.when(me >= pair[2])
        def _():
            pair[1].wait_send()

    share = rows // spans
    my_rows = pl.ds(pl.multiple_of(span * share, share), share)

    def hand_on(at, count, below, above):
        def copies(start, sem):
            return [
                pltpu.make_async_remote_copy(
                    cap.at[pl.ds(start, count), my_rows], cap.at[pl.ds(start, count), my_rows],
                    fs.at[sem, k], fr.at[sem, k],
                    device_id={"tm": (span + k) % spans}, device_id_type=MESH)
                for k in range(1, spans)
            ]

        return copies(below, at), copies(above, at + 1)

    def each(pair, act):
        @pl.when(me > 0)
        def _():
            for copy in pair[0]:
                act(copy)

        @pl.when(me < parts - 1)
        def _():
            for copy in pair[1]:
                act(copy)

    def hops(k):
        z, y = k // 4, k % 4
        return min(z, parts // 4 - z) + min(y, 4 - y)

    def gather(source, target, sends, recvs, offsets, to):
        return [
            pltpu.make_async_remote_copy(
                source, target, sends.at[k], recvs.at[k],
                device_id={"space": (me + k) % parts, **to}, device_id_type=MESH)
            for k in sorted(offsets, key=lambda k: -hops(k))
        ]

    d = depth
    onward = {"tm": (span + 1) % spans}
    near = halo(c0, hs, hr, 0, 2, (2 * d - 1, d - 1), (d + 1, 2 * d + 1))
    far = halo(c0, hs, hr, 2, d - 2, (d + 1, 1), (d + 3, 2 * d + 3))
    beyond = halo(c0, hs, hr, 4, 1, (2 * d, 0), (d + 1, 3 * d + 1), reach=2)
    source = halo(src1, hs, hr, 6, 2, (d, 0), (2, d + 2))
    third = halo(c1x, hs, hr, 8, 1, (d, 0), (5, d + 5))
    cap_near = halo(cap, ks, kr, 0, 1, (2 * d - 1, d - 1), (d, 2 * d))
    cap_far = halo(cap, ks, kr, 2, d - 1, (d, 0), (d + 1, 2 * d + 1), rows_at=my_rows)
    pass_far = hand_on(0, d - 1, 0, 2 * d + 1)
    gather_r = [
        gather(gr.at[0, me], gr.at[0, me], gs.at[0], gv.at[0], range(1, parts), {}),
        gather(r_sent, gr.at[1, me], gs.at[1], gv.at[1], range(parts), onward),
    ]
    cap_window = window(cw, cw.at[2], ws.at[0], wr.at[0], 1, 2)
    c_window = [
        window(vw.at[0], vw.at[0, 3], ws.at[1], wr.at[1], 1, 3),
        window(vw.at[1], c_sent, ws.at[2], wr.at[2], 0, 2, onward),
    ]
    fin_onward = pltpu.make_async_remote_copy(
        fin.at[0], fin.at[1], ts.at[0], ts.at[1],
        device_id={"tm": (span + 1) % spans}, device_id_type=MESH)

    def clear(ref, start, stop):
        ref[start:stop] = jnp.zeros((stop - start, rows, lanes), F32)

    @pl.when(me == 0)
    def _():
        clear(cap, 0, d)
        clear(c0, 0, d + 1)
        clear(c1x, 0, 3)
        clear(src1, 0, 2)

    @pl.when(me == 1)
    def _():
        clear(c0, 0, 1)

    @pl.when(me == parts - 2)
    def _():
        clear(c0, 3 * d + 1, 3 * d + 2)

    @pl.when(me == parts - 1)
    def _():
        clear(cap, 2 * d, 3 * d)
        clear(c0, 2 * d + 1, 3 * d + 2)
        clear(c1x, d + 3, d + 6)
        clear(src1, d + 2, d + 4)

    loads[0].wait()
    mine = cap[d:2 * d]
    loads[1].wait()
    loads[2].wait()
    b = mine * u0[...] + src0[...]
    own[...] = b
    c0[d + 1:2 * d + 1] = b * (W / (mine + 6.0))
    cap1 = pack(mine)
    cw[2] = cap1
    loads[3].wait()

    pl.semaphore_wait(barrier, len(close) + spans - 1)
    begin(near)
    begin(cap_near)
    window_start(cap_window)
    for k in close:
        pl.semaphore_signal(far_sem, inc=1, device_id={"space": (me + k) % parts}, device_id_type=MESH)
    begin(far)
    begin(beyond)
    begin(cap_far)
    cap2_sent = to_2(cap1[None], groups - 1)

    def weights(start, count):
        plane = (me - 1) * depth + start + iota((count, 1, 1), 0)
        inside = (plane >= 0) & (plane < parts * depth)
        return jnp.where(inside, W / (cap[start:start + count] + 6.0), 0.0)

    def inverse_1(start, stop):
        block = me - 2 + start + iota((stop - start, 1, 1), 0)
        diagonal = cw[start:stop] + 3.0
        return diagonal, jnp.where((block >= 0) & (block < parts), W / diagonal, 0.0)

    arrive(cap_near)
    a = weights(d - 1, d + 2)

    none = jnp.zeros((1, rows // 2, lanes), F32)

    def padded(x):
        return jnp.concatenate([none, x[None], none], 0)

    def first_sweeps(b, c, a):
        x = 1.2 * c[1:-1] + a * sum_inner(c, lanes)
        r = b - (cap[d:2 * d] + 6.0) * x[1:-1] + sum_inner(x, lanes)
        return x, pack(r)

    def spread(b1, c1, d1, a1):
        c1 = padded(c1)
        y1 = 1.2 * c1 + a1 * sum_packed(c1, half)
        r1 = padded(b1) - d1 * y1 + 0.5 * sum_packed(y1, half)
        return to_2(r1[1:2], 0) + to_2(r1[0:1], 1) + to_2(r1[2:3], 2)

    def level_2(got, cap2, i2, a2, i3, a3):
        b2 = unpack(got, 0) + after(unpack(got, 1)) + before(unpack(got, 2))
        c2 = b2 * i2
        y2 = 1.2 * c2 + a2 * sum_grouped(c2)
        r2 = b2 - (cap2 + 1.5) * y2 + 0.25 * sum_grouped(y2)
        c3 = to_3(r2) * i3
        y3 = coarse_solve(c3, a3)
        lift = twice_rows(dot(flat(y3), up_3), stack // 2)
        lift = jnp.broadcast_to(lift[:, None], (stack // 2, 2) + lift.shape[1:]).reshape(y2.shape)
        y2 = y2 + lift
        for _ in range(2):
            y2 = (0.2 * y2 + c2) + a2 * sum_grouped(y2)
        y2s[...] = y2
        lifts = []
        for k in range(-2, 3):
            at = (me + k + parts) % parts
            plane = pltpu.roll(y2s[at % stack], (lanes - GROUP * (at // stack)) % lanes, 1)
            lifts.append(jnp.where(within(k), plane, 0.0))
        return twice_rows(dot(jnp.concatenate(lifts, 0), up_2), 5)

    def lift_0(y1, skip):
        n = rows // 2
        around = flat(y1)
        even, odd = dot(around, up_lo), dot(around, up_hi)
        halves = [part[n * k:n * k + n] for k in range(3) for part in (even, odd)]
        halves = halves[skip:len(halves) - skip]
        planes = len(halves)
        lift = twice_rows(jnp.concatenate(halves, 0), planes)
        return jnp.broadcast_to(lift[:, None], (planes, 2) + lift.shape[1:]).reshape(2 * planes, rows, lanes)

    arrive(near)
    x, b1 = first_sweeps(own[...], c0[d - 1:2 * d + 3], a)
    window_arrive(cap_window[:2])
    d1, i1 = inverse_1(1, 4)
    vw[0, 3] = b1 * i1[1]
    beside = spread(b1, b1 * i1[1], d1, 0.5 * i1) + cap2_sent
    gr[0, me] = beside
    pl.semaphore_wait(far_sem, len(close))
    for copy in gather_r[0]:
        copy.start()
    window_start(c_window[0])
    begin(source)
    arrive(cap_far)
    each(pass_far, lambda copy: copy.start())
    window_arrive(cap_window[2:])
    a1 = 0.5 * inverse_1(0, 5)[1]
    arrive(far)
    arrive(beyond)
    each(pass_far, lambda copy: copy.wait_recv())
    a_lo, a_hi = weights(0, d - 1), weights(2 * d + 1, d - 1)
    first = 1.2 * c0[1:d] + a_lo * sum_inner(c0[0:d + 1], lanes)
    final = 1.2 * c0[2 * d + 2:3 * d + 1] + a_hi * sum_inner(c0[2 * d + 1:3 * d + 2], lanes)
    wide = jnp.concatenate([a_lo, a, a_hi], 0)
    x = jnp.concatenate([first, x, final], 0)
    for copy in gather_r[0]:
        copy.wait_recv()
    window_arrive(c_window[0])

    got = gr[0]
    cap2 = unpack(got, 3)
    i2 = W / (cap2 + 1.5)
    cap3 = to_3(cap2)
    i3 = jnp.where(iota(cap3.shape, 2) % GROUP < GROUP // 2, W / (cap3 + 0.75), 0.0)
    coarse = cap2, i2, 0.25 * i2, i3, 0.125 * i3
    c1 = vw[0]
    y1 = 1.2 * c1[1:-1] + a1 * sum_packed(c1, half)[1:-1] + level_2(got, *coarse)
    c1 = c1[1:-1]
    y1 = (0.2 * y1 + c1) + a1 * sum_packed(y1, half)
    y1 = ((0.2 * y1 + c1) + a1 * sum_packed(y1, half))[1:-1]
    x = x + lift_0(y1, 0)
    x = (0.2 * x[1:-1] + c0[2:3 * d]) + wide[1:-1] * sum_inner(x, lanes)
    x = (0.2 * x[1:-1] + c0[3:3 * d - 1]) + wide[2:-2] * sum_inner(x, lanes)
    fp_ref[...] = x[2:-2]
    arrive(source)
    b = cap[2:3 * d - 2] * x + src1[...]
    c1x[1:d + 5] = b * wide[2:-2]

    x, b1 = first_sweeps(b[2:-2], c1x[1:d + 5], a)
    c1 = b1 * i1[1]
    c_sent[...] = c1
    r_sent[...] = spread(b1, c1, d1, 0.5 * i1)

    @pl.when(span < spans - 1)
    def _():
        for copy in gather_r[1]:
            copy.start()
        window_start(c_window[1])

    begin(third)
    arrive(third)
    first = 1.2 * c1x[1:2] + wide[2:3] * sum_inner(c1x[0:3], lanes)
    final = 1.2 * c1x[d + 4:d + 5] + wide[-3:-2] * sum_inner(c1x[d + 3:d + 6], lanes)
    x = jnp.concatenate([first, x, final], 0)
    x = (0.2 * x[1:-1] + c1x[2:d + 4]) + a * sum_inner(x, lanes)
    fin[0] = (0.2 * x[1:-1] + c1x[3:d + 3]) + a[1:-1] * sum_inner(x, lanes)

    @pl.when(span < spans - 1)
    def _():
        fin_onward.start()

    for pair in (near, far, beyond, source, third, cap_near, cap_far):
        sent(pair)
    each(pass_far, lambda copy: copy.wait_send())
    for copies in (cap_window, c_window[0]):
        window_sent(copies)
    for copy in gather_r[0]:
        copy.wait_send()

    @pl.when(span == 0)
    def _():
        up_ref[...] = u0[...]

    @pl.when(span > 0)
    def _():
        for copy in gather_r[1]:
            copy.wait_recv()
        window_arrive(c_window[1])
        fin_onward.wait_recv()
        c1 = vw[1, 1:6]
        y1 = 1.2 * c1 + a1 * sum_packed(c1, half) + level_2(gr[1], *coarse)
        y1 = ((0.2 * y1 + c1) + a1 * sum_packed(y1, half))[1:-1]
        y1 = (0.2 * y1 + c1[1:-1]) + a1[1:-1] * sum_packed(y1, half)
        x = lift_0(y1, 1)
        x = 0.2 * x[1:-1] + a * sum_inner(x, lanes)
        up_ref[...] = fin[1] + (0.2 * x[1:-1] + a[1:-1] * sum_inner(x, lanes))

    @pl.when(span < spans - 1)
    def _():
        for copy in gather_r[1]:
            copy.wait_send()
        window_sent(c_window[1])
        fin_onward.wait_send()


def shards(span_opening, source_power, warmth_retention):
    parts, spans = lax.axis_size("space"), lax.axis_size("tm")
    steps = source_power.shape[1]
    depth, rows, lanes = warmth_retention.shape
    assert steps == 2 and depth == 4
    slab = jax.ShapeDtypeStruct((depth, rows, lanes), F32)
    vmem = pl.BlockSpec(memory_space=pltpu.VMEM)
    dma = pltpu.SemaphoreType.DMA
    fpoint, updated = pl.pallas_call(
        functools.partial(kernel, parts, spans, steps),
        out_shape=(pltpu.VMEM(slab.shape, F32),) * 2,
        in_specs=[pl.BlockSpec(memory_space=pl.ANY)] * 3,
        out_specs=(vmem, vmem),
        scratch_shapes=[
            pltpu.VMEM((depth, rows, lanes), F32),
            pltpu.VMEM((depth, rows, lanes), F32),
            pltpu.VMEM((depth + 4, rows, lanes), F32),
            pltpu.VMEM((3 * depth, rows, lanes), F32),
            pltpu.VMEM((3 * depth + 2, rows, lanes), F32),
            pltpu.VMEM((depth + 6, rows, lanes), F32),
            pltpu.VMEM((5, rows // 2, lanes), F32),
            pltpu.VMEM((steps, 7, rows // 2, lanes), F32),
            pltpu.VMEM((rows // 2, lanes), F32),
            pltpu.VMEM((steps, parts, rows // 4, lanes), F32),
            pltpu.VMEM((rows // 4, lanes), F32),
            pltpu.VMEM((parts * GROUP // lanes, rows // 4, lanes), F32),
            pltpu.VMEM((depth, rows, lanes), F32),
            pltpu.VMEM((6 * rows, lanes), F32),
            pltpu.VMEM((2, depth, rows, lanes), F32),
            pltpu.SemaphoreType.REGULAR,
            dma((4,)), dma((10,)), dma((10,)), dma((4,)), dma((4,)), dma((2, spans)), dma((2, spans)),
            dma((steps, parts)), dma((steps, parts)), dma((1 + steps, 7)), dma((1 + steps, 7)), dma((2,)),
        ],
        compiler_params=pltpu.CompilerParams(
            collective_id=0, has_side_effects=True, vmem_limit_bytes=67043328 - 2 * 4 * slab.size
        ),
    )(span_opening[0], source_power[0], warmth_retention)
    return fpoint[None], updated[None]


def solution(mesh):
    in_specs = (
        P("tm", "space", None, None),
        P("tm", None, "space", None, None),
        P("space", None, None),
    )
    out_specs = (P("tm", "space", None, None), P("tm", "space", None, None))
    return jax.shard_map(shards, mesh=mesh, in_specs=in_specs, out_specs=out_specs, check_vma=False)
```

```python
import functools

import jax
import jax.numpy as jnp
from jax import lax
from jax.experimental import pallas as pl
from jax.experimental.pallas import tpu as pltpu
from jax.sharding import PartitionSpec as P

COARSE_SWEEPS = 24
W = 0.8
GROUP = 32
NEAR = (1, 2, 3, 4, 8, 12)
F32 = jnp.float32
MESH = pl.DeviceIdType.MESH


def iota(shape, dim):
    return lax.broadcasted_iota(jnp.int32, shape, dim)


def dot(a, b):
    total = None
    for _ in range(3):
        part = a.astype(jnp.bfloat16)
        a = a - part.astype(F32)
        term = jnp.dot(part, b, preferred_element_type=F32)
        total = term if total is None else total + term
    return total


def picks(lanes, pick, scale):
    src, dst = iota((lanes, lanes), 0), iota((lanes, lanes), 1)
    return jnp.where(pick(src, dst), scale, 0.0).astype(jnp.bfloat16)


def in_plane(x, width):
    rows, lanes = x.shape[1], x.shape[2]
    lane, row = iota(x.shape, 2), iota(x.shape, 1)
    left, right = pltpu.roll(x, 1, 2), pltpu.roll(x, lanes - 1, 2)
    if width:
        left = jnp.where(lane % width == 0, 0.0, left)
        right = jnp.where(lane % width == width - 1, 0.0, right)
    up = jnp.where(row == 0, 0.0, pltpu.roll(x, 1, 1))
    down = jnp.where(row == rows - 1, 0.0, pltpu.roll(x, rows - 1, 1))
    return (left + right) + (up + down)


def shifted(x):
    zero = jnp.zeros((1,) + x.shape[1:], F32)
    return jnp.concatenate([zero, x[:-1]], 0), jnp.concatenate([x[1:], zero], 0)


def earlier(x, by=1, shift=0):
    lanes = x.shape[2]
    moved = pltpu.roll(x[-by:], (GROUP + shift) % lanes, 2)
    return jnp.where(iota(moved.shape, 2) < GROUP, 0.0, moved)


def later(x, by=1, shift=0):
    lanes = x.shape[2]
    moved = pltpu.roll(x[:by], (lanes - GROUP + shift) % lanes, 2)
    return jnp.where(iota(moved.shape, 2) >= lanes - GROUP, 0.0, moved)


def sum_grouped(x):
    ends = jnp.concatenate([earlier(x), x, later(x)], 0)
    return in_plane(x, GROUP) + (ends[:-2] + ends[2:])


def sum_planes(x):
    before, after = shifted(x)
    return in_plane(x, None) + (before + after)


def plane_padded(x, by):
    zero = jnp.zeros((by,) + x.shape[1:], F32)
    return jnp.concatenate([zero, x, zero], 0)


def sum_packed(x, width):
    half = pltpu.roll(x, width, 2)
    before, after = shifted(half)
    return in_plane(x, width) + (half + jnp.where(iota(x.shape, 2) < width, before, after))


def sum_inner(x, width):
    return in_plane(x[1:-1], width) + (x[:-2] + x[2:])


def column_sum(x):
    rows = x.shape[1]
    mid = x[1:-1]
    row = iota(mid.shape, 1)
    up = jnp.where(row == 0, 0.0, pltpu.roll(mid, 1, 1))
    down = jnp.where(row == rows - 1, 0.0, pltpu.roll(mid, rows - 1, 1))
    return (x[:-2] + x[2:]) + (up + down)


def coarse_solve(c, a):
    n, lanes = c.shape[0], c.shape[2]

    def turned(x, by):
        return x if by == 0 else pltpu.roll(x, by % lanes, 2)

    def longer(x, by, reach=1):
        return jnp.concatenate([earlier(x, reach, by), turned(x, by), later(x, reach, by)], 0)

    c_at, a_at = [[longer(x, 0) if by == 0 else turned(x, by) for by in (1, 0, -1)] for x in (c, a)]

    def sweep(y, side, c, a):
        return (0.2 * y[1:-1] + c) + a * (side + column_sum(y))

    def two_sweeps(_, y):
        left, mid, right = longer(y, 1), longer(y, 0, 2), longer(y, -1)
        once_left = sweep(left, turned(y, 2) + y, c_at[0], a_at[0])
        once_mid = sweep(mid, left + right, c_at[1], a_at[1])
        once_right = sweep(right, y + turned(y, -2), c_at[2], a_at[2])
        return sweep(once_mid, once_left + once_right, c, a)

    left = COARSE_SWEEPS - 1
    y = c
    if left % 2:
        y = 1.2 * c + a * sum_grouped(c)
    return lax.fori_loop(0, left // 2, two_sweeps, y, unroll=True)


def flat(x):
    return x.reshape(x.shape[0] * x.shape[1], x.shape[2])


def kernel(
    parts, spans, steps,
    open_ref, src_ref, cap_in,
    fp_ref, up_ref,
    u0, src0, src1, cap, c0, c1x, cw, vw, c_sent, bw, b_sent, gr, r_sent, r2s, y3s, own, tmp, fin,
    far_sem, in_sem, hs, hr, ks, kr, fs, fr, gs, gv, ws, wr, ts,
):
    me, span = lax.axis_index("space"), lax.axis_index("tm")
    depth, rows, lanes = open_ref.shape
    half = lanes // 2
    groups = lanes // GROUP
    assert parts == 32 and lanes == 128 and rows == 64
    close = sorted({k % parts for k in NEAR} | {-k % parts for k in NEAR})
    assert {(a + b) % parts for a in close + [0] for b in close + [0]} == set(range(parts))

    cw[...] = jnp.zeros(cw.shape, F32)
    vw[...] = jnp.zeros(vw.shape, F32)
    bw[...] = jnp.zeros(bw.shape, F32)
    r2s[...] = jnp.zeros(r2s.shape, F32)

    barrier = pltpu.get_barrier_semaphore()
    for k in close:
        pl.semaphore_signal(barrier, inc=1, device_id={"space": (me + k) % parts}, device_id_type=MESH)
    for k in range(1, spans):
        pl.semaphore_signal(barrier, inc=1, device_id={"tm": (span + k) % spans}, device_id_type=MESH)

    loads = [
        pltpu.make_async_copy(cap_in, cap.at[pl.ds(depth, depth)], in_sem.at[0]),
        pltpu.make_async_copy(open_ref, u0, in_sem.at[1]),
        pltpu.make_async_copy(src_ref.at[0], src0, in_sem.at[2]),
        pltpu.make_async_copy(src_ref.at[1], src1.at[pl.ds(2, depth)], in_sem.at[3]),
    ]
    for load in loads:
        load.start()

    down_lo = picks(lanes, lambda s, d: (s // 2 == d) & (d < half), 0.125)
    down_hi = picks(lanes, lambda s, d: s // 2 + half == d, 0.125)
    down_2 = picks(lanes, lambda s, d: (s % half) // 2 == d, 0.125)
    down_3 = picks(lanes, lambda s, d: (s < GROUP) & (d % GROUP == s // 2), 0.125)
    down_cap = picks(lanes, lambda s, d: (s < GROUP) & (d % GROUP == s // 2 + GROUP // 2), 0.125)
    up_lo = picks(lanes, lambda s, d: d // 2 == s, 1.0)
    up_hi = picks(lanes, lambda s, d: d // 2 + half == s, 1.0)
    up_2 = picks(lanes, lambda s, d: (d % half) // 2 == s, 1.0)
    up_3 = picks(lanes, lambda s, d: (d < GROUP) & (d // 2 == s), 1.0)

    def pair_rows(x):
        n, r, w = x.shape
        tmp[pl.ds(0, n * r), :] = flat(x)
        return tmp[pl.ds(0, n * r // 2, 2), :] + tmp[pl.ds(1, n * r // 2, 2), :]

    def twice_rows(x, planes):
        r = x.shape[0]
        tmp[pl.ds(0, r, 2), :] = x
        tmp[pl.ds(1, r, 2), :] = x
        return tmp[pl.ds(0, 2 * r), :].reshape(planes, 2 * r // planes, lanes)

    def pack(x):
        s = pair_rows(x.reshape(depth // 2, 2, rows, lanes).sum(1))
        n = rows // 2
        return dot(s[:n], down_lo) + dot(s[n:], down_hi)

    def to_2(x):
        return dot(pair_rows(x), down_2).reshape(x.shape[0], rows // 4, lanes)

    lane = iota((rows // 8, lanes), 1)

    def turn(planes, off):
        out = []
        for k in range(groups):
            total = None
            for g in range(groups):
                by = (GROUP * (g - k) - off) % lanes
                moved = pltpu.roll(planes[g], by, 1) if by else planes[g]
                total = moved if total is None else jnp.where(lane // GROUP == g, moved, total)
            out.append(total[None])
        return jnp.concatenate(out, 0)

    def level_3(got):
        pairs = [got[0]] + [got[2 * i - 1] + got[2 * i] for i in range(1, parts // 2)] + [got[parts - 1]]
        out = []
        for k in range(groups):
            total = pairs[4 * k + 2]
            for i, keep in (
                (4 * k - 1, lane < GROUP), (4 * k, lane < 2 * GROUP), (4 * k + 1, lane < 3 * GROUP),
                (4 * k + 3, lane >= GROUP), (4 * k + 4, lane >= 2 * GROUP), (4 * k + 5, lane >= 3 * GROUP),
            ):
                if 0 <= i < len(pairs):
                    total = total + jnp.where(keep, pairs[i], 0.0)
            out.append(total)
        return turn(out, 0)

    def capacity_3(got):
        out = []
        for k in range(groups):
            total = None
            for g in range(groups):
                i = 2 * (4 * k + g)
                pair = got[i] + got[i + 1]
                total = pair if total is None else jnp.where(lane // GROUP == g, pair, total)
            out.append(total)
        return turn(out, GROUP // 2)

    def within(k):
        return (me + k >= 0) & (me + k < parts)

    def window(buf, source, sends, recvs, nearest, reach, to={}):
        middle = buf.shape[0] // 2
        return [
            (k, pltpu.make_async_remote_copy(
                source, buf.at[middle - k], sends.at[middle + k], recvs.at[middle + k],
                device_id={"space": (me + k + parts) % parts, **to}, device_id_type=MESH))
            for far in range(nearest, reach + 1) for k in ((far, -far) if far else (0,))
        ]

    def where_within(copies, sign, act):
        for k, copy in copies:
            @pl.when(within(sign * k))
            def _(copy=copy):
                act(copy)

    def window_start(copies):
        where_within(copies, 1, lambda copy: copy.start())

    def window_arrive(copies):
        where_within(copies, -1, lambda copy: copy.wait_recv())

    def window_sent(copies):
        where_within(copies, 1, lambda copy: copy.wait_send())

    def halo(buf, sends, recvs, at, count, up, down, reach=1, rows_at=None):
        def cut(start):
            return buf.at[pl.ds(start, count)] if rows_at is None else buf.at[pl.ds(start, count), rows_at]

        ways = ((up, reach, at), (down, parts - reach, at + 1))
        pair = [
            pltpu.make_async_remote_copy(
                cut(way[0]), cut(way[1]), sends.at[sem], recvs.at[sem],
                device_id={"space": (me + by) % parts}, device_id_type=MESH)
            for way, by, sem in ways
        ]
        return pair + [reach]

    def begin(pair):
        @pl.when(me < parts - pair[2])
        def _():
            pair[0].start()

        @pl.when(me >= pair[2])
        def _():
            pair[1].start()

    def arrive(pair):
        @pl.when(me >= pair[2])
        def _():
            pair[0].wait_recv()

        @pl.when(me < parts - pair[2])
        def _():
            pair[1].wait_recv()

    def sent(pair):
        @pl.when(me < parts - pair[2])
        def _():
            pair[0].wait_send()

        @pl.when(me >= pair[2])
        def _():
            pair[1].wait_send()

    share = rows // spans
    my_rows = pl.ds(pl.multiple_of(span * share, share), share)

    def hand_on(at, count, below, above):
        def copies(start, sem):
            return [
                pltpu.make_async_remote_copy(
                    cap.at[pl.ds(start, count), my_rows], cap.at[pl.ds(start, count), my_rows],
                    fs.at[sem, k], fr.at[sem, k],
                    device_id={"tm": (span + k) % spans}, device_id_type=MESH)
                for k in range(1, spans)
            ]

        return copies(below, at), copies(above, at + 1)

    def each(pair, act):
        @pl.when(me > 0)
        def _():
            for copy in pair[0]:
                act(copy)

        @pl.when(me < parts - 1)
        def _():
            for copy in pair[1]:
                act(copy)

    def hops(k):
        z, y = k // 4, k % 4
        return min(z, parts // 4 - z) + min(y, 4 - y)

    def gather(source, target, sends, recvs, offsets, to):
        return [
            pltpu.make_async_remote_copy(
                source, target, sends.at[k], recvs.at[k],
                device_id={"space": (me + k) % parts, **to}, device_id_type=MESH)
            for k in sorted(offsets, key=lambda k: -hops(k))
        ]

    d = depth
    onward = {"tm": (span + 1) % spans}
    near = halo(c0, hs, hr, 0, 2, (2 * d - 1, d - 1), (d + 1, 2 * d + 1))
    far = halo(c0, hs, hr, 2, d - 2, (d + 1, 1), (d + 3, 2 * d + 3))
    beyond = halo(c0, hs, hr, 4, 1, (2 * d, 0), (d + 1, 3 * d + 1), reach=2)
    source = halo(src1, hs, hr, 6, 2, (d, 0), (2, d + 2))
    third = halo(c1x, hs, hr, 8, 1, (d, 0), (5, d + 5))
    cap_near = halo(cap, ks, kr, 0, 1, (2 * d - 1, d - 1), (d, 2 * d))
    cap_far = halo(cap, ks, kr, 2, d - 1, (d, 0), (d + 1, 2 * d + 1), rows_at=my_rows)
    pass_far = hand_on(0, d - 1, 0, 2 * d + 1)
    gather_r = [
        gather(gr.at[0, me], gr.at[0, me], gs.at[0], gv.at[0], range(1, parts), {}),
        gather(r_sent, gr.at[1, me], gs.at[1], gv.at[1], range(parts), onward),
    ]
    cap_window = window(cw, cw.at[5], ws.at[0], wr.at[0], 1, 5)
    c_window = [
        window(vw.at[0], vw.at[0, 3], ws.at[1], wr.at[1], 1, 3),
        window(vw.at[1], c_sent, ws.at[2], wr.at[2], 0, 2, onward),
    ]
    b_window = [
        window(bw.at[0], bw.at[0, 6], ws.at[3], wr.at[3], 1, 6),
        window(bw.at[1], b_sent, ws.at[4], wr.at[4], 0, 6, onward),
    ]
    fin_onward = pltpu.make_async_remote_copy(
        fin.at[0], fin.at[1], ts.at[0], ts.at[1],
        device_id={"tm": (span + 1) % spans}, device_id_type=MESH)

    def clear(ref, start, stop):
        ref[start:stop] = jnp.zeros((stop - start, rows, lanes), F32)

    @pl.when(me == 0)
    def _():
        clear(cap, 0, d)
        clear(c0, 0, d + 1)
        clear(c1x, 0, 3)
        clear(src1, 0, 2)

    @pl.when(me == 1)
    def _():
        clear(c0, 0, 1)

    @pl.when(me == parts - 2)
    def _():
        clear(c0, 3 * d + 1, 3 * d + 2)

    @pl.when(me == parts - 1)
    def _():
        clear(cap, 2 * d, 3 * d)
        clear(c0, 2 * d + 1, 3 * d + 2)
        clear(c1x, d + 3, d + 6)
        clear(src1, d + 2, d + 4)

    loads[0].wait()
    mine = cap[d:2 * d]
    loads[1].wait()
    loads[2].wait()
    b = mine * u0[...] + src0[...]
    own[...] = b
    c0[d + 1:2 * d + 1] = b * (W / (mine + 6.0))
    cap1 = pack(mine)
    cw[5] = cap1
    loads[3].wait()

    pl.semaphore_wait(barrier, len(close) + spans - 1)
    begin(near)
    begin(cap_near)
    window_start(cap_window[:4])
    for k in close:
        pl.semaphore_signal(far_sem, inc=1, device_id={"space": (me + k) % parts}, device_id_type=MESH)
    begin(far)
    begin(beyond)
    begin(cap_far)
    cap_sent = dot(pair_rows(to_2(cap1[None])), down_cap)

    def weights(start, count):
        plane = (me - 1) * depth + start + iota((count, 1, 1), 0)
        inside = (plane >= 0) & (plane < parts * depth)
        return jnp.where(inside, W / (cap[start:start + count] + 6.0), 0.0)

    def inverse(diagonal, start, reach):
        block = me - reach + start + iota((diagonal.shape[0], 1, 1), 0)
        return jnp.where((block >= 0) & (block < parts), W / diagonal, 0.0)

    def inverse_1(start, stop):
        diagonal = cw[start:stop] + 3.0
        return diagonal, inverse(diagonal, start, 5)

    def inverse_2(start, stop):
        diagonal = to_2(cw[start:stop]) + 1.5
        return diagonal, jnp.where(iota(diagonal.shape, 2) < GROUP, inverse(diagonal, start, 5), 0.0)

    window_arrive(cap_window[:4])
    d1, i1 = inverse_1(4, 7)
    d2, i2 = inverse_2(3, 8)
    near_1 = i1, d1, 0.5 * i1, i2, d2, 0.25 * i2
    arrive(cap_near)
    a = weights(d - 1, d + 2)

    def first_sweeps(b, c, a):
        x = 1.2 * c[1:-1] + a * sum_inner(c, lanes)
        r = b - (cap[d:2 * d] + 6.0) * x[1:-1] + sum_inner(x, lanes)
        return x, pack(r)

    def spread(b1, c1, i1, d1, a1, i2, d2, a2):
        c1 = plane_padded(c1[None], 1)
        y1 = 1.2 * c1 + a1 * sum_packed(c1, half)
        b2 = to_2(plane_padded(b1[None], 1) - d1 * y1 + 0.5 * sum_packed(y1, half))
        c2 = plane_padded(b2 * i2[1:4], 1)
        y2 = 1.2 * c2 + a2 * sum_planes(c2)
        r2s[1:8] = plane_padded(b2, 2) - plane_padded(d2 * y2, 1) + 0.25 * sum_planes(plane_padded(y2, 1))
        pairs = r2s[pl.ds(me % 2, 8)].reshape(4, 2, rows // 4, lanes).sum(1)
        b3 = dot(pair_rows(pairs), down_3).reshape(4, rows // 8, lanes)
        first = (me + 4 + me % 2) // 2
        return b2, sum(jnp.where(lane // GROUP == (first + q) % groups, b3[q], 0.0) for q in range(4))

    def side_by_side(b2):
        return b2[1] + (pltpu.roll(b2[0], GROUP, 1) + pltpu.roll(b2[2], 2 * GROUP, 1))

    def level_2(b, c3, i2, a2, a3):
        b2 = b[1:-1] + (pltpu.roll(b[2:], lanes - GROUP, 2) + pltpu.roll(b[:-2], lanes - 2 * GROUP, 2))
        c2 = b2 * i2
        y2 = 1.2 * c2[1:-1] + a2 * sum_planes(c2)[1:-1]
        c2 = c2[1:-1]
        y3s[...] = coarse_solve(c3, a3)
        lifts = []
        for q in range(-2, 3):
            at = me // 2 + q
            inside = (at >= 0) & (at < parts // 2)
            at = (at + parts // 2) % (parts // 2)
            plane = pltpu.roll(y3s[at % groups], (lanes - GROUP * (at // groups)) % lanes, 1)
            lifts.append(jnp.where(inside, plane, 0.0))
        lift = twice_rows(dot(jnp.concatenate(lifts, 0), up_3), 5)
        lift = jnp.broadcast_to(lift[:, None], (5, 2) + lift.shape[1:]).reshape((10,) + lift.shape[1:])
        y2 = y2 + jnp.where(me % 2 == 1, lift[1:], lift[:-1])
        y2 = ((0.2 * y2 + c2) + a2 * sum_planes(y2))[1:-1]
        y2 = ((0.2 * y2 + c2[1:-1]) + a2[1:-1] * sum_planes(y2))[1:-1]
        return twice_rows(dot(flat(y2), up_2), 5)

    def lift_0(y1, skip):
        n = rows // 2
        around = flat(y1)
        even, odd = dot(around, up_lo), dot(around, up_hi)
        halves = [part[n * k:n * k + n] for k in range(3) for part in (even, odd)]
        halves = halves[skip:len(halves) - skip]
        planes = len(halves)
        lift = twice_rows(jnp.concatenate(halves, 0), planes)
        return jnp.broadcast_to(lift[:, None], (planes, 2) + lift.shape[1:]).reshape(2 * planes, rows, lanes)

    arrive(near)
    x, b1 = first_sweeps(own[...], c0[d - 1:2 * d + 3], a)
    c1 = b1 * i1[1]
    vw[0, 3] = c1
    b2, b3 = spread(b1, c1, *near_1)
    gr[0, me] = b3 + cap_sent
    bw[0, 6] = side_by_side(b2)
    pl.semaphore_wait(far_sem, len(close))
    for copy in gather_r[0]:
        copy.start()
    window_start(b_window[0])
    window_start(c_window[0])
    window_start(cap_window[4:])
    begin(source)
    arrive(cap_far)
    each(pass_far, lambda copy: copy.start())
    a1 = 0.5 * inverse_1(3, 8)[1]
    arrive(far)
    arrive(beyond)
    window_arrive(cap_window[4:])
    i2 = inverse_2(0, 11)[1]
    a2 = 0.25 * i2[1:-1]
    each(pass_far, lambda copy: copy.wait_recv())
    a_lo, a_hi = weights(0, d - 1), weights(2 * d + 1, d - 1)
    first = 1.2 * c0[1:d] + a_lo * sum_inner(c0[0:d + 1], lanes)
    final = 1.2 * c0[2 * d + 2:3 * d + 1] + a_hi * sum_inner(c0[2 * d + 1:3 * d + 2], lanes)
    wide = jnp.concatenate([a_lo, a, a_hi], 0)
    x = jnp.concatenate([first, x, final], 0)
    for copy in gather_r[0]:
        copy.wait_recv()
    window_arrive(b_window[0])
    window_arrive(c_window[0])

    got = gr[0]
    cap3 = capacity_3(got)
    i3 = jnp.where(iota(cap3.shape, 2) % GROUP < GROUP // 2, W / (cap3 + 0.75), 0.0)
    a3 = 0.125 * i3
    c1 = vw[0]
    y1 = 1.2 * c1[1:-1] + a1 * sum_packed(c1, half)[1:-1] + level_2(bw[0], level_3(got) * i3, i2, a2, a3)
    c1 = c1[1:-1]
    y1 = (0.2 * y1 + c1) + a1 * sum_packed(y1, half)
    y1 = ((0.2 * y1 + c1) + a1 * sum_packed(y1, half))[1:-1]
    x = x + lift_0(y1, 0)
    x = (0.2 * x[1:-1] + c0[2:3 * d]) + wide[1:-1] * sum_inner(x, lanes)
    x = (0.2 * x[1:-1] + c0[3:3 * d - 1]) + wide[2:-2] * sum_inner(x, lanes)
    fp_ref[...] = x[2:-2]
    arrive(source)
    b = cap[2:3 * d - 2] * x + src1[...]
    c1x[1:d + 5] = b * wide[2:-2]
    begin(third)

    x, b1 = first_sweeps(b[2:-2], c1x[1:d + 5], a)
    c1 = b1 * i1[1]
    c_sent[...] = c1
    b2, b3 = spread(b1, c1, *near_1)
    r_sent[...] = b3
    b_sent[...] = side_by_side(b2)

    @pl.when(span < spans - 1)
    def _():
        for copy in gather_r[1]:
            copy.start()
        window_start(b_window[1])
        window_start(c_window[1])

    arrive(third)
    first = 1.2 * c1x[1:2] + wide[2:3] * sum_inner(c1x[0:3], lanes)
    final = 1.2 * c1x[d + 4:d + 5] + wide[-3:-2] * sum_inner(c1x[d + 3:d + 6], lanes)
    x = jnp.concatenate([first, x, final], 0)
    x = (0.2 * x[1:-1] + c1x[2:d + 4]) + a * sum_inner(x, lanes)
    fin[0] = (0.2 * x[1:-1] + c1x[3:d + 3]) + a[1:-1] * sum_inner(x, lanes)

    @pl.when(span < spans - 1)
    def _():
        fin_onward.start()

    for pair in (near, far, beyond, source, third, cap_near, cap_far):
        sent(pair)
    each(pass_far, lambda copy: copy.wait_send())
    for copies in (cap_window, b_window[0], c_window[0]):
        window_sent(copies)
    for copy in gather_r[0]:
        copy.wait_send()

    @pl.when(span == 0)
    def _():
        up_ref[...] = u0[...]

    @pl.when(span > 0)
    def _():
        for copy in gather_r[1]:
            copy.wait_recv()
        window_arrive(b_window[1])
        window_arrive(c_window[1])
        fin_onward.wait_recv()
        c1 = vw[1, 1:6]
        y1 = 1.2 * c1 + a1 * sum_packed(c1, half) + level_2(bw[1], level_3(gr[1]) * i3, i2, a2, a3)
        y1 = ((0.2 * y1 + c1) + a1 * sum_packed(y1, half))[1:-1]
        y1 = (0.2 * y1 + c1[1:-1]) + a1[1:-1] * sum_packed(y1, half)
        x = lift_0(y1, 1)
        x = 0.2 * x[1:-1] + a * sum_inner(x, lanes)
        up_ref[...] = fin[1] + (0.2 * x[1:-1] + a[1:-1] * sum_inner(x, lanes))

    @pl.when(span < spans - 1)
    def _():
        for copy in gather_r[1]:
            copy.wait_send()
        window_sent(b_window[1])
        window_sent(c_window[1])
        fin_onward.wait_send()


def shards(span_opening, source_power, warmth_retention):
    parts, spans = lax.axis_size("space"), lax.axis_size("tm")
    steps = source_power.shape[1]
    depth, rows, lanes = warmth_retention.shape
    assert steps == 2 and depth == 4
    slab = jax.ShapeDtypeStruct((depth, rows, lanes), F32)
    vmem = pl.BlockSpec(memory_space=pltpu.VMEM)
    dma = pltpu.SemaphoreType.DMA
    fpoint, updated = pl.pallas_call(
        functools.partial(kernel, parts, spans, steps),
        out_shape=(pltpu.VMEM(slab.shape, F32),) * 2,
        in_specs=[pl.BlockSpec(memory_space=pl.ANY)] * 3,
        out_specs=(vmem, vmem),
        scratch_shapes=[
            pltpu.VMEM((depth, rows, lanes), F32),
            pltpu.VMEM((depth, rows, lanes), F32),
            pltpu.VMEM((depth + 4, rows, lanes), F32),
            pltpu.VMEM((3 * depth, rows, lanes), F32),
            pltpu.VMEM((3 * depth + 2, rows, lanes), F32),
            pltpu.VMEM((depth + 6, rows, lanes), F32),
            pltpu.VMEM((11, rows // 2, lanes), F32),
            pltpu.VMEM((steps, 7, rows // 2, lanes), F32),
            pltpu.VMEM((rows // 2, lanes), F32),
            pltpu.VMEM((steps, 13, rows // 4, lanes), F32),
            pltpu.VMEM((rows // 4, lanes), F32),
            pltpu.VMEM((steps, parts, rows // 8, lanes), F32),
            pltpu.VMEM((rows // 8, lanes), F32),
            pltpu.VMEM((9, rows // 4, lanes), F32),
            pltpu.VMEM((parts * GROUP // lanes // 2, rows // 8, lanes), F32),
            pltpu.VMEM((depth, rows, lanes), F32),
            pltpu.VMEM((6 * rows, lanes), F32),
            pltpu.VMEM((2, depth, rows, lanes), F32),
            pltpu.SemaphoreType.REGULAR,
            dma((4,)), dma((10,)), dma((10,)), dma((4,)), dma((4,)), dma((2, spans)), dma((2, spans)),
            dma((steps, parts)), dma((steps, parts)), dma((5, 13)), dma((5, 13)), dma((2,)),
        ],
        compiler_params=pltpu.CompilerParams(
            collective_id=0, has_side_effects=True, vmem_limit_bytes=67043328 - 2 * 4 * slab.size
        ),
    )(span_opening[0], source_power[0], warmth_retention)
    return fpoint[None], updated[None]


def solution(mesh):
    in_specs = (
        P("tm", "space", None, None),
        P("tm", None, "space", None, None),
        P("space", None, None),
    )
    out_specs = (P("tm", "space", None, None), P("tm", "space", None, None))
    return jax.shard_map(shards, mesh=mesh, in_specs=in_specs, out_specs=out_specs, check_vma=False)
```

```python
import functools

import jax
import jax.numpy as jnp
from jax import lax
from jax.experimental import pallas as pl
from jax.experimental.pallas import tpu as pltpu
from jax.sharding import PartitionSpec as P

COARSE_SWEEPS = 24
W = 0.8
GROUP = 32
NEAR = (1, 2, 3, 4, 8, 12)
F32 = jnp.float32
MESH = pl.DeviceIdType.MESH


def iota(shape, dim):
    return lax.broadcasted_iota(jnp.int32, shape, dim)


def dot(a, b):
    total = None
    for _ in range(3):
        part = a.astype(jnp.bfloat16)
        a = a - part.astype(F32)
        term = jnp.dot(part, b, preferred_element_type=F32)
        total = term if total is None else total + term
    return total


def picks(lanes, pick, scale):
    src, dst = iota((lanes, lanes), 0), iota((lanes, lanes), 1)
    return jnp.where(pick(src, dst), scale, 0.0).astype(jnp.bfloat16)


def in_plane(x, width):
    rows, lanes = x.shape[1], x.shape[2]
    lane, row = iota(x.shape, 2), iota(x.shape, 1)
    left, right = pltpu.roll(x, 1, 2), pltpu.roll(x, lanes - 1, 2)
    if width:
        left = jnp.where(lane % width == 0, 0.0, left)
        right = jnp.where(lane % width == width - 1, 0.0, right)
    up = jnp.where(row == 0, 0.0, pltpu.roll(x, 1, 1))
    down = jnp.where(row == rows - 1, 0.0, pltpu.roll(x, rows - 1, 1))
    return (left + right) + (up + down)


def shifted(x):
    zero = jnp.zeros((1,) + x.shape[1:], F32)
    return jnp.concatenate([zero, x[:-1]], 0), jnp.concatenate([x[1:], zero], 0)


def earlier(x, by=1, shift=0):
    lanes = x.shape[2]
    moved = pltpu.roll(x[-by:], (GROUP + shift) % lanes, 2)
    return jnp.where(iota(moved.shape, 2) < GROUP, 0.0, moved)


def later(x, by=1, shift=0):
    lanes = x.shape[2]
    moved = pltpu.roll(x[:by], (lanes - GROUP + shift) % lanes, 2)
    return jnp.where(iota(moved.shape, 2) >= lanes - GROUP, 0.0, moved)


def sum_grouped(x):
    ends = jnp.concatenate([earlier(x), x, later(x)], 0)
    return in_plane(x, GROUP) + (ends[:-2] + ends[2:])


def sum_planes(x):
    before, after = shifted(x)
    return in_plane(x, None) + (before + after)


def plane_padded(x, by):
    zero = jnp.zeros((by,) + x.shape[1:], F32)
    return jnp.concatenate([zero, x, zero], 0)


def sum_packed(x, width):
    half = pltpu.roll(x, width, 2)
    before, after = shifted(half)
    return in_plane(x, width) + (half + jnp.where(iota(x.shape, 2) < width, before, after))


def sum_inner(x, width):
    return in_plane(x[1:-1], width) + (x[:-2] + x[2:])


def column_sum(x):
    rows = x.shape[1]
    mid = x[1:-1]
    row = iota(mid.shape, 1)
    up = jnp.where(row == 0, 0.0, pltpu.roll(mid, 1, 1))
    down = jnp.where(row == rows - 1, 0.0, pltpu.roll(mid, rows - 1, 1))
    return (x[:-2] + x[2:]) + (up + down)


def coarse_solve(c, a):
    n, lanes = c.shape[0], c.shape[2]

    def turned(x, by):
        return x if by == 0 else pltpu.roll(x, by % lanes, 2)

    def longer(x, by, reach=1):
        return jnp.concatenate([earlier(x, reach, by), turned(x, by), later(x, reach, by)], 0)

    c_at, a_at = [[longer(x, 0) if by == 0 else turned(x, by) for by in (1, 0, -1)] for x in (c, a)]

    def sweep(y, side, c, a):
        return (0.2 * y[1:-1] + c) + a * (side + column_sum(y))

    def two_sweeps(_, y):
        left, mid, right = longer(y, 1), longer(y, 0, 2), longer(y, -1)
        once_left = sweep(left, turned(y, 2) + y, c_at[0], a_at[0])
        once_mid = sweep(mid, left + right, c_at[1], a_at[1])
        once_right = sweep(right, y + turned(y, -2), c_at[2], a_at[2])
        return sweep(once_mid, once_left + once_right, c, a)

    left = COARSE_SWEEPS - 1
    y = c
    if left % 2:
        y = 1.2 * c + a * sum_grouped(c)
    return lax.fori_loop(0, left // 2, two_sweeps, y, unroll=True)


def flat(x):
    return x.reshape(x.shape[0] * x.shape[1], x.shape[2])


def kernel(
    parts, spans, steps,
    open_ref, src_ref, cap_in,
    fp_ref, up_ref,
    u0, src0, src1, cap, c0, c1x, cw, kw, vw, c_sent, bw, b_sent, gr, r_sent, r2s, y3s, own, tmp, fin,
    far_sem, in_sem, hs, hr, ks, kr, fs, fr, gs, gv, ws, wr, ts,
):
    me, span = lax.axis_index("space"), lax.axis_index("tm")
    depth, rows, lanes = open_ref.shape
    half = lanes // 2
    groups = lanes // GROUP
    assert parts == 32 and lanes == 128 and rows == 64
    close = sorted({k % parts for k in NEAR} | {-k % parts for k in NEAR})
    assert {(a + b) % parts for a in close + [0] for b in close + [0]} == set(range(parts))

    cw[...] = jnp.zeros(cw.shape, F32)
    kw[...] = jnp.zeros(kw.shape, F32)
    vw[...] = jnp.zeros(vw.shape, F32)
    bw[...] = jnp.zeros(bw.shape, F32)
    r2s[...] = jnp.zeros(r2s.shape, F32)

    barrier = pltpu.get_barrier_semaphore()
    for k in close:
        pl.semaphore_signal(barrier, inc=1, device_id={"space": (me + k) % parts}, device_id_type=MESH)
    for k in range(1, spans):
        pl.semaphore_signal(barrier, inc=1, device_id={"tm": (span + k) % spans}, device_id_type=MESH)

    loads = [
        pltpu.make_async_copy(cap_in, cap.at[pl.ds(depth, depth)], in_sem.at[0]),
        pltpu.make_async_copy(open_ref, u0, in_sem.at[1]),
        pltpu.make_async_copy(src_ref.at[0], src0, in_sem.at[2]),
        pltpu.make_async_copy(src_ref.at[1], src1.at[pl.ds(2, depth)], in_sem.at[3]),
    ]
    for load in loads:
        load.start()

    down_lo = picks(lanes, lambda s, d: (s // 2 == d) & (d < half), 0.125)
    down_hi = picks(lanes, lambda s, d: s // 2 + half == d, 0.125)
    down_2 = picks(lanes, lambda s, d: (s % half) // 2 == d, 0.125)
    down_3 = picks(lanes, lambda s, d: (s < GROUP) & (d % GROUP == s // 2), 0.125)
    down_cap = picks(lanes, lambda s, d: (s < GROUP) & (d % GROUP == s // 2 + GROUP // 2), 0.125)
    up_lo = picks(lanes, lambda s, d: d // 2 == s, 1.0)
    up_hi = picks(lanes, lambda s, d: d // 2 + half == s, 1.0)
    up_2 = picks(lanes, lambda s, d: (d % half) // 2 == s, 1.0)
    up_3 = picks(lanes, lambda s, d: (d < GROUP) & (d // 2 == s), 1.0)

    def pair_rows(x):
        n, r, w = x.shape
        tmp[pl.ds(0, n * r), :] = flat(x)
        return tmp[pl.ds(0, n * r // 2, 2), :] + tmp[pl.ds(1, n * r // 2, 2), :]

    def twice_rows(x, planes):
        r = x.shape[0]
        tmp[pl.ds(0, r, 2), :] = x
        tmp[pl.ds(1, r, 2), :] = x
        return tmp[pl.ds(0, 2 * r), :].reshape(planes, 2 * r // planes, lanes)

    def pack(x):
        s = pair_rows(x.reshape(depth // 2, 2, rows, lanes).sum(1))
        n = rows // 2
        return dot(s[:n], down_lo) + dot(s[n:], down_hi)

    def to_2(x):
        return dot(pair_rows(x), down_2).reshape(x.shape[0], rows // 4, lanes)

    lane = iota((rows // 8, lanes), 1)

    def turn(planes, off):
        out = []
        for k in range(groups):
            total = None
            for g in range(groups):
                by = (GROUP * (g - k) - off) % lanes
                moved = pltpu.roll(planes[g], by, 1) if by else planes[g]
                total = moved if total is None else jnp.where(lane // GROUP == g, moved, total)
            out.append(total[None])
        return jnp.concatenate(out, 0)

    def level_3(got):
        pairs = [got[0]] + [got[2 * i - 1] + got[2 * i] for i in range(1, parts // 2)] + [got[parts - 1]]
        out = []
        for k in range(groups):
            total = pairs[4 * k + 2]
            for i, keep in (
                (4 * k - 1, lane < GROUP), (4 * k, lane < 2 * GROUP), (4 * k + 1, lane < 3 * GROUP),
                (4 * k + 3, lane >= GROUP), (4 * k + 4, lane >= 2 * GROUP), (4 * k + 5, lane >= 3 * GROUP),
            ):
                if 0 <= i < len(pairs):
                    total = total + jnp.where(keep, pairs[i], 0.0)
            out.append(total)
        return turn(out, 0)

    def capacity_3(got):
        out = []
        for k in range(groups):
            total = None
            for g in range(groups):
                i = 2 * (4 * k + g)
                pair = got[i] + got[i + 1]
                total = pair if total is None else jnp.where(lane // GROUP == g, pair, total)
            out.append(total)
        return turn(out, GROUP // 2)

    def within(k):
        return (me + k >= 0) & (me + k < parts)

    def window(buf, source, sends, recvs, nearest, reach, to={}):
        middle = buf.shape[0] // 2
        return [
            (k, pltpu.make_async_remote_copy(
                source, buf.at[middle - k], sends.at[middle + k], recvs.at[middle + k],
                device_id={"space": (me + k + parts) % parts, **to}, device_id_type=MESH))
            for far in range(nearest, reach + 1) for k in ((far, -far) if far else (0,))
        ]

    def where_within(copies, sign, act):
        for k, copy in copies:
            @pl.when(within(sign * k))
            def _(copy=copy):
                act(copy)

    def window_start(copies):
        where_within(copies, 1, lambda copy: copy.start())

    def window_arrive(copies):
        where_within(copies, -1, lambda copy: copy.wait_recv())

    def window_sent(copies):
        where_within(copies, 1, lambda copy: copy.wait_send())

    def halo(buf, sends, recvs, at, count, up, down, reach=1, rows_at=None):
        def cut(start):
            return buf.at[pl.ds(start, count)] if rows_at is None else buf.at[pl.ds(start, count), rows_at]

        ways = ((up, reach, at), (down, parts - reach, at + 1))
        pair = [
            pltpu.make_async_remote_copy(
                cut(way[0]), cut(way[1]), sends.at[sem], recvs.at[sem],
                device_id={"space": (me + by) % parts}, device_id_type=MESH)
            for way, by, sem in ways
        ]
        return pair + [reach]

    def begin(pair):
        @pl.when(me < parts - pair[2])
        def _():
            pair[0].start()

        @pl.when(me >= pair[2])
        def _():
            pair[1].start()

    def arrive(pair):
        @pl.when(me >= pair[2])
        def _():
            pair[0].wait_recv()

        @pl.when(me < parts - pair[2])
        def _():
            pair[1].wait_recv()

    def sent(pair):
        @pl.when(me < parts - pair[2])
        def _():
            pair[0].wait_send()

        @pl.when(me >= pair[2])
        def _():
            pair[1].wait_send()

    share = rows // spans
    my_rows = pl.ds(pl.multiple_of(span * share, share), share)

    def hand_on(at, count, below, above):
        def copies(start, sem):
            return [
                pltpu.make_async_remote_copy(
                    cap.at[pl.ds(start, count), my_rows], cap.at[pl.ds(start, count), my_rows],
                    fs.at[sem, k], fr.at[sem, k],
                    device_id={"tm": (span + k) % spans}, device_id_type=MESH)
                for k in range(1, spans)
            ]

        return copies(below, at), copies(above, at + 1)

    def each(pair, act):
        @pl.when(me > 0)
        def _():
            for copy in pair[0]:
                act(copy)

        @pl.when(me < parts - 1)
        def _():
            for copy in pair[1]:
                act(copy)

    def hops(k):
        z, y = k // 4, k % 4
        return min(z, parts // 4 - z) + min(y, 4 - y)

    def gather(source, target, sends, recvs, offsets, to):
        return [
            pltpu.make_async_remote_copy(
                source, target, sends.at[k], recvs.at[k],
                device_id={"space": (me + k) % parts, **to}, device_id_type=MESH)
            for k in sorted(offsets, key=lambda k: -hops(k))
        ]

    d = depth
    onward = {"tm": (span + 1) % spans}
    near = halo(c0, hs, hr, 0, 2, (2 * d - 1, d - 1), (d + 1, 2 * d + 1))
    far = halo(c0, hs, hr, 2, 1, (2 * d - 2, d - 2), (d + 3, 2 * d + 3))
    known = halo(src1, hs, hr, 6, 2, (d, 0), (2, d + 2))
    third = halo(c1x, hs, hr, 8, 1, (d, 0), (5, d + 5))
    cap_near = halo(cap, ks, kr, 0, 1, (2 * d - 1, d - 1), (d, 2 * d))
    cap_far = halo(cap, ks, kr, 2, d - 2, (d + 1, 1), (d + 1, 2 * d + 1), rows_at=my_rows)
    pass_far = hand_on(0, d - 2, 1, 2 * d + 1)
    gather_r = [
        gather(gr.at[0, me], gr.at[0, me], gs.at[0], gv.at[0], range(1, parts), {}),
        gather(r_sent, gr.at[1, me], gs.at[1], gv.at[1], range(parts), onward),
    ]
    cap_window = window(cw, cw.at[2], ws.at[0], wr.at[0], 1, 2)
    cap2_window = window(kw, kw.at[5], ws.at[5], wr.at[5], 1, 5)
    c_window = [
        window(vw.at[0], vw.at[0, 3], ws.at[1], wr.at[1], 1, 3),
        window(vw.at[1], c_sent, ws.at[2], wr.at[2], 0, 2, onward),
    ]
    b_window = [
        window(bw.at[0], bw.at[0, 6], ws.at[3], wr.at[3], 1, 6),
        window(bw.at[1], b_sent, ws.at[4], wr.at[4], 0, 6, onward),
    ]
    fin_onward = pltpu.make_async_remote_copy(
        fin.at[0], fin.at[1], ts.at[0], ts.at[1],
        device_id={"tm": (span + 1) % spans}, device_id_type=MESH)

    def clear(ref, start, stop):
        ref[start:stop] = jnp.zeros((stop - start, rows, lanes), F32)

    @pl.when(me == 0)
    def _():
        clear(cap, 0, d)
        clear(c0, 0, d + 1)
        clear(c1x, 0, 3)
        clear(src1, 0, 2)

    @pl.when(me == parts - 1)
    def _():
        clear(cap, 2 * d, 3 * d)
        clear(c0, 2 * d + 1, 3 * d + 2)
        clear(c1x, d + 3, d + 6)
        clear(src1, d + 2, d + 4)

    loads[0].wait()
    mine = cap[d:2 * d]
    loads[1].wait()
    loads[2].wait()
    b = mine * u0[...] + src0[...]
    own[...] = b
    c0[d + 1:2 * d + 1] = b * (W / (mine + 6.0))

    pl.semaphore_wait(barrier, len(close) + spans - 1)
    begin(cap_far)
    begin(near)
    begin(cap_near)
    for k in close:
        pl.semaphore_signal(far_sem, inc=1, device_id={"space": (me + k) % parts}, device_id_type=MESH)
    cap1 = pack(mine)
    cw[2] = cap1
    window_start(cap_window[:2])
    cap2 = to_2(cap1[None])
    kw[5] = cap2[0, :rows // 8] + pltpu.roll(cap2[0, rows // 8:], GROUP, 1)
    window_start(cap2_window[:4])
    begin(far)
    window_start(cap_window[2:])
    window_start(cap2_window[4:8])
    cap_sent = dot(pair_rows(cap2), down_cap)
    loads[3].wait()

    def weights(start, count):
        plane = (me - 1) * depth + start + iota((count, 1, 1), 0)
        inside = (plane >= 0) & (plane < parts * depth)
        return jnp.where(inside, W / (cap[start:start + count] + 6.0), 0.0)

    def inverse(diagonal, start, reach):
        block = me - reach + start + iota((diagonal.shape[0], 1, 1), 0)
        return jnp.where((block >= 0) & (block < parts), W / diagonal, 0.0)

    def inverse_1(start, stop):
        diagonal = cw[start:stop] + 3.0
        return diagonal, inverse(diagonal, start, 2)

    def inverse_2(start, stop):
        packed = kw[start:stop]
        diagonal = jnp.concatenate([packed, pltpu.roll(packed, lanes - GROUP, 2)], 1) + 1.5
        return diagonal, jnp.where(iota(diagonal.shape, 2) < GROUP, inverse(diagonal, start, 5), 0.0)

    arrive(cap_near)
    a = weights(d - 1, d + 2)
    arrive(cap_far)
    each(pass_far, lambda copy: copy.start())

    def first_sweeps(b, c, a):
        x = 1.2 * c[1:-1] + a * sum_inner(c, lanes)
        r = b - (cap[d:2 * d] + 6.0) * x[1:-1] + sum_inner(x, lanes)
        return x, pack(r)

    def spread(b1, c1, i1, d1, a1, i2, d2, a2):
        c1 = plane_padded(c1[None], 1)
        y1 = 1.2 * c1 + a1 * sum_packed(c1, half)
        b2 = to_2(plane_padded(b1[None], 1) - d1 * y1 + 0.5 * sum_packed(y1, half))
        c2 = plane_padded(b2 * i2[1:4], 1)
        y2 = 1.2 * c2 + a2 * sum_planes(c2)
        r2s[1:8] = plane_padded(b2, 2) - plane_padded(d2 * y2, 1) + 0.25 * sum_planes(plane_padded(y2, 1))
        pairs = r2s[pl.ds(me % 2, 8)].reshape(4, 2, rows // 4, lanes).sum(1)
        b3 = dot(pair_rows(pairs), down_3).reshape(4, rows // 8, lanes)
        first = (me + 4 + me % 2) // 2
        return b2, sum(jnp.where(lane // GROUP == (first + q) % groups, b3[q], 0.0) for q in range(4))

    def side_by_side(b2):
        return b2[1] + (pltpu.roll(b2[0], GROUP, 1) + pltpu.roll(b2[2], 2 * GROUP, 1))

    def level_2(b, c3, i2, a2, a3):
        b2 = b[1:-1] + (pltpu.roll(b[2:], lanes - GROUP, 2) + pltpu.roll(b[:-2], lanes - 2 * GROUP, 2))
        c2 = b2 * i2
        y2 = 1.2 * c2[1:-1] + a2 * sum_planes(c2)[1:-1]
        c2 = c2[1:-1]
        y3s[...] = coarse_solve(c3, a3)
        lifts = []
        for q in range(-2, 3):
            at = me // 2 + q
            inside = (at >= 0) & (at < parts // 2)
            at = (at + parts // 2) % (parts // 2)
            plane = pltpu.roll(y3s[at % groups], (lanes - GROUP * (at // groups)) % lanes, 1)
            lifts.append(jnp.where(inside, plane, 0.0))
        lift = twice_rows(dot(jnp.concatenate(lifts, 0), up_3), 5)
        lift = jnp.broadcast_to(lift[:, None], (5, 2) + lift.shape[1:]).reshape((10,) + lift.shape[1:])
        y2 = y2 + jnp.where(me % 2 == 1, lift[1:], lift[:-1])
        y2 = ((0.2 * y2 + c2) + a2 * sum_planes(y2))[1:-1]
        y2 = ((0.2 * y2 + c2[1:-1]) + a2[1:-1] * sum_planes(y2))[1:-1]
        return twice_rows(dot(flat(y2), up_2), 5)

    def lift_0(y1, skip):
        n = rows // 2
        around = flat(y1)
        even, odd = dot(around, up_lo), dot(around, up_hi)
        halves = [part[n * k:n * k + n] for k in range(3) for part in (even, odd)]
        halves = halves[skip:len(halves) - skip]
        planes = len(halves)
        lift = twice_rows(jnp.concatenate(halves, 0), planes)
        return jnp.broadcast_to(lift[:, None], (planes, 2) + lift.shape[1:]).reshape(2 * planes, rows, lanes)

    arrive(near)
    x, b1 = first_sweeps(own[...], c0[d - 1:2 * d + 3], a)
    window_arrive(cap_window[:2])
    window_arrive(cap2_window[:4])
    d1, i1 = inverse_1(1, 4)
    d2, i2 = inverse_2(3, 8)
    near_1 = i1, d1, 0.5 * i1, i2, d2, 0.25 * i2
    c1 = b1 * i1[1]
    vw[0, 3] = c1
    b2, b3 = spread(b1, c1, *near_1)
    gr[0, me] = b3 + cap_sent
    bw[0, 6] = side_by_side(b2)
    pl.semaphore_wait(far_sem, len(close))
    for copy in gather_r[0]:
        copy.start()
    window_start(b_window[0])
    window_start(c_window[0])
    window_start(cap2_window[8:])
    arrive(far)
    each(pass_far, lambda copy: copy.wait_recv())
    wide = weights(1, 3 * d - 2)
    first = 1.2 * c0[d - 1:d] + wide[1:2] * sum_inner(c0[d - 2:d + 1], lanes)
    final = 1.2 * c0[2 * d + 2:2 * d + 3] + wide[-2:-1] * sum_inner(c0[2 * d + 1:2 * d + 4], lanes)

    def last_sweeps(x, c):
        x = (0.2 * x[1:-1] + c) + a * sum_inner(x, lanes)
        return (0.2 * x[1:-1] + c[1:-1]) + a[1:-1] * sum_inner(x, lanes)

    alone = last_sweeps(jnp.concatenate([first, x, final], 0), c0[d:2 * d + 2])
    fp_ref[...] = alone
    src1[2:d + 2] = cap[d:2 * d] * alone + src1[2:d + 2]
    begin(known)
    window_arrive(cap_window[2:])
    a1 = 0.5 * inverse_1(0, 5)[1]
    window_arrive(cap2_window[4:])
    i2 = inverse_2(0, 11)[1]
    a2 = 0.25 * i2[1:-1]
    for copy in gather_r[0]:
        copy.wait_recv()
    window_arrive(b_window[0])
    window_arrive(c_window[0])

    got = gr[0]
    cap3 = capacity_3(got)
    i3 = jnp.where(iota(cap3.shape, 2) % GROUP < GROUP // 2, W / (cap3 + 0.75), 0.0)
    a3 = 0.125 * i3
    c1 = vw[0]
    y1 = 1.2 * c1[1:-1] + a1 * sum_packed(c1, half)[1:-1] + level_2(bw[0], level_3(got) * i3, i2, a2, a3)
    c1 = c1[1:-1]
    y1 = (0.2 * y1 + c1) + a1 * sum_packed(y1, half)
    y1 = ((0.2 * y1 + c1) + a1 * sum_packed(y1, half))[1:-1]
    x = lift_0(y1, 0)
    x = 0.2 * x[1:-1] + wide * sum_inner(x, lanes)
    x = 0.2 * x[1:-1] + wide[1:-1] * sum_inner(x, lanes)
    fp_ref[...] = fp_ref[...] + x[2:-2]
    arrive(known)
    b = cap[2:3 * d - 2] * x + src1[...]
    c1x[1:d + 5] = b * wide[1:-1]
    begin(third)

    x, b1 = first_sweeps(b[2:-2], c1x[1:d + 5], a)
    c1 = b1 * i1[1]
    c_sent[...] = c1
    b2, b3 = spread(b1, c1, *near_1)
    r_sent[...] = b3
    b_sent[...] = side_by_side(b2)

    @pl.when(span < spans - 1)
    def _():
        for copy in gather_r[1]:
            copy.start()
        window_start(b_window[1])
        window_start(c_window[1])

    arrive(third)
    first = 1.2 * c1x[1:2] + wide[1:2] * sum_inner(c1x[0:3], lanes)
    final = 1.2 * c1x[d + 4:d + 5] + wide[-2:-1] * sum_inner(c1x[d + 3:d + 6], lanes)
    fin[0] = last_sweeps(jnp.concatenate([first, x, final], 0), c1x[2:d + 4])

    @pl.when(span < spans - 1)
    def _():
        fin_onward.start()

    for pair in (near, far, known, third, cap_near, cap_far):
        sent(pair)
    each(pass_far, lambda copy: copy.wait_send())
    for copies in (cap_window, cap2_window, b_window[0], c_window[0]):
        window_sent(copies)
    for copy in gather_r[0]:
        copy.wait_send()

    @pl.when(span == 0)
    def _():
        up_ref[...] = u0[...]

    @pl.when(span > 0)
    def _():
        for copy in gather_r[1]:
            copy.wait_recv()
        window_arrive(b_window[1])
        window_arrive(c_window[1])
        fin_onward.wait_recv()
        c1 = vw[1, 1:6]
        y1 = 1.2 * c1 + a1 * sum_packed(c1, half) + level_2(bw[1], level_3(gr[1]) * i3, i2, a2, a3)
        y1 = ((0.2 * y1 + c1) + a1 * sum_packed(y1, half))[1:-1]
        y1 = (0.2 * y1 + c1[1:-1]) + a1[1:-1] * sum_packed(y1, half)
        x = lift_0(y1, 1)
        x = 0.2 * x[1:-1] + a * sum_inner(x, lanes)
        up_ref[...] = fin[1] + (0.2 * x[1:-1] + a[1:-1] * sum_inner(x, lanes))

    @pl.when(span < spans - 1)
    def _():
        for copy in gather_r[1]:
            copy.wait_send()
        window_sent(b_window[1])
        window_sent(c_window[1])
        fin_onward.wait_send()


def shards(span_opening, source_power, warmth_retention):
    parts, spans = lax.axis_size("space"), lax.axis_size("tm")
    steps = source_power.shape[1]
    depth, rows, lanes = warmth_retention.shape
    assert steps == 2 and depth == 4
    slab = jax.ShapeDtypeStruct((depth, rows, lanes), F32)
    vmem = pl.BlockSpec(memory_space=pltpu.VMEM)
    dma = pltpu.SemaphoreType.DMA
    fpoint, updated = pl.pallas_call(
        functools.partial(kernel, parts, spans, steps),
        out_shape=(pltpu.VMEM(slab.shape, F32),) * 2,
        in_specs=[pl.BlockSpec(memory_space=pl.ANY)] * 3,
        out_specs=(vmem, vmem),
        scratch_shapes=[
            pltpu.VMEM((depth, rows, lanes), F32),
            pltpu.VMEM((depth, rows, lanes), F32),
            pltpu.VMEM((depth + 4, rows, lanes), F32),
            pltpu.VMEM((3 * depth, rows, lanes), F32),
            pltpu.VMEM((3 * depth + 2, rows, lanes), F32),
            pltpu.VMEM((depth + 6, rows, lanes), F32),
            pltpu.VMEM((5, rows // 2, lanes), F32),
            pltpu.VMEM((11, rows // 8, lanes), F32),
            pltpu.VMEM((steps, 7, rows // 2, lanes), F32),
            pltpu.VMEM((rows // 2, lanes), F32),
            pltpu.VMEM((steps, 13, rows // 4, lanes), F32),
            pltpu.VMEM((rows // 4, lanes), F32),
            pltpu.VMEM((steps, parts, rows // 8, lanes), F32),
            pltpu.VMEM((rows // 8, lanes), F32),
            pltpu.VMEM((9, rows // 4, lanes), F32),
            pltpu.VMEM((parts * GROUP // lanes // 2, rows // 8, lanes), F32),
            pltpu.VMEM((depth, rows, lanes), F32),
            pltpu.VMEM((6 * rows, lanes), F32),
            pltpu.VMEM((2, depth, rows, lanes), F32),
            pltpu.SemaphoreType.REGULAR,
            dma((4,)), dma((10,)), dma((10,)), dma((4,)), dma((4,)), dma((2, spans)), dma((2, spans)),
            dma((steps, parts)), dma((steps, parts)), dma((6, 13)), dma((6, 13)), dma((2,)),
        ],
        compiler_params=pltpu.CompilerParams(
            collective_id=0, has_side_effects=True, vmem_limit_bytes=67043328 - 2 * 4 * slab.size
        ),
    )(span_opening[0], source_power[0], warmth_retention)
    return fpoint[None], updated[None]


def solution(mesh):
    in_specs = (
        P("tm", "space", None, None),
        P("tm", None, "space", None, None),
        P("space", None, None),
    )
    out_specs = (P("tm", "space", None, None), P("tm", "space", None, None))
    return jax.shard_map(shards, mesh=mesh, in_specs=in_specs, out_specs=out_specs, check_vma=False)
```

```python
import functools

import jax
import jax.numpy as jnp
from jax import lax
from jax.experimental import pallas as pl
from jax.experimental.pallas import tpu as pltpu
from jax.sharding import PartitionSpec as P

COARSE_SWEEPS = 24
W = 0.8
GROUP = 32
NEAR = (1, 2, 3, 4, 5, 8, 12)
F32 = jnp.float32
MESH = pl.DeviceIdType.MESH


def iota(shape, dim):
    return lax.broadcasted_iota(jnp.int32, shape, dim)


def dot(a, b):
    total = None
    for _ in range(3):
        part = a.astype(jnp.bfloat16)
        a = a - part.astype(F32)
        term = jnp.dot(part, b, preferred_element_type=F32)
        total = term if total is None else total + term
    return total


def picks(lanes, pick, scale):
    src, dst = iota((lanes, lanes), 0), iota((lanes, lanes), 1)
    return jnp.where(pick(src, dst), scale, 0.0).astype(jnp.bfloat16)


def in_plane(x, width):
    rows, lanes = x.shape[1], x.shape[2]
    lane, row = iota(x.shape, 2), iota(x.shape, 1)
    left, right = pltpu.roll(x, 1, 2), pltpu.roll(x, lanes - 1, 2)
    if width:
        left = jnp.where(lane % width == 0, 0.0, left)
        right = jnp.where(lane % width == width - 1, 0.0, right)
    up = jnp.where(row == 0, 0.0, pltpu.roll(x, 1, 1))
    down = jnp.where(row == rows - 1, 0.0, pltpu.roll(x, rows - 1, 1))
    return (left + right) + (up + down)


def shifted(x):
    zero = jnp.zeros((1,) + x.shape[1:], F32)
    return jnp.concatenate([zero, x[:-1]], 0), jnp.concatenate([x[1:], zero], 0)


def earlier(x, by=1, shift=0):
    lanes = x.shape[2]
    moved = pltpu.roll(x[-by:], (GROUP + shift) % lanes, 2)
    return jnp.where(iota(moved.shape, 2) < GROUP, 0.0, moved)


def later(x, by=1, shift=0):
    lanes = x.shape[2]
    moved = pltpu.roll(x[:by], (lanes - GROUP + shift) % lanes, 2)
    return jnp.where(iota(moved.shape, 2) >= lanes - GROUP, 0.0, moved)


def sum_grouped(x):
    ends = jnp.concatenate([earlier(x), x, later(x)], 0)
    return in_plane(x, GROUP) + (ends[:-2] + ends[2:])


def sum_planes(x):
    before, after = shifted(x)
    return in_plane(x, None) + (before + after)


def plane_padded(x, by):
    zero = jnp.zeros((by,) + x.shape[1:], F32)
    return jnp.concatenate([zero, x, zero], 0)


def sum_packed(x, width):
    half = pltpu.roll(x, width, 2)
    before, after = shifted(half)
    return in_plane(x, width) + (half + jnp.where(iota(x.shape, 2) < width, before, after))


def sum_inner(x, width):
    return in_plane(x[1:-1], width) + (x[:-2] + x[2:])


def column_sum(x):
    rows = x.shape[1]
    mid = x[1:-1]
    row = iota(mid.shape, 1)
    up = jnp.where(row == 0, 0.0, pltpu.roll(mid, 1, 1))
    down = jnp.where(row == rows - 1, 0.0, pltpu.roll(mid, rows - 1, 1))
    return (x[:-2] + x[2:]) + (up + down)


def coarse_solve(c, a):
    n, lanes = c.shape[0], c.shape[2]

    def turned(x, by):
        return x if by == 0 else pltpu.roll(x, by % lanes, 2)

    def longer(x, by, reach=1):
        return jnp.concatenate([earlier(x, reach, by), turned(x, by), later(x, reach, by)], 0)

    c_at, a_at = [[longer(x, 0) if by == 0 else turned(x, by) for by in (1, 0, -1)] for x in (c, a)]

    def sweep(y, side, c, a):
        return (0.2 * y[1:-1] + c) + a * (side + column_sum(y))

    def two_sweeps(_, y):
        left, mid, right = longer(y, 1), longer(y, 0, 2), longer(y, -1)
        once_left = sweep(left, turned(y, 2) + y, c_at[0], a_at[0])
        once_mid = sweep(mid, left + right, c_at[1], a_at[1])
        once_right = sweep(right, y + turned(y, -2), c_at[2], a_at[2])
        return sweep(once_mid, once_left + once_right, c, a)

    left = COARSE_SWEEPS - 1
    y = c
    if left % 2:
        y = 1.2 * c + a * sum_grouped(c)
    return lax.fori_loop(0, left // 2, two_sweeps, y, unroll=True)


def flat(x):
    return x.reshape(x.shape[0] * x.shape[1], x.shape[2])


def kernel(
    parts, spans, steps,
    open_ref, src_ref, cap_in,
    fp_ref, up_ref,
    u0, src0, src1, cap, c0, c1x, cw, kw, vw, c_sent, bw, b_sent, gr, r_sent, r2s, y3s, own, tmp, fin,
    far_sem, in_sem, send_sem, recv_sem,
):
    me, span = lax.axis_index("space"), lax.axis_index("tm")
    depth, rows, lanes = open_ref.shape
    half = lanes // 2
    groups = lanes // GROUP
    assert parts == 32 and lanes == 128 and rows == 64
    close = sorted({k % parts for k in NEAR} | {-k % parts for k in NEAR})
    assert {(a + b) % parts for a in close + [0] for b in close + [0]} == set(range(parts))

    r2s[...] = jnp.zeros(r2s.shape, F32)

    barrier = pltpu.get_barrier_semaphore()
    for k in close:
        pl.semaphore_signal(barrier, inc=1, device_id={"space": (me + k) % parts}, device_id_type=MESH)
    for k in range(1, spans):
        pl.semaphore_signal(barrier, inc=1, device_id={"tm": (span + k) % spans}, device_id_type=MESH)

    loads = [
        pltpu.make_async_copy(cap_in, cap.at[pl.ds(depth, depth)], in_sem.at[0]),
        pltpu.make_async_copy(open_ref, u0, in_sem.at[1]),
        pltpu.make_async_copy(src_ref.at[0], src0, in_sem.at[2]),
        pltpu.make_async_copy(src_ref.at[1], src1.at[pl.ds(2, depth)], in_sem.at[3]),
    ]
    for load in loads:
        load.start()

    down_lo = picks(lanes, lambda s, d: (s // 2 == d) & (d < half), 0.125)
    down_hi = picks(lanes, lambda s, d: s // 2 + half == d, 0.125)
    down_2 = picks(lanes, lambda s, d: (s % half) // 2 == d, 0.125)
    down_3 = picks(lanes, lambda s, d: (s < GROUP) & (d % GROUP == s // 2), 0.125)
    down_cap = picks(lanes, lambda s, d: (s < GROUP) & (d % GROUP == s // 2 + GROUP // 2), 0.125)
    up_lo = picks(lanes, lambda s, d: d // 2 == s, 1.0)
    up_hi = picks(lanes, lambda s, d: d // 2 + half == s, 1.0)
    up_2 = picks(lanes, lambda s, d: (d % half) // 2 == s, 1.0)
    up_3 = picks(lanes, lambda s, d: (d < GROUP) & (d // 2 == s), 1.0)

    def pair_rows(x):
        n, r, w = x.shape
        tmp[pl.ds(0, n * r), :] = flat(x)
        return tmp[pl.ds(0, n * r // 2, 2), :] + tmp[pl.ds(1, n * r // 2, 2), :]

    def twice_rows(x, planes):
        r = x.shape[0]
        tmp[pl.ds(0, r, 2), :] = x
        tmp[pl.ds(1, r, 2), :] = x
        return tmp[pl.ds(0, 2 * r), :].reshape(planes, 2 * r // planes, lanes)

    def pack(x):
        s = pair_rows(x.reshape(depth // 2, 2, rows, lanes).sum(1))
        n = rows // 2
        return dot(s[:n], down_lo) + dot(s[n:], down_hi)

    def to_2(x):
        return dot(pair_rows(x), down_2).reshape(x.shape[0], rows // 4, lanes)

    lane = iota((rows // 8, lanes), 1)

    def turn(planes, off):
        out = []
        for k in range(groups):
            total = None
            for g in range(groups):
                by = (GROUP * (g - k) - off) % lanes
                moved = pltpu.roll(planes[g], by, 1) if by else planes[g]
                total = moved if total is None else jnp.where(lane // GROUP == g, moved, total)
            out.append(total[None])
        return jnp.concatenate(out, 0)

    def level_3(got):
        pairs = [got[0]] + [got[2 * i - 1] + got[2 * i] for i in range(1, parts // 2)] + [got[parts - 1]]
        out = []
        for k in range(groups):
            total = pairs[4 * k + 2]
            for i, keep in (
                (4 * k - 1, lane < GROUP), (4 * k, lane < 2 * GROUP), (4 * k + 1, lane < 3 * GROUP),
                (4 * k + 3, lane >= GROUP), (4 * k + 4, lane >= 2 * GROUP), (4 * k + 5, lane >= 3 * GROUP),
            ):
                if 0 <= i < len(pairs):
                    total = total + jnp.where(keep, pairs[i], 0.0)
            out.append(total)
        return turn(out, 0)

    def capacity_3(got):
        out = []
        for k in range(groups):
            total = None
            for g in range(groups):
                i = 2 * (4 * k + g)
                pair = got[i] + got[i + 1]
                total = pair if total is None else jnp.where(lane // GROUP == g, pair, total)
            out.append(total)
        return turn(out, GROUP // 2)

    def valid(start, count, of):
        at = start + iota((count, 1, 1), 0)
        return (at >= 0) & (at < of)

    batches = []

    def batch(pieces, total):
        at = len(batches)

        def copy(source, target, to):
            return pltpu.make_async_remote_copy(
                source, target, send_sem.at[at], recv_sem.at[at], device_id=to, device_id_type=MESH)

        made = [copy(*piece) for piece in pieces], copy(total, total, pieces[0][2])
        batches.append(made)
        return made

    def begin(made):
        for copy in made[0]:
            copy.start()

    def arrive(made):
        made[1].wait_recv()

    def sent(made):
        made[1].wait_send()

    def beside(k):
        return {"space": (me + k + parts) % parts}

    share = rows // spans
    my_rows = pl.ds(pl.multiple_of(span * share, share), share)

    def halo(buf, count, up, down, rows_at=None):
        def part(start):
            return buf.at[pl.ds(start, count)] if rows_at is None else buf.at[pl.ds(start, count), rows_at]

        total = buf.at[pl.ds(0, 2 * count)] if rows_at is None else buf.at[pl.ds(0, 2 * count), pl.ds(0, share)]
        return batch([(part(way[0]), part(way[1]), beside(k)) for way, k in ((up, 1), (down, -1))], total)

    def window(buf, source, nearest, reach, to={}):
        middle = buf.shape[0] // 2
        offsets = [k for far in range(nearest, reach + 1) for k in ((far, -far) if far else (0,))]
        return batch([(source, buf.at[middle - k], {**beside(k), **to}) for k in offsets], buf.at[pl.ds(0, len(offsets))])

    def hops(k):
        z, y = k // 4, k % 4
        return min(z, parts // 4 - z) + min(y, 4 - y)

    def gather(buf, source, offsets, to={}):
        offsets = sorted(offsets, key=lambda k: -hops(k))
        return batch([(source, buf.at[me], {**beside(k), **to}) for k in offsets], buf.at[pl.ds(0, len(offsets))])

    d = depth
    onward = {"tm": (span + 1) % spans}
    near = halo(c0, 2, (2 * d - 1, d - 1), (d + 1, 2 * d + 1))
    far = halo(c0, 1, (2 * d - 2, d - 2), (d + 3, 2 * d + 3))
    known = halo(src1, 2, (d, 0), (2, d + 2))
    third = halo(c1x, 1, (d, 0), (5, d + 5))
    cap_near = halo(cap, 1, (2 * d - 1, d - 1), (d, 2 * d))
    cap_far = halo(cap, 2, (d + 1, 1), (d + 1, 2 * d + 1), my_rows)
    pass_far = batch(
        [
            (cap.at[pl.ds(start, 2), my_rows], cap.at[pl.ds(start, 2), my_rows], {"tm": (span + k) % spans})
            for start in (1, 2 * d + 1) for k in range(1, spans)
        ], cap.at[pl.ds(0, 4), pl.ds(0, (spans - 1) * share)])
    cap_window = window(cw, cw.at[2], 1, 1), window(cw, cw.at[2], 2, 2)
    cap2_window = window(kw, kw.at[5], 1, 2), window(kw, kw.at[5], 3, 5)
    gather_r = gather(gr.at[0], gr.at[0, me], range(1, parts)), gather(gr.at[1], r_sent, range(parts), onward)
    c_window = window(vw.at[0], vw.at[0, 3], 1, 3), window(vw.at[1], c_sent, 0, 2, onward)
    b_window = window(bw.at[0], bw.at[0, 6], 1, 6), window(bw.at[1], b_sent, 0, 6, onward)
    fin_onward = batch([(fin.at[0], fin.at[1], onward)], fin.at[0])

    loads[0].wait()
    mine = cap[d:2 * d]
    loads[1].wait()
    loads[2].wait()
    b = mine * u0[...] + src0[...]
    own[...] = b
    c0[d + 1:2 * d + 1] = b * (W / (mine + 6.0))

    pl.semaphore_wait(barrier, len(close) + spans - 1)
    begin(cap_far)
    begin(near)
    begin(cap_near)
    for k in close:
        pl.semaphore_signal(far_sem, inc=1, device_id={"space": (me + k) % parts}, device_id_type=MESH)
    cap1 = pack(mine)
    cw[2] = cap1
    begin(cap_window[0])
    cap2 = to_2(cap1[None])
    kw[5] = cap2[0, :rows // 8] + pltpu.roll(cap2[0, rows // 8:], GROUP, 1)
    begin(cap2_window[0])
    begin(far)
    begin(cap_window[1])
    begin(cap2_window[1])
    cap_sent = dot(pair_rows(cap2), down_cap)
    loads[3].wait()

    def weights(start, count):
        inside = valid((me - 1) * depth + start, count, parts * depth)
        return jnp.where(inside, W / (cap[start:start + count] + 6.0), 0.0)

    def inverse(diagonal, start, reach):
        return jnp.where(valid(me - reach + start, diagonal.shape[0], parts), W / diagonal, 0.0)

    def planes_of(buf, own, start, count):
        return jnp.where(valid(me * depth + start - own, count, parts * depth), buf[start:start + count], 0.0)

    def inverse_1(start, stop):
        diagonal = cw[start:stop] + 3.0
        return diagonal, inverse(diagonal, start, 2)

    def inverse_2(start, stop):
        packed = kw[start:stop]
        diagonal = jnp.concatenate([packed, pltpu.roll(packed, lanes - GROUP, 2)], 1) + 1.5
        return diagonal, jnp.where(iota(diagonal.shape, 2) < GROUP, inverse(diagonal, start, 5), 0.0)

    arrive(cap_near)
    a = weights(d - 1, d + 2)
    arrive(cap_far)
    begin(pass_far)

    def first_sweeps(b, c, a):
        x = 1.2 * c[1:-1] + a * sum_inner(c, lanes)
        r = b - (cap[d:2 * d] + 6.0) * x[1:-1] + sum_inner(x, lanes)
        return x, pack(r)

    def spread(b1, c1, i1, d1, a1, i2, d2, a2):
        c1 = plane_padded(c1[None], 1)
        y1 = 1.2 * c1 + a1 * sum_packed(c1, half)
        b2 = to_2(plane_padded(b1[None], 1) - d1 * y1 + 0.5 * sum_packed(y1, half))
        c2 = plane_padded(b2 * i2[1:4], 1)
        y2 = 1.2 * c2 + a2 * sum_planes(c2)
        r2s[1:8] = plane_padded(b2, 2) - plane_padded(d2 * y2, 1) + 0.25 * sum_planes(plane_padded(y2, 1))
        pairs = r2s[pl.ds(me % 2, 8)].reshape(4, 2, rows // 4, lanes).sum(1)
        b3 = dot(pair_rows(pairs), down_3).reshape(4, rows // 8, lanes)
        first = (me + 4 + me % 2) // 2
        return b2, sum(jnp.where(lane // GROUP == (first + q) % groups, b3[q], 0.0) for q in range(4))

    def side_by_side(b2):
        return b2[1] + (pltpu.roll(b2[0], GROUP, 1) + pltpu.roll(b2[2], 2 * GROUP, 1))

    def level_2(t, c3, i2, a2, a3):
        b = jnp.where(valid(me - 6, 13, parts), bw[t], 0.0)
        b2 = b[1:-1] + (pltpu.roll(b[2:], lanes - GROUP, 2) + pltpu.roll(b[:-2], lanes - 2 * GROUP, 2))
        c2 = b2 * i2
        y2 = 1.2 * c2[1:-1] + a2 * sum_planes(c2)[1:-1]
        c2 = c2[1:-1]
        y3s[...] = coarse_solve(c3, a3)
        lifts = []
        for q in range(-2, 3):
            at = me // 2 + q
            inside = (at >= 0) & (at < parts // 2)
            at = (at + parts // 2) % (parts // 2)
            plane = pltpu.roll(y3s[at % groups], (lanes - GROUP * (at // groups)) % lanes, 1)
            lifts.append(jnp.where(inside, plane, 0.0))
        lift = twice_rows(dot(jnp.concatenate(lifts, 0), up_3), 5)
        lift = jnp.broadcast_to(lift[:, None], (5, 2) + lift.shape[1:]).reshape((10,) + lift.shape[1:])
        y2 = y2 + jnp.where(me % 2 == 1, lift[1:], lift[:-1])
        y2 = ((0.2 * y2 + c2) + a2 * sum_planes(y2))[1:-1]
        y2 = ((0.2 * y2 + c2[1:-1]) + a2[1:-1] * sum_planes(y2))[1:-1]
        return twice_rows(dot(flat(y2), up_2), 5)

    def lift_0(y1, skip):
        n = rows // 2
        around = flat(y1)
        even, odd = dot(around, up_lo), dot(around, up_hi)
        halves = [part[n * k:n * k + n] for k in range(3) for part in (even, odd)]
        halves = halves[skip:len(halves) - skip]
        planes = len(halves)
        lift = twice_rows(jnp.concatenate(halves, 0), planes)
        return jnp.broadcast_to(lift[:, None], (planes, 2) + lift.shape[1:]).reshape(2 * planes, rows, lanes)

    arrive(near)
    x, b1 = first_sweeps(own[...], planes_of(c0, d + 1, d - 1, d + 4), a)
    arrive(cap_window[0])
    arrive(cap2_window[0])
    d1, i1 = inverse_1(1, 4)
    d2, i2 = inverse_2(3, 8)
    near_1 = i1, d1, 0.5 * i1, i2, d2, 0.25 * i2
    c1 = b1 * i1[1]
    vw[0, 3] = c1
    b2, b3 = spread(b1, c1, *near_1)
    gr[0, me] = b3 + cap_sent
    bw[0, 6] = side_by_side(b2)
    pl.semaphore_wait(far_sem, len(close))
    begin(gather_r[0])
    begin(b_window[0])
    begin(c_window[0])
    arrive(far)
    arrive(pass_far)
    wide = weights(1, 3 * d - 2)
    c = planes_of(c0, d + 1, d - 2, d + 6)
    first = 1.2 * c[1:2] + wide[1:2] * sum_inner(c[0:3], lanes)
    final = 1.2 * c[-2:-1] + wide[-2:-1] * sum_inner(c[-3:], lanes)

    def last_sweeps(x, c):
        x = (0.2 * x[1:-1] + c) + a * sum_inner(x, lanes)
        return (0.2 * x[1:-1] + c[1:-1]) + a[1:-1] * sum_inner(x, lanes)

    alone = last_sweeps(jnp.concatenate([first, x, final], 0), c[2:-2])
    fp_ref[...] = alone
    src1[2:d + 2] = cap[d:2 * d] * alone + src1[2:d + 2]
    begin(known)
    arrive(cap_window[1])
    a1 = 0.5 * inverse_1(0, 5)[1]
    arrive(cap2_window[1])
    i2 = inverse_2(0, 11)[1]
    a2 = 0.25 * i2[1:-1]
    arrive(gather_r[0])
    arrive(b_window[0])
    arrive(c_window[0])

    got = gr[0]
    cap3 = capacity_3(got)
    i3 = jnp.where(iota(cap3.shape, 2) % GROUP < GROUP // 2, W / (cap3 + 0.75), 0.0)
    a3 = 0.125 * i3
    c1 = jnp.where(valid(me - 3, 7, parts), vw[0], 0.0)
    y1 = 1.2 * c1[1:-1] + a1 * sum_packed(c1, half)[1:-1] + level_2(0, level_3(got) * i3, i2, a2, a3)
    c1 = c1[1:-1]
    y1 = (0.2 * y1 + c1) + a1 * sum_packed(y1, half)
    y1 = ((0.2 * y1 + c1) + a1 * sum_packed(y1, half))[1:-1]
    x = lift_0(y1, 0)
    x = 0.2 * x[1:-1] + wide * sum_inner(x, lanes)
    x = 0.2 * x[1:-1] + wide[1:-1] * sum_inner(x, lanes)
    fp_ref[...] = fp_ref[...] + x[2:-2]
    arrive(known)
    b = cap[2:3 * d - 2] * x + src1[...]
    c1x[1:d + 5] = b * wide[1:-1]
    begin(third)

    x, b1 = first_sweeps(b[2:-2], c1x[1:d + 5], a)
    c1 = b1 * i1[1]
    c_sent[...] = c1
    b2, b3 = spread(b1, c1, *near_1)
    r_sent[...] = b3
    b_sent[...] = side_by_side(b2)

    @pl.when(span < spans - 1)
    def _():
        begin(gather_r[1])
        begin(b_window[1])
        begin(c_window[1])

    arrive(third)
    c = planes_of(c1x, 3, 0, d + 6)
    first = 1.2 * c[1:2] + wide[1:2] * sum_inner(c[0:3], lanes)
    final = 1.2 * c[-2:-1] + wide[-2:-1] * sum_inner(c[-3:], lanes)
    fin[0] = last_sweeps(jnp.concatenate([first, x, final], 0), c[2:-2])

    @pl.when(span < spans - 1)
    def _():
        begin(fin_onward)

    handed = gather_r[1], b_window[1], c_window[1], fin_onward
    for made in batches:
        if not any(made is other for other in handed):
            sent(made)

    @pl.when(span == 0)
    def _():
        up_ref[...] = u0[...]

    @pl.when(span > 0)
    def _():
        for made in handed:
            arrive(made)
        c1 = jnp.where(valid(me - 2, 5, parts), vw[1, 1:6], 0.0)
        y1 = 1.2 * c1 + a1 * sum_packed(c1, half) + level_2(1, level_3(gr[1]) * i3, i2, a2, a3)
        y1 = ((0.2 * y1 + c1) + a1 * sum_packed(y1, half))[1:-1]
        y1 = (0.2 * y1 + c1[1:-1]) + a1[1:-1] * sum_packed(y1, half)
        x = lift_0(y1, 1)
        x = 0.2 * x[1:-1] + a * sum_inner(x, lanes)
        up_ref[...] = fin[1] + (0.2 * x[1:-1] + a[1:-1] * sum_inner(x, lanes))

    @pl.when(span < spans - 1)
    def _():
        for made in handed:
            sent(made)


def shards(span_opening, source_power, warmth_retention):
    parts, spans = lax.axis_size("space"), lax.axis_size("tm")
    steps = source_power.shape[1]
    depth, rows, lanes = warmth_retention.shape
    assert steps == 2 and depth == 4
    slab = jax.ShapeDtypeStruct((depth, rows, lanes), F32)
    vmem = pl.BlockSpec(memory_space=pltpu.VMEM)
    dma = pltpu.SemaphoreType.DMA
    fpoint, updated = pl.pallas_call(
        functools.partial(kernel, parts, spans, steps),
        out_shape=(pltpu.VMEM(slab.shape, F32),) * 2,
        in_specs=[pl.BlockSpec(memory_space=pl.ANY)] * 3,
        out_specs=(vmem, vmem),
        scratch_shapes=[
            pltpu.VMEM((depth, rows, lanes), F32),
            pltpu.VMEM((depth, rows, lanes), F32),
            pltpu.VMEM((depth + 4, rows, lanes), F32),
            pltpu.VMEM((3 * depth, rows, lanes), F32),
            pltpu.VMEM((3 * depth + 2, rows, lanes), F32),
            pltpu.VMEM((depth + 6, rows, lanes), F32),
            pltpu.VMEM((5, rows // 2, lanes), F32),
            pltpu.VMEM((11, rows // 8, lanes), F32),
            pltpu.VMEM((steps, 7, rows // 2, lanes), F32),
            pltpu.VMEM((rows // 2, lanes), F32),
            pltpu.VMEM((steps, 13, rows // 4, lanes), F32),
            pltpu.VMEM((rows // 4, lanes), F32),
            pltpu.VMEM((steps, parts, rows // 8, lanes), F32),
            pltpu.VMEM((rows // 8, lanes), F32),
            pltpu.VMEM((9, rows // 4, lanes), F32),
            pltpu.VMEM((parts * GROUP // lanes // 2, rows // 8, lanes), F32),
            pltpu.VMEM((depth, rows, lanes), F32),
            pltpu.VMEM((6 * rows, lanes), F32),
            pltpu.VMEM((2, depth, rows, lanes), F32),
            pltpu.SemaphoreType.REGULAR,
            dma((4,)), dma((18,)), dma((18,)),
        ],
        compiler_params=pltpu.CompilerParams(
            collective_id=0, has_side_effects=True, vmem_limit_bytes=67043328 - 2 * 4 * slab.size
        ),
    )(span_opening[0], source_power[0], warmth_retention)
    return fpoint[None], updated[None]


def solution(mesh):
    in_specs = (
        P("tm", "space", None, None),
        P("tm", None, "space", None, None),
        P("space", None, None),
    )
    out_specs = (P("tm", "space", None, None), P("tm", "space", None, None))
    return jax.shard_map(shards, mesh=mesh, in_specs=in_specs, out_specs=out_specs, check_vma=False)
```

```python
import functools

import jax
import jax.numpy as jnp
from jax import lax
from jax.experimental import pallas as pl
from jax.experimental.pallas import tpu as pltpu
from jax.sharding import PartitionSpec as P

COARSE_SWEEPS = 24
W = 0.8
GROUP = 32
NEAR = (1, 3, 4)
F32 = jnp.float32
MESH = pl.DeviceIdType.MESH


def iota(shape, dim):
    return lax.broadcasted_iota(jnp.int32, shape, dim)


def dot(a, b):
    total = None
    for _ in range(2):
        part = a.astype(jnp.bfloat16)
        a = a - part.astype(F32)
        term = jnp.dot(part, b, preferred_element_type=F32)
        total = term if total is None else total + term
    return total


def picks(lanes, pick, scale):
    src, dst = iota((lanes, lanes), 0), iota((lanes, lanes), 1)
    return jnp.where(pick(src, dst), scale, 0.0).astype(jnp.bfloat16)


def from_sides(lanes, pick, width, scale):
    def shifted_pick(by):
        return picks(lanes, lambda s, d: (s % width + by >= 0) & (s % width + by < width) & pick(s + by, d), scale)

    return shifted_pick(-1) + shifted_pick(1)


def to_sides(lanes, pick, width):
    def shifted_pick(by):
        return picks(lanes, lambda s, d: (d % width + by >= 0) & (d % width + by < width) & pick(s, d + by), 1.0)

    return shifted_pick(-1) + shifted_pick(1)


def up_down(x):
    rows = x.shape[1]
    row = iota(x.shape, 1)
    up = jnp.where(row == 0, 0.0, pltpu.roll(x, 1, 1))
    return up + jnp.where(row == rows - 1, 0.0, pltpu.roll(x, rows - 1, 1))


def in_plane(x, width):
    lanes = x.shape[2]
    lane = iota(x.shape, 2)
    left, right = pltpu.roll(x, 1, 2), pltpu.roll(x, lanes - 1, 2)
    if width:
        left = jnp.where(lane % width == 0, 0.0, left)
        right = jnp.where(lane % width == width - 1, 0.0, right)
    return (left + right) + up_down(x)


def shifted(x):
    zero = jnp.zeros((1,) + x.shape[1:], F32)
    return jnp.concatenate([zero, x[:-1]], 0), jnp.concatenate([x[1:], zero], 0)


def earlier(x, by=1, shift=0):
    lanes = x.shape[2]
    moved = pltpu.roll(x[-by:], (GROUP + shift) % lanes, 2)
    return jnp.where(iota(moved.shape, 2) < GROUP, 0.0, moved)


def later(x, by=1, shift=0):
    lanes = x.shape[2]
    moved = pltpu.roll(x[:by], (lanes - GROUP + shift) % lanes, 2)
    return jnp.where(iota(moved.shape, 2) >= lanes - GROUP, 0.0, moved)


def sum_grouped(x):
    ends = jnp.concatenate([earlier(x), x, later(x)], 0)
    return in_plane(x, GROUP) + (ends[:-2] + ends[2:])


def sum_planes(x):
    before, after = shifted(x)
    return in_plane(x, None) + (before + after)


def plane_padded(x, by):
    zero = jnp.zeros((by,) + x.shape[1:], F32)
    return jnp.concatenate([zero, x, zero], 0)


def sum_packed(x, width):
    half = pltpu.roll(x, width, 2)
    before, after = shifted(half)
    return in_plane(x, width) + (half + jnp.where(iota(x.shape, 2) < width, before, after))


def sum_inner(x, width):
    return in_plane(x[1:-1], width) + (x[:-2] + x[2:])


def column_sum(x):
    rows = x.shape[1]
    mid = x[1:-1]
    row = iota(mid.shape, 1)
    up = jnp.where(row == 0, 0.0, pltpu.roll(mid, 1, 1))
    down = jnp.where(row == rows - 1, 0.0, pltpu.roll(mid, rows - 1, 1))
    return (x[:-2] + x[2:]) + (up + down)


def coarse_solve(c, a):
    n, lanes = c.shape[0], c.shape[2]

    def turned(x, by):
        return x if by == 0 else pltpu.roll(x, by % lanes, 2)

    def longer(x, by, reach=1):
        return jnp.concatenate([earlier(x, reach, by), turned(x, by), later(x, reach, by)], 0)

    c_at, a_at = [[longer(x, 0) if by == 0 else turned(x, by) for by in (1, 0, -1)] for x in (c, a)]

    def sweep(y, side, c, a):
        return (0.2 * y[1:-1] + c) + a * (side + column_sum(y))

    def two_sweeps(_, y):
        left, mid, right = longer(y, 1), longer(y, 0, 2), longer(y, -1)
        once_left = sweep(left, turned(y, 2) + y, c_at[0], a_at[0])
        once_mid = sweep(mid, left + right, c_at[1], a_at[1])
        once_right = sweep(right, y + turned(y, -2), c_at[2], a_at[2])
        return sweep(once_mid, once_left + once_right, c, a)

    left = COARSE_SWEEPS - 1
    y = c
    if left % 2:
        y = 1.2 * c + a * sum_grouped(c)
    return lax.fori_loop(0, left // 2, two_sweeps, y, unroll=True)


def flat(x):
    return x.reshape(x.shape[0] * x.shape[1], x.shape[2])


def kernel(
    parts, spans, steps,
    open_ref, src_ref, cap_in,
    fp_ref, up_ref,
    u0, src0, src1, cap, c0, c1x, cw, kw, vw, c_sent, bw, b_sent, gr, r_sent, r2s, y3s, own, tmp, fin,
    near_sem, far_sem, in_sem, send_sem, recv_sem,
):
    me, span = lax.axis_index("space"), lax.axis_index("tm")
    depth, rows, lanes = open_ref.shape
    half = lanes // 2
    groups = lanes // GROUP
    assert parts == 32 and lanes == 128 and rows == 64
    close = sorted({k % parts for k in NEAR} | {-k % parts for k in NEAR})
    nearby = sorted({(a + b) % parts for a in close for b in close + [0]} - {0})
    assert {(a + b) % parts for a in nearby for b in nearby + [0]} == set(range(parts))
    assert set(range(1, 6)) <= set(nearby)

    loads = [
        pltpu.make_async_copy(cap_in, cap.at[pl.ds(depth, depth)], in_sem.at[0]),
        pltpu.make_async_copy(open_ref, u0, in_sem.at[1]),
        pltpu.make_async_copy(src_ref.at[0], src0, in_sem.at[2]),
        pltpu.make_async_copy(src_ref.at[1], src1.at[pl.ds(2, depth)], in_sem.at[3]),
    ]
    for load in loads:
        load.start()
    barrier = pltpu.get_barrier_semaphore()
    for k in close:
        pl.semaphore_signal(barrier, inc=1, device_id={"space": lax.rem(me + k, parts)}, device_id_type=MESH)
    for k in range(1, spans):
        pl.semaphore_signal(barrier, inc=1, device_id={"tm": lax.rem(span + k, spans)}, device_id_type=MESH)

    r2s[...] = jnp.zeros(r2s.shape, F32)
    y3s[...] = jnp.zeros(y3s.shape, F32)

    def pick_lo(s, d):
        return (s // 2 == d) & (d < half)

    def pick_hi(s, d):
        return s // 2 + half == d

    def pick_2(s, d):
        return (s % half) // 2 == d

    def pick_3(s, d):
        return (s < GROUP) & (d % GROUP == s // 2)

    def swap(pick):
        return lambda s, d: pick(d, s)

    down_0 = jnp.concatenate([
        picks(lanes, pick_lo, 0.125), from_sides(lanes, pick_lo, lanes, 0.125),
        picks(lanes, pick_hi, 0.125), from_sides(lanes, pick_hi, lanes, 0.125),
    ], 0)
    down_cap1 = jnp.concatenate([picks(lanes, pick_lo, 0.125), picks(lanes, pick_hi, 0.125)], 0)
    down_2 = picks(lanes, pick_2, 0.125)
    down_1 = jnp.concatenate([
        down_2, from_sides(lanes, pick_2, half, 0.0625) + picks(lanes, pick_2, 0.0625),
        picks(lanes, lambda s, d: pick_2(s, d) & (s >= half), 0.0625),
        picks(lanes, lambda s, d: pick_2(s, d) & (s < half), 0.0625),
    ], 0)
    down_3 = jnp.concatenate([picks(lanes, pick_3, 0.125), from_sides(lanes, pick_3, GROUP, 0.03125)], 0)
    down_cap = picks(lanes, lambda s, d: (s < GROUP) & (d % GROUP == s // 2 + GROUP // 2), 0.125)
    def rises(pick, width):
        return [picks(lanes, pick, 1.0), to_sides(lanes, pick, width)]

    up_lo = jnp.concatenate(rises(lambda s, d: d // 2 == s, lanes), 1)
    up_hi = jnp.concatenate(rises(lambda s, d: d // 2 + half == s, lanes), 1)
    up_2 = jnp.concatenate(rises(swap(pick_2), half), 1)
    up_3 = jnp.concatenate([
        rise for g in range(groups)
        for rise in rises(lambda s, d: (d < GROUP) & (d // 2 + g * GROUP == s), GROUP)
    ], 1)

    def pair_rows(x, at=0):
        n, r, w = x.shape
        tmp[pl.ds(at, n * r), :] = flat(x)
        return tmp[pl.ds(at, n * r // 2, 2), :] + tmp[pl.ds(at + 1, n * r // 2, 2), :]

    def twice_rows(x, planes):
        parts_of = [x[:, at:at + lanes] for at in range(0, x.shape[1], lanes)]
        x = jnp.concatenate(parts_of, 0)
        r = x.shape[0]
        tmp[pl.ds(0, r, 2), :] = x
        tmp[pl.ds(1, r, 2), :] = x
        out = tmp[pl.ds(0, 2 * r), :].reshape(len(parts_of) * planes, -1, lanes)
        return [out[at:at + planes] for at in range(0, out.shape[0], planes)]

    def twice_planes(x):
        return jnp.broadcast_to(x[:, None], (x.shape[0], 2) + x.shape[1:]).reshape((2 * x.shape[0],) + x.shape[1:])

    def slab_pairs(x, at=0):
        s = pair_rows(x.reshape(depth // 2, 2, rows, lanes).sum(1), at)
        return s[:rows // 2], s[rows // 2:]

    def to_2(x):
        return dot(pair_rows(x), down_2).reshape(x.shape[0], rows // 4, lanes)

    lane = iota((rows // 8, lanes), 1)

    def turn(planes, off):
        out = []
        for k in range(groups):
            total = None
            for g in range(groups):
                by = (GROUP * (g - k) - off) % lanes
                moved = pltpu.roll(planes[g], by, 1) if by else planes[g]
                total = moved if total is None else jnp.where(lane // GROUP == g, moved, total)
            out.append(total[None])
        return jnp.concatenate(out, 0)

    def level_3(got):
        pairs = [got[0]] + [got[2 * i - 1] + got[2 * i] for i in range(1, parts // 2)] + [got[parts - 1]]
        out = []
        for k in range(groups):
            total = pairs[4 * k + 2]
            for i, keep in (
                (4 * k - 1, lane < GROUP), (4 * k, lane < 2 * GROUP), (4 * k + 1, lane < 3 * GROUP),
                (4 * k + 3, lane >= GROUP), (4 * k + 4, lane >= 2 * GROUP), (4 * k + 5, lane >= 3 * GROUP),
            ):
                if 0 <= i < len(pairs):
                    total = total + jnp.where(keep, pairs[i], 0.0)
            out.append(total)
        return turn(out, 0)

    def capacity_3(got):
        out = []
        for k in range(groups):
            total = None
            for g in range(groups):
                i = 2 * (4 * k + g)
                pair = got[i] + got[i + 1]
                total = pair if total is None else jnp.where(lane // GROUP == g, pair, total)
            out.append(total)
        return turn(out, GROUP // 2)

    def valid(start, count, of):
        at = start + iota((count, 1, 1), 0)
        return (at >= 0) & (at < of)

    batches = []

    def batch(pieces, total):
        at = len(batches)

        def copy(source, target, to):
            return pltpu.make_async_remote_copy(
                source, target, send_sem.at[at], recv_sem.at[at], device_id=to, device_id_type=MESH)

        made = [copy(*piece) for piece in pieces], copy(total, total, pieces[0][2])
        batches.append(made)
        return made

    def begin(made):
        for copy in made[0]:
            copy.start()

    def arrive(made):
        made[1].wait_recv()

    def sent(made):
        made[1].wait_send()

    def beside(k):
        return {"space": lax.rem(me + (k + parts) % parts, parts)}

    share = rows // spans
    my_rows = pl.ds(pl.multiple_of(span * share, share), share)

    def halo(buf, count, up, down, rows_at=None):
        def part(start):
            return buf.at[pl.ds(start, count)] if rows_at is None else buf.at[pl.ds(start, count), rows_at]

        total = buf.at[pl.ds(0, 2 * count)] if rows_at is None else buf.at[pl.ds(0, 2 * count), pl.ds(0, share)]
        return batch([(part(way[0]), part(way[1]), beside(k)) for way, k in ((up, 1), (down, -1))], total)

    def window(buf, source, nearest, reach, to={}):
        middle = buf.shape[0] // 2
        offsets = [k for far in range(nearest, reach + 1) for k in ((far, -far) if far else (0,))]
        return batch([(source, buf.at[middle - k], {**beside(k), **to}) for k in offsets], buf.at[pl.ds(0, len(offsets))])

    def hops(k):
        z, y = k // 4, k % 4
        return min(z, parts // 4 - z) + min(y, 4 - y)

    def gather(buf, source, offsets, to={}):
        offsets = sorted(offsets, key=lambda k: -hops(k))
        return batch([(source, buf.at[me], {**beside(k), **to}) for k in offsets], buf.at[pl.ds(0, len(offsets))])

    d = depth
    onward = {"tm": (span + 1) % spans}
    near = halo(c0, 2, (2 * d - 1, d - 1), (d + 1, 2 * d + 1))
    far = halo(c0, 1, (2 * d - 2, d - 2), (d + 3, 2 * d + 3))
    known = halo(src1, 2, (d, 0), (2, d + 2))
    third = halo(c1x, 1, (d, 0), (5, d + 5))
    cap_near = halo(cap, 1, (2 * d - 1, d - 1), (d, 2 * d))
    cap_far = halo(cap, 2, (d + 1, 1), (d + 1, 2 * d + 1), my_rows)
    pass_far = batch(
        [
            (cap.at[pl.ds(start, 2), my_rows], cap.at[pl.ds(start, 2), my_rows], {"tm": (span + k) % spans})
            for start in (1, 2 * d + 1) for k in range(1, spans)
        ], cap.at[pl.ds(0, 4), pl.ds(0, (spans - 1) * share)])
    cap_window = window(cw, cw.at[2], 1, 1), window(cw, cw.at[2], 2, 2)
    cap2_window = window(kw, kw.at[5], 1, 2), window(kw, kw.at[5], 3, 5)
    gather_r = gather(gr.at[0], gr.at[0, me], range(1, parts)), gather(gr.at[1], r_sent, range(parts), onward)
    c_window = window(vw.at[0], vw.at[0, 3], 1, 3), window(vw.at[1], c_sent, 0, 2, onward)
    b_window = window(bw.at[0], bw.at[0, 6], 1, 6), window(bw.at[1], b_sent, 0, 6, onward)
    fin_onward = batch([(fin.at[0], fin.at[1], onward)], fin.at[0])

    loads[0].wait()
    mine = cap[d:2 * d]
    loads[1].wait()
    loads[2].wait()
    b = mine * u0[...] + src0[...]
    own[...] = b
    c0[d + 1:2 * d + 1] = b * (W / (mine + 6.0))

    pl.semaphore_wait(barrier, len(close) + spans - 1)
    begin(cap_far)
    begin(near)
    begin(cap_near)
    for k in close:
        pl.semaphore_signal(near_sem, inc=1, device_id=beside(k), device_id_type=MESH)
    cap1 = dot(jnp.concatenate(slab_pairs(mine), 1), down_cap1)
    cw[2] = cap1
    begin(cap_window[0])
    cap2 = to_2(cap1[None])
    kw[5] = cap2[0, :rows // 8] + pltpu.roll(cap2[0, rows // 8:], GROUP, 1)
    begin(far)
    pl.semaphore_wait(near_sem, len(close))
    begin(cap2_window[0])
    for k in nearby:
        pl.semaphore_signal(far_sem, inc=1, device_id=beside(k), device_id_type=MESH)
    begin(cap_window[1])
    begin(cap2_window[1])
    cap_sent = dot(pair_rows(cap2), down_cap)
    loads[3].wait()

    def weights(start, count):
        inside = valid((me - 1) * depth + start, count, parts * depth)
        return jnp.where(inside, W / (cap[start:start + count] + 6.0), 0.0)

    def inverse(diagonal, start, reach):
        return jnp.where(valid(me - reach + start, diagonal.shape[0], parts), W / diagonal, 0.0)

    def planes_of(buf, own, start, count):
        return jnp.where(valid(me * depth + start - own, count, parts * depth), buf[start:start + count], 0.0)

    def inverse_1(start, stop):
        diagonal = cw[start:stop] + 3.0
        return diagonal, inverse(diagonal, start, 2)

    def inverse_2(start, stop):
        packed = kw[start:stop]
        diagonal = jnp.concatenate([packed, pltpu.roll(packed, lanes - GROUP, 2)], 1) + 1.5
        return diagonal, jnp.where(iota(diagonal.shape, 2) < GROUP, inverse(diagonal, start, 5), 0.0)

    arrive(cap_near)
    a = weights(d - 1, d + 2)
    arrive(cap_far)
    begin(pass_far)

    def first_sweeps(b, c, a):
        x = 1.2 * c[1:-1] + a * sum_inner(c, lanes)
        inner = x[1:-1]
        r = b - (cap[d:2 * d] + 6.0) * inner + up_down(inner) + (x[:-2] + x[2:])
        (r_lo, r_hi), (x_lo, x_hi) = slab_pairs(r), slab_pairs(inner, depth * rows // 2)
        return x, dot(jnp.concatenate([r_lo, x_lo, r_hi, x_hi], 1), down_0)

    def spread(b1, c1, i1, d1, a1, i2, d2, a2):
        c1 = plane_padded(c1[None], 1)
        y1 = 1.2 * c1 + a1 * sum_packed(c1, half)
        r1 = pair_rows(plane_padded(b1[None], 1) - d1 * y1 + 0.5 * up_down(y1))
        y1 = pair_rows(y1, 3 * rows // 2)
        n = rows // 4
        none = jnp.zeros((n, lanes), F32)
        around = jnp.concatenate([none, y1[:-n]], 0), jnp.concatenate([y1[n:], none], 0)
        b2 = dot(jnp.concatenate([r1, y1, *around], 1), down_1).reshape(3, n, lanes)
        c2 = plane_padded(b2 * i2[1:4], 1)
        y2 = 1.2 * c2 + a2 * sum_planes(c2)
        r2 = plane_padded(b2, 2) - plane_padded(d2 * y2, 1)
        y2 = plane_padded(y2, 1)
        before, after = shifted(y2)
        r2s[0, 1:8] = r2 + 0.25 * (up_down(y2) + (before + after))
        r2s[1, 1:8] = y2
        pairs = [
            pair_rows(r2s[i, pl.ds(me % 2, 8)].reshape(4, 2, n, lanes).sum(1), i * 4 * n)
            for i in range(2)
        ]
        b3 = dot(jnp.concatenate(pairs, 1), down_3).reshape(4, n // 2, lanes)
        first = (me + 4 + me % 2) // 2
        return b2, sum(jnp.where(lane // GROUP == (first + q) % groups, b3[q], 0.0) for q in range(4))

    def side_by_side(b2):
        return b2[1] + (pltpu.roll(b2[0], GROUP, 1) + pltpu.roll(b2[2], 2 * GROUP, 1))

    def level_2(t, c3, i2, a2, a3):
        b = jnp.where(valid(me - 6, 13, parts), bw[t], 0.0)
        b2 = b[1:-1] + (pltpu.roll(b[2:], lanes - GROUP, 2) + pltpu.roll(b[:-2], lanes - 2 * GROUP, 2))
        c2 = b2 * i2
        y2 = 1.2 * c2[1:-1] + a2 * sum_planes(c2)[1:-1]
        c2 = c2[1:-1]
        y2 = ((0.2 * y2 + c2) + a2 * sum_planes(y2))[1:-1]
        y3 = dot(flat(coarse_solve(c3, a3)), up_3)
        for g in range(groups):
            y3s[2 + 4 * g:6 + 4 * g] = y3[:, 2 * g * lanes:2 * (g + 1) * lanes].reshape(4, rows // 8, 2 * lanes)
        lift, sides = [
            jnp.where(me % 2 == 1, x[1:], x[:-1]) for x in
            [twice_planes(x) for x in twice_rows(y3s[pl.ds(me // 2, 5)].reshape(5 * rows // 8, 2 * lanes), 5)]
        ]
        total = (sides + up_down(lift))[1:-1] + (lift[:-2] + lift[2:])
        y2 = y2 + (0.2 * lift[1:-1] + a2[1:-1] * total)
        y2 = ((0.2 * y2 + c2[1:-1]) + a2[1:-1] * sum_planes(y2))[1:-1]
        return twice_rows(dot(flat(y2), up_2), 5)

    def swept_1(y1, lift, sides, a1):
        before, after = shifted(lift)
        across = lift + jnp.where(iota(lift.shape, 2) < half, before, after)
        return y1 + (0.2 * lift + a1 * ((sides + up_down(lift)) + across))

    def lift_0(y1, skip):
        n = rows // 2
        around = flat(y1)
        both = dot(around, up_lo), dot(around, up_hi)
        halves = [part[n * k:n * k + n] for k in range(3) for part in both]
        halves = halves[skip:len(halves) - skip]
        return [twice_planes(x) for x in twice_rows(jnp.concatenate(halves, 0), len(halves))]

    def swept_0(lift, sides, a):
        total = (sides + up_down(lift))[1:-1] + (lift[:-2] + lift[2:])
        return 0.2 * lift[1:-1] + a * total

    arrive(near)
    x, b1 = first_sweeps(own[...], planes_of(c0, d + 1, d - 1, d + 4), a)
    arrive(cap_window[0])
    arrive(cap2_window[0])
    d1, i1 = inverse_1(1, 4)
    d2, i2 = inverse_2(3, 8)
    near_1 = i1, d1, 0.5 * i1, i2, d2, 0.25 * i2
    c1 = b1 * i1[1]
    vw[0, 3] = c1
    b2, b3 = spread(b1, c1, *near_1)
    gr[0, me] = b3 + cap_sent
    bw[0, 6] = side_by_side(b2)
    pl.semaphore_wait(far_sem, len(nearby))
    begin(gather_r[0])
    begin(b_window[0])
    begin(c_window[0])
    arrive(far)
    arrive(pass_far)
    wide = weights(1, 3 * d - 2)
    c = planes_of(c0, d + 1, d - 2, d + 6)
    first = 1.2 * c[1:2] + wide[1:2] * sum_inner(c[0:3], lanes)
    final = 1.2 * c[-2:-1] + wide[-2:-1] * sum_inner(c[-3:], lanes)

    def last_sweeps(x, c):
        x = (0.2 * x[1:-1] + c) + a * sum_inner(x, lanes)
        return (0.2 * x[1:-1] + c[1:-1]) + a[1:-1] * sum_inner(x, lanes)

    alone = last_sweeps(jnp.concatenate([first, x, final], 0), c[2:-2])
    fp_ref[...] = alone
    src1[2:d + 2] = cap[d:2 * d] * alone + src1[2:d + 2]
    begin(known)
    arrive(cap_window[1])
    a1 = 0.5 * inverse_1(0, 5)[1]
    arrive(cap2_window[1])
    i2 = inverse_2(0, 11)[1]
    a2 = 0.25 * i2[1:-1]
    arrive(gather_r[0])
    arrive(b_window[0])
    arrive(c_window[0])

    got = gr[0]
    cap3 = capacity_3(got)
    i3 = jnp.where(iota(cap3.shape, 2) % GROUP < GROUP // 2, W / (cap3 + 0.75), 0.0)
    a3 = 0.125 * i3
    c1 = jnp.where(valid(me - 3, 7, parts), vw[0], 0.0)
    y1 = 1.2 * c1[1:-1] + a1 * sum_packed(c1, half)[1:-1]
    c1 = c1[1:-1]
    y1 = (0.2 * y1 + c1) + a1 * sum_packed(y1, half)
    y1 = swept_1(y1, *level_2(0, level_3(got) * i3, i2, a2, a3), a1)
    y1 = ((0.2 * y1 + c1) + a1 * sum_packed(y1, half))[1:-1]
    x = swept_0(*lift_0(y1, 0), wide)
    x = 0.2 * x[1:-1] + wide[1:-1] * sum_inner(x, lanes)
    fp_ref[...] = fp_ref[...] + x[2:-2]
    arrive(known)
    b = cap[2:3 * d - 2] * x + src1[...]
    c1x[1:d + 5] = b * wide[1:-1]
    begin(third)

    x, b1 = first_sweeps(b[2:-2], c1x[1:d + 5], a)
    c1 = b1 * i1[1]
    c_sent[...] = c1
    b2, b3 = spread(b1, c1, *near_1)
    r_sent[...] = b3
    b_sent[...] = side_by_side(b2)

    @pl.when(span < spans - 1)
    def _():
        begin(gather_r[1])
        begin(b_window[1])
        begin(c_window[1])

    arrive(third)
    c = planes_of(c1x, 3, 0, d + 6)
    first = 1.2 * c[1:2] + wide[1:2] * sum_inner(c[0:3], lanes)
    final = 1.2 * c[-2:-1] + wide[-2:-1] * sum_inner(c[-3:], lanes)
    fin[0] = last_sweeps(jnp.concatenate([first, x, final], 0), c[2:-2])

    @pl.when(span < spans - 1)
    def _():
        begin(fin_onward)

    handed = gather_r[1], b_window[1], c_window[1], fin_onward
    for made in batches:
        if not any(made is other for other in handed):
            sent(made)

    @pl.when(span == 0)
    def _():
        up_ref[...] = u0[...]

    @pl.when(span > 0)
    def _():
        for made in handed:
            arrive(made)
        c1 = jnp.where(valid(me - 2, 5, parts), vw[1, 1:6], 0.0)
        y1 = 1.2 * c1 + a1 * sum_packed(c1, half)
        y1 = (0.2 * y1 + c1) + a1 * sum_packed(y1, half)
        y1 = swept_1(y1, *level_2(1, level_3(gr[1]) * i3, i2, a2, a3), a1)[1:-1]
        y1 = (0.2 * y1 + c1[1:-1]) + a1[1:-1] * sum_packed(y1, half)
        x = swept_0(*lift_0(y1, 1), a)
        up_ref[...] = fin[1] + (0.2 * x[1:-1] + a[1:-1] * sum_inner(x, lanes))

    @pl.when(span < spans - 1)
    def _():
        for made in handed:
            sent(made)


def shards(span_opening, source_power, warmth_retention):
    parts, spans = lax.axis_size("space"), lax.axis_size("tm")
    steps = source_power.shape[1]
    depth, rows, lanes = warmth_retention.shape
    assert steps == 2 and depth == 4
    slab = jax.ShapeDtypeStruct((depth, rows, lanes), F32)
    vmem = pl.BlockSpec(memory_space=pltpu.VMEM)
    dma = pltpu.SemaphoreType.DMA
    fpoint, updated = pl.pallas_call(
        functools.partial(kernel, parts, spans, steps),
        out_shape=(pltpu.VMEM(slab.shape, F32),) * 2,
        in_specs=[pl.BlockSpec(memory_space=pl.ANY)] * 3,
        out_specs=(vmem, vmem),
        scratch_shapes=[
            pltpu.VMEM((depth, rows, lanes), F32),
            pltpu.VMEM((depth, rows, lanes), F32),
            pltpu.VMEM((depth + 4, rows, lanes), F32),
            pltpu.VMEM((3 * depth, rows, lanes), F32),
            pltpu.VMEM((3 * depth + 2, rows, lanes), F32),
            pltpu.VMEM((depth + 6, rows, lanes), F32),
            pltpu.VMEM((5, rows // 2, lanes), F32),
            pltpu.VMEM((11, rows // 8, lanes), F32),
            pltpu.VMEM((steps, 7, rows // 2, lanes), F32),
            pltpu.VMEM((rows // 2, lanes), F32),
            pltpu.VMEM((steps, 13, rows // 4, lanes), F32),
            pltpu.VMEM((rows // 4, lanes), F32),
            pltpu.VMEM((steps, parts, rows // 8, lanes), F32),
            pltpu.VMEM((rows // 8, lanes), F32),
            pltpu.VMEM((2, 9, rows // 4, lanes), F32),
            pltpu.VMEM((parts // 2 + 4, rows // 8, 2 * lanes), F32),
            pltpu.VMEM((depth, rows, lanes), F32),
            pltpu.VMEM((12 * rows, lanes), F32),
            pltpu.VMEM((2, depth, rows, lanes), F32),
            pltpu.SemaphoreType.REGULAR,
            pltpu.SemaphoreType.REGULAR,
            dma((4,)), dma((18,)), dma((18,)),
        ],
        compiler_params=pltpu.CompilerParams(
            collective_id=0, has_side_effects=True, vmem_limit_bytes=67043328 - 2 * 4 * slab.size
        ),
    )(span_opening[0], source_power[0], warmth_retention)
    return fpoint[None], updated[None]


def solution(mesh):
    in_specs = (
        P("tm", "space", None, None),
        P("tm", None, "space", None, None),
        P("space", None, None),
    )
    out_specs = (P("tm", "space", None, None), P("tm", "space", None, None))
    return jax.shard_map(shards, mesh=mesh, in_specs=in_specs, out_specs=out_specs, check_vma=False)
```

```python
import functools

import jax
import jax.numpy as jnp
from jax import lax
from jax.experimental import pallas as pl
from jax.experimental.pallas import tpu as pltpu
from jax.sharding import PartitionSpec as P

COARSE_SWEEPS = 24
W = 0.8
GROUP = 32
NEAR = (1, 3, 4)
F32 = jnp.float32
MESH = pl.DeviceIdType.MESH


def iota(shape, dim):
    return lax.broadcasted_iota(jnp.int32, shape, dim)


def dot(a, b):
    total = None
    for _ in range(2):
        part = a.astype(jnp.bfloat16)
        a = a - part.astype(F32)
        term = jnp.dot(part, b, preferred_element_type=F32)
        total = term if total is None else total + term
    return total


def picks(lanes, pick, scale):
    src, dst = iota((lanes, lanes), 0), iota((lanes, lanes), 1)
    return jnp.where(pick(src, dst), scale, 0.0).astype(jnp.bfloat16)


def from_sides(lanes, pick, width, scale):
    def shifted_pick(by):
        return picks(lanes, lambda s, d: (s % width + by >= 0) & (s % width + by < width) & pick(s + by, d), scale)

    return shifted_pick(-1) + shifted_pick(1)


def to_sides(lanes, pick, width):
    def shifted_pick(by):
        return picks(lanes, lambda s, d: (d % width + by >= 0) & (d % width + by < width) & pick(s, d + by), 1.0)

    return shifted_pick(-1) + shifted_pick(1)


def up_down(x):
    rows = x.shape[1]
    row = iota(x.shape, 1)
    up = jnp.where(row == 0, 0.0, pltpu.roll(x, 1, 1))
    return up + jnp.where(row == rows - 1, 0.0, pltpu.roll(x, rows - 1, 1))


def in_plane(x, width):
    lanes = x.shape[2]
    lane = iota(x.shape, 2)
    left, right = pltpu.roll(x, 1, 2), pltpu.roll(x, lanes - 1, 2)
    if width:
        left = jnp.where(lane % width == 0, 0.0, left)
        right = jnp.where(lane % width == width - 1, 0.0, right)
    return (left + right) + up_down(x)


def shifted(x):
    zero = jnp.zeros((1,) + x.shape[1:], F32)
    return jnp.concatenate([zero, x[:-1]], 0), jnp.concatenate([x[1:], zero], 0)


def earlier(x, by=1, shift=0):
    lanes = x.shape[2]
    moved = pltpu.roll(x[-by:], (GROUP + shift) % lanes, 2)
    return jnp.where(iota(moved.shape, 2) < GROUP, 0.0, moved)


def later(x, by=1, shift=0):
    lanes = x.shape[2]
    moved = pltpu.roll(x[:by], (lanes - GROUP + shift) % lanes, 2)
    return jnp.where(iota(moved.shape, 2) >= lanes - GROUP, 0.0, moved)


def sum_grouped(x):
    ends = jnp.concatenate([earlier(x), x, later(x)], 0)
    return in_plane(x, GROUP) + (ends[:-2] + ends[2:])


def sum_planes(x):
    before, after = shifted(x)
    return in_plane(x, None) + (before + after)


def plane_padded(x, by):
    zero = jnp.zeros((by,) + x.shape[1:], F32)
    return jnp.concatenate([zero, x, zero], 0)


def sum_packed(x, width):
    half = pltpu.roll(x, width, 2)
    before, after = shifted(half)
    return in_plane(x, width) + (half + jnp.where(iota(x.shape, 2) < width, before, after))


def sum_inner(x, width):
    return in_plane(x[1:-1], width) + (x[:-2] + x[2:])


def column_sum(x):
    rows = x.shape[1]
    mid = x[1:-1]
    row = iota(mid.shape, 1)
    up = jnp.where(row == 0, 0.0, pltpu.roll(mid, 1, 1))
    down = jnp.where(row == rows - 1, 0.0, pltpu.roll(mid, rows - 1, 1))
    return (x[:-2] + x[2:]) + (up + down)


def coarse_solve(c, a):
    n, lanes = c.shape[0], c.shape[2]

    def turned(x, by):
        return x if by == 0 else pltpu.roll(x, by % lanes, 2)

    def longer(x, by, reach=1):
        return jnp.concatenate([earlier(x, reach, by), turned(x, by), later(x, reach, by)], 0)

    c_at, a_at = [[longer(x, 0) if by == 0 else turned(x, by) for by in (1, 0, -1)] for x in (c, a)]

    def sweep(y, side, c, a):
        return (0.2 * y[1:-1] + c) + a * (side + column_sum(y))

    def two_sweeps(_, y):
        left, mid, right = longer(y, 1), longer(y, 0, 2), longer(y, -1)
        once_left = sweep(left, turned(y, 2) + y, c_at[0], a_at[0])
        once_mid = sweep(mid, left + right, c_at[1], a_at[1])
        once_right = sweep(right, y + turned(y, -2), c_at[2], a_at[2])
        return sweep(once_mid, once_left + once_right, c, a)

    left = COARSE_SWEEPS - 1
    y = c
    if left % 2:
        y = 1.2 * c + a * sum_grouped(c)
    return lax.fori_loop(0, left // 2, two_sweeps, y, unroll=True)


def flat(x):
    return x.reshape(x.shape[0] * x.shape[1], x.shape[2])


def kernel(
    parts, spans, steps,
    open_ref, src_ref, cap_in,
    fp_ref, up_ref,
    u0, src0, src1, cap, c0, c1x, cw, kw, vw, c_sent, bw, b_sent, b_own, b_got, gr, r_sent, r2s, y3s, own, tmp, fin,
    near_sem, far_sem, in_sem, send_sem, recv_sem,
):
    me, span = lax.axis_index("space"), lax.axis_index("tm")
    depth, rows, lanes = open_ref.shape
    half = lanes // 2
    groups = lanes // GROUP
    assert parts == 32 and lanes == 128 and rows == 64
    close = sorted({k % parts for k in NEAR} | {-k % parts for k in NEAR})
    nearby = sorted({(a + b) % parts for a in close for b in close + [0]} - {0})
    assert {(a + b) % parts for a in nearby for b in nearby + [0]} == set(range(parts))
    assert set(range(1, 6)) <= set(nearby)

    loads = [
        pltpu.make_async_copy(cap_in, cap.at[pl.ds(depth, depth)], in_sem.at[0]),
        pltpu.make_async_copy(open_ref, u0, in_sem.at[1]),
        pltpu.make_async_copy(src_ref.at[0], src0, in_sem.at[2]),
        pltpu.make_async_copy(src_ref.at[1], src1.at[pl.ds(2, depth)], in_sem.at[3]),
    ]
    for load in loads:
        load.start()
    barrier = pltpu.get_barrier_semaphore()
    for k in close:
        pl.semaphore_signal(barrier, inc=1, device_id={"space": lax.rem(me + k, parts)}, device_id_type=MESH)
    for k in range(1, spans):
        pl.semaphore_signal(barrier, inc=1, device_id={"tm": lax.rem(span + k, spans)}, device_id_type=MESH)

    r2s[...] = jnp.zeros(r2s.shape, F32)
    y3s[...] = jnp.zeros(y3s.shape, F32)

    def pick_lo(s, d):
        return (s // 2 == d) & (d < half)

    def pick_hi(s, d):
        return s // 2 + half == d

    def pick_2(s, d):
        return (s % half) // 2 == d

    def pick_3(s, d):
        return (s < GROUP) & (d % GROUP == s // 2)

    def swap(pick):
        return lambda s, d: pick(d, s)

    down_0 = jnp.concatenate([
        picks(lanes, pick_lo, 0.125), from_sides(lanes, pick_lo, lanes, 0.125),
        picks(lanes, pick_hi, 0.125), from_sides(lanes, pick_hi, lanes, 0.125),
    ], 0)
    down_cap1 = jnp.concatenate([picks(lanes, pick_lo, 0.125), picks(lanes, pick_hi, 0.125)], 0)
    down_2 = picks(lanes, pick_2, 0.125)
    down_1 = jnp.concatenate([
        down_2, from_sides(lanes, pick_2, half, 0.0625) + picks(lanes, pick_2, 0.0625),
        picks(lanes, lambda s, d: pick_2(s, d) & (s >= half), 0.0625),
        picks(lanes, lambda s, d: pick_2(s, d) & (s < half), 0.0625),
    ], 0)
    down_3 = jnp.concatenate([picks(lanes, pick_3, 0.125), from_sides(lanes, pick_3, GROUP, 0.03125)], 0)
    down_cap = picks(lanes, lambda s, d: (s < GROUP) & (d % GROUP == s // 2 + GROUP // 2), 0.125)
    def rises(pick, width):
        return [picks(lanes, pick, 1.0), to_sides(lanes, pick, width)]

    up_lo = jnp.concatenate(rises(lambda s, d: d // 2 == s, lanes), 1)
    up_hi = jnp.concatenate(rises(lambda s, d: d // 2 + half == s, lanes), 1)
    up_2 = jnp.concatenate(rises(swap(pick_2), half), 1)
    up_3 = jnp.concatenate([
        rise for g in range(groups)
        for rise in rises(lambda s, d: (d < GROUP) & (d // 2 + g * GROUP == s), GROUP)
    ], 1)

    def pair_rows(x, at=0):
        n, r, w = x.shape
        tmp[pl.ds(at, n * r), :] = flat(x)
        return tmp[pl.ds(at, n * r // 2, 2), :] + tmp[pl.ds(at + 1, n * r // 2, 2), :]

    def twice_rows(x, planes):
        parts_of = [x[:, at:at + lanes] for at in range(0, x.shape[1], lanes)]
        x = jnp.concatenate(parts_of, 0)
        r = x.shape[0]
        tmp[pl.ds(0, r, 2), :] = x
        tmp[pl.ds(1, r, 2), :] = x
        out = tmp[pl.ds(0, 2 * r), :].reshape(len(parts_of) * planes, -1, lanes)
        return [out[at:at + planes] for at in range(0, out.shape[0], planes)]

    def twice_planes(x):
        return jnp.broadcast_to(x[:, None], (x.shape[0], 2) + x.shape[1:]).reshape((2 * x.shape[0],) + x.shape[1:])

    def slab_pairs(x, at=0):
        s = pair_rows(x.reshape(depth // 2, 2, rows, lanes).sum(1), at)
        return s[:rows // 2], s[rows // 2:]

    def to_2(x):
        return dot(pair_rows(x), down_2).reshape(x.shape[0], rows // 4, lanes)

    lane = iota((rows // 8, lanes), 1)

    def turn(planes, off):
        out = []
        for k in range(groups):
            total = None
            for g in range(groups):
                by = (GROUP * (g - k) - off) % lanes
                moved = pltpu.roll(planes[g], by, 1) if by else planes[g]
                total = moved if total is None else jnp.where(lane // GROUP == g, moved, total)
            out.append(total[None])
        return jnp.concatenate(out, 0)

    def level_3(got):
        pairs = [got[0]] + [got[2 * i - 1] + got[2 * i] for i in range(1, parts // 2)] + [got[parts - 1]]
        out = []
        for k in range(groups):
            total = pairs[4 * k + 2]
            for i, keep in (
                (4 * k - 1, lane < GROUP), (4 * k, lane < 2 * GROUP), (4 * k + 1, lane < 3 * GROUP),
                (4 * k + 3, lane >= GROUP), (4 * k + 4, lane >= 2 * GROUP), (4 * k + 5, lane >= 3 * GROUP),
            ):
                if 0 <= i < len(pairs):
                    total = total + jnp.where(keep, pairs[i], 0.0)
            out.append(total)
        return turn(out, 0)

    def capacity_3(got):
        out = []
        for k in range(groups):
            total = None
            for g in range(groups):
                i = 2 * (4 * k + g)
                pair = got[i] + got[i + 1]
                total = pair if total is None else jnp.where(lane // GROUP == g, pair, total)
            out.append(total)
        return turn(out, GROUP // 2)

    def valid(start, count, of):
        at = start + iota((count, 1, 1), 0)
        return (at >= 0) & (at < of)

    batches = []

    def batch(pieces, total):
        at = len(batches)

        def copy(source, target, to):
            return pltpu.make_async_remote_copy(
                source, target, send_sem.at[at], recv_sem.at[at], device_id=to, device_id_type=MESH)

        made = [copy(*piece) for piece in pieces], copy(total, total, pieces[0][2])
        batches.append(made)
        return made

    def begin(made):
        for copy in made[0]:
            copy.start()

    def arrive(made):
        made[1].wait_recv()

    def sent(made):
        made[1].wait_send()

    def beside(k):
        return {"space": lax.rem(me + (k + parts) % parts, parts)}

    share = rows // spans
    my_rows = pl.ds(pl.multiple_of(span * share, share), share)

    def halo(buf, count, up, down, rows_at=None):
        def part(start):
            return buf.at[pl.ds(start, count)] if rows_at is None else buf.at[pl.ds(start, count), rows_at]

        total = buf.at[pl.ds(0, 2 * count)] if rows_at is None else buf.at[pl.ds(0, 2 * count), pl.ds(0, share)]
        return batch([(part(way[0]), part(way[1]), beside(k)) for way, k in ((up, 1), (down, -1))], total)

    def window(buf, source, nearest, reach, to={}):
        middle = buf.shape[0] // 2
        offsets = [k for far in range(nearest, reach + 1) for k in ((far, -far) if far else (0,))]
        return batch([(source, buf.at[middle - k], {**beside(k), **to}) for k in offsets], buf.at[pl.ds(0, len(offsets))])

    def hops(k):
        z, y = k // 4, k % 4
        return min(z, parts // 4 - z) + min(y, 4 - y)

    def gather(buf, source, offsets, to={}):
        offsets = sorted(offsets, key=lambda k: -hops(k))
        return batch([(source, buf.at[me], {**beside(k), **to}) for k in offsets], buf.at[pl.ds(0, len(offsets))])

    d = depth
    onward = {"tm": (span + 1) % spans}
    near = halo(c0, 2, (2 * d - 1, d - 1), (d + 1, 2 * d + 1))
    far = halo(c0, 1, (2 * d - 2, d - 2), (d + 3, 2 * d + 3))
    known = halo(src1, 2, (d, 0), (2, d + 2))
    third = halo(c1x, 1, (d, 0), (5, d + 5))
    cap_near = halo(cap, 1, (2 * d - 1, d - 1), (d, 2 * d))
    cap_far = halo(cap, 2, (d + 1, 1), (d + 1, 2 * d + 1), my_rows)
    pass_far = batch(
        [
            (cap.at[pl.ds(start, 2), my_rows], cap.at[pl.ds(start, 2), my_rows], {"tm": (span + k) % spans})
            for start in (1, 2 * d + 1) for k in range(1, spans)
        ], cap.at[pl.ds(0, 4), pl.ds(0, (spans - 1) * share)])
    cap_window = window(cw, cw.at[2], 1, 1), window(cw, cw.at[2], 2, 2)
    cap2_window = window(kw, kw.at[5], 1, 2), window(kw, kw.at[5], 3, 5)
    gather_r = gather(gr.at[0], gr.at[0, me], range(1, parts)), gather(gr.at[1], r_sent, range(parts), onward)
    c_window = window(vw.at[0], vw.at[0, 3], 1, 3), window(vw.at[1], c_sent, 0, 2, onward)
    b_window = window(bw.at[0], bw.at[0, 5], 1, 5), window(bw.at[1], b_sent, 0, 5, onward)
    b_near = [
        batch([(b_own.at[t, 2], b_got.at[t, 0], beside(1)), (b_own.at[t, 0], b_got.at[t, 1], beside(-1))], b_got.at[t])
        for t in range(steps)
    ]
    fin_onward = batch([(fin.at[0], fin.at[1], onward)], fin.at[0])

    def pack_2(x):
        return x[:rows // 8] + pltpu.roll(x[rows // 8:], GROUP, 1)

    def unpack_2(x):
        return jnp.concatenate([x, pltpu.roll(x, lanes - GROUP, 2)], 1)

    loads[0].wait()
    mine = cap[d:2 * d]
    loads[1].wait()
    loads[2].wait()
    b = mine * u0[...] + src0[...]
    own[...] = b
    c0[d + 1:2 * d + 1] = b * (W / (mine + 6.0))

    pl.semaphore_wait(barrier, len(close) + spans - 1)
    begin(cap_far)
    begin(near)
    begin(cap_near)
    for k in close:
        pl.semaphore_signal(near_sem, inc=1, device_id=beside(k), device_id_type=MESH)
    cap1 = dot(jnp.concatenate(slab_pairs(mine), 1), down_cap1)
    cw[2] = cap1
    begin(cap_window[0])
    cap2 = to_2(cap1[None])
    kw[5] = pack_2(cap2[0])
    pl.semaphore_wait(near_sem, len(close))
    begin(cap2_window[0])
    begin(far)
    for k in nearby:
        pl.semaphore_signal(far_sem, inc=1, device_id=beside(k), device_id_type=MESH)
    begin(cap_window[1])
    begin(cap2_window[1])
    cap_sent = dot(pair_rows(cap2), down_cap)
    loads[3].wait()

    def weights(start, count):
        inside = valid((me - 1) * depth + start, count, parts * depth)
        return jnp.where(inside, W / (cap[start:start + count] + 6.0), 0.0)

    def inverse(diagonal, start, reach):
        return jnp.where(valid(me - reach + start, diagonal.shape[0], parts), W / diagonal, 0.0)

    def planes_of(buf, own, start, count):
        return jnp.where(valid(me * depth + start - own, count, parts * depth), buf[start:start + count], 0.0)

    def inverse_1(start, stop):
        diagonal = cw[start:stop] + 3.0
        return diagonal, inverse(diagonal, start, 2)

    def inverse_2(start, stop):
        diagonal = unpack_2(kw[start:stop]) + 1.5
        return diagonal, jnp.where(iota(diagonal.shape, 2) < GROUP, inverse(diagonal, start, 5), 0.0)

    arrive(cap_near)
    a = weights(d - 1, d + 2)
    arrive(cap_far)
    begin(pass_far)

    def first_sweeps(b, c, a):
        x = 1.2 * c[1:-1] + a * sum_inner(c, lanes)
        inner = x[1:-1]
        r = b - (cap[d:2 * d] + 6.0) * inner + up_down(inner) + (x[:-2] + x[2:])
        (r_lo, r_hi), (x_lo, x_hi) = slab_pairs(r), slab_pairs(inner, depth * rows // 2)
        return x, dot(jnp.concatenate([r_lo, x_lo, r_hi, x_hi], 1), down_0)

    def spread(t, b1, c1, i1, d1, a1, i2, d2, a2):
        c1 = plane_padded(c1[None], 1)
        y1 = 1.2 * c1 + a1 * sum_packed(c1, half)
        r1 = pair_rows(plane_padded(b1[None], 1) - d1 * y1 + 0.5 * up_down(y1))
        y1 = pair_rows(y1, 3 * rows // 2)
        n = rows // 4
        none = jnp.zeros((n, lanes), F32)
        around = jnp.concatenate([none, y1[:-n]], 0), jnp.concatenate([y1[n:], none], 0)
        b2 = dot(jnp.concatenate([r1, y1, *around], 1), down_1).reshape(3, n, lanes)
        b_own[t] = b2
        begin(b_near[t])
        c2 = plane_padded(b2 * i2[1:4], 1)
        y2 = 1.2 * c2 + a2 * sum_planes(c2)
        r2 = plane_padded(b2, 2) - plane_padded(d2 * y2, 1)
        y2 = plane_padded(y2, 1)
        before, after = shifted(y2)
        r2s[0, 1:8] = r2 + 0.25 * (up_down(y2) + (before + after))
        r2s[1, 1:8] = y2
        pairs = [
            pair_rows(r2s[i, pl.ds(me % 2, 8)].reshape(4, 2, n, lanes).sum(1), i * 4 * n)
            for i in range(2)
        ]
        b3 = dot(jnp.concatenate(pairs, 1), down_3).reshape(4, n // 2, lanes)
        first = (me + 4 + me % 2) // 2
        return sum(jnp.where(lane // GROUP == (first + q) % groups, b3[q], 0.0) for q in range(4))

    def level_2(t, c3, i2, a2, a3):
        c2 = unpack_2(bw[t]) * i2
        y2 = 1.2 * c2[1:-1] + a2 * sum_planes(c2)[1:-1]
        c2 = c2[1:-1]
        y2 = ((0.2 * y2 + c2) + a2 * sum_planes(y2))[1:-1]
        y3 = dot(flat(coarse_solve(c3, a3)), up_3)
        for g in range(groups):
            y3s[2 + 4 * g:6 + 4 * g] = y3[:, 2 * g * lanes:2 * (g + 1) * lanes].reshape(4, rows // 8, 2 * lanes)
        lift, sides = [
            jnp.where(me % 2 == 1, x[1:], x[:-1]) for x in
            [twice_planes(x) for x in twice_rows(y3s[pl.ds(me // 2, 5)].reshape(5 * rows // 8, 2 * lanes), 5)]
        ]
        total = (sides + up_down(lift))[1:-1] + (lift[:-2] + lift[2:])
        y2 = y2 + (0.2 * lift[1:-1] + a2[1:-1] * total)
        y2 = ((0.2 * y2 + c2[1:-1]) + a2[1:-1] * sum_planes(y2))[1:-1]
        return twice_rows(dot(flat(y2), up_2), 5)

    def swept_1(y1, lift, sides, a1):
        before, after = shifted(lift)
        across = lift + jnp.where(iota(lift.shape, 2) < half, before, after)
        return y1 + (0.2 * lift + a1 * ((sides + up_down(lift)) + across))

    def right_2(t):
        arrive(b_near[t])
        got = jnp.where(valid(me - 1, 1, parts), b_got[t, 0:1], 0.0) + jnp.where(valid(me + 1, 1, parts), b_got[t, 1:2], 0.0)
        return pack_2(b_own[t, 1] + got[0])

    def lift_0(y1, skip):
        n = rows // 2
        around = flat(y1)
        both = dot(around, up_lo), dot(around, up_hi)
        halves = [part[n * k:n * k + n] for k in range(3) for part in both]
        halves = halves[skip:len(halves) - skip]
        return [twice_planes(x) for x in twice_rows(jnp.concatenate(halves, 0), len(halves))]

    def swept_0(lift, sides, a):
        total = (sides + up_down(lift))[1:-1] + (lift[:-2] + lift[2:])
        return 0.2 * lift[1:-1] + a * total

    arrive(near)
    x, b1 = first_sweeps(own[...], planes_of(c0, d + 1, d - 1, d + 4), a)
    arrive(cap_window[0])
    arrive(cap2_window[0])
    d1, i1 = inverse_1(1, 4)
    d2, i2 = inverse_2(3, 8)
    near_1 = i1, d1, 0.5 * i1, i2, d2, 0.25 * i2
    c1 = b1 * i1[1]
    vw[0, 3] = c1
    gr[0, me] = spread(0, b1, c1, *near_1) + cap_sent
    pl.semaphore_wait(far_sem, len(nearby))
    begin(gather_r[0])
    begin(c_window[0])
    bw[0, 5] = right_2(0)
    begin(b_window[0])
    arrive(far)
    arrive(pass_far)
    wide = weights(1, 3 * d - 2)
    c = planes_of(c0, d + 1, d - 2, d + 6)
    first = 1.2 * c[1:2] + wide[1:2] * sum_inner(c[0:3], lanes)
    final = 1.2 * c[-2:-1] + wide[-2:-1] * sum_inner(c[-3:], lanes)

    def last_sweeps(x, c):
        x = (0.2 * x[1:-1] + c) + a * sum_inner(x, lanes)
        return (0.2 * x[1:-1] + c[1:-1]) + a[1:-1] * sum_inner(x, lanes)

    alone = last_sweeps(jnp.concatenate([first, x, final], 0), c[2:-2])
    fp_ref[...] = alone
    src1[2:d + 2] = cap[d:2 * d] * alone + src1[2:d + 2]
    begin(known)
    arrive(cap_window[1])
    a1 = 0.5 * inverse_1(0, 5)[1]
    arrive(cap2_window[1])
    i2 = inverse_2(0, 11)[1]
    a2 = 0.25 * i2[1:-1]
    arrive(gather_r[0])
    arrive(b_window[0])
    arrive(c_window[0])

    got = gr[0]
    cap3 = capacity_3(got)
    i3 = jnp.where(iota(cap3.shape, 2) % GROUP < GROUP // 2, W / (cap3 + 0.75), 0.0)
    a3 = 0.125 * i3
    c1 = jnp.where(valid(me - 3, 7, parts), vw[0], 0.0)
    y1 = 1.2 * c1[1:-1] + a1 * sum_packed(c1, half)[1:-1]
    c1 = c1[1:-1]
    y1 = (0.2 * y1 + c1) + a1 * sum_packed(y1, half)
    y1 = swept_1(y1, *level_2(0, level_3(got) * i3, i2, a2, a3), a1)
    y1 = ((0.2 * y1 + c1) + a1 * sum_packed(y1, half))[1:-1]
    x = swept_0(*lift_0(y1, 0), wide)
    x = 0.2 * x[1:-1] + wide[1:-1] * sum_inner(x, lanes)
    fp_ref[...] = fp_ref[...] + x[2:-2]
    arrive(known)
    b = cap[2:3 * d - 2] * x + src1[...]
    c1x[1:d + 5] = b * wide[1:-1]
    begin(third)

    x, b1 = first_sweeps(b[2:-2], c1x[1:d + 5], a)
    c1 = b1 * i1[1]
    c_sent[...] = c1
    r_sent[...] = spread(1, b1, c1, *near_1)

    @pl.when(span < spans - 1)
    def _():
        begin(gather_r[1])
        begin(c_window[1])

    b_sent[...] = right_2(1)

    @pl.when(span < spans - 1)
    def _():
        begin(b_window[1])

    arrive(third)
    c = planes_of(c1x, 3, 0, d + 6)
    first = 1.2 * c[1:2] + wide[1:2] * sum_inner(c[0:3], lanes)
    final = 1.2 * c[-2:-1] + wide[-2:-1] * sum_inner(c[-3:], lanes)
    fin[0] = last_sweeps(jnp.concatenate([first, x, final], 0), c[2:-2])

    @pl.when(span < spans - 1)
    def _():
        begin(fin_onward)

    handed = gather_r[1], b_window[1], c_window[1], fin_onward
    for made in batches:
        if not any(made is other for other in handed):
            sent(made)

    @pl.when(span == 0)
    def _():
        up_ref[...] = u0[...]

    @pl.when(span > 0)
    def _():
        for made in handed:
            arrive(made)
        c1 = jnp.where(valid(me - 2, 5, parts), vw[1, 1:6], 0.0)
        y1 = 1.2 * c1 + a1 * sum_packed(c1, half)
        y1 = (0.2 * y1 + c1) + a1 * sum_packed(y1, half)
        y1 = swept_1(y1, *level_2(1, level_3(gr[1]) * i3, i2, a2, a3), a1)[1:-1]
        y1 = (0.2 * y1 + c1[1:-1]) + a1[1:-1] * sum_packed(y1, half)
        x = swept_0(*lift_0(y1, 1), a)
        up_ref[...] = fin[1] + (0.2 * x[1:-1] + a[1:-1] * sum_inner(x, lanes))

    @pl.when(span < spans - 1)
    def _():
        for made in handed:
            sent(made)


def shards(span_opening, source_power, warmth_retention):
    parts, spans = lax.axis_size("space"), lax.axis_size("tm")
    steps = source_power.shape[1]
    depth, rows, lanes = warmth_retention.shape
    assert steps == 2 and depth == 4
    slab = jax.ShapeDtypeStruct((depth, rows, lanes), F32)
    vmem = pl.BlockSpec(memory_space=pltpu.VMEM)
    dma = pltpu.SemaphoreType.DMA
    fpoint, updated = pl.pallas_call(
        functools.partial(kernel, parts, spans, steps),
        out_shape=(pltpu.VMEM(slab.shape, F32),) * 2,
        in_specs=[pl.BlockSpec(memory_space=pl.ANY)] * 3,
        out_specs=(vmem, vmem),
        scratch_shapes=[
            pltpu.VMEM((depth, rows, lanes), F32),
            pltpu.VMEM((depth, rows, lanes), F32),
            pltpu.VMEM((depth + 4, rows, lanes), F32),
            pltpu.VMEM((3 * depth, rows, lanes), F32),
            pltpu.VMEM((3 * depth + 2, rows, lanes), F32),
            pltpu.VMEM((depth + 6, rows, lanes), F32),
            pltpu.VMEM((5, rows // 2, lanes), F32),
            pltpu.VMEM((11, rows // 8, lanes), F32),
            pltpu.VMEM((steps, 7, rows // 2, lanes), F32),
            pltpu.VMEM((rows // 2, lanes), F32),
            pltpu.VMEM((steps, 11, rows // 8, lanes), F32),
            pltpu.VMEM((rows // 8, lanes), F32),
            pltpu.VMEM((steps, 3, rows // 4, lanes), F32),
            pltpu.VMEM((steps, 2, rows // 4, lanes), F32),
            pltpu.VMEM((steps, parts, rows // 8, lanes), F32),
            pltpu.VMEM((rows // 8, lanes), F32),
            pltpu.VMEM((2, 9, rows // 4, lanes), F32),
            pltpu.VMEM((parts // 2 + 4, rows // 8, 2 * lanes), F32),
            pltpu.VMEM((depth, rows, lanes), F32),
            pltpu.VMEM((12 * rows, lanes), F32),
            pltpu.VMEM((2, depth, rows, lanes), F32),
            pltpu.SemaphoreType.REGULAR,
            pltpu.SemaphoreType.REGULAR,
            dma((4,)), dma((20,)), dma((20,)),
        ],
        compiler_params=pltpu.CompilerParams(
            collective_id=0, has_side_effects=True, vmem_limit_bytes=67043328 - 2 * 4 * slab.size
        ),
    )(span_opening[0], source_power[0], warmth_retention)
    return fpoint[None], updated[None]


def solution(mesh):
    in_specs = (
        P("tm", "space", None, None),
        P("tm", None, "space", None, None),
        P("space", None, None),
    )
    out_specs = (P("tm", "space", None, None), P("tm", "space", None, None))
    return jax.shard_map(shards, mesh=mesh, in_specs=in_specs, out_specs=out_specs, check_vma=False)
```

```python
import functools

import jax
import jax.numpy as jnp
from jax import lax
from jax.experimental import pallas as pl
from jax.experimental.pallas import tpu as pltpu
from jax.sharding import PartitionSpec as P

COARSE_SWEEPS = 24
W = 0.8
GROUP = 32
NEAR = 4
F32 = jnp.float32
MESH = pl.DeviceIdType.MESH


def iota(shape, dim):
    return lax.broadcasted_iota(jnp.int32, shape, dim)


def dot(a, b):
    total = None
    for _ in range(2):
        part = a.astype(jnp.bfloat16)
        a = a - part.astype(F32)
        term = jnp.dot(part, b, preferred_element_type=F32)
        total = term if total is None else total + term
    return total


def picks(lanes, pick, scale):
    src, dst = iota((lanes, lanes), 0), iota((lanes, lanes), 1)
    return jnp.where(pick(src, dst), scale, 0.0).astype(jnp.bfloat16)


def from_sides(lanes, pick, width, scale):
    def shifted_pick(by):
        return picks(lanes, lambda s, d: (s % width + by >= 0) & (s % width + by < width) & pick(s + by, d), scale)

    return shifted_pick(-1) + shifted_pick(1)


def to_sides(lanes, pick, width):
    def shifted_pick(by):
        return picks(lanes, lambda s, d: (d % width + by >= 0) & (d % width + by < width) & pick(s, d + by), 1.0)

    return shifted_pick(-1) + shifted_pick(1)


def up_down(x):
    rows = x.shape[1]
    row = iota(x.shape, 1)
    up = jnp.where(row == 0, 0.0, pltpu.roll(x, 1, 1))
    return up + jnp.where(row == rows - 1, 0.0, pltpu.roll(x, rows - 1, 1))


def in_plane(x, width):
    lanes = x.shape[2]
    lane = iota(x.shape, 2)
    left, right = pltpu.roll(x, 1, 2), pltpu.roll(x, lanes - 1, 2)
    if width:
        left = jnp.where(lane % width == 0, 0.0, left)
        right = jnp.where(lane % width == width - 1, 0.0, right)
    return (left + right) + up_down(x)


def shifted(x):
    zero = jnp.zeros((1,) + x.shape[1:], F32)
    return jnp.concatenate([zero, x[:-1]], 0), jnp.concatenate([x[1:], zero], 0)


def earlier(x, by=1, shift=0):
    lanes = x.shape[2]
    moved = pltpu.roll(x[-by:], (GROUP + shift) % lanes, 2)
    return jnp.where(iota(moved.shape, 2) < GROUP, 0.0, moved)


def later(x, by=1, shift=0):
    lanes = x.shape[2]
    moved = pltpu.roll(x[:by], (lanes - GROUP + shift) % lanes, 2)
    return jnp.where(iota(moved.shape, 2) >= lanes - GROUP, 0.0, moved)


def sum_grouped(x):
    ends = jnp.concatenate([earlier(x), x, later(x)], 0)
    return in_plane(x, GROUP) + (ends[:-2] + ends[2:])


def sum_planes(x):
    before, after = shifted(x)
    return in_plane(x, None) + (before + after)


def plane_padded(x, by):
    zero = jnp.zeros((by,) + x.shape[1:], F32)
    return jnp.concatenate([zero, x, zero], 0)


def sum_packed(x, width):
    half = pltpu.roll(x, width, 2)
    before, after = shifted(half)
    return in_plane(x, width) + (half + jnp.where(iota(x.shape, 2) < width, before, after))


def sum_inner(x, width):
    return in_plane(x[1:-1], width) + (x[:-2] + x[2:])


def column_sum(x):
    rows = x.shape[1]
    mid = x[1:-1]
    row = iota(mid.shape, 1)
    up = jnp.where(row == 0, 0.0, pltpu.roll(mid, 1, 1))
    down = jnp.where(row == rows - 1, 0.0, pltpu.roll(mid, rows - 1, 1))
    return (x[:-2] + x[2:]) + (up + down)


def coarse_solve(c, a):
    n, lanes = c.shape[0], c.shape[2]

    def turned(x, by):
        return x if by == 0 else pltpu.roll(x, by % lanes, 2)

    def longer(x, by, reach=1):
        return jnp.concatenate([earlier(x, reach, by), turned(x, by), later(x, reach, by)], 0)

    c_at, a_at = [[longer(x, 0) if by == 0 else turned(x, by) for by in (1, 0, -1)] for x in (c, a)]

    def sweep(y, side, c, a):
        return (0.2 * y[1:-1] + c) + a * (side + column_sum(y))

    def two_sweeps(_, y):
        left, mid, right = longer(y, 1), longer(y, 0, 2), longer(y, -1)
        once_left = sweep(left, turned(y, 2) + y, c_at[0], a_at[0])
        once_mid = sweep(mid, left + right, c_at[1], a_at[1])
        once_right = sweep(right, y + turned(y, -2), c_at[2], a_at[2])
        return sweep(once_mid, once_left + once_right, c, a)

    left = COARSE_SWEEPS - 1
    y = c
    if left % 2:
        y = 1.2 * c + a * sum_grouped(c)
    return lax.fori_loop(0, left // 2, two_sweeps, y, unroll=True)


def flat(x):
    return x.reshape(x.shape[0] * x.shape[1], x.shape[2])


def kernel(
    parts, spans, steps,
    open_ref, src_ref, cap_in,
    fp_ref, up_ref,
    u0, src0, src1, cap, c0, c1x, cw, kw, vw, c_sent, bw, b_sent, gr, r_sent, r2s, y3s, own, tmp, fin,
    near_sem, far_sem, in_sem, send_sem, recv_sem,
):
    me, span = lax.axis_index("space"), lax.axis_index("tm")
    depth, rows, lanes = open_ref.shape
    half = lanes // 2
    groups = lanes // GROUP
    assert parts == 32 and lanes == 128 and rows == 64
    assert parts == 8 * NEAR
    close = [k for k in range(-NEAR, NEAR + 1) if k]

    loads = [
        pltpu.make_async_copy(cap_in, cap.at[pl.ds(depth, depth)], in_sem.at[0]),
        pltpu.make_async_copy(open_ref, u0, in_sem.at[1]),
        pltpu.make_async_copy(src_ref.at[0], src0, in_sem.at[2]),
        pltpu.make_async_copy(src_ref.at[1], src1.at[pl.ds(2, depth)], in_sem.at[3]),
    ]
    for load in loads:
        load.start()
    barrier = pltpu.get_barrier_semaphore()
    for k in close:
        pl.semaphore_signal(barrier, inc=1, device_id={"space": lax.rem(me + k % parts, parts)}, device_id_type=MESH)
    for k in range(1, spans):
        pl.semaphore_signal(barrier, inc=1, device_id={"tm": lax.rem(span + k, spans)}, device_id_type=MESH)

    r2s[...] = jnp.zeros(r2s.shape, F32)
    y3s[...] = jnp.zeros(y3s.shape, F32)

    def pick_lo(s, d):
        return (s // 2 == d) & (d < half)

    def pick_hi(s, d):
        return s // 2 + half == d

    def pick_2(s, d):
        return (s % half) // 2 == d

    def pick_3(s, d):
        return (s < GROUP) & (d % GROUP == s // 2)

    def swap(pick):
        return lambda s, d: pick(d, s)

    down_0 = jnp.concatenate([
        picks(lanes, pick_lo, 0.125), from_sides(lanes, pick_lo, lanes, 0.125),
        picks(lanes, pick_hi, 0.125), from_sides(lanes, pick_hi, lanes, 0.125),
    ], 0)
    down_cap1 = jnp.concatenate([picks(lanes, pick_lo, 0.125), picks(lanes, pick_hi, 0.125)], 0)
    down_2 = picks(lanes, pick_2, 0.125)
    down_1 = jnp.concatenate([
        down_2, from_sides(lanes, pick_2, half, 0.0625) + picks(lanes, pick_2, 0.0625),
        picks(lanes, lambda s, d: pick_2(s, d) & (s >= half), 0.0625),
        picks(lanes, lambda s, d: pick_2(s, d) & (s < half), 0.0625),
    ], 0)
    down_3 = jnp.concatenate([picks(lanes, pick_3, 0.125), from_sides(lanes, pick_3, GROUP, 0.03125)], 0)
    down_cap = picks(lanes, lambda s, d: (s < GROUP) & (d % GROUP == s // 2 + GROUP // 2), 0.125)
    def rises(pick, width):
        return [picks(lanes, pick, 1.0), to_sides(lanes, pick, width)]

    up_lo = jnp.concatenate(rises(lambda s, d: d // 2 == s, lanes), 1)
    up_hi = jnp.concatenate(rises(lambda s, d: d // 2 + half == s, lanes), 1)
    up_2 = jnp.concatenate(rises(swap(pick_2), half), 1)
    up_3 = jnp.concatenate([
        rise for g in range(groups)
        for rise in rises(lambda s, d: (d < GROUP) & (d // 2 + g * GROUP == s), GROUP)
    ], 1)

    def pair_rows(x, at=0):
        n, r, w = x.shape
        tmp[pl.ds(at, n * r), :] = flat(x)
        return tmp[pl.ds(at, n * r // 2, 2), :] + tmp[pl.ds(at + 1, n * r // 2, 2), :]

    def twice_rows(x, planes):
        parts_of = [x[:, at:at + lanes] for at in range(0, x.shape[1], lanes)]
        x = jnp.concatenate(parts_of, 0)
        r = x.shape[0]
        tmp[pl.ds(0, r, 2), :] = x
        tmp[pl.ds(1, r, 2), :] = x
        out = tmp[pl.ds(0, 2 * r), :].reshape(len(parts_of) * planes, -1, lanes)
        return [out[at:at + planes] for at in range(0, out.shape[0], planes)]

    def twice_planes(x):
        return jnp.broadcast_to(x[:, None], (x.shape[0], 2) + x.shape[1:]).reshape((2 * x.shape[0],) + x.shape[1:])

    def slab_pairs(x, at=0):
        s = pair_rows(x.reshape(depth // 2, 2, rows, lanes).sum(1), at)
        return s[:rows // 2], s[rows // 2:]

    def to_2(x):
        return dot(pair_rows(x), down_2).reshape(x.shape[0], rows // 4, lanes)

    lane = iota((rows // 8, lanes), 1)

    def turn(planes, off):
        out = []
        for k in range(groups):
            total = None
            for g in range(groups):
                by = (GROUP * (g - k) - off) % lanes
                moved = pltpu.roll(planes[g], by, 1) if by else planes[g]
                total = moved if total is None else jnp.where(lane // GROUP == g, moved, total)
            out.append(total[None])
        return jnp.concatenate(out, 0)

    def level_3(got):
        pairs = [got[0]] + [got[2 * i - 1] + got[2 * i] for i in range(1, parts // 2)] + [got[parts - 1]]
        out = []
        for k in range(groups):
            total = pairs[4 * k + 2]
            for i, keep in (
                (4 * k - 1, lane < GROUP), (4 * k, lane < 2 * GROUP), (4 * k + 1, lane < 3 * GROUP),
                (4 * k + 3, lane >= GROUP), (4 * k + 4, lane >= 2 * GROUP), (4 * k + 5, lane >= 3 * GROUP),
            ):
                if 0 <= i < len(pairs):
                    total = total + jnp.where(keep, pairs[i], 0.0)
            out.append(total)
        return turn(out, 0)

    def capacity_3(got):
        out = []
        for k in range(groups):
            total = None
            for g in range(groups):
                i = 2 * (4 * k + g)
                pair = got[i] + got[i + 1]
                total = pair if total is None else jnp.where(lane // GROUP == g, pair, total)
            out.append(total)
        return turn(out, GROUP // 2)

    def valid(start, count, of):
        at = start + iota((count, 1, 1), 0)
        return (at >= 0) & (at < of)

    batches = []

    def batch(pieces, total):
        at = len(batches)

        def copy(source, target, to):
            return pltpu.make_async_remote_copy(
                source, target, send_sem.at[at], recv_sem.at[at], device_id=to, device_id_type=MESH)

        made = [copy(*piece) for piece in pieces], copy(total, total, pieces[0][2])
        batches.append(made)
        return made

    def begin(made):
        for copy in made[0]:
            copy.start()

    def arrive(made):
        made[1].wait_recv()

    def sent(made):
        made[1].wait_send()

    def beside(k):
        return {"space": lax.rem(me + (k + parts) % parts, parts)}

    share = rows // spans
    my_rows = pl.ds(pl.multiple_of(span * share, share), share)

    def halo(buf, count, up, down, rows_at=None):
        def part(start):
            return buf.at[pl.ds(start, count)] if rows_at is None else buf.at[pl.ds(start, count), rows_at]

        total = buf.at[pl.ds(0, 2 * count)] if rows_at is None else buf.at[pl.ds(0, 2 * count), pl.ds(0, share)]
        return batch([(part(way[0]), part(way[1]), beside(k)) for way, k in ((up, 1), (down, -1))], total)

    def window(buf, source, nearest, reach, to={}):
        middle = buf.shape[0] // 2
        offsets = [k for far in range(reach, nearest - 1, -1) for k in ((far, -far) if far else (0,))]
        return batch([(source, buf.at[middle - k], {**beside(k), **to}) for k in offsets], buf.at[pl.ds(0, len(offsets))])

    def hops(k):
        z, y = k // 4, k % 4
        return min(z, parts // 4 - z) + min(y, 4 - y)

    def gather(buf, source, offsets, to={}):
        offsets = sorted(offsets, key=lambda k: -hops(k))
        return batch([(source, buf.at[me], {**beside(k), **to}) for k in offsets], buf.at[pl.ds(0, len(offsets))])

    d = depth
    onward = {"tm": (span + 1) % spans}
    near = halo(c0, 2, (2 * d - 1, d - 1), (d + 1, 2 * d + 1))
    far = halo(c0, 1, (2 * d - 2, d - 2), (d + 3, 2 * d + 3))
    known = halo(src1, 2, (d, 0), (2, d + 2))
    third = halo(c1x, 1, (d, 0), (5, d + 5))
    cap_near = halo(cap, 1, (2 * d - 1, d - 1), (d, 2 * d))
    cap_far = halo(cap, 2, (d + 1, 1), (d + 1, 2 * d + 1), my_rows)
    pass_far = batch(
        [
            (cap.at[pl.ds(start, 2), my_rows], cap.at[pl.ds(start, 2), my_rows], {"tm": (span + k) % spans})
            for start in (1, 2 * d + 1) for k in range(1, spans)
        ], cap.at[pl.ds(0, 4), pl.ds(0, (spans - 1) * share)])
    cap_window = window(cw, cw.at[2], 1, 1), window(cw, cw.at[2], 2, 2)
    cap2_window = window(kw, kw.at[5], 1, 2), window(kw, kw.at[5], 3, 5)
    gather_r = gather(gr.at[0], gr.at[0, me], range(1, parts)), gather(gr.at[1], r_sent, range(parts), onward)
    c_window = window(vw.at[0], vw.at[0, 3], 1, 3), window(vw.at[1], c_sent, 0, 2, onward)
    b_window = window(bw.at[0], bw.at[0, 6], 1, 6), window(bw.at[1], b_sent, 0, 6, onward)
    fin_onward = batch([(fin.at[0], fin.at[1], onward)], fin.at[0])

    loads[0].wait()
    mine = cap[d:2 * d]
    loads[1].wait()
    loads[2].wait()
    b = mine * u0[...] + src0[...]
    own[...] = b
    c0[d + 1:2 * d + 1] = b * (W / (mine + 6.0))

    pl.semaphore_wait(barrier, len(close) + spans - 1)
    begin(cap_far)
    begin(near)
    begin(cap_near)
    for k in (NEAR, -NEAR):
        pl.semaphore_signal(near_sem, inc=1, device_id=beside(k), device_id_type=MESH)
    cap1 = dot(jnp.concatenate(slab_pairs(mine), 1), down_cap1)
    cw[2] = cap1
    begin(cap_window[0])
    cap2 = to_2(cap1[None])
    kw[5] = cap2[0, :rows // 8] + pltpu.roll(cap2[0, rows // 8:], GROUP, 1)
    begin(cap2_window[0])
    begin(far)
    pl.semaphore_wait(near_sem, 2)
    for k in (2 * NEAR, -2 * NEAR):
        pl.semaphore_signal(far_sem, inc=1, device_id=beside(k), device_id_type=MESH)
    begin(cap_window[1])
    begin(cap2_window[1])
    cap_sent = dot(pair_rows(cap2), down_cap)
    loads[3].wait()

    def weights(start, count):
        inside = valid((me - 1) * depth + start, count, parts * depth)
        return jnp.where(inside, W / (cap[start:start + count] + 6.0), 0.0)

    def inverse(diagonal, start, reach):
        return jnp.where(valid(me - reach + start, diagonal.shape[0], parts), W / diagonal, 0.0)

    def planes_of(buf, own, start, count):
        return jnp.where(valid(me * depth + start - own, count, parts * depth), buf[start:start + count], 0.0)

    def inverse_1(start, stop):
        diagonal = cw[start:stop] + 3.0
        return diagonal, inverse(diagonal, start, 2)

    def inverse_2(start, stop):
        packed = kw[start:stop]
        diagonal = jnp.concatenate([packed, pltpu.roll(packed, lanes - GROUP, 2)], 1) + 1.5
        return diagonal, jnp.where(iota(diagonal.shape, 2) < GROUP, inverse(diagonal, start, 5), 0.0)

    arrive(cap_near)
    a = weights(d - 1, d + 2)
    arrive(cap_far)
    begin(pass_far)

    def first_sweeps(b, c, a):
        x = 1.2 * c[1:-1] + a * sum_inner(c, lanes)
        inner = x[1:-1]
        r = b - (cap[d:2 * d] + 6.0) * inner + up_down(inner) + (x[:-2] + x[2:])
        (r_lo, r_hi), (x_lo, x_hi) = slab_pairs(r), slab_pairs(inner, depth * rows // 2)
        return x, dot(jnp.concatenate([r_lo, x_lo, r_hi, x_hi], 1), down_0)

    def spread(b1, c1, i1, d1, a1, i2, d2, a2):
        c1 = plane_padded(c1[None], 1)
        y1 = 1.2 * c1 + a1 * sum_packed(c1, half)
        r1 = pair_rows(plane_padded(b1[None], 1) - d1 * y1 + 0.5 * up_down(y1))
        y1 = pair_rows(y1, 3 * rows // 2)
        n = rows // 4
        none = jnp.zeros((n, lanes), F32)
        around = jnp.concatenate([none, y1[:-n]], 0), jnp.concatenate([y1[n:], none], 0)
        b2 = dot(jnp.concatenate([r1, y1, *around], 1), down_1).reshape(3, n, lanes)
        c2 = plane_padded(b2 * i2[1:4], 1)
        y2 = 1.2 * c2 + a2 * sum_planes(c2)
        r2 = plane_padded(b2, 2) - plane_padded(d2 * y2, 1)
        y2 = plane_padded(y2, 1)
        before, after = shifted(y2)
        r2s[0, 1:8] = r2 + 0.25 * (up_down(y2) + (before + after))
        r2s[1, 1:8] = y2
        pairs = [
            pair_rows(r2s[i, pl.ds(me % 2, 8)].reshape(4, 2, n, lanes).sum(1), i * 4 * n)
            for i in range(2)
        ]
        b3 = dot(jnp.concatenate(pairs, 1), down_3).reshape(4, n // 2, lanes)
        first = (me + 4 + me % 2) // 2
        return b2, sum(jnp.where(lane // GROUP == (first + q) % groups, b3[q], 0.0) for q in range(4))

    def side_by_side(b2):
        return b2[1] + (pltpu.roll(b2[0], GROUP, 1) + pltpu.roll(b2[2], 2 * GROUP, 1))

    def level_2(t, c3, i2, a2, a3):
        b = jnp.where(valid(me - 6, 13, parts), bw[t], 0.0)
        b2 = b[1:-1] + (pltpu.roll(b[2:], lanes - GROUP, 2) + pltpu.roll(b[:-2], lanes - 2 * GROUP, 2))
        c2 = b2 * i2
        y2 = 1.2 * c2[1:-1] + a2 * sum_planes(c2)[1:-1]
        c2 = c2[1:-1]
        y2 = ((0.2 * y2 + c2) + a2 * sum_planes(y2))[1:-1]
        y3 = dot(flat(coarse_solve(c3, a3)), up_3)
        for g in range(groups):
            y3s[2 + 4 * g:6 + 4 * g] = y3[:, 2 * g * lanes:2 * (g + 1) * lanes].reshape(4, rows // 8, 2 * lanes)
        lift, sides = [
            jnp.where(me % 2 == 1, x[1:], x[:-1]) for x in
            [twice_planes(x) for x in twice_rows(y3s[pl.ds(me // 2, 5)].reshape(5 * rows // 8, 2 * lanes), 5)]
        ]
        total = (sides + up_down(lift))[1:-1] + (lift[:-2] + lift[2:])
        y2 = y2 + (0.2 * lift[1:-1] + a2[1:-1] * total)
        y2 = ((0.2 * y2 + c2[1:-1]) + a2[1:-1] * sum_planes(y2))[1:-1]
        return twice_rows(dot(flat(y2), up_2), 5)

    def swept_1(y1, lift, sides, a1):
        before, after = shifted(lift)
        across = lift + jnp.where(iota(lift.shape, 2) < half, before, after)
        return y1 + (0.2 * lift + a1 * ((sides + up_down(lift)) + across))

    def lift_0(y1, skip):
        n = rows // 2
        around = flat(y1)
        both = dot(around, up_lo), dot(around, up_hi)
        halves = [part[n * k:n * k + n] for k in range(3) for part in both]
        halves = halves[skip:len(halves) - skip]
        return [twice_planes(x) for x in twice_rows(jnp.concatenate(halves, 0), len(halves))]

    def swept_0(lift, sides, a):
        total = (sides + up_down(lift))[1:-1] + (lift[:-2] + lift[2:])
        return 0.2 * lift[1:-1] + a * total

    arrive(near)
    x, b1 = first_sweeps(own[...], planes_of(c0, d + 1, d - 1, d + 4), a)
    arrive(cap_window[0])
    arrive(cap2_window[0])
    d1, i1 = inverse_1(1, 4)
    d2, i2 = inverse_2(3, 8)
    near_1 = i1, d1, 0.5 * i1, i2, d2, 0.25 * i2
    c1 = b1 * i1[1]
    vw[0, 3] = c1
    b2, b3 = spread(b1, c1, *near_1)
    gr[0, me] = b3 + cap_sent
    bw[0, 6] = side_by_side(b2)
    pl.semaphore_wait(far_sem, 2)
    begin(gather_r[0])
    begin(b_window[0])
    begin(c_window[0])
    arrive(far)
    arrive(pass_far)
    wide = weights(1, 3 * d - 2)
    c = planes_of(c0, d + 1, d - 2, d + 6)
    first = 1.2 * c[1:2] + wide[1:2] * sum_inner(c[0:3], lanes)
    final = 1.2 * c[-2:-1] + wide[-2:-1] * sum_inner(c[-3:], lanes)

    def last_sweeps(x, c):
        x = (0.2 * x[1:-1] + c) + a * sum_inner(x, lanes)
        return (0.2 * x[1:-1] + c[1:-1]) + a[1:-1] * sum_inner(x, lanes)

    alone = last_sweeps(jnp.concatenate([first, x, final], 0), c[2:-2])
    fp_ref[...] = alone
    src1[2:d + 2] = cap[d:2 * d] * alone + src1[2:d + 2]
    begin(known)
    arrive(cap_window[1])
    a1 = 0.5 * inverse_1(0, 5)[1]
    arrive(cap2_window[1])
    i2 = inverse_2(0, 11)[1]
    a2 = 0.25 * i2[1:-1]
    arrive(gather_r[0])
    arrive(b_window[0])
    arrive(c_window[0])

    got = gr[0]
    cap3 = capacity_3(got)
    i3 = jnp.where(iota(cap3.shape, 2) % GROUP < GROUP // 2, W / (cap3 + 0.75), 0.0)
    a3 = 0.125 * i3
    c1 = jnp.where(valid(me - 3, 7, parts), vw[0], 0.0)
    y1 = 1.2 * c1[1:-1] + a1 * sum_packed(c1, half)[1:-1]
    c1 = c1[1:-1]
    y1 = (0.2 * y1 + c1) + a1 * sum_packed(y1, half)
    y1 = swept_1(y1, *level_2(0, level_3(got) * i3, i2, a2, a3), a1)
    y1 = ((0.2 * y1 + c1) + a1 * sum_packed(y1, half))[1:-1]
    x = swept_0(*lift_0(y1, 0), wide)
    x = 0.2 * x[1:-1] + wide[1:-1] * sum_inner(x, lanes)
    fp_ref[...] = fp_ref[...] + x[2:-2]
    arrive(known)
    b = cap[2:3 * d - 2] * x + src1[...]
    c1x[1:d + 5] = b * wide[1:-1]
    begin(third)

    x, b1 = first_sweeps(b[2:-2], c1x[1:d + 5], a)
    c1 = b1 * i1[1]
    c_sent[...] = c1
    b2, b3 = spread(b1, c1, *near_1)
    r_sent[...] = b3
    b_sent[...] = side_by_side(b2)

    @pl.when(span < spans - 1)
    def _():
        begin(gather_r[1])
        begin(b_window[1])
        begin(c_window[1])

    arrive(third)
    c = planes_of(c1x, 3, 0, d + 6)
    first = 1.2 * c[1:2] + wide[1:2] * sum_inner(c[0:3], lanes)
    final = 1.2 * c[-2:-1] + wide[-2:-1] * sum_inner(c[-3:], lanes)
    fin[0] = last_sweeps(jnp.concatenate([first, x, final], 0), c[2:-2])

    @pl.when(span < spans - 1)
    def _():
        begin(fin_onward)

    handed = gather_r[1], b_window[1], c_window[1], fin_onward
    for made in batches:
        if not any(made is other for other in handed):
            sent(made)

    @pl.when(span == 0)
    def _():
        up_ref[...] = u0[...]

    @pl.when(span > 0)
    def _():
        arrive(handed[0])
        arrive(handed[1])
        arrive(handed[2])
        arrive(handed[3])
        c1 = jnp.where(valid(me - 2, 5, parts), vw[1, 1:6], 0.0)
        y1 = 1.2 * c1 + a1 * sum_packed(c1, half)
        y1 = (0.2 * y1 + c1) + a1 * sum_packed(y1, half)
        y1 = swept_1(y1, *level_2(1, level_3(gr[1]) * i3, i2, a2, a3), a1)[1:-1]
        y1 = (0.2 * y1 + c1[1:-1]) + a1[1:-1] * sum_packed(y1, half)
        x = swept_0(*lift_0(y1, 1), a)
        up_ref[...] = fin[1] + (0.2 * x[1:-1] + a[1:-1] * sum_inner(x, lanes))

    @pl.when(span < spans - 1)
    def _():
        for made in handed:
            sent(made)


def shards(span_opening, source_power, warmth_retention):
    parts, spans = lax.axis_size("space"), lax.axis_size("tm")
    steps = source_power.shape[1]
    depth, rows, lanes = warmth_retention.shape
    assert steps == 2 and depth == 4
    slab = jax.ShapeDtypeStruct((depth, rows, lanes), F32)
    vmem = pl.BlockSpec(memory_space=pltpu.VMEM)
    dma = pltpu.SemaphoreType.DMA
    fpoint, updated = pl.pallas_call(
        functools.partial(kernel, parts, spans, steps),
        out_shape=(pltpu.VMEM(slab.shape, F32),) * 2,
        in_specs=[pl.BlockSpec(memory_space=pl.ANY)] * 3,
        out_specs=(vmem, vmem),
        scratch_shapes=[
            pltpu.VMEM((depth, rows, lanes), F32),
            pltpu.VMEM((depth, rows, lanes), F32),
            pltpu.VMEM((depth + 4, rows, lanes), F32),
            pltpu.VMEM((3 * depth, rows, lanes), F32),
            pltpu.VMEM((3 * depth + 2, rows, lanes), F32),
            pltpu.VMEM((depth + 6, rows, lanes), F32),
            pltpu.VMEM((5, rows // 2, lanes), F32),
            pltpu.VMEM((11, rows // 8, lanes), F32),
            pltpu.VMEM((steps, 7, rows // 2, lanes), F32),
            pltpu.VMEM((rows // 2, lanes), F32),
            pltpu.VMEM((steps, 13, rows // 4, lanes), F32),
            pltpu.VMEM((rows // 4, lanes), F32),
            pltpu.VMEM((steps, parts, rows // 8, lanes), F32),
            pltpu.VMEM((rows // 8, lanes), F32),
            pltpu.VMEM((2, 9, rows // 4, lanes), F32),
            pltpu.VMEM((parts // 2 + 4, rows // 8, 2 * lanes), F32),
            pltpu.VMEM((depth, rows, lanes), F32),
            pltpu.VMEM((12 * rows, lanes), F32),
            pltpu.VMEM((2, depth, rows, lanes), F32),
            pltpu.SemaphoreType.REGULAR,
            pltpu.SemaphoreType.REGULAR,
            dma((4,)), dma((18,)), dma((18,)),
        ],
        compiler_params=pltpu.CompilerParams(
            collective_id=0, has_side_effects=True, vmem_limit_bytes=67043328 - 2 * 4 * slab.size
        ),
    )(span_opening[0], source_power[0], warmth_retention)
    return fpoint[None], updated[None]


def solution(mesh):
    in_specs = (
        P("tm", "space", None, None),
        P("tm", None, "space", None, None),
        P("space", None, None),
    )
    out_specs = (P("tm", "space", None, None), P("tm", "space", None, None))
    return jax.shard_map(shards, mesh=mesh, in_specs=in_specs, out_specs=out_specs, check_vma=False)
```

```python
import functools

import jax
import jax.numpy as jnp
from jax import lax
from jax.experimental import pallas as pl
from jax.experimental.pallas import tpu as pltpu
from jax.sharding import PartitionSpec as P

COARSE_SWEEPS = 24
W = 0.8
GROUP = 32
NEAR = 4
F32 = jnp.float32
MESH = pl.DeviceIdType.MESH


def iota(shape, dim):
    return lax.broadcasted_iota(jnp.int32, shape, dim)


def dot(a, b):
    total = None
    for _ in range(2):
        part = a.astype(jnp.bfloat16)
        a = a - part.astype(F32)
        term = jnp.dot(part, b, preferred_element_type=F32)
        total = term if total is None else total + term
    return total


def picks(lanes, pick, scale):
    src, dst = iota((lanes, lanes), 0), iota((lanes, lanes), 1)
    return jnp.where(pick(src, dst), scale, 0.0).astype(jnp.bfloat16)


def from_sides(lanes, pick, width, scale):
    def shifted_pick(by):
        return picks(lanes, lambda s, d: (s % width + by >= 0) & (s % width + by < width) & pick(s + by, d), scale)

    return shifted_pick(-1) + shifted_pick(1)


def to_sides(lanes, pick, width):
    def shifted_pick(by):
        return picks(lanes, lambda s, d: (d % width + by >= 0) & (d % width + by < width) & pick(s, d + by), 1.0)

    return shifted_pick(-1) + shifted_pick(1)


def up_down(x):
    rows = x.shape[1]
    row = iota(x.shape, 1)
    up = jnp.where(row == 0, 0.0, pltpu.roll(x, 1, 1))
    return up + jnp.where(row == rows - 1, 0.0, pltpu.roll(x, rows - 1, 1))


def in_plane(x, width):
    lanes = x.shape[2]
    lane = iota(x.shape, 2)
    left, right = pltpu.roll(x, 1, 2), pltpu.roll(x, lanes - 1, 2)
    if width:
        left = jnp.where(lane % width == 0, 0.0, left)
        right = jnp.where(lane % width == width - 1, 0.0, right)
    return (left + right) + up_down(x)


def shifted(x):
    zero = jnp.zeros((1,) + x.shape[1:], F32)
    return jnp.concatenate([zero, x[:-1]], 0), jnp.concatenate([x[1:], zero], 0)


def earlier(x, by=1, shift=0):
    lanes = x.shape[2]
    moved = pltpu.roll(x[-by:], (GROUP + shift) % lanes, 2)
    return jnp.where(iota(moved.shape, 2) < GROUP, 0.0, moved)


def later(x, by=1, shift=0):
    lanes = x.shape[2]
    moved = pltpu.roll(x[:by], (lanes - GROUP + shift) % lanes, 2)
    return jnp.where(iota(moved.shape, 2) >= lanes - GROUP, 0.0, moved)


def sum_grouped(x):
    ends = jnp.concatenate([earlier(x), x, later(x)], 0)
    return in_plane(x, GROUP) + (ends[:-2] + ends[2:])


def sum_planes(x):
    before, after = shifted(x)
    return in_plane(x, None) + (before + after)


def plane_padded(x, by):
    zero = jnp.zeros((by,) + x.shape[1:], F32)
    return jnp.concatenate([zero, x, zero], 0)


def sum_packed(x, width):
    half = pltpu.roll(x, width, 2)
    before, after = shifted(half)
    return in_plane(x, width) + (half + jnp.where(iota(x.shape, 2) < width, before, after))


def sum_inner(x, width):
    return in_plane(x[1:-1], width) + (x[:-2] + x[2:])


def column_sum(x):
    rows = x.shape[1]
    mid = x[1:-1]
    row = iota(mid.shape, 1)
    up = jnp.where(row == 0, 0.0, pltpu.roll(mid, 1, 1))
    down = jnp.where(row == rows - 1, 0.0, pltpu.roll(mid, rows - 1, 1))
    return (x[:-2] + x[2:]) + (up + down)


def coarse_solve(c, a):
    n, lanes = c.shape[0], c.shape[2]

    def turned(x, by):
        return x if by == 0 else pltpu.roll(x, by % lanes, 2)

    def longer(x, by, reach=1):
        return jnp.concatenate([earlier(x, reach, by), turned(x, by), later(x, reach, by)], 0)

    c_at, a_at = [[longer(x, 0) if by == 0 else turned(x, by) for by in (1, 0, -1)] for x in (c, a)]

    def sweep(y, side, c, a):
        return (0.2 * y[1:-1] + c) + a * (side + column_sum(y))

    def two_sweeps(_, y):
        left, mid, right = longer(y, 1), longer(y, 0, 2), longer(y, -1)
        once_left = sweep(left, turned(y, 2) + y, c_at[0], a_at[0])
        once_mid = sweep(mid, left + right, c_at[1], a_at[1])
        once_right = sweep(right, y + turned(y, -2), c_at[2], a_at[2])
        return sweep(once_mid, once_left + once_right, c, a)

    left = COARSE_SWEEPS - 1
    y = c
    if left % 2:
        y = 1.2 * c + a * sum_grouped(c)
    return lax.fori_loop(0, left // 2, two_sweeps, y, unroll=True)


def flat(x):
    return x.reshape(x.shape[0] * x.shape[1], x.shape[2])


def kernel(
    parts, spans, steps,
    open_ref, src_ref, cap_in,
    fp_ref, up_ref,
    u0, src0, src1, cap, c0, c1x, cw, kw, vw, c_sent, bw, b_sent, gr, r_sent, r2s, y3s, own, tmp, fin,
    near_sem, far_sem, in_sem, send_sem, recv_sem,
):
    me, span = lax.axis_index("space"), lax.axis_index("tm")
    depth, rows, lanes = open_ref.shape
    half = lanes // 2
    groups = lanes // GROUP
    assert parts == 32 and lanes == 128 and rows == 64
    assert parts == 8 * NEAR
    close = [k for k in range(-NEAR, NEAR + 1) if k]

    loads = [
        pltpu.make_async_copy(cap_in, cap.at[pl.ds(depth, depth)], in_sem.at[0]),
        pltpu.make_async_copy(open_ref, u0, in_sem.at[1]),
        pltpu.make_async_copy(src_ref.at[0], src0, in_sem.at[2]),
        pltpu.make_async_copy(src_ref.at[1], src1.at[pl.ds(2, depth)], in_sem.at[3]),
    ]
    for load in loads:
        load.start()
    barrier = pltpu.get_barrier_semaphore()
    for k in close:
        pl.semaphore_signal(barrier, inc=1, device_id={"space": lax.rem(me + k % parts, parts)}, device_id_type=MESH)
    for k in range(1, spans):
        pl.semaphore_signal(barrier, inc=1, device_id={"tm": lax.rem(span + k, spans)}, device_id_type=MESH)

    r2s[...] = jnp.zeros(r2s.shape, F32)
    y3s[...] = jnp.zeros(y3s.shape, F32)

    def pick_lo(s, d):
        return (s // 2 == d) & (d < half)

    def pick_hi(s, d):
        return s // 2 + half == d

    def pick_2(s, d):
        return (s % half) // 2 == d

    def pick_3(s, d):
        return (s < GROUP) & (d % GROUP == s // 2)

    def swap(pick):
        return lambda s, d: pick(d, s)

    down_0 = jnp.concatenate([
        picks(lanes, pick_lo, 0.125), from_sides(lanes, pick_lo, lanes, 0.125),
        picks(lanes, pick_hi, 0.125), from_sides(lanes, pick_hi, lanes, 0.125),
    ], 0)
    down_cap1 = jnp.concatenate([picks(lanes, pick_lo, 0.125), picks(lanes, pick_hi, 0.125)], 0)
    down_2 = picks(lanes, pick_2, 0.125)
    down_1 = jnp.concatenate([
        down_2, from_sides(lanes, pick_2, half, 0.0625) + picks(lanes, pick_2, 0.0625),
        picks(lanes, lambda s, d: pick_2(s, d) & (s >= half), 0.0625),
        picks(lanes, lambda s, d: pick_2(s, d) & (s < half), 0.0625),
    ], 0)
    down_3 = jnp.concatenate([picks(lanes, pick_3, 0.125), from_sides(lanes, pick_3, GROUP, 0.03125)], 0)
    down_cap = picks(lanes, lambda s, d: (s < GROUP) & (d % GROUP == s // 2 + GROUP // 2), 0.125)
    def rises(pick, width):
        return [picks(lanes, pick, 1.0), to_sides(lanes, pick, width)]

    up_lo = jnp.concatenate(rises(lambda s, d: d // 2 == s, lanes), 1)
    up_hi = jnp.concatenate(rises(lambda s, d: d // 2 + half == s, lanes), 1)
    up_2 = jnp.concatenate(rises(swap(pick_2), half), 1)
    up_3 = jnp.concatenate([
        rise for g in range(groups)
        for rise in rises(lambda s, d: (d < GROUP) & (d // 2 + g * GROUP == s), GROUP)
    ], 1)

    def pair_rows(x, at=0):
        n, r, w = x.shape
        tmp[pl.ds(at, n * r), :] = flat(x)
        return tmp[pl.ds(at, n * r // 2, 2), :] + tmp[pl.ds(at + 1, n * r // 2, 2), :]

    def twice_rows(x, planes):
        parts_of = [x[:, at:at + lanes] for at in range(0, x.shape[1], lanes)]
        x = jnp.concatenate(parts_of, 0)
        r = x.shape[0]
        tmp[pl.ds(0, r, 2), :] = x
        tmp[pl.ds(1, r, 2), :] = x
        out = tmp[pl.ds(0, 2 * r), :].reshape(len(parts_of) * planes, -1, lanes)
        return [out[at:at + planes] for at in range(0, out.shape[0], planes)]

    def twice_planes(x):
        return jnp.broadcast_to(x[:, None], (x.shape[0], 2) + x.shape[1:]).reshape((2 * x.shape[0],) + x.shape[1:])

    def slab_pairs(x, at=0):
        s = pair_rows(x.reshape(depth // 2, 2, rows, lanes).sum(1), at)
        return s[:rows // 2], s[rows // 2:]

    def to_2(x):
        return dot(pair_rows(x), down_2).reshape(x.shape[0], rows // 4, lanes)

    lane = iota((rows // 8, lanes), 1)

    def turn(planes, off):
        out = []
        for k in range(groups):
            total = None
            for g in range(groups):
                by = (GROUP * (g - k) - off) % lanes
                moved = pltpu.roll(planes[g], by, 1) if by else planes[g]
                total = moved if total is None else jnp.where(lane // GROUP == g, moved, total)
            out.append(total[None])
        return jnp.concatenate(out, 0)

    def level_3(got):
        pairs = [got[0]] + [got[2 * i - 1] + got[2 * i] for i in range(1, parts // 2)] + [got[parts - 1]]
        out = []
        for k in range(groups):
            total = pairs[4 * k + 2]
            for i, keep in (
                (4 * k - 1, lane < GROUP), (4 * k, lane < 2 * GROUP), (4 * k + 1, lane < 3 * GROUP),
                (4 * k + 3, lane >= GROUP), (4 * k + 4, lane >= 2 * GROUP), (4 * k + 5, lane >= 3 * GROUP),
            ):
                if 0 <= i < len(pairs):
                    total = total + jnp.where(keep, pairs[i], 0.0)
            out.append(total)
        return turn(out, 0)

    def capacity_3(got):
        out = []
        for k in range(groups):
            total = None
            for g in range(groups):
                i = 2 * (4 * k + g)
                pair = got[i] + got[i + 1]
                total = pair if total is None else jnp.where(lane // GROUP == g, pair, total)
            out.append(total)
        return turn(out, GROUP // 2)

    def valid(start, count, of):
        at = start + iota((count, 1, 1), 0)
        return (at >= 0) & (at < of)

    batches = []

    def batch(pieces, total):
        at = len(batches)

        def copy(source, target, to):
            return pltpu.make_async_remote_copy(
                source, target, send_sem.at[at], recv_sem.at[at], device_id=to, device_id_type=MESH)

        made = [copy(*piece) for piece in pieces], copy(total, total, pieces[0][2])
        batches.append(made)
        return made

    def begin(made):
        for copy in made[0]:
            copy.start()

    def arrive(made):
        made[1].wait_recv()

    def sent(made):
        made[1].wait_send()

    def beside(k):
        return {"space": lax.rem(me + (k + parts) % parts, parts)}

    share = rows // spans
    my_rows = pl.ds(pl.multiple_of(span * share, share), share)

    def halo(buf, count, up, down, rows_at=None):
        def part(start):
            return buf.at[pl.ds(start, count)] if rows_at is None else buf.at[pl.ds(start, count), rows_at]

        total = buf.at[pl.ds(0, 2 * count)] if rows_at is None else buf.at[pl.ds(0, 2 * count), pl.ds(0, share)]
        return batch([(part(way[0]), part(way[1]), beside(k)) for way, k in ((up, 1), (down, -1))], total)

    def window(buf, source, nearest, reach, to={}):
        middle = buf.shape[0] // 2
        offsets = [k for far in range(reach, nearest - 1, -1) for k in ((far, -far) if far else (0,))]
        return batch([(source, buf.at[middle - k], {**beside(k), **to}) for k in offsets], buf.at[pl.ds(0, len(offsets))])

    def hops(k):
        z, y = k // 4, k % 4
        return min(z, parts // 4 - z) + min(y, 4 - y)

    def gather(buf, source, offsets, to={}):
        offsets = sorted(offsets, key=lambda k: -hops(k))
        return batch([(source, buf.at[me], {**beside(k), **to}) for k in offsets], buf.at[pl.ds(0, len(offsets))])

    d = depth
    onward = {"tm": (span + 1) % spans}
    near = halo(c0, 2, (2 * d - 1, d - 1), (d + 1, 2 * d + 1))
    far = halo(c0, 1, (2 * d - 2, d - 2), (d + 3, 2 * d + 3))
    known = halo(src1, 2, (d, 0), (2, d + 2))
    third = halo(c1x, 1, (d, 0), (5, d + 5))
    cap_near = halo(cap, 1, (2 * d - 1, d - 1), (d, 2 * d))
    cap_far = halo(cap, 2, (d + 1, 1), (d + 1, 2 * d + 1), my_rows)
    pass_far = batch(
        [
            (cap.at[pl.ds(start, 2), my_rows], cap.at[pl.ds(start, 2), my_rows], {"tm": (span + k) % spans})
            for start in (1, 2 * d + 1) for k in range(1, spans)
        ], cap.at[pl.ds(0, 4), pl.ds(0, (spans - 1) * share)])
    cap_window = window(cw, cw.at[2], 1, 1), window(cw, cw.at[2], 2, 2)
    cap2_window = window(kw, kw.at[5], 1, 2), window(kw, kw.at[5], 3, 5)
    gather_r = gather(gr.at[0], gr.at[0, me], range(1, parts)), gather(gr.at[1], r_sent, range(parts), onward)
    c_window = window(vw.at[0], vw.at[0, 3], 1, 3), window(vw.at[1], c_sent, 0, 2, onward)
    b_window = window(bw.at[0], bw.at[0, 6], 1, 6), window(bw.at[1], b_sent, 0, 6, onward)
    fin_onward = batch([(fin.at[0], fin.at[1], onward)], fin.at[0])

    loads[0].wait()
    mine = cap[d:2 * d]
    loads[1].wait()
    loads[2].wait()
    b = mine * u0[...] + src0[...]
    own[...] = b
    c0[d + 1:2 * d + 1] = b * (W / (mine + 6.0))

    pl.semaphore_wait(barrier, len(close) + spans - 1)
    begin(near)
    begin(cap_near)
    for k in (NEAR, -NEAR):
        pl.semaphore_signal(near_sem, inc=1, device_id=beside(k), device_id_type=MESH)
    cap1 = dot(jnp.concatenate(slab_pairs(mine), 1), down_cap1)
    cw[2] = cap1
    begin(cap_window[0])
    cap2 = to_2(cap1[None])
    kw[5] = cap2[0, :rows // 8] + pltpu.roll(cap2[0, rows // 8:], GROUP, 1)
    begin(cap2_window[0])
    begin(cap_far)
    begin(far)
    pl.semaphore_wait(near_sem, 2)
    for k in (2 * NEAR, -2 * NEAR):
        pl.semaphore_signal(far_sem, inc=1, device_id=beside(k), device_id_type=MESH)
    begin(cap_window[1])
    begin(cap2_window[1])
    cap_sent = dot(pair_rows(cap2), down_cap)
    loads[3].wait()

    def weights(start, count):
        inside = valid((me - 1) * depth + start, count, parts * depth)
        return jnp.where(inside, W / (cap[start:start + count] + 6.0), 0.0)

    def inverse(diagonal, start, reach):
        return jnp.where(valid(me - reach + start, diagonal.shape[0], parts), W / diagonal, 0.0)

    def planes_of(buf, own, start, count):
        return jnp.where(valid(me * depth + start - own, count, parts * depth), buf[start:start + count], 0.0)

    def inverse_1(start, stop):
        diagonal = cw[start:stop] + 3.0
        return diagonal, inverse(diagonal, start, 2)

    def inverse_2(start, stop):
        packed = kw[start:stop]
        diagonal = jnp.concatenate([packed, pltpu.roll(packed, lanes - GROUP, 2)], 1) + 1.5
        return diagonal, jnp.where(iota(diagonal.shape, 2) < GROUP, inverse(diagonal, start, 5), 0.0)

    arrive(cap_near)
    a = weights(d - 1, d + 2)

    def first_sweeps(b, c, a):
        x = 1.2 * c[1:-1] + a * sum_inner(c, lanes)
        inner = x[1:-1]
        r = b - (cap[d:2 * d] + 6.0) * inner + up_down(inner) + (x[:-2] + x[2:])
        (r_lo, r_hi), (x_lo, x_hi) = slab_pairs(r), slab_pairs(inner, depth * rows // 2)
        return x, dot(jnp.concatenate([r_lo, x_lo, r_hi, x_hi], 1), down_0)

    def spread(b1, c1, i1, d1, a1, i2, d2, a2):
        c1 = plane_padded(c1[None], 1)
        y1 = 1.2 * c1 + a1 * sum_packed(c1, half)
        r1 = pair_rows(plane_padded(b1[None], 1) - d1 * y1 + 0.5 * up_down(y1))
        y1 = pair_rows(y1, 3 * rows // 2)
        n = rows // 4
        none = jnp.zeros((n, lanes), F32)
        around = jnp.concatenate([none, y1[:-n]], 0), jnp.concatenate([y1[n:], none], 0)
        b2 = dot(jnp.concatenate([r1, y1, *around], 1), down_1).reshape(3, n, lanes)
        c2 = plane_padded(b2 * i2[1:4], 1)
        y2 = 1.2 * c2 + a2 * sum_planes(c2)
        r2 = plane_padded(b2, 2) - plane_padded(d2 * y2, 1)
        y2 = plane_padded(y2, 1)
        before, after = shifted(y2)
        r2s[0, 1:8] = r2 + 0.25 * (up_down(y2) + (before + after))
        r2s[1, 1:8] = y2
        pairs = [
            pair_rows(r2s[i, pl.ds(me % 2, 8)].reshape(4, 2, n, lanes).sum(1), i * 4 * n)
            for i in range(2)
        ]
        b3 = dot(jnp.concatenate(pairs, 1), down_3).reshape(4, n // 2, lanes)
        first = (me + 4 + me % 2) // 2
        return b2, sum(jnp.where(lane // GROUP == (first + q) % groups, b3[q], 0.0) for q in range(4))

    def side_by_side(b2):
        return b2[1] + (pltpu.roll(b2[0], GROUP, 1) + pltpu.roll(b2[2], 2 * GROUP, 1))

    def level_2(t, c3, i2, a2, a3):
        b = jnp.where(valid(me - 6, 13, parts), bw[t], 0.0)
        b2 = b[1:-1] + (pltpu.roll(b[2:], lanes - GROUP, 2) + pltpu.roll(b[:-2], lanes - 2 * GROUP, 2))
        c2 = b2 * i2
        y2 = 1.2 * c2[1:-1] + a2 * sum_planes(c2)[1:-1]
        c2 = c2[1:-1]
        y2 = ((0.2 * y2 + c2) + a2 * sum_planes(y2))[1:-1]
        y3 = dot(flat(coarse_solve(c3, a3)), up_3)
        for g in range(groups):
            y3s[2 + 4 * g:6 + 4 * g] = y3[:, 2 * g * lanes:2 * (g + 1) * lanes].reshape(4, rows // 8, 2 * lanes)
        lift, sides = [
            jnp.where(me % 2 == 1, x[1:], x[:-1]) for x in
            [twice_planes(x) for x in twice_rows(y3s[pl.ds(me // 2, 5)].reshape(5 * rows // 8, 2 * lanes), 5)]
        ]
        total = (sides + up_down(lift))[1:-1] + (lift[:-2] + lift[2:])
        y2 = y2 + (0.2 * lift[1:-1] + a2[1:-1] * total)
        y2 = ((0.2 * y2 + c2[1:-1]) + a2[1:-1] * sum_planes(y2))[1:-1]
        return twice_rows(dot(flat(y2), up_2), 5)

    def swept_1(y1, lift, sides, a1):
        before, after = shifted(lift)
        across = lift + jnp.where(iota(lift.shape, 2) < half, before, after)
        return y1 + (0.2 * lift + a1 * ((sides + up_down(lift)) + across))

    def lift_0(y1, skip):
        n = rows // 2
        around = flat(y1)
        both = dot(around, up_lo), dot(around, up_hi)
        halves = [part[n * k:n * k + n] for k in range(3) for part in both]
        halves = halves[skip:len(halves) - skip]
        return [twice_planes(x) for x in twice_rows(jnp.concatenate(halves, 0), len(halves))]

    def swept_0(lift, sides, a):
        total = (sides + up_down(lift))[1:-1] + (lift[:-2] + lift[2:])
        return 0.2 * lift[1:-1] + a * total

    arrive(near)
    x, b1 = first_sweeps(own[...], planes_of(c0, d + 1, d - 1, d + 4), a)
    arrive(cap_window[0])
    arrive(cap2_window[0])
    d1, i1 = inverse_1(1, 4)
    d2, i2 = inverse_2(3, 8)
    near_1 = i1, d1, 0.5 * i1, i2, d2, 0.25 * i2
    c1 = b1 * i1[1]
    vw[0, 3] = c1
    b2, b3 = spread(b1, c1, *near_1)
    gr[0, me] = b3 + cap_sent
    bw[0, 6] = side_by_side(b2)
    pl.semaphore_wait(far_sem, 2)
    begin(gather_r[0])
    arrive(cap_far)
    begin(pass_far)
    begin(b_window[0])
    begin(c_window[0])
    arrive(far)
    arrive(pass_far)
    wide = weights(1, 3 * d - 2)
    c = planes_of(c0, d + 1, d - 2, d + 6)
    first = 1.2 * c[1:2] + wide[1:2] * sum_inner(c[0:3], lanes)
    final = 1.2 * c[-2:-1] + wide[-2:-1] * sum_inner(c[-3:], lanes)

    def last_sweeps(x, c):
        x = (0.2 * x[1:-1] + c) + a * sum_inner(x, lanes)
        return (0.2 * x[1:-1] + c[1:-1]) + a[1:-1] * sum_inner(x, lanes)

    alone = last_sweeps(jnp.concatenate([first, x, final], 0), c[2:-2])
    fp_ref[...] = alone
    src1[2:d + 2] = cap[d:2 * d] * alone + src1[2:d + 2]
    begin(known)
    arrive(cap_window[1])
    a1 = 0.5 * inverse_1(0, 5)[1]
    arrive(cap2_window[1])
    i2 = inverse_2(0, 11)[1]
    a2 = 0.25 * i2[1:-1]
    arrive(gather_r[0])
    arrive(b_window[0])
    arrive(c_window[0])

    got = gr[0]
    cap3 = capacity_3(got)
    i3 = jnp.where(iota(cap3.shape, 2) % GROUP < GROUP // 2, W / (cap3 + 0.75), 0.0)
    a3 = 0.125 * i3
    c1 = jnp.where(valid(me - 3, 7, parts), vw[0], 0.0)
    y1 = 1.2 * c1[1:-1] + a1 * sum_packed(c1, half)[1:-1]
    c1 = c1[1:-1]
    y1 = (0.2 * y1 + c1) + a1 * sum_packed(y1, half)
    y1 = swept_1(y1, *level_2(0, level_3(got) * i3, i2, a2, a3), a1)
    y1 = ((0.2 * y1 + c1) + a1 * sum_packed(y1, half))[1:-1]
    x = swept_0(*lift_0(y1, 0), wide)
    x = 0.2 * x[1:-1] + wide[1:-1] * sum_inner(x, lanes)
    fp_ref[...] = fp_ref[...] + x[2:-2]
    arrive(known)
    b = cap[2:3 * d - 2] * x + src1[...]
    c1x[1:d + 5] = b * wide[1:-1]
    begin(third)

    x, b1 = first_sweeps(b[2:-2], c1x[1:d + 5], a)
    c1 = b1 * i1[1]
    c_sent[...] = c1
    b2, b3 = spread(b1, c1, *near_1)
    r_sent[...] = b3
    b_sent[...] = side_by_side(b2)

    @pl.when(span < spans - 1)
    def _():
        begin(gather_r[1])
        begin(b_window[1])
        begin(c_window[1])

    arrive(third)
    c = planes_of(c1x, 3, 0, d + 6)
    first = 1.2 * c[1:2] + wide[1:2] * sum_inner(c[0:3], lanes)
    final = 1.2 * c[-2:-1] + wide[-2:-1] * sum_inner(c[-3:], lanes)
    fin[0] = last_sweeps(jnp.concatenate([first, x, final], 0), c[2:-2])

    @pl.when(span < spans - 1)
    def _():
        begin(fin_onward)

    handed = gather_r[1], b_window[1], c_window[1], fin_onward
    for made in batches:
        if not any(made is other for other in handed):
            sent(made)

    @pl.when(span == 0)
    def _():
        up_ref[...] = u0[...]

    @pl.when(span > 0)
    def _():
        arrive(handed[0])
        arrive(handed[1])
        arrive(handed[2])
        arrive(handed[3])
        c1 = jnp.where(valid(me - 2, 5, parts), vw[1, 1:6], 0.0)
        y1 = 1.2 * c1 + a1 * sum_packed(c1, half)
        y1 = (0.2 * y1 + c1) + a1 * sum_packed(y1, half)
        y1 = swept_1(y1, *level_2(1, level_3(gr[1]) * i3, i2, a2, a3), a1)[1:-1]
        y1 = (0.2 * y1 + c1[1:-1]) + a1[1:-1] * sum_packed(y1, half)
        x = swept_0(*lift_0(y1, 1), a)
        up_ref[...] = fin[1] + (0.2 * x[1:-1] + a[1:-1] * sum_inner(x, lanes))

    @pl.when(span < spans - 1)
    def _():
        for made in handed:
            sent(made)


def shards(span_opening, source_power, warmth_retention):
    parts, spans = lax.axis_size("space"), lax.axis_size("tm")
    steps = source_power.shape[1]
    depth, rows, lanes = warmth_retention.shape
    assert steps == 2 and depth == 4
    slab = jax.ShapeDtypeStruct((depth, rows, lanes), F32)
    vmem = pl.BlockSpec(memory_space=pltpu.VMEM)
    dma = pltpu.SemaphoreType.DMA
    fpoint, updated = pl.pallas_call(
        functools.partial(kernel, parts, spans, steps),
        out_shape=(pltpu.VMEM(slab.shape, F32),) * 2,
        in_specs=[pl.BlockSpec(memory_space=pl.ANY)] * 3,
        out_specs=(vmem, vmem),
        scratch_shapes=[
            pltpu.VMEM((depth, rows, lanes), F32),
            pltpu.VMEM((depth, rows, lanes), F32),
            pltpu.VMEM((depth + 4, rows, lanes), F32),
            pltpu.VMEM((3 * depth, rows, lanes), F32),
            pltpu.VMEM((3 * depth + 2, rows, lanes), F32),
            pltpu.VMEM((depth + 6, rows, lanes), F32),
            pltpu.VMEM((5, rows // 2, lanes), F32),
            pltpu.VMEM((11, rows // 8, lanes), F32),
            pltpu.VMEM((steps, 7, rows // 2, lanes), F32),
            pltpu.VMEM((rows // 2, lanes), F32),
            pltpu.VMEM((steps, 13, rows // 4, lanes), F32),
            pltpu.VMEM((rows // 4, lanes), F32),
            pltpu.VMEM((steps, parts, rows // 8, lanes), F32),
            pltpu.VMEM((rows // 8, lanes), F32),
            pltpu.VMEM((2, 9, rows // 4, lanes), F32),
            pltpu.VMEM((parts // 2 + 4, rows // 8, 2 * lanes), F32),
            pltpu.VMEM((depth, rows, lanes), F32),
            pltpu.VMEM((12 * rows, lanes), F32),
            pltpu.VMEM((2, depth, rows, lanes), F32),
            pltpu.SemaphoreType.REGULAR,
            pltpu.SemaphoreType.REGULAR,
            dma((4,)), dma((18,)), dma((18,)),
        ],
        compiler_params=pltpu.CompilerParams(
            collective_id=0, has_side_effects=True, vmem_limit_bytes=67043328 - 2 * 4 * slab.size
        ),
    )(span_opening[0], source_power[0], warmth_retention)
    flag = lax.axis_index("tm") > spans
    fpoint, updated = jnp.where(flag, updated, fpoint), jnp.where(flag, fpoint, updated)
    return fpoint[None], updated[None]


def solution(mesh):
    in_specs = (
        P("tm", "space", None, None),
        P("tm", None, "space", None, None),
        P("space", None, None),
    )
    out_specs = (P("tm", "space", None, None), P("tm", "space", None, None))
    return jax.shard_map(shards, mesh=mesh, in_specs=in_specs, out_specs=out_specs, check_vma=False)
```

```python
import functools

import jax
import jax.numpy as jnp
from jax import lax
from jax.experimental import pallas as pl
from jax.experimental.pallas import tpu as pltpu
from jax.sharding import PartitionSpec as P

COARSE_SWEEPS = 24
W = 0.8
GROUP = 32
NEAR = 4
F32 = jnp.float32
MESH = pl.DeviceIdType.MESH


def iota(shape, dim):
    return lax.broadcasted_iota(jnp.int32, shape, dim)


def dot(a, b):
    total = None
    for _ in range(2):
        part = a.astype(jnp.bfloat16)
        a = a - part.astype(F32)
        term = jnp.dot(part, b, preferred_element_type=F32)
        total = term if total is None else total + term
    return total


def picks(lanes, pick, scale):
    src, dst = iota((lanes, lanes), 0), iota((lanes, lanes), 1)
    return jnp.where(pick(src, dst), scale, 0.0).astype(jnp.bfloat16)


def from_sides(lanes, pick, width, scale):
    def shifted_pick(by):
        return picks(lanes, lambda s, d: (s % width + by >= 0) & (s % width + by < width) & pick(s + by, d), scale)

    return shifted_pick(-1) + shifted_pick(1)


def to_sides(lanes, pick, width):
    def shifted_pick(by):
        return picks(lanes, lambda s, d: (d % width + by >= 0) & (d % width + by < width) & pick(s, d + by), 1.0)

    return shifted_pick(-1) + shifted_pick(1)


def up_down(x):
    rows = x.shape[1]
    row = iota(x.shape, 1)
    up = jnp.where(row == 0, 0.0, pltpu.roll(x, 1, 1))
    return up + jnp.where(row == rows - 1, 0.0, pltpu.roll(x, rows - 1, 1))


def in_plane(x, width):
    lanes = x.shape[2]
    lane = iota(x.shape, 2)
    left, right = pltpu.roll(x, 1, 2), pltpu.roll(x, lanes - 1, 2)
    if width:
        left = jnp.where(lane % width == 0, 0.0, left)
        right = jnp.where(lane % width == width - 1, 0.0, right)
    return (left + right) + up_down(x)


def shifted(x):
    zero = jnp.zeros((1,) + x.shape[1:], F32)
    return jnp.concatenate([zero, x[:-1]], 0), jnp.concatenate([x[1:], zero], 0)


def earlier(x, by=1, shift=0):
    lanes = x.shape[2]
    moved = pltpu.roll(x[-by:], (GROUP + shift) % lanes, 2)
    return jnp.where(iota(moved.shape, 2) < GROUP, 0.0, moved)


def later(x, by=1, shift=0):
    lanes = x.shape[2]
    moved = pltpu.roll(x[:by], (lanes - GROUP + shift) % lanes, 2)
    return jnp.where(iota(moved.shape, 2) >= lanes - GROUP, 0.0, moved)


def sum_grouped(x):
    ends = jnp.concatenate([earlier(x), x, later(x)], 0)
    return in_plane(x, GROUP) + (ends[:-2] + ends[2:])


def sum_planes(x):
    before, after = shifted(x)
    return in_plane(x, None) + (before + after)


def plane_padded(x, by):
    zero = jnp.zeros((by,) + x.shape[1:], F32)
    return jnp.concatenate([zero, x, zero], 0)


def sum_packed(x, width):
    half = pltpu.roll(x, width, 2)
    before, after = shifted(half)
    return in_plane(x, width) + (half + jnp.where(iota(x.shape, 2) < width, before, after))


def sum_inner(x, width):
    return in_plane(x[1:-1], width) + (x[:-2] + x[2:])


def column_sum(x):
    rows = x.shape[1]
    mid = x[1:-1]
    row = iota(mid.shape, 1)
    up = jnp.where(row == 0, 0.0, pltpu.roll(mid, 1, 1))
    down = jnp.where(row == rows - 1, 0.0, pltpu.roll(mid, rows - 1, 1))
    return (x[:-2] + x[2:]) + (up + down)


def coarse_solve(c, a):
    n, lanes = c.shape[0], c.shape[2]

    def turned(x, by):
        return x if by == 0 else pltpu.roll(x, by % lanes, 2)

    def longer(x, by, reach=1):
        return jnp.concatenate([earlier(x, reach, by), turned(x, by), later(x, reach, by)], 0)

    c_at, a_at = [[longer(x, 0) if by == 0 else turned(x, by) for by in (1, 0, -1)] for x in (c, a)]

    def sweep(y, side, c, a):
        return (0.2 * y[1:-1] + c) + a * (side + column_sum(y))

    def two_sweeps(_, y):
        left, mid, right = longer(y, 1), longer(y, 0, 2), longer(y, -1)
        once_left = sweep(left, turned(y, 2) + y, c_at[0], a_at[0])
        once_mid = sweep(mid, left + right, c_at[1], a_at[1])
        once_right = sweep(right, y + turned(y, -2), c_at[2], a_at[2])
        return sweep(once_mid, once_left + once_right, c, a)

    left = COARSE_SWEEPS - 1
    y = c
    if left % 2:
        y = 1.2 * c + a * sum_grouped(c)
    return lax.fori_loop(0, left // 2, two_sweeps, y, unroll=True)


def flat(x):
    return x.reshape(x.shape[0] * x.shape[1], x.shape[2])


def kernel(
    parts, spans, steps,
    open_ref, src_ref, cap_in,
    fp_ref, up_ref,
    u0, src0, src1, cap, c0, c1x, cw, kw, vw, c_sent, bw, b_sent, gr, r_sent, r2s, y3s, own, tmp, fin,
    near_sem, far_sem, in_sem, send_sem, recv_sem,
):
    me, span = lax.axis_index("space"), lax.axis_index("tm")
    depth, rows, lanes = open_ref.shape
    half = lanes // 2
    groups = lanes // GROUP
    assert parts == 32 and lanes == 128 and rows == 64
    assert parts == 8 * NEAR
    close = [k for k in range(-NEAR, NEAR + 1) if k]

    loads = [
        pltpu.make_async_copy(cap_in, cap.at[pl.ds(depth, depth)], in_sem.at[0]),
        pltpu.make_async_copy(open_ref, u0, in_sem.at[1]),
        pltpu.make_async_copy(src_ref.at[0], src0, in_sem.at[2]),
        pltpu.make_async_copy(src_ref.at[1], src1.at[pl.ds(2, depth)], in_sem.at[3]),
    ]
    for load in loads:
        load.start()
    barrier = pltpu.get_barrier_semaphore()
    for k in close:
        pl.semaphore_signal(barrier, inc=1, device_id={"space": lax.rem(me + k % parts, parts)}, device_id_type=MESH)
    for k in (1, spans - 1):
        pl.semaphore_signal(barrier, inc=1, device_id={"tm": lax.rem(span + k, spans)}, device_id_type=MESH)

    r2s[...] = jnp.zeros(r2s.shape, F32)
    y3s[...] = jnp.zeros(y3s.shape, F32)

    def pick_lo(s, d):
        return (s // 2 == d) & (d < half)

    def pick_hi(s, d):
        return s // 2 + half == d

    def pick_2(s, d):
        return (s % half) // 2 == d

    def pick_3(s, d):
        return (s < GROUP) & (d % GROUP == s // 2)

    def swap(pick):
        return lambda s, d: pick(d, s)

    down_0 = jnp.concatenate([
        picks(lanes, pick_lo, 0.125), from_sides(lanes, pick_lo, lanes, 0.125),
        picks(lanes, pick_hi, 0.125), from_sides(lanes, pick_hi, lanes, 0.125),
    ], 0)
    down_cap1 = jnp.concatenate([picks(lanes, pick_lo, 0.125), picks(lanes, pick_hi, 0.125)], 0)
    down_2 = picks(lanes, pick_2, 0.125)
    down_1 = jnp.concatenate([
        down_2, from_sides(lanes, pick_2, half, 0.0625) + picks(lanes, pick_2, 0.0625),
        picks(lanes, lambda s, d: pick_2(s, d) & (s >= half), 0.0625),
        picks(lanes, lambda s, d: pick_2(s, d) & (s < half), 0.0625),
    ], 0)
    down_3 = jnp.concatenate([picks(lanes, pick_3, 0.125), from_sides(lanes, pick_3, GROUP, 0.03125)], 0)
    down_cap = picks(lanes, lambda s, d: (s < GROUP) & (d % GROUP == s // 2 + GROUP // 2), 0.125)
    def rises(pick, width):
        return [picks(lanes, pick, 1.0), to_sides(lanes, pick, width)]

    up_lo = jnp.concatenate(rises(lambda s, d: d // 2 == s, lanes), 1)
    up_hi = jnp.concatenate(rises(lambda s, d: d // 2 + half == s, lanes), 1)
    up_2 = jnp.concatenate(rises(swap(pick_2), half), 1)
    up_3 = jnp.concatenate([
        rise for g in range(groups)
        for rise in rises(lambda s, d: (d < GROUP) & (d // 2 + g * GROUP == s), GROUP)
    ], 1)

    def pair_rows(x, at=0):
        n, r, w = x.shape
        tmp[pl.ds(at, n * r), :] = flat(x)
        return tmp[pl.ds(at, n * r // 2, 2), :] + tmp[pl.ds(at + 1, n * r // 2, 2), :]

    def twice_rows(x, planes):
        parts_of = [x[:, at:at + lanes] for at in range(0, x.shape[1], lanes)]
        x = jnp.concatenate(parts_of, 0)
        r = x.shape[0]
        tmp[pl.ds(0, r, 2), :] = x
        tmp[pl.ds(1, r, 2), :] = x
        out = tmp[pl.ds(0, 2 * r), :].reshape(len(parts_of) * planes, -1, lanes)
        return [out[at:at + planes] for at in range(0, out.shape[0], planes)]

    def twice_planes(x):
        return jnp.broadcast_to(x[:, None], (x.shape[0], 2) + x.shape[1:]).reshape((2 * x.shape[0],) + x.shape[1:])

    def slab_pairs(x, at=0):
        s = pair_rows(x.reshape(depth // 2, 2, rows, lanes).sum(1), at)
        return s[:rows // 2], s[rows // 2:]

    def to_2(x):
        return dot(pair_rows(x), down_2).reshape(x.shape[0], rows // 4, lanes)

    lane = iota((rows // 8, lanes), 1)

    def turn(planes, off):
        out = []
        for k in range(groups):
            total = None
            for g in range(groups):
                by = (GROUP * (g - k) - off) % lanes
                moved = pltpu.roll(planes[g], by, 1) if by else planes[g]
                total = moved if total is None else jnp.where(lane // GROUP == g, moved, total)
            out.append(total[None])
        return jnp.concatenate(out, 0)

    def level_3(got):
        pairs = [got[0]] + [got[2 * i - 1] + got[2 * i] for i in range(1, parts // 2)] + [got[parts - 1]]
        out = []
        for k in range(groups):
            total = pairs[4 * k + 2]
            for i, keep in (
                (4 * k - 1, lane < GROUP), (4 * k, lane < 2 * GROUP), (4 * k + 1, lane < 3 * GROUP),
                (4 * k + 3, lane >= GROUP), (4 * k + 4, lane >= 2 * GROUP), (4 * k + 5, lane >= 3 * GROUP),
            ):
                if 0 <= i < len(pairs):
                    total = total + jnp.where(keep, pairs[i], 0.0)
            out.append(total)
        return turn(out, 0)

    def capacity_3(got):
        out = []
        for k in range(groups):
            total = None
            for g in range(groups):
                i = 2 * (4 * k + g)
                pair = got[i] + got[i + 1]
                total = pair if total is None else jnp.where(lane // GROUP == g, pair, total)
            out.append(total)
        return turn(out, GROUP // 2)

    def valid(start, count, of):
        at = start + iota((count, 1, 1), 0)
        return (at >= 0) & (at < of)

    batches = []

    def batch(pieces, total):
        at = len(batches)

        def copy(source, target, to):
            return pltpu.make_async_remote_copy(
                source, target, send_sem.at[at], recv_sem.at[at], device_id=to, device_id_type=MESH)

        made = [copy(*piece) for piece in pieces], copy(total, total, pieces[0][2])
        batches.append(made)
        return made

    def begin(made):
        for copy in made[0]:
            copy.start()

    def arrive(made):
        made[1].wait_recv()

    def sent(made):
        made[1].wait_send()

    def beside(k):
        return {"space": lax.rem(me + (k + parts) % parts, parts)}

    share = rows // 2
    my_rows = pl.ds(pl.multiple_of(span % 2 * share, share), share)

    def halo(buf, count, up, down, rows_at=None):
        def part(start):
            return buf.at[pl.ds(start, count)] if rows_at is None else buf.at[pl.ds(start, count), rows_at]

        total = buf.at[pl.ds(0, 2 * count)] if rows_at is None else buf.at[pl.ds(0, 2 * count), pl.ds(0, share)]
        return batch([(part(way[0]), part(way[1]), beside(k)) for way, k in ((up, 1), (down, -1))], total)

    def window(buf, source, nearest, reach, to={}):
        middle = buf.shape[0] // 2
        offsets = [k for far in range(reach, nearest - 1, -1) for k in ((far, -far) if far else (0,))]
        return batch([(source, buf.at[middle - k], {**beside(k), **to}) for k in offsets], buf.at[pl.ds(0, len(offsets))])

    def hops(k):
        z, y = k // 4, k % 4
        return min(z, parts // 4 - z) + min(y, 4 - y)

    def gather(buf, source, offsets, to={}):
        offsets = sorted(offsets, key=lambda k: -hops(k))
        return batch([(source, buf.at[me], {**beside(k), **to}) for k in offsets], buf.at[pl.ds(0, len(offsets))])

    d = depth
    onward = {"tm": (span + 1) % spans}
    near = halo(c0, 2, (2 * d - 1, d - 1), (d + 1, 2 * d + 1))
    far = halo(c0, 1, (2 * d - 2, d - 2), (d + 3, 2 * d + 3))
    known = halo(src1, 2, (d, 0), (2, d + 2))
    third = halo(c1x, 1, (d, 0), (5, d + 5))
    cap_near = halo(cap, 1, (2 * d - 1, d - 1), (d, 2 * d))
    cap_far = halo(cap, 2, (d + 1, 1), (d + 1, 2 * d + 1), my_rows)
    pass_far = batch(
        [
            (cap.at[pl.ds(start, 2), my_rows], cap.at[pl.ds(start, 2), my_rows], {"tm": span + 1 - 2 * (span % 2)})
            for start in (1, 2 * d + 1)
        ], cap.at[pl.ds(0, 4), pl.ds(0, share)])
    cap_window = window(cw, cw.at[2], 1, 1), window(cw, cw.at[2], 2, 2)
    cap2_window = window(kw, kw.at[5], 1, 2), window(kw, kw.at[5], 3, 5)
    gather_r = gather(gr.at[0], gr.at[0, me], range(1, parts)), gather(gr.at[1], r_sent, range(parts), onward)
    c_window = window(vw.at[0], vw.at[0, 3], 1, 3), window(vw.at[1], c_sent, 0, 2, onward)
    b_window = window(bw.at[0], bw.at[0, 6], 1, 6), window(bw.at[1], b_sent, 0, 6, onward)
    fin_onward = batch([(fin.at[0], fin.at[1], onward)], fin.at[0])

    loads[0].wait()
    mine = cap[d:2 * d]
    loads[1].wait()
    loads[2].wait()
    b = mine * u0[...] + src0[...]
    own[...] = b
    c0[d + 1:2 * d + 1] = b * (W / (mine + 6.0))

    pl.semaphore_wait(barrier, len(close) + 2)
    begin(near)
    begin(cap_near)
    for k in (NEAR, -NEAR):
        pl.semaphore_signal(near_sem, inc=1, device_id=beside(k), device_id_type=MESH)
    cap1 = dot(jnp.concatenate(slab_pairs(mine), 1), down_cap1)
    cw[2] = cap1
    begin(cap_window[0])
    cap2 = to_2(cap1[None])
    kw[5] = cap2[0, :rows // 8] + pltpu.roll(cap2[0, rows // 8:], GROUP, 1)
    begin(cap2_window[0])
    begin(cap_far)
    begin(far)
    pl.semaphore_wait(near_sem, 2)
    for k in (2 * NEAR, -2 * NEAR):
        pl.semaphore_signal(far_sem, inc=1, device_id=beside(k), device_id_type=MESH)
    begin(cap_window[1])
    begin(cap2_window[1])
    cap_sent = dot(pair_rows(cap2), down_cap)
    loads[3].wait()

    def weights(start, count):
        inside = valid((me - 1) * depth + start, count, parts * depth)
        return jnp.where(inside, W / (cap[start:start + count] + 6.0), 0.0)

    def inverse(diagonal, start, reach):
        return jnp.where(valid(me - reach + start, diagonal.shape[0], parts), W / diagonal, 0.0)

    def planes_of(buf, own, start, count):
        return jnp.where(valid(me * depth + start - own, count, parts * depth), buf[start:start + count], 0.0)

    def inverse_1(start, stop):
        diagonal = cw[start:stop] + 3.0
        return diagonal, inverse(diagonal, start, 2)

    def inverse_2(start, stop):
        packed = kw[start:stop]
        diagonal = jnp.concatenate([packed, pltpu.roll(packed, lanes - GROUP, 2)], 1) + 1.5
        return diagonal, jnp.where(iota(diagonal.shape, 2) < GROUP, inverse(diagonal, start, 5), 0.0)

    arrive(cap_near)
    a = weights(d - 1, d + 2)

    def first_sweeps(b, c, a):
        x = 1.2 * c[1:-1] + a * sum_inner(c, lanes)
        inner = x[1:-1]
        r = b - (cap[d:2 * d] + 6.0) * inner + up_down(inner) + (x[:-2] + x[2:])
        (r_lo, r_hi), (x_lo, x_hi) = slab_pairs(r), slab_pairs(inner, depth * rows // 2)
        return x, dot(jnp.concatenate([r_lo, x_lo, r_hi, x_hi], 1), down_0)

    def spread(b1, c1, i1, d1, a1, i2, d2, a2):
        c1 = plane_padded(c1[None], 1)
        y1 = 1.2 * c1 + a1 * sum_packed(c1, half)
        r1 = pair_rows(plane_padded(b1[None], 1) - d1 * y1 + 0.5 * up_down(y1))
        y1 = pair_rows(y1, 3 * rows // 2)
        n = rows // 4
        none = jnp.zeros((n, lanes), F32)
        around = jnp.concatenate([none, y1[:-n]], 0), jnp.concatenate([y1[n:], none], 0)
        b2 = dot(jnp.concatenate([r1, y1, *around], 1), down_1).reshape(3, n, lanes)
        c2 = plane_padded(b2 * i2[1:4], 1)
        y2 = 1.2 * c2 + a2 * sum_planes(c2)
        r2 = plane_padded(b2, 2) - plane_padded(d2 * y2, 1)
        y2 = plane_padded(y2, 1)
        before, after = shifted(y2)
        r2s[0, 1:8] = r2 + 0.25 * (up_down(y2) + (before + after))
        r2s[1, 1:8] = y2
        pairs = [
            pair_rows(r2s[i, pl.ds(me % 2, 8)].reshape(4, 2, n, lanes).sum(1), i * 4 * n)
            for i in range(2)
        ]
        b3 = dot(jnp.concatenate(pairs, 1), down_3).reshape(4, n // 2, lanes)
        first = (me + 4 + me % 2) // 2
        return b2, sum(jnp.where(lane // GROUP == (first + q) % groups, b3[q], 0.0) for q in range(4))

    def side_by_side(b2):
        return b2[1] + (pltpu.roll(b2[0], GROUP, 1) + pltpu.roll(b2[2], 2 * GROUP, 1))

    def level_2(t, c3, i2, a2, a3):
        b = jnp.where(valid(me - 6, 13, parts), bw[t], 0.0)
        b2 = b[1:-1] + (pltpu.roll(b[2:], lanes - GROUP, 2) + pltpu.roll(b[:-2], lanes - 2 * GROUP, 2))
        c2 = b2 * i2
        y2 = 1.2 * c2[1:-1] + a2 * sum_planes(c2)[1:-1]
        c2 = c2[1:-1]
        y2 = ((0.2 * y2 + c2) + a2 * sum_planes(y2))[1:-1]
        y3 = dot(flat(coarse_solve(c3, a3)), up_3)
        for g in range(groups):
            y3s[2 + 4 * g:6 + 4 * g] = y3[:, 2 * g * lanes:2 * (g + 1) * lanes].reshape(4, rows // 8, 2 * lanes)
        lift, sides = [
            jnp.where(me % 2 == 1, x[1:], x[:-1]) for x in
            [twice_planes(x) for x in twice_rows(y3s[pl.ds(me // 2, 5)].reshape(5 * rows // 8, 2 * lanes), 5)]
        ]
        total = (sides + up_down(lift))[1:-1] + (lift[:-2] + lift[2:])
        y2 = y2 + (0.2 * lift[1:-1] + a2[1:-1] * total)
        y2 = ((0.2 * y2 + c2[1:-1]) + a2[1:-1] * sum_planes(y2))[1:-1]
        return twice_rows(dot(flat(y2), up_2), 5)

    def swept_1(y1, lift, sides, a1):
        before, after = shifted(lift)
        across = lift + jnp.where(iota(lift.shape, 2) < half, before, after)
        return y1 + (0.2 * lift + a1 * ((sides + up_down(lift)) + across))

    def lift_0(y1, skip):
        n = rows // 2
        around = flat(y1)
        both = dot(around, up_lo), dot(around, up_hi)
        halves = [part[n * k:n * k + n] for k in range(3) for part in both]
        halves = halves[skip:len(halves) - skip]
        return [twice_planes(x) for x in twice_rows(jnp.concatenate(halves, 0), len(halves))]

    def swept_0(lift, sides, a):
        total = (sides + up_down(lift))[1:-1] + (lift[:-2] + lift[2:])
        return 0.2 * lift[1:-1] + a * total

    arrive(near)
    x, b1 = first_sweeps(own[...], planes_of(c0, d + 1, d - 1, d + 4), a)
    arrive(cap_window[0])
    arrive(cap2_window[0])
    d1, i1 = inverse_1(1, 4)
    d2, i2 = inverse_2(3, 8)
    near_1 = i1, d1, 0.5 * i1, i2, d2, 0.25 * i2
    c1 = b1 * i1[1]
    vw[0, 3] = c1
    b2, b3 = spread(b1, c1, *near_1)
    gr[0, me] = b3 + cap_sent
    bw[0, 6] = side_by_side(b2)
    pl.semaphore_wait(far_sem, 2)
    begin(gather_r[0])
    arrive(cap_far)
    begin(pass_far)
    begin(b_window[0])
    begin(c_window[0])
    arrive(far)
    arrive(pass_far)
    wide = weights(1, 3 * d - 2)
    c = planes_of(c0, d + 1, d - 2, d + 6)
    first = 1.2 * c[1:2] + wide[1:2] * sum_inner(c[0:3], lanes)
    final = 1.2 * c[-2:-1] + wide[-2:-1] * sum_inner(c[-3:], lanes)

    def last_sweeps(x, c):
        x = (0.2 * x[1:-1] + c) + a * sum_inner(x, lanes)
        return (0.2 * x[1:-1] + c[1:-1]) + a[1:-1] * sum_inner(x, lanes)

    alone = last_sweeps(jnp.concatenate([first, x, final], 0), c[2:-2])
    fp_ref[...] = alone
    src1[2:d + 2] = cap[d:2 * d] * alone + src1[2:d + 2]
    begin(known)
    arrive(cap_window[1])
    a1 = 0.5 * inverse_1(0, 5)[1]
    arrive(cap2_window[1])
    i2 = inverse_2(0, 11)[1]
    a2 = 0.25 * i2[1:-1]
    arrive(gather_r[0])
    arrive(b_window[0])
    arrive(c_window[0])

    got = gr[0]
    cap3 = capacity_3(got)
    i3 = jnp.where(iota(cap3.shape, 2) % GROUP < GROUP // 2, W / (cap3 + 0.75), 0.0)
    a3 = 0.125 * i3
    c1 = jnp.where(valid(me - 3, 7, parts), vw[0], 0.0)
    y1 = 1.2 * c1[1:-1] + a1 * sum_packed(c1, half)[1:-1]
    c1 = c1[1:-1]
    y1 = (0.2 * y1 + c1) + a1 * sum_packed(y1, half)
    y1 = swept_1(y1, *level_2(0, level_3(got) * i3, i2, a2, a3), a1)
    y1 = ((0.2 * y1 + c1) + a1 * sum_packed(y1, half))[1:-1]
    x = swept_0(*lift_0(y1, 0), wide)
    x = 0.2 * x[1:-1] + wide[1:-1] * sum_inner(x, lanes)
    fp_ref[...] = fp_ref[...] + x[2:-2]
    arrive(known)
    b = cap[2:3 * d - 2] * x + src1[...]
    c1x[1:d + 5] = b * wide[1:-1]
    begin(third)

    x, b1 = first_sweeps(b[2:-2], c1x[1:d + 5], a)
    c1 = b1 * i1[1]
    c_sent[...] = c1
    b2, b3 = spread(b1, c1, *near_1)
    r_sent[...] = b3
    b_sent[...] = side_by_side(b2)

    @pl.when(span < spans - 1)
    def _():
        begin(gather_r[1])
        begin(b_window[1])
        begin(c_window[1])

    arrive(third)
    c = planes_of(c1x, 3, 0, d + 6)
    first = 1.2 * c[1:2] + wide[1:2] * sum_inner(c[0:3], lanes)
    final = 1.2 * c[-2:-1] + wide[-2:-1] * sum_inner(c[-3:], lanes)
    fin[0] = last_sweeps(jnp.concatenate([first, x, final], 0), c[2:-2])

    @pl.when(span < spans - 1)
    def _():
        begin(fin_onward)

    handed = gather_r[1], b_window[1], c_window[1], fin_onward
    for made in batches:
        if not any(made is other for other in handed):
            sent(made)

    @pl.when(span == 0)
    def _():
        up_ref[...] = u0[...]

    @pl.when(span > 0)
    def _():
        arrive(handed[0])
        arrive(handed[1])
        arrive(handed[2])
        arrive(handed[3])
        c1 = jnp.where(valid(me - 2, 5, parts), vw[1, 1:6], 0.0)
        y1 = 1.2 * c1 + a1 * sum_packed(c1, half)
        y1 = (0.2 * y1 + c1) + a1 * sum_packed(y1, half)
        y1 = swept_1(y1, *level_2(1, level_3(gr[1]) * i3, i2, a2, a3), a1)[1:-1]
        y1 = (0.2 * y1 + c1[1:-1]) + a1[1:-1] * sum_packed(y1, half)
        x = swept_0(*lift_0(y1, 1), a)
        up_ref[...] = fin[1] + (0.2 * x[1:-1] + a[1:-1] * sum_inner(x, lanes))

    @pl.when(span < spans - 1)
    def _():
        for made in handed:
            sent(made)


def shards(span_opening, source_power, warmth_retention):
    parts, spans = lax.axis_size("space"), lax.axis_size("tm")
    steps = source_power.shape[1]
    depth, rows, lanes = warmth_retention.shape
    assert steps == 2 and depth == 4
    slab = jax.ShapeDtypeStruct((depth, rows, lanes), F32)
    vmem = pl.BlockSpec(memory_space=pltpu.VMEM)
    dma = pltpu.SemaphoreType.DMA
    fpoint, updated = pl.pallas_call(
        functools.partial(kernel, parts, spans, steps),
        out_shape=(pltpu.VMEM(slab.shape, F32),) * 2,
        in_specs=[pl.BlockSpec(memory_space=pl.ANY)] * 3,
        out_specs=(vmem, vmem),
        scratch_shapes=[
            pltpu.VMEM((depth, rows, lanes), F32),
            pltpu.VMEM((depth, rows, lanes), F32),
            pltpu.VMEM((depth + 4, rows, lanes), F32),
            pltpu.VMEM((3 * depth, rows, lanes), F32),
            pltpu.VMEM((3 * depth + 2, rows, lanes), F32),
            pltpu.VMEM((depth + 6, rows, lanes), F32),
            pltpu.VMEM((5, rows // 2, lanes), F32),
            pltpu.VMEM((11, rows // 8, lanes), F32),
            pltpu.VMEM((steps, 7, rows // 2, lanes), F32),
            pltpu.VMEM((rows // 2, lanes), F32),
            pltpu.VMEM((steps, 13, rows // 4, lanes), F32),
            pltpu.VMEM((rows // 4, lanes), F32),
            pltpu.VMEM((steps, parts, rows // 8, lanes), F32),
            pltpu.VMEM((rows // 8, lanes), F32),
            pltpu.VMEM((2, 9, rows // 4, lanes), F32),
            pltpu.VMEM((parts // 2 + 4, rows // 8, 2 * lanes), F32),
            pltpu.VMEM((depth, rows, lanes), F32),
            pltpu.VMEM((12 * rows, lanes), F32),
            pltpu.VMEM((2, depth, rows, lanes), F32),
            pltpu.SemaphoreType.REGULAR,
            pltpu.SemaphoreType.REGULAR,
            dma((4,)), dma((18,)), dma((18,)),
        ],
        compiler_params=pltpu.CompilerParams(
            collective_id=0, has_side_effects=True, vmem_limit_bytes=67043328 - 2 * 4 * slab.size
        ),
    )(span_opening[0], source_power[0], warmth_retention)
    flag = lax.axis_index("tm") > spans
    fpoint, updated = jnp.where(flag, updated, fpoint), jnp.where(flag, fpoint, updated)
    return fpoint[None], updated[None]


def solution(mesh):
    in_specs = (
        P("tm", "space", None, None),
        P("tm", None, "space", None, None),
        P("space", None, None),
    )
    out_specs = (P("tm", "space", None, None), P("tm", "space", None, None))
    return jax.shard_map(shards, mesh=mesh, in_specs=in_specs, out_specs=out_specs, check_vma=False)
```

```python
import functools

import jax
import jax.numpy as jnp
from jax import lax
from jax.experimental import pallas as pl
from jax.experimental.pallas import tpu as pltpu
from jax.sharding import PartitionSpec as P

COARSE_SWEEPS = 24
W = 0.8
GROUP = 32
NEAR = 4
F32 = jnp.float32
MESH = pl.DeviceIdType.MESH


def iota(shape, dim):
    return lax.broadcasted_iota(jnp.int32, shape, dim)


def dot(a, b):
    total = None
    for _ in range(2):
        part = a.astype(jnp.bfloat16)
        a = a - part.astype(F32)
        term = jnp.dot(part, b, preferred_element_type=F32)
        total = term if total is None else total + term
    return total


def picks(lanes, pick, scale):
    src, dst = iota((lanes, lanes), 0), iota((lanes, lanes), 1)
    return jnp.where(pick(src, dst), scale, 0.0).astype(jnp.bfloat16)


def from_sides(lanes, pick, width, scale):
    def shifted_pick(by):
        return picks(lanes, lambda s, d: (s % width + by >= 0) & (s % width + by < width) & pick(s + by, d), scale)

    return shifted_pick(-1) + shifted_pick(1)


def to_sides(lanes, pick, width):
    def shifted_pick(by):
        return picks(lanes, lambda s, d: (d % width + by >= 0) & (d % width + by < width) & pick(s, d + by), 1.0)

    return shifted_pick(-1) + shifted_pick(1)


def up_down(x):
    rows = x.shape[1]
    row = iota(x.shape, 1)
    up = jnp.where(row == 0, 0.0, pltpu.roll(x, 1, 1))
    return up + jnp.where(row == rows - 1, 0.0, pltpu.roll(x, rows - 1, 1))


def in_plane(x, width):
    lanes = x.shape[2]
    lane = iota(x.shape, 2)
    left, right = pltpu.roll(x, 1, 2), pltpu.roll(x, lanes - 1, 2)
    if width:
        left = jnp.where(lane % width == 0, 0.0, left)
        right = jnp.where(lane % width == width - 1, 0.0, right)
    return (left + right) + up_down(x)


def shifted(x):
    zero = jnp.zeros((1,) + x.shape[1:], F32)
    return jnp.concatenate([zero, x[:-1]], 0), jnp.concatenate([x[1:], zero], 0)


def earlier(x, by=1, shift=0):
    lanes = x.shape[2]
    moved = pltpu.roll(x[-by:], (GROUP + shift) % lanes, 2)
    return jnp.where(iota(moved.shape, 2) < GROUP, 0.0, moved)


def later(x, by=1, shift=0):
    lanes = x.shape[2]
    moved = pltpu.roll(x[:by], (lanes - GROUP + shift) % lanes, 2)
    return jnp.where(iota(moved.shape, 2) >= lanes - GROUP, 0.0, moved)


def sum_grouped(x):
    ends = jnp.concatenate([earlier(x), x, later(x)], 0)
    return in_plane(x, GROUP) + (ends[:-2] + ends[2:])


def sum_planes(x):
    before, after = shifted(x)
    return in_plane(x, None) + (before + after)


def plane_padded(x, by):
    zero = jnp.zeros((by,) + x.shape[1:], F32)
    return jnp.concatenate([zero, x, zero], 0)


def sum_packed(x, width):
    half = pltpu.roll(x, width, 2)
    before, after = shifted(half)
    return in_plane(x, width) + (half + jnp.where(iota(x.shape, 2) < width, before, after))


def sum_inner(x, width):
    return in_plane(x[1:-1], width) + (x[:-2] + x[2:])


def column_sum(x):
    rows = x.shape[1]
    mid = x[1:-1]
    row = iota(mid.shape, 1)
    up = jnp.where(row == 0, 0.0, pltpu.roll(mid, 1, 1))
    down = jnp.where(row == rows - 1, 0.0, pltpu.roll(mid, rows - 1, 1))
    return (x[:-2] + x[2:]) + (up + down)


def coarse_solve(c, a):
    n, lanes = c.shape[0], c.shape[2]

    def turned(x, by):
        return x if by == 0 else pltpu.roll(x, by % lanes, 2)

    def longer(x, by, reach=1):
        return jnp.concatenate([earlier(x, reach, by), turned(x, by), later(x, reach, by)], 0)

    c_at, a_at = [[longer(x, 0) if by == 0 else turned(x, by) for by in (1, 0, -1)] for x in (c, a)]

    def sweep(y, side, c, a):
        return (0.2 * y[1:-1] + c) + a * (side + column_sum(y))

    def two_sweeps(_, y):
        left, mid, right = longer(y, 1), longer(y, 0, 2), longer(y, -1)
        once_left = sweep(left, turned(y, 2) + y, c_at[0], a_at[0])
        once_mid = sweep(mid, left + right, c_at[1], a_at[1])
        once_right = sweep(right, y + turned(y, -2), c_at[2], a_at[2])
        return sweep(once_mid, once_left + once_right, c, a)

    left = COARSE_SWEEPS - 1
    y = c
    if left % 2:
        y = 1.2 * c + a * sum_grouped(c)
    return lax.fori_loop(0, left // 2, two_sweeps, y, unroll=True)


def flat(x):
    return x.reshape(x.shape[0] * x.shape[1], x.shape[2])


def kernel(
    parts, spans, steps,
    open_ref, src_ref, cap_in,
    fp_ref, up_ref,
    u0, src0, src1, cap, c0, c1x, cw, kw, vw, c_sent, bw, b_sent, gr, r_sent, r2s, y3s, own, tmp, fin,
    near_sem, far_sem, in_sem, send_sem, recv_sem,
):
    me, span = lax.axis_index("space"), lax.axis_index("tm")
    depth, rows, lanes = open_ref.shape
    half = lanes // 2
    groups = lanes // GROUP
    assert parts == 32 and lanes == 128 and rows == 64
    assert parts == 8 * NEAR
    close = [k for k in range(-NEAR, NEAR + 1) if k]

    loads = [
        pltpu.make_async_copy(cap_in, cap.at[pl.ds(depth, depth)], in_sem.at[0]),
        pltpu.make_async_copy(open_ref, u0, in_sem.at[1]),
        pltpu.make_async_copy(src_ref.at[0], src0, in_sem.at[2]),
        pltpu.make_async_copy(src_ref.at[1], src1.at[pl.ds(2, depth)], in_sem.at[3]),
    ]
    for load in loads:
        load.start()
    barrier = pltpu.get_barrier_semaphore()
    for k in close:
        pl.semaphore_signal(barrier, inc=1, device_id={"space": lax.rem(me + k % parts, parts)}, device_id_type=MESH)
    for k in (1, spans - 1):
        pl.semaphore_signal(barrier, inc=1, device_id={"tm": lax.rem(span + k, spans)}, device_id_type=MESH)

    r2s[...] = jnp.zeros(r2s.shape, F32)
    y3s[...] = jnp.zeros(y3s.shape, F32)

    def pick_lo(s, d):
        return (s // 2 == d) & (d < half)

    def pick_hi(s, d):
        return s // 2 + half == d

    def pick_2(s, d):
        return (s % half) // 2 == d

    def pick_3(s, d):
        return (s < GROUP) & (d % GROUP == s // 2)

    def swap(pick):
        return lambda s, d: pick(d, s)

    down_0 = jnp.concatenate([
        picks(lanes, pick_lo, 0.125), from_sides(lanes, pick_lo, lanes, 0.125),
        picks(lanes, pick_hi, 0.125), from_sides(lanes, pick_hi, lanes, 0.125),
    ], 0)
    down_cap1 = jnp.concatenate([picks(lanes, pick_lo, 0.125), picks(lanes, pick_hi, 0.125)], 0)
    down_2 = picks(lanes, pick_2, 0.125)
    down_1 = jnp.concatenate([
        down_2, from_sides(lanes, pick_2, half, 0.0625) + picks(lanes, pick_2, 0.0625),
        picks(lanes, lambda s, d: pick_2(s, d) & (s >= half), 0.0625),
        picks(lanes, lambda s, d: pick_2(s, d) & (s < half), 0.0625),
    ], 0)
    down_3 = jnp.concatenate([picks(lanes, pick_3, 0.125), from_sides(lanes, pick_3, GROUP, 0.03125)], 0)
    down_cap = picks(lanes, lambda s, d: (s < GROUP) & (d % GROUP == s // 2 + GROUP // 2), 0.125)
    def rises(pick, width):
        return [picks(lanes, pick, 1.0), to_sides(lanes, pick, width)]

    up_lo = jnp.concatenate(rises(lambda s, d: d // 2 == s, lanes), 1)
    up_hi = jnp.concatenate(rises(lambda s, d: d // 2 + half == s, lanes), 1)
    up_2 = jnp.concatenate(rises(swap(pick_2), half), 1)
    up_3 = jnp.concatenate([
        rise for g in range(groups)
        for rise in rises(lambda s, d: (d < GROUP) & (d // 2 + g * GROUP == s), GROUP)
    ], 1)

    def pair_rows(x, at=0):
        n, r, w = x.shape
        tmp[pl.ds(at, n * r), :] = flat(x)
        return tmp[pl.ds(at, n * r // 2, 2), :] + tmp[pl.ds(at + 1, n * r // 2, 2), :]

    def twice_rows(x, planes):
        parts_of = [x[:, at:at + lanes] for at in range(0, x.shape[1], lanes)]
        x = jnp.concatenate(parts_of, 0)
        r = x.shape[0]
        tmp[pl.ds(0, r, 2), :] = x
        tmp[pl.ds(1, r, 2), :] = x
        out = tmp[pl.ds(0, 2 * r), :].reshape(len(parts_of) * planes, -1, lanes)
        return [out[at:at + planes] for at in range(0, out.shape[0], planes)]

    def twice_planes(x):
        return jnp.broadcast_to(x[:, None], (x.shape[0], 2) + x.shape[1:]).reshape((2 * x.shape[0],) + x.shape[1:])

    def slab_pairs(x, at=0):
        s = pair_rows(x.reshape(depth // 2, 2, rows, lanes).sum(1), at)
        return s[:rows // 2], s[rows // 2:]

    def to_2(x):
        return dot(pair_rows(x), down_2).reshape(x.shape[0], rows // 4, lanes)

    lane = iota((rows // 8, lanes), 1)

    def turn(planes, off):
        out = []
        for k in range(groups):
            total = None
            for g in range(groups):
                by = (GROUP * (g - k) - off) % lanes
                moved = pltpu.roll(planes[g], by, 1) if by else planes[g]
                total = moved if total is None else jnp.where(lane // GROUP == g, moved, total)
            out.append(total[None])
        return jnp.concatenate(out, 0)

    def level_3(got):
        pairs = [got[0]] + [got[2 * i - 1] + got[2 * i] for i in range(1, parts // 2)] + [got[parts - 1]]
        out = []
        for k in range(groups):
            total = pairs[4 * k + 2]
            for i, keep in (
                (4 * k - 1, lane < GROUP), (4 * k, lane < 2 * GROUP), (4 * k + 1, lane < 3 * GROUP),
                (4 * k + 3, lane >= GROUP), (4 * k + 4, lane >= 2 * GROUP), (4 * k + 5, lane >= 3 * GROUP),
            ):
                if 0 <= i < len(pairs):
                    total = total + jnp.where(keep, pairs[i], 0.0)
            out.append(total)
        return turn(out, 0)

    def capacity_3(got):
        out = []
        for k in range(groups):
            total = None
            for g in range(groups):
                i = 2 * (4 * k + g)
                pair = got[i] + got[i + 1]
                total = pair if total is None else jnp.where(lane // GROUP == g, pair, total)
            out.append(total)
        return turn(out, GROUP // 2)

    def valid(start, count, of):
        at = start + iota((count, 1, 1), 0)
        return (at >= 0) & (at < of)

    batches = []

    def batch(pieces, total):
        at = len(batches)

        def copy(source, target, to):
            return pltpu.make_async_remote_copy(
                source, target, send_sem.at[at], recv_sem.at[at], device_id=to, device_id_type=MESH)

        made = [copy(*piece) for piece in pieces], copy(total, total, pieces[0][2])
        batches.append(made)
        return made

    def begin(made):
        for copy in made[0]:
            copy.start()

    def arrive(made):
        made[1].wait_recv()

    def sent(made):
        made[1].wait_send()

    def beside(k):
        return {"space": lax.rem(me + (k + parts) % parts, parts)}

    share = rows // 2
    my_rows = pl.ds(pl.multiple_of(span % 2 * share, share), share)

    def halo(buf, count, up, down, rows_at=None):
        def part(start):
            return buf.at[pl.ds(start, count)] if rows_at is None else buf.at[pl.ds(start, count), rows_at]

        total = buf.at[pl.ds(0, 2 * count)] if rows_at is None else buf.at[pl.ds(0, 2 * count), pl.ds(0, share)]
        return batch([(part(way[0]), part(way[1]), beside(k)) for way, k in ((up, 1), (down, -1))], total)

    def window(buf, source, nearest, reach, to={}):
        middle = buf.shape[0] // 2
        offsets = [k for far in range(reach, nearest - 1, -1) for k in ((far, -far) if far else (0,))]
        return batch([(source, buf.at[middle - k], {**beside(k), **to}) for k in offsets], buf.at[pl.ds(0, len(offsets))])

    def hops(k):
        z, y = k // 4, k % 4
        return min(z, parts // 4 - z) + min(y, 4 - y)

    def gather(buf, source, offsets, to={}):
        offsets = sorted(offsets, key=lambda k: -hops(k))
        return batch([(source, buf.at[me], {**beside(k), **to}) for k in offsets], buf.at[pl.ds(0, len(offsets))])

    d = depth
    onward = {"tm": (span + 1) % spans}
    near = halo(c0, 2, (2 * d - 1, d - 1), (d + 1, 2 * d + 1))
    far = halo(c0, 1, (2 * d - 2, d - 2), (d + 3, 2 * d + 3))
    known = halo(src1, 2, (d, 0), (2, d + 2))
    third = halo(c1x, 1, (d, 0), (5, d + 5))
    cap_near = halo(cap, 1, (2 * d - 1, d - 1), (d, 2 * d))
    cap_far = halo(cap, 2, (d + 1, 1), (d + 1, 2 * d + 1), my_rows)
    pass_far = batch(
        [
            (cap.at[pl.ds(start, 2), my_rows], cap.at[pl.ds(start, 2), my_rows], {"tm": span + 1 - 2 * (span % 2)})
            for start in (1, 2 * d + 1)
        ], cap.at[pl.ds(0, 4), pl.ds(0, share)])
    half_block = pl.ds(pl.multiple_of(span % 2 * (share // 2), share // 2), share // 2)
    half_total = cw.at[pl.ds(0, 2), pl.ds(0, share // 2)]
    cap_window = window(cw, cw.at[2], 1, 1), batch(
        [(cw.at[2, half_block], cw.at[2 - k, half_block], beside(k)) for k in (2, -2)], half_total)
    pass_window = batch(
        [(cw.at[i, half_block], cw.at[i, half_block], {"tm": span + 1 - 2 * (span % 2)}) for i in (0, 4)], half_total)
    cap2_window = window(kw, kw.at[5], 1, 2), window(kw, kw.at[5], 3, 5)
    gather_r = gather(gr.at[0], gr.at[0, me], range(1, parts)), gather(gr.at[1], r_sent, range(parts), onward)
    c_window = window(vw.at[0], vw.at[0, 3], 1, 3), window(vw.at[1], c_sent, 0, 2, onward)
    b_window = window(bw.at[0], bw.at[0, 6], 1, 6), window(bw.at[1], b_sent, 0, 6, onward)
    fin_onward = batch([(fin.at[0], fin.at[1], onward)], fin.at[0])

    loads[0].wait()
    mine = cap[d:2 * d]
    loads[1].wait()
    loads[2].wait()
    b = mine * u0[...] + src0[...]
    own[...] = b
    c0[d + 1:2 * d + 1] = b * (W / (mine + 6.0))

    pl.semaphore_wait(barrier, len(close) + 2)
    begin(near)
    begin(cap_near)
    for k in (NEAR, -NEAR):
        pl.semaphore_signal(near_sem, inc=1, device_id=beside(k), device_id_type=MESH)
    cap1 = dot(jnp.concatenate(slab_pairs(mine), 1), down_cap1)
    cw[2] = cap1
    begin(cap_window[0])
    cap2 = to_2(cap1[None])
    kw[5] = cap2[0, :rows // 8] + pltpu.roll(cap2[0, rows // 8:], GROUP, 1)
    begin(cap2_window[0])
    begin(cap_far)
    begin(far)
    begin(cap_window[1])
    pl.semaphore_wait(near_sem, 2)
    for k in (2 * NEAR, -2 * NEAR):
        pl.semaphore_signal(far_sem, inc=1, device_id=beside(k), device_id_type=MESH)
    begin(cap2_window[1])
    cap_sent = dot(pair_rows(cap2), down_cap)
    loads[3].wait()

    def weights(start, count):
        inside = valid((me - 1) * depth + start, count, parts * depth)
        return jnp.where(inside, W / (cap[start:start + count] + 6.0), 0.0)

    def inverse(diagonal, start, reach):
        return jnp.where(valid(me - reach + start, diagonal.shape[0], parts), W / diagonal, 0.0)

    def planes_of(buf, own, start, count):
        return jnp.where(valid(me * depth + start - own, count, parts * depth), buf[start:start + count], 0.0)

    def inverse_1(start, stop):
        diagonal = cw[start:stop] + 3.0
        return diagonal, inverse(diagonal, start, 2)

    def inverse_2(start, stop):
        packed = kw[start:stop]
        diagonal = jnp.concatenate([packed, pltpu.roll(packed, lanes - GROUP, 2)], 1) + 1.5
        return diagonal, jnp.where(iota(diagonal.shape, 2) < GROUP, inverse(diagonal, start, 5), 0.0)

    arrive(cap_near)
    a = weights(d - 1, d + 2)

    def first_sweeps(b, c, a):
        x = 1.2 * c[1:-1] + a * sum_inner(c, lanes)
        inner = x[1:-1]
        r = b - (cap[d:2 * d] + 6.0) * inner + up_down(inner) + (x[:-2] + x[2:])
        (r_lo, r_hi), (x_lo, x_hi) = slab_pairs(r), slab_pairs(inner, depth * rows // 2)
        return x, dot(jnp.concatenate([r_lo, x_lo, r_hi, x_hi], 1), down_0)

    def spread(b1, c1, i1, d1, a1, i2, d2, a2):
        c1 = plane_padded(c1[None], 1)
        y1 = 1.2 * c1 + a1 * sum_packed(c1, half)
        r1 = pair_rows(plane_padded(b1[None], 1) - d1 * y1 + 0.5 * up_down(y1))
        y1 = pair_rows(y1, 3 * rows // 2)
        n = rows // 4
        none = jnp.zeros((n, lanes), F32)
        around = jnp.concatenate([none, y1[:-n]], 0), jnp.concatenate([y1[n:], none], 0)
        b2 = dot(jnp.concatenate([r1, y1, *around], 1), down_1).reshape(3, n, lanes)
        c2 = plane_padded(b2 * i2[1:4], 1)
        y2 = 1.2 * c2 + a2 * sum_planes(c2)
        r2 = plane_padded(b2, 2) - plane_padded(d2 * y2, 1)
        y2 = plane_padded(y2, 1)
        before, after = shifted(y2)
        r2s[0, 1:8] = r2 + 0.25 * (up_down(y2) + (before + after))
        r2s[1, 1:8] = y2
        pairs = [
            pair_rows(r2s[i, pl.ds(me % 2, 8)].reshape(4, 2, n, lanes).sum(1), i * 4 * n)
            for i in range(2)
        ]
        b3 = dot(jnp.concatenate(pairs, 1), down_3).reshape(4, n // 2, lanes)
        first = (me + 4 + me % 2) // 2
        return b2, sum(jnp.where(lane // GROUP == (first + q) % groups, b3[q], 0.0) for q in range(4))

    def side_by_side(b2):
        return b2[1] + (pltpu.roll(b2[0], GROUP, 1) + pltpu.roll(b2[2], 2 * GROUP, 1))

    def level_2(t, c3, i2, a2, a3):
        b = jnp.where(valid(me - 6, 13, parts), bw[t], 0.0)
        b2 = b[1:-1] + (pltpu.roll(b[2:], lanes - GROUP, 2) + pltpu.roll(b[:-2], lanes - 2 * GROUP, 2))
        c2 = b2 * i2
        y2 = 1.2 * c2[1:-1] + a2 * sum_planes(c2)[1:-1]
        c2 = c2[1:-1]
        y2 = ((0.2 * y2 + c2) + a2 * sum_planes(y2))[1:-1]
        y3 = dot(flat(coarse_solve(c3, a3)), up_3)
        for g in range(groups):
            y3s[2 + 4 * g:6 + 4 * g] = y3[:, 2 * g * lanes:2 * (g + 1) * lanes].reshape(4, rows // 8, 2 * lanes)
        lift, sides = [
            jnp.where(me % 2 == 1, x[1:], x[:-1]) for x in
            [twice_planes(x) for x in twice_rows(y3s[pl.ds(me // 2, 5)].reshape(5 * rows // 8, 2 * lanes), 5)]
        ]
        total = (sides + up_down(lift))[1:-1] + (lift[:-2] + lift[2:])
        y2 = y2 + (0.2 * lift[1:-1] + a2[1:-1] * total)
        y2 = ((0.2 * y2 + c2[1:-1]) + a2[1:-1] * sum_planes(y2))[1:-1]
        return twice_rows(dot(flat(y2), up_2), 5)

    def swept_1(y1, lift, sides, a1):
        before, after = shifted(lift)
        across = lift + jnp.where(iota(lift.shape, 2) < half, before, after)
        return y1 + (0.2 * lift + a1 * ((sides + up_down(lift)) + across))

    def lift_0(y1, skip):
        n = rows // 2
        around = flat(y1)
        both = dot(around, up_lo), dot(around, up_hi)
        halves = [part[n * k:n * k + n] for k in range(3) for part in both]
        halves = halves[skip:len(halves) - skip]
        return [twice_planes(x) for x in twice_rows(jnp.concatenate(halves, 0), len(halves))]

    def swept_0(lift, sides, a):
        total = (sides + up_down(lift))[1:-1] + (lift[:-2] + lift[2:])
        return 0.2 * lift[1:-1] + a * total

    arrive(near)
    x, b1 = first_sweeps(own[...], planes_of(c0, d + 1, d - 1, d + 4), a)
    arrive(cap_window[0])
    arrive(cap2_window[0])
    d1, i1 = inverse_1(1, 4)
    d2, i2 = inverse_2(3, 8)
    near_1 = i1, d1, 0.5 * i1, i2, d2, 0.25 * i2
    c1 = b1 * i1[1]
    vw[0, 3] = c1
    b2, b3 = spread(b1, c1, *near_1)
    gr[0, me] = b3 + cap_sent
    bw[0, 6] = side_by_side(b2)
    pl.semaphore_wait(far_sem, 2)
    begin(gather_r[0])
    begin(b_window[0])
    begin(c_window[0])
    arrive(cap_far)
    begin(pass_far)
    arrive(cap_window[1])
    begin(pass_window)
    arrive(far)
    arrive(pass_far)
    wide = weights(1, 3 * d - 2)
    c = planes_of(c0, d + 1, d - 2, d + 6)
    first = 1.2 * c[1:2] + wide[1:2] * sum_inner(c[0:3], lanes)
    final = 1.2 * c[-2:-1] + wide[-2:-1] * sum_inner(c[-3:], lanes)

    def last_sweeps(x, c):
        x = (0.2 * x[1:-1] + c) + a * sum_inner(x, lanes)
        return (0.2 * x[1:-1] + c[1:-1]) + a[1:-1] * sum_inner(x, lanes)

    alone = last_sweeps(jnp.concatenate([first, x, final], 0), c[2:-2])
    fp_ref[...] = alone
    src1[2:d + 2] = cap[d:2 * d] * alone + src1[2:d + 2]
    begin(known)
    arrive(pass_window)
    a1 = 0.5 * inverse_1(0, 5)[1]
    arrive(cap2_window[1])
    i2 = inverse_2(0, 11)[1]
    a2 = 0.25 * i2[1:-1]
    arrive(gather_r[0])
    arrive(b_window[0])
    arrive(c_window[0])

    got = gr[0]
    cap3 = capacity_3(got)
    i3 = jnp.where(iota(cap3.shape, 2) % GROUP < GROUP // 2, W / (cap3 + 0.75), 0.0)
    a3 = 0.125 * i3
    c1 = jnp.where(valid(me - 3, 7, parts), vw[0], 0.0)
    y1 = 1.2 * c1[1:-1] + a1 * sum_packed(c1, half)[1:-1]
    c1 = c1[1:-1]
    y1 = (0.2 * y1 + c1) + a1 * sum_packed(y1, half)
    y1 = swept_1(y1, *level_2(0, level_3(got) * i3, i2, a2, a3), a1)
    y1 = ((0.2 * y1 + c1) + a1 * sum_packed(y1, half))[1:-1]
    x = swept_0(*lift_0(y1, 0), wide)
    x = 0.2 * x[1:-1] + wide[1:-1] * sum_inner(x, lanes)
    fp_ref[...] = fp_ref[...] + x[2:-2]
    arrive(known)
    b = cap[2:3 * d - 2] * x + src1[...]
    c1x[1:d + 5] = b * wide[1:-1]
    begin(third)

    x, b1 = first_sweeps(b[2:-2], c1x[1:d + 5], a)
    c1 = b1 * i1[1]
    c_sent[...] = c1
    b2, b3 = spread(b1, c1, *near_1)
    r_sent[...] = b3
    b_sent[...] = side_by_side(b2)

    @pl.when(span < spans - 1)
    def _():
        begin(gather_r[1])
        begin(b_window[1])
        begin(c_window[1])

    arrive(third)
    c = planes_of(c1x, 3, 0, d + 6)
    first = 1.2 * c[1:2] + wide[1:2] * sum_inner(c[0:3], lanes)
    final = 1.2 * c[-2:-1] + wide[-2:-1] * sum_inner(c[-3:], lanes)
    fin[0] = last_sweeps(jnp.concatenate([first, x, final], 0), c[2:-2])

    @pl.when(span < spans - 1)
    def _():
        begin(fin_onward)

    handed = gather_r[1], b_window[1], c_window[1], fin_onward
    for made in batches:
        if not any(made is other for other in handed):
            sent(made)

    @pl.when(span == 0)
    def _():
        up_ref[...] = u0[...]

    @pl.when(span > 0)
    def _():
        arrive(handed[0])
        arrive(handed[1])
        arrive(handed[2])
        arrive(handed[3])
        c1 = jnp.where(valid(me - 2, 5, parts), vw[1, 1:6], 0.0)
        y1 = 1.2 * c1 + a1 * sum_packed(c1, half)
        y1 = (0.2 * y1 + c1) + a1 * sum_packed(y1, half)
        y1 = swept_1(y1, *level_2(1, level_3(gr[1]) * i3, i2, a2, a3), a1)[1:-1]
        y1 = (0.2 * y1 + c1[1:-1]) + a1[1:-1] * sum_packed(y1, half)
        x = swept_0(*lift_0(y1, 1), a)
        up_ref[...] = fin[1] + (0.2 * x[1:-1] + a[1:-1] * sum_inner(x, lanes))

    @pl.when(span < spans - 1)
    def _():
        for made in handed:
            sent(made)


def shards(span_opening, source_power, warmth_retention):
    parts, spans = lax.axis_size("space"), lax.axis_size("tm")
    steps = source_power.shape[1]
    depth, rows, lanes = warmth_retention.shape
    assert steps == 2 and depth == 4
    slab = jax.ShapeDtypeStruct((depth, rows, lanes), F32)
    vmem = pl.BlockSpec(memory_space=pltpu.VMEM)
    dma = pltpu.SemaphoreType.DMA
    fpoint, updated = pl.pallas_call(
        functools.partial(kernel, parts, spans, steps),
        out_shape=(pltpu.VMEM(slab.shape, F32),) * 2,
        in_specs=[pl.BlockSpec(memory_space=pl.ANY)] * 3,
        out_specs=(vmem, vmem),
        scratch_shapes=[
            pltpu.VMEM((depth, rows, lanes), F32),
            pltpu.VMEM((depth, rows, lanes), F32),
            pltpu.VMEM((depth + 4, rows, lanes), F32),
            pltpu.VMEM((3 * depth, rows, lanes), F32),
            pltpu.VMEM((3 * depth + 2, rows, lanes), F32),
            pltpu.VMEM((depth + 6, rows, lanes), F32),
            pltpu.VMEM((5, rows // 2, lanes), F32),
            pltpu.VMEM((11, rows // 8, lanes), F32),
            pltpu.VMEM((steps, 7, rows // 2, lanes), F32),
            pltpu.VMEM((rows // 2, lanes), F32),
            pltpu.VMEM((steps, 13, rows // 4, lanes), F32),
            pltpu.VMEM((rows // 4, lanes), F32),
            pltpu.VMEM((steps, parts, rows // 8, lanes), F32),
            pltpu.VMEM((rows // 8, lanes), F32),
            pltpu.VMEM((2, 9, rows // 4, lanes), F32),
            pltpu.VMEM((parts // 2 + 4, rows // 8, 2 * lanes), F32),
            pltpu.VMEM((depth, rows, lanes), F32),
            pltpu.VMEM((12 * rows, lanes), F32),
            pltpu.VMEM((2, depth, rows, lanes), F32),
            pltpu.SemaphoreType.REGULAR,
            pltpu.SemaphoreType.REGULAR,
            dma((4,)), dma((19,)), dma((19,)),
        ],
        compiler_params=pltpu.CompilerParams(
            collective_id=0, has_side_effects=True, vmem_limit_bytes=67043328 - 2 * 4 * slab.size
        ),
    )(span_opening[0], source_power[0], warmth_retention)
    flag = lax.axis_index("tm") > spans
    fpoint, updated = jnp.where(flag, updated, fpoint), jnp.where(flag, fpoint, updated)
    return fpoint[None], updated[None]


def solution(mesh):
    in_specs = (
        P("tm", "space", None, None),
        P("tm", None, "space", None, None),
        P("space", None, None),
    )
    out_specs = (P("tm", "space", None, None), P("tm", "space", None, None))
    return jax.shard_map(shards, mesh=mesh, in_specs=in_specs, out_specs=out_specs, check_vma=False)
```

```python
import functools
import math

import jax
import jax.numpy as jnp
from jax import lax
from jax.experimental import pallas as pl
from jax.experimental.pallas import tpu as pltpu
from jax.sharding import PartitionSpec as P

COARSE_SWEEPS = 24
W = 0.8
GROUP = 32
NEAR = 4
F32 = jnp.float32
MESH = pl.DeviceIdType.MESH


def iota(shape, dim):
    return lax.broadcasted_iota(jnp.int32, shape, dim)


def dot(a, b):
    total = None
    for _ in range(2):
        part = a.astype(jnp.bfloat16)
        a = a - part.astype(F32)
        term = jnp.dot(part, b, preferred_element_type=F32)
        total = term if total is None else total + term
    return total


def picks(lanes, pick, scale):
    src, dst = iota((lanes, lanes), 0), iota((lanes, lanes), 1)
    return jnp.where(pick(src, dst), scale, 0.0).astype(jnp.bfloat16)


def from_sides(lanes, pick, width, scale):
    def shifted_pick(by):
        return picks(lanes, lambda s, d: (s % width + by >= 0) & (s % width + by < width) & pick(s + by, d), scale)

    return shifted_pick(-1) + shifted_pick(1)


def to_sides(lanes, pick, width):
    def shifted_pick(by):
        return picks(lanes, lambda s, d: (d % width + by >= 0) & (d % width + by < width) & pick(s, d + by), 1.0)

    return shifted_pick(-1) + shifted_pick(1)


def up_down(x):
    rows = x.shape[1]
    row = iota(x.shape, 1)
    up = jnp.where(row == 0, 0.0, pltpu.roll(x, 1, 1))
    return up + jnp.where(row == rows - 1, 0.0, pltpu.roll(x, rows - 1, 1))


def in_plane(x, width):
    lanes = x.shape[2]
    lane = iota(x.shape, 2)
    left, right = pltpu.roll(x, 1, 2), pltpu.roll(x, lanes - 1, 2)
    if width:
        left = jnp.where(lane % width == 0, 0.0, left)
        right = jnp.where(lane % width == width - 1, 0.0, right)
    return (left + right) + up_down(x)


def shifted(x):
    zero = jnp.zeros((1,) + x.shape[1:], F32)
    return jnp.concatenate([zero, x[:-1]], 0), jnp.concatenate([x[1:], zero], 0)


def earlier(x, by=1, shift=0):
    lanes = x.shape[2]
    moved = pltpu.roll(x[-by:], (GROUP + shift) % lanes, 2)
    return jnp.where(iota(moved.shape, 2) < GROUP, 0.0, moved)


def later(x, by=1, shift=0):
    lanes = x.shape[2]
    moved = pltpu.roll(x[:by], (lanes - GROUP + shift) % lanes, 2)
    return jnp.where(iota(moved.shape, 2) >= lanes - GROUP, 0.0, moved)


def sum_grouped(x):
    ends = jnp.concatenate([earlier(x), x, later(x)], 0)
    return in_plane(x, GROUP) + (ends[:-2] + ends[2:])


def sum_planes(x):
    before, after = shifted(x)
    return in_plane(x, None) + (before + after)


def plane_padded(x, by):
    zero = jnp.zeros((by,) + x.shape[1:], F32)
    return jnp.concatenate([zero, x, zero], 0)


def sum_packed(x, width):
    half = pltpu.roll(x, width, 2)
    before, after = shifted(half)
    return in_plane(x, width) + (half + jnp.where(iota(x.shape, 2) < width, before, after))


def sum_inner(x, width):
    return in_plane(x[1:-1], width) + (x[:-2] + x[2:])


def column_sum(x):
    rows = x.shape[1]
    mid = x[1:-1]
    row = iota(mid.shape, 1)
    up = jnp.where(row == 0, 0.0, pltpu.roll(mid, 1, 1))
    down = jnp.where(row == rows - 1, 0.0, pltpu.roll(mid, rows - 1, 1))
    return (x[:-2] + x[2:]) + (up + down)


def coarse_solve(c, a):
    n, lanes = c.shape[0], c.shape[2]

    def turned(x, by):
        return x if by == 0 else pltpu.roll(x, by % lanes, 2)

    def longer(x, by, reach=1):
        return jnp.concatenate([earlier(x, reach, by), turned(x, by), later(x, reach, by)], 0)

    c_at, a_at = [[longer(x, 0) if by == 0 else turned(x, by) for by in (1, 0, -1)] for x in (c, a)]

    def sweep(y, side, c, a):
        return (0.2 * y[1:-1] + c) + a * (side + column_sum(y))

    def two_sweeps(_, y):
        left, mid, right = longer(y, 1), longer(y, 0, 2), longer(y, -1)
        once_left = sweep(left, turned(y, 2) + y, c_at[0], a_at[0])
        once_mid = sweep(mid, left + right, c_at[1], a_at[1])
        once_right = sweep(right, y + turned(y, -2), c_at[2], a_at[2])
        return sweep(once_mid, once_left + once_right, c, a)

    left = COARSE_SWEEPS - 1
    y = c
    if left % 2:
        y = 1.2 * c + a * sum_grouped(c)
    return lax.fori_loop(0, left // 2, two_sweeps, y, unroll=True)


def flat(x):
    return x.reshape(x.shape[0] * x.shape[1], x.shape[2])


def kernel(
    parts, spans, steps,
    open_ref, src_ref, cap_in,
    fp_ref, up_ref,
    u0, src0, src1, cap, c0, c1x, cw, kw, vw, c_sent, bw, b_sent, gr, r_sent, r2s, y3s, own, tmp, fin, spare,
    near_sem, far_sem, in_sem, send_sem, recv_sem,
):
    me, span = lax.axis_index("space"), lax.axis_index("tm")
    depth, rows, lanes = open_ref.shape
    half = lanes // 2
    groups = lanes // GROUP
    assert parts == 32 and lanes == 128 and rows == 64
    assert parts == 8 * NEAR
    close = [k for k in range(-NEAR, NEAR + 1) if k]

    loads = [
        pltpu.make_async_copy(cap_in, cap.at[pl.ds(depth, depth)], in_sem.at[0]),
        pltpu.make_async_copy(open_ref, u0, in_sem.at[0]),
        pltpu.make_async_copy(src_ref.at[0], src0, in_sem.at[0]),
        pltpu.make_async_copy(src_ref.at[1], src1.at[pl.ds(2, depth)], in_sem.at[1]),
    ]
    for load in loads:
        load.start()
    barrier = pltpu.get_barrier_semaphore()
    for k in close:
        pl.semaphore_signal(barrier, inc=1, device_id={"space": lax.rem(me + k % parts, parts)}, device_id_type=MESH)
    for k in (1, spans - 1):
        pl.semaphore_signal(barrier, inc=1, device_id={"tm": lax.rem(span + k, spans)}, device_id_type=MESH)

    r2s[...] = jnp.zeros(r2s.shape, F32)
    y3s[...] = jnp.zeros(y3s.shape, F32)

    def pick_lo(s, d):
        return (s // 2 == d) & (d < half)

    def pick_hi(s, d):
        return s // 2 + half == d

    def pick_2(s, d):
        return (s % half) // 2 == d

    def pick_3(s, d):
        return (s < GROUP) & (d % GROUP == s // 2)

    def swap(pick):
        return lambda s, d: pick(d, s)

    down_0 = jnp.concatenate([
        picks(lanes, pick_lo, 0.125), from_sides(lanes, pick_lo, lanes, 0.125),
        picks(lanes, pick_hi, 0.125), from_sides(lanes, pick_hi, lanes, 0.125),
    ], 0)
    down_cap1 = jnp.concatenate([picks(lanes, pick_lo, 0.125), picks(lanes, pick_hi, 0.125)], 0)
    down_2 = picks(lanes, pick_2, 0.125)
    down_1 = jnp.concatenate([
        down_2, from_sides(lanes, pick_2, half, 0.0625) + picks(lanes, pick_2, 0.0625),
        picks(lanes, lambda s, d: pick_2(s, d) & (s >= half), 0.0625),
        picks(lanes, lambda s, d: pick_2(s, d) & (s < half), 0.0625),
    ], 0)
    down_3 = jnp.concatenate([picks(lanes, pick_3, 0.125), from_sides(lanes, pick_3, GROUP, 0.03125)], 0)
    down_cap = picks(lanes, lambda s, d: (s < GROUP) & (d % GROUP == s // 2 + GROUP // 2), 0.125)
    def rises(pick, width):
        return [picks(lanes, pick, 1.0), to_sides(lanes, pick, width)]

    up_lo = jnp.concatenate(rises(lambda s, d: d // 2 == s, lanes), 1)
    up_hi = jnp.concatenate(rises(lambda s, d: d // 2 + half == s, lanes), 1)
    up_2 = jnp.concatenate(rises(swap(pick_2), half), 1)
    up_3 = jnp.concatenate([
        rise for g in range(groups)
        for rise in rises(lambda s, d: (d < GROUP) & (d // 2 + g * GROUP == s), GROUP)
    ], 1)

    def pair_rows(x, at=0):
        n, r, w = x.shape
        tmp[pl.ds(at, n * r), :] = flat(x)
        return tmp[pl.ds(at, n * r // 2, 2), :] + tmp[pl.ds(at + 1, n * r // 2, 2), :]

    def twice_rows(x, planes):
        parts_of = [x[:, at:at + lanes] for at in range(0, x.shape[1], lanes)]
        x = jnp.concatenate(parts_of, 0)
        r = x.shape[0]
        tmp[pl.ds(0, r, 2), :] = x
        tmp[pl.ds(1, r, 2), :] = x
        out = tmp[pl.ds(0, 2 * r), :].reshape(len(parts_of) * planes, -1, lanes)
        return [out[at:at + planes] for at in range(0, out.shape[0], planes)]

    def twice_planes(x):
        return jnp.broadcast_to(x[:, None], (x.shape[0], 2) + x.shape[1:]).reshape((2 * x.shape[0],) + x.shape[1:])

    def slab_pairs(x, at=0):
        s = pair_rows(x.reshape(depth // 2, 2, rows, lanes).sum(1), at)
        return s[:rows // 2], s[rows // 2:]

    def to_2(x):
        return dot(pair_rows(x), down_2).reshape(x.shape[0], rows // 4, lanes)

    lane = iota((rows // 8, lanes), 1)

    def turn(planes, off):
        out = []
        for k in range(groups):
            total = None
            for g in range(groups):
                by = (GROUP * (g - k) - off) % lanes
                moved = pltpu.roll(planes[g], by, 1) if by else planes[g]
                total = moved if total is None else jnp.where(lane // GROUP == g, moved, total)
            out.append(total[None])
        return jnp.concatenate(out, 0)

    def level_3(got):
        pairs = [got[0]] + [got[2 * i - 1] + got[2 * i] for i in range(1, parts // 2)] + [got[parts - 1]]
        out = []
        for k in range(groups):
            total = pairs[4 * k + 2]
            for i, keep in (
                (4 * k - 1, lane < GROUP), (4 * k, lane < 2 * GROUP), (4 * k + 1, lane < 3 * GROUP),
                (4 * k + 3, lane >= GROUP), (4 * k + 4, lane >= 2 * GROUP), (4 * k + 5, lane >= 3 * GROUP),
            ):
                if 0 <= i < len(pairs):
                    total = total + jnp.where(keep, pairs[i], 0.0)
            out.append(total)
        return turn(out, 0)

    def capacity_3(got):
        out = []
        for k in range(groups):
            total = None
            for g in range(groups):
                i = 2 * (4 * k + g)
                pair = got[i] + got[i + 1]
                total = pair if total is None else jnp.where(lane // GROUP == g, pair, total)
            out.append(total)
        return turn(out, GROUP // 2)

    def valid(start, count, of):
        at = start + iota((count, 1, 1), 0)
        return (at >= 0) & (at < of)

    own_span, next_span = 0, 1
    sent_rows, groups_of = [0, 0], {}

    def batch(pieces, total, group=None, side=own_span):
        at = groups_of.setdefault(group or len(groups_of), len(groups_of))
        count = total.size // lanes if hasattr(total, "size") else math.prod(total.shape) // lanes
        sent_rows[side] += count
        return [
            pltpu.make_async_remote_copy(
                source, target, send_sem.at[side], recv_sem.at[at], device_id=to, device_id_type=MESH)
            for source, target, to in pieces
        ], count, at, side

    def waiting(count, at, side):
        rows_of = spare.at[pl.ds(0, count)]
        return pltpu.make_async_remote_copy(
            rows_of, rows_of, send_sem.at[side], recv_sem.at[at], device_id=beside(1), device_id_type=MESH)

    def begin(made):
        for copy in made[0]:
            copy.start()

    def arrive(*made):
        assert len({one[2] for one in made}) == 1
        waiting(sum(one[1] for one in made), *made[0][2:]).wait_recv()

    def sent(side):
        waiting(sent_rows[side], 0, side).wait_send()

    def beside(k):
        return {"space": lax.rem(me + (k + parts) % parts, parts)}

    share = rows // 2
    my_rows = pl.ds(pl.multiple_of(span % 2 * share, share), share)

    def halo(buf, count, up, down, rows_at=None):
        def part(start):
            return buf.at[pl.ds(start, count)] if rows_at is None else buf.at[pl.ds(start, count), rows_at]

        total = buf.at[pl.ds(0, 2 * count)] if rows_at is None else buf.at[pl.ds(0, 2 * count), pl.ds(0, share)]
        return batch([(part(way[0]), part(way[1]), beside(k)) for way, k in ((up, 1), (down, -1))], total)

    def window(buf, source, nearest, reach, to={}, group=None, side=own_span):
        middle = buf.shape[0] // 2
        offsets = [k for far in range(reach, nearest - 1, -1) for k in ((far, -far) if far else (0,))]
        return batch([(source, buf.at[middle - k], {**beside(k), **to}) for k in offsets], buf.at[pl.ds(0, len(offsets))], group, side)

    def hops(k):
        z, y = k // 4, k % 4
        return min(z, parts // 4 - z) + min(y, 4 - y)

    def gather(buf, source, offsets, to={}, group=None, side=own_span):
        offsets = sorted(offsets, key=lambda k: -hops(k))
        return batch([(source, buf.at[me], {**beside(k), **to}) for k in offsets], buf.at[pl.ds(0, len(offsets))], group, side)

    d = depth
    onward = {"tm": (span + 1) % spans}
    near = halo(c0, 2, (2 * d - 1, d - 1), (d + 1, 2 * d + 1))
    far = halo(c0, 1, (2 * d - 2, d - 2), (d + 3, 2 * d + 3))
    known = halo(src1, 2, (d, 0), (2, d + 2))
    third = halo(c1x, 1, (d, 0), (5, d + 5))
    cap_near = halo(cap, 1, (2 * d - 1, d - 1), (d, 2 * d))
    cap_far = halo(cap, 2, (d + 1, 1), (d + 1, 2 * d + 1), my_rows)
    pass_far = batch(
        [
            (cap.at[pl.ds(start, 2), my_rows], cap.at[pl.ds(start, 2), my_rows], {"tm": span + 1 - 2 * (span % 2)})
            for start in (1, 2 * d + 1)
        ], cap.at[pl.ds(0, 4), pl.ds(0, share)])
    half_block = pl.ds(pl.multiple_of(span % 2 * (share // 2), share // 2), share // 2)
    half_total = cw.at[pl.ds(0, 2), pl.ds(0, share // 2)]
    cap_window = window(cw, cw.at[2], 1, 1, group="first"), batch(
        [(cw.at[2, half_block], cw.at[2 - k, half_block], beside(k)) for k in (2, -2)], half_total)
    pass_window = batch(
        [(cw.at[i, half_block], cw.at[i, half_block], {"tm": span + 1 - 2 * (span % 2)}) for i in (0, 4)], half_total)
    cap2_window = window(kw, kw.at[5], 1, 2, group="first"), window(kw, kw.at[5], 3, 5)
    to_next = {"to": onward, "group": "next", "side": next_span}
    gather_r = gather(gr.at[0], gr.at[0, me], range(1, parts), group="own"), gather(gr.at[1], r_sent, range(parts), **to_next)
    c_window = window(vw.at[0], vw.at[0, 3], 1, 3, group="own"), window(vw.at[1], c_sent, 0, 2, **to_next)
    b_window = window(bw.at[0], bw.at[0, 6], 1, 6, group="own"), window(bw.at[1], b_sent, 0, 6, **to_next)
    fin_onward = batch([(fin.at[0], fin.at[1], onward)], fin.at[0], "next", next_span)

    loaded = spare.at[pl.ds(0, 3 * depth * rows)]
    pltpu.make_async_copy(loaded, loaded, in_sem.at[0]).wait()
    mine = cap[d:2 * d]
    b = mine * u0[...] + src0[...]
    own[...] = b
    c0[d + 1:2 * d + 1] = b * (W / (mine + 6.0))

    pl.semaphore_wait(barrier, len(close) + 2)
    begin(near)
    begin(cap_near)
    for k in (NEAR, -NEAR):
        pl.semaphore_signal(near_sem, inc=1, device_id=beside(k), device_id_type=MESH)
    cap1 = dot(jnp.concatenate(slab_pairs(mine), 1), down_cap1)
    cw[2] = cap1
    begin(cap_window[0])
    cap2 = to_2(cap1[None])
    kw[5] = cap2[0, :rows // 8] + pltpu.roll(cap2[0, rows // 8:], GROUP, 1)
    begin(cap2_window[0])
    begin(cap_far)
    begin(far)
    begin(cap_window[1])
    pl.semaphore_wait(near_sem, 2)
    for k in (2 * NEAR, -2 * NEAR):
        pl.semaphore_signal(far_sem, inc=1, device_id=beside(k), device_id_type=MESH)
    begin(cap2_window[1])
    cap_sent = dot(pair_rows(cap2), down_cap)
    loads[3].wait()

    def weights(start, count):
        inside = valid((me - 1) * depth + start, count, parts * depth)
        return jnp.where(inside, W / (cap[start:start + count] + 6.0), 0.0)

    def inverse(diagonal, start, reach):
        return jnp.where(valid(me - reach + start, diagonal.shape[0], parts), W / diagonal, 0.0)

    def planes_of(buf, own, start, count):
        return jnp.where(valid(me * depth + start - own, count, parts * depth), buf[start:start + count], 0.0)

    def inverse_1(start, stop):
        diagonal = cw[start:stop] + 3.0
        return diagonal, inverse(diagonal, start, 2)

    def inverse_2(start, stop):
        packed = kw[start:stop]
        diagonal = jnp.concatenate([packed, pltpu.roll(packed, lanes - GROUP, 2)], 1) + 1.5
        return diagonal, jnp.where(iota(diagonal.shape, 2) < GROUP, inverse(diagonal, start, 5), 0.0)

    arrive(cap_near)
    a = weights(d - 1, d + 2)

    assert len(groups_of) == 13 and max(sent_rows) <= spare.shape[0]

    def first_sweeps(b, c, a):
        x = 1.2 * c[1:-1] + a * sum_inner(c, lanes)
        inner = x[1:-1]
        r = b - (cap[d:2 * d] + 6.0) * inner + up_down(inner) + (x[:-2] + x[2:])
        (r_lo, r_hi), (x_lo, x_hi) = slab_pairs(r), slab_pairs(inner, depth * rows // 2)
        return x, dot(jnp.concatenate([r_lo, x_lo, r_hi, x_hi], 1), down_0)

    def spread(b1, c1, i1, d1, a1, i2, d2, a2):
        c1 = plane_padded(c1[None], 1)
        y1 = 1.2 * c1 + a1 * sum_packed(c1, half)
        r1 = pair_rows(plane_padded(b1[None], 1) - d1 * y1 + 0.5 * up_down(y1))
        y1 = pair_rows(y1, 3 * rows // 2)
        n = rows // 4
        none = jnp.zeros((n, lanes), F32)
        around = jnp.concatenate([none, y1[:-n]], 0), jnp.concatenate([y1[n:], none], 0)
        b2 = dot(jnp.concatenate([r1, y1, *around], 1), down_1).reshape(3, n, lanes)
        c2 = plane_padded(b2 * i2[1:4], 1)
        y2 = 1.2 * c2 + a2 * sum_planes(c2)
        r2 = plane_padded(b2, 2) - plane_padded(d2 * y2, 1)
        y2 = plane_padded(y2, 1)
        before, after = shifted(y2)
        r2s[0, 1:8] = r2 + 0.25 * (up_down(y2) + (before + after))
        r2s[1, 1:8] = y2
        pairs = [
            pair_rows(r2s[i, pl.ds(me % 2, 8)].reshape(4, 2, n, lanes).sum(1), i * 4 * n)
            for i in range(2)
        ]
        b3 = dot(jnp.concatenate(pairs, 1), down_3).reshape(4, n // 2, lanes)
        first = (me + 4 + me % 2) // 2
        return b2, sum(jnp.where(lane // GROUP == (first + q) % groups, b3[q], 0.0) for q in range(4))

    def side_by_side(b2):
        return b2[1] + (pltpu.roll(b2[0], GROUP, 1) + pltpu.roll(b2[2], 2 * GROUP, 1))

    def level_2(t, c3, i2, a2, a3):
        b = jnp.where(valid(me - 6, 13, parts), bw[t], 0.0)
        b2 = b[1:-1] + (pltpu.roll(b[2:], lanes - GROUP, 2) + pltpu.roll(b[:-2], lanes - 2 * GROUP, 2))
        c2 = b2 * i2
        y2 = 1.2 * c2[1:-1] + a2 * sum_planes(c2)[1:-1]
        c2 = c2[1:-1]
        y2 = ((0.2 * y2 + c2) + a2 * sum_planes(y2))[1:-1]
        y3 = dot(flat(coarse_solve(c3, a3)), up_3)
        for g in range(groups):
            y3s[2 + 4 * g:6 + 4 * g] = y3[:, 2 * g * lanes:2 * (g + 1) * lanes].reshape(4, rows // 8, 2 * lanes)
        lift, sides = [
            jnp.where(me % 2 == 1, x[1:], x[:-1]) for x in
            [twice_planes(x) for x in twice_rows(y3s[pl.ds(me // 2, 5)].reshape(5 * rows // 8, 2 * lanes), 5)]
        ]
        total = (sides + up_down(lift))[1:-1] + (lift[:-2] + lift[2:])
        y2 = y2 + (0.2 * lift[1:-1] + a2[1:-1] * total)
        y2 = ((0.2 * y2 + c2[1:-1]) + a2[1:-1] * sum_planes(y2))[1:-1]
        return twice_rows(dot(flat(y2), up_2), 5)

    def swept_1(y1, lift, sides, a1):
        before, after = shifted(lift)
        across = lift + jnp.where(iota(lift.shape, 2) < half, before, after)
        return y1 + (0.2 * lift + a1 * ((sides + up_down(lift)) + across))

    def lift_0(y1, skip):
        n = rows // 2
        around = flat(y1)
        both = dot(around, up_lo), dot(around, up_hi)
        halves = [part[n * k:n * k + n] for k in range(3) for part in both]
        halves = halves[skip:len(halves) - skip]
        return [twice_planes(x) for x in twice_rows(jnp.concatenate(halves, 0), len(halves))]

    def swept_0(lift, sides, a):
        total = (sides + up_down(lift))[1:-1] + (lift[:-2] + lift[2:])
        return 0.2 * lift[1:-1] + a * total

    arrive(near)
    x, b1 = first_sweeps(own[...], planes_of(c0, d + 1, d - 1, d + 4), a)
    arrive(cap_window[0], cap2_window[0])
    d1, i1 = inverse_1(1, 4)
    d2, i2 = inverse_2(3, 8)
    near_1 = i1, d1, 0.5 * i1, i2, d2, 0.25 * i2
    c1 = b1 * i1[1]
    vw[0, 3] = c1
    b2, b3 = spread(b1, c1, *near_1)
    gr[0, me] = b3 + cap_sent
    bw[0, 6] = side_by_side(b2)
    pl.semaphore_wait(far_sem, 2)
    begin(gather_r[0])
    begin(b_window[0])
    begin(c_window[0])
    arrive(cap_far)
    begin(pass_far)
    arrive(cap_window[1])
    begin(pass_window)
    arrive(far)
    arrive(pass_far)
    wide = weights(1, 3 * d - 2)
    c = planes_of(c0, d + 1, d - 2, d + 6)
    first = 1.2 * c[1:2] + wide[1:2] * sum_inner(c[0:3], lanes)
    final = 1.2 * c[-2:-1] + wide[-2:-1] * sum_inner(c[-3:], lanes)

    def last_sweeps(x, c):
        x = (0.2 * x[1:-1] + c) + a * sum_inner(x, lanes)
        return (0.2 * x[1:-1] + c[1:-1]) + a[1:-1] * sum_inner(x, lanes)

    alone = last_sweeps(jnp.concatenate([first, x, final], 0), c[2:-2])
    fp_ref[...] = alone
    src1[2:d + 2] = cap[d:2 * d] * alone + src1[2:d + 2]
    begin(known)
    arrive(pass_window)
    a1 = 0.5 * inverse_1(0, 5)[1]
    arrive(cap2_window[1])
    i2 = inverse_2(0, 11)[1]
    a2 = 0.25 * i2[1:-1]
    arrive(gather_r[0], b_window[0], c_window[0])

    got = gr[0]
    cap3 = capacity_3(got)
    i3 = jnp.where(iota(cap3.shape, 2) % GROUP < GROUP // 2, W / (cap3 + 0.75), 0.0)
    a3 = 0.125 * i3
    c1 = jnp.where(valid(me - 3, 7, parts), vw[0], 0.0)
    y1 = 1.2 * c1[1:-1] + a1 * sum_packed(c1, half)[1:-1]
    c1 = c1[1:-1]
    y1 = (0.2 * y1 + c1) + a1 * sum_packed(y1, half)
    y1 = swept_1(y1, *level_2(0, level_3(got) * i3, i2, a2, a3), a1)
    y1 = ((0.2 * y1 + c1) + a1 * sum_packed(y1, half))[1:-1]
    x = swept_0(*lift_0(y1, 0), wide)
    x = 0.2 * x[1:-1] + wide[1:-1] * sum_inner(x, lanes)
    fp_ref[...] = fp_ref[...] + x[2:-2]
    arrive(known)
    b = cap[2:3 * d - 2] * x + src1[...]
    c1x[1:d + 5] = b * wide[1:-1]
    begin(third)

    x, b1 = first_sweeps(b[2:-2], c1x[1:d + 5], a)
    c1 = b1 * i1[1]
    c_sent[...] = c1
    b2, b3 = spread(b1, c1, *near_1)
    r_sent[...] = b3
    b_sent[...] = side_by_side(b2)

    @pl.when(span < spans - 1)
    def _():
        begin(gather_r[1])
        begin(b_window[1])
        begin(c_window[1])

    arrive(third)
    c = planes_of(c1x, 3, 0, d + 6)
    first = 1.2 * c[1:2] + wide[1:2] * sum_inner(c[0:3], lanes)
    final = 1.2 * c[-2:-1] + wide[-2:-1] * sum_inner(c[-3:], lanes)
    fin[0] = last_sweeps(jnp.concatenate([first, x, final], 0), c[2:-2])

    @pl.when(span < spans - 1)
    def _():
        begin(fin_onward)

    sent(own_span)

    @pl.when(span == 0)
    def _():
        up_ref[...] = u0[...]

    @pl.when(span > 0)
    def _():
        arrive(gather_r[1], b_window[1], c_window[1], fin_onward)
        c1 = jnp.where(valid(me - 2, 5, parts), vw[1, 1:6], 0.0)
        y1 = 1.2 * c1 + a1 * sum_packed(c1, half)
        y1 = (0.2 * y1 + c1) + a1 * sum_packed(y1, half)
        y1 = swept_1(y1, *level_2(1, level_3(gr[1]) * i3, i2, a2, a3), a1)[1:-1]
        y1 = (0.2 * y1 + c1[1:-1]) + a1[1:-1] * sum_packed(y1, half)
        x = swept_0(*lift_0(y1, 1), a)
        up_ref[...] = fin[1] + (0.2 * x[1:-1] + a[1:-1] * sum_inner(x, lanes))

    @pl.when(span < spans - 1)
    def _():
        sent(next_span)


def shards(span_opening, source_power, warmth_retention):
    parts, spans = lax.axis_size("space"), lax.axis_size("tm")
    steps = source_power.shape[1]
    depth, rows, lanes = warmth_retention.shape
    assert steps == 2 and depth == 4
    slab = jax.ShapeDtypeStruct((depth, rows, lanes), F32)
    vmem = pl.BlockSpec(memory_space=pltpu.VMEM)
    dma = pltpu.SemaphoreType.DMA
    fpoint, updated = pl.pallas_call(
        functools.partial(kernel, parts, spans, steps),
        out_shape=(pltpu.VMEM(slab.shape, F32),) * 2,
        in_specs=[pl.BlockSpec(memory_space=pl.ANY)] * 3,
        out_specs=(vmem, vmem),
        scratch_shapes=[
            pltpu.VMEM((depth, rows, lanes), F32),
            pltpu.VMEM((depth, rows, lanes), F32),
            pltpu.VMEM((depth + 4, rows, lanes), F32),
            pltpu.VMEM((3 * depth, rows, lanes), F32),
            pltpu.VMEM((3 * depth + 2, rows, lanes), F32),
            pltpu.VMEM((depth + 6, rows, lanes), F32),
            pltpu.VMEM((5, rows // 2, lanes), F32),
            pltpu.VMEM((11, rows // 8, lanes), F32),
            pltpu.VMEM((steps, 7, rows // 2, lanes), F32),
            pltpu.VMEM((rows // 2, lanes), F32),
            pltpu.VMEM((steps, 13, rows // 4, lanes), F32),
            pltpu.VMEM((rows // 4, lanes), F32),
            pltpu.VMEM((steps, parts, rows // 8, lanes), F32),
            pltpu.VMEM((rows // 8, lanes), F32),
            pltpu.VMEM((2, 9, rows // 4, lanes), F32),
            pltpu.VMEM((parts // 2 + 4, rows // 8, 2 * lanes), F32),
            pltpu.VMEM((depth, rows, lanes), F32),
            pltpu.VMEM((12 * rows, lanes), F32),
            pltpu.VMEM((2, depth, rows, lanes), F32),
            pltpu.VMEM((2048, lanes), F32),
            pltpu.SemaphoreType.REGULAR,
            pltpu.SemaphoreType.REGULAR,
            dma((2,)), dma((2,)), dma((13,)),
        ],
        compiler_params=pltpu.CompilerParams(
            collective_id=0, has_side_effects=True, vmem_limit_bytes=67043328 - 2 * 4 * slab.size
        ),
    )(span_opening[0], source_power[0], warmth_retention)
    flag = lax.axis_index("tm") > spans
    fpoint, updated = jnp.where(flag, updated, fpoint), jnp.where(flag, fpoint, updated)
    return fpoint[None], updated[None]


def solution(mesh):
    in_specs = (
        P("tm", "space", None, None),
        P("tm", None, "space", None, None),
        P("space", None, None),
    )
    out_specs = (P("tm", "space", None, None), P("tm", "space", None, None))
    return jax.shard_map(shards, mesh=mesh, in_specs=in_specs, out_specs=out_specs, check_vma=False)
```

```python
import functools
import math

import jax
import jax.numpy as jnp
from jax import lax
from jax.experimental import pallas as pl
from jax.experimental.pallas import tpu as pltpu
from jax.sharding import PartitionSpec as P

COARSE_SWEEPS = 24
W = 0.8
GROUP = 32
NEAR = 4
F32 = jnp.float32
MESH = pl.DeviceIdType.MESH


def iota(shape, dim):
    return lax.broadcasted_iota(jnp.int32, shape, dim)


def dot(a, b):
    total = None
    for _ in range(2):
        part = a.astype(jnp.bfloat16)
        a = a - part.astype(F32)
        term = jnp.dot(part, b, preferred_element_type=F32)
        total = term if total is None else total + term
    return total


def picks(lanes, pick, scale):
    src, dst = iota((lanes, lanes), 0), iota((lanes, lanes), 1)
    return jnp.where(pick(src, dst), scale, 0.0).astype(jnp.bfloat16)


def from_sides(lanes, pick, width, scale):
    def shifted_pick(by):
        return picks(lanes, lambda s, d: (s % width + by >= 0) & (s % width + by < width) & pick(s + by, d), scale)

    return shifted_pick(-1) + shifted_pick(1)


def to_sides(lanes, pick, width):
    def shifted_pick(by):
        return picks(lanes, lambda s, d: (d % width + by >= 0) & (d % width + by < width) & pick(s, d + by), 1.0)

    return shifted_pick(-1) + shifted_pick(1)


def up_down(x):
    rows = x.shape[1]
    row = iota(x.shape, 1)
    up = jnp.where(row == 0, 0.0, pltpu.roll(x, 1, 1))
    return up + jnp.where(row == rows - 1, 0.0, pltpu.roll(x, rows - 1, 1))


def in_plane(x, width):
    lanes = x.shape[2]
    lane = iota(x.shape, 2)
    left, right = pltpu.roll(x, 1, 2), pltpu.roll(x, lanes - 1, 2)
    if width:
        left = jnp.where(lane % width == 0, 0.0, left)
        right = jnp.where(lane % width == width - 1, 0.0, right)
    return (left + right) + up_down(x)


def shifted(x):
    zero = jnp.zeros((1,) + x.shape[1:], F32)
    return jnp.concatenate([zero, x[:-1]], 0), jnp.concatenate([x[1:], zero], 0)


def earlier(x, by=1, shift=0):
    lanes = x.shape[2]
    moved = pltpu.roll(x[-by:], (GROUP + shift) % lanes, 2)
    return jnp.where(iota(moved.shape, 2) < GROUP, 0.0, moved)


def later(x, by=1, shift=0):
    lanes = x.shape[2]
    moved = pltpu.roll(x[:by], (lanes - GROUP + shift) % lanes, 2)
    return jnp.where(iota(moved.shape, 2) >= lanes - GROUP, 0.0, moved)


def sum_grouped(x):
    ends = jnp.concatenate([earlier(x), x, later(x)], 0)
    return in_plane(x, GROUP) + (ends[:-2] + ends[2:])


def sum_planes(x):
    before, after = shifted(x)
    return in_plane(x, None) + (before + after)


def plane_padded(x, by):
    zero = jnp.zeros((by,) + x.shape[1:], F32)
    return jnp.concatenate([zero, x, zero], 0)


def sum_packed(x, width):
    half = pltpu.roll(x, width, 2)
    before, after = shifted(half)
    return in_plane(x, width) + (half + jnp.where(iota(x.shape, 2) < width, before, after))


def sum_inner(x, width):
    return in_plane(x[1:-1], width) + (x[:-2] + x[2:])


def column_sum(x):
    rows = x.shape[1]
    mid = x[1:-1]
    row = iota(mid.shape, 1)
    up = jnp.where(row == 0, 0.0, pltpu.roll(mid, 1, 1))
    down = jnp.where(row == rows - 1, 0.0, pltpu.roll(mid, rows - 1, 1))
    return (x[:-2] + x[2:]) + (up + down)


def coarse_solve(c, a):
    n, lanes = c.shape[0], c.shape[2]

    def turned(x, by):
        return x if by == 0 else pltpu.roll(x, by % lanes, 2)

    def longer(x, by, reach=1):
        return jnp.concatenate([earlier(x, reach, by), turned(x, by), later(x, reach, by)], 0)

    c_at, a_at = [[longer(x, 0) if by == 0 else turned(x, by) for by in (1, 0, -1)] for x in (c, a)]

    def sweep(y, side, c, a):
        return (0.2 * y[1:-1] + c) + a * (side + column_sum(y))

    def two_sweeps(_, y):
        left, mid, right = longer(y, 1), longer(y, 0, 2), longer(y, -1)
        once_left = sweep(left, turned(y, 2) + y, c_at[0], a_at[0])
        once_mid = sweep(mid, left + right, c_at[1], a_at[1])
        once_right = sweep(right, y + turned(y, -2), c_at[2], a_at[2])
        return sweep(once_mid, once_left + once_right, c, a)

    left = COARSE_SWEEPS - 1
    y = c
    if left % 2:
        y = 1.2 * c + a * sum_grouped(c)
    return lax.fori_loop(0, left // 2, two_sweeps, y, unroll=True)


def flat(x):
    return x.reshape(x.shape[0] * x.shape[1], x.shape[2])


def kernel(
    parts, spans, steps,
    open_ref, src_ref, cap_in,
    fp_ref, up_ref,
    u0, src0, src1, cap, c0, c1x, cw, kw, vw, c_sent, bw, b_sent, gr, r_sent, r2s, y3s, own, tmp, fin, spare,
    near_sem, far_sem, in_sem, send_sem, recv_sem,
):
    me, span = lax.axis_index("space"), lax.axis_index("tm")
    depth, rows, lanes = open_ref.shape
    half = lanes // 2
    groups = lanes // GROUP
    assert parts == 32 and lanes == 128 and rows == 64
    assert parts == 8 * NEAR
    close = [k for k in range(-NEAR, NEAR + 1) if k]

    loads = [
        pltpu.make_async_copy(cap_in, cap.at[pl.ds(depth, depth)], in_sem.at[0]),
        pltpu.make_async_copy(open_ref, u0, in_sem.at[0]),
        pltpu.make_async_copy(src_ref.at[0], src0, in_sem.at[0]),
        pltpu.make_async_copy(src_ref.at[1], src1.at[pl.ds(2, depth)], in_sem.at[1]),
    ]
    for load in loads:
        load.start()
    barrier = pltpu.get_barrier_semaphore()
    for k in close:
        pl.semaphore_signal(barrier, inc=1, device_id={"space": lax.rem(me + k % parts, parts)}, device_id_type=MESH)
    for k in (1, spans - 1):
        pl.semaphore_signal(barrier, inc=1, device_id={"tm": lax.rem(span + k, spans)}, device_id_type=MESH)

    r2s[...] = jnp.zeros(r2s.shape, F32)
    y3s[...] = jnp.zeros(y3s.shape, F32)

    def pick_lo(s, d):
        return (s // 2 == d) & (d < half)

    def pick_hi(s, d):
        return s // 2 + half == d

    def pick_2(s, d):
        return (s % half) // 2 == d

    def pick_3(s, d):
        return (s < GROUP) & (d % GROUP == s // 2)

    def swap(pick):
        return lambda s, d: pick(d, s)

    down_0 = jnp.concatenate([
        picks(lanes, pick_lo, 0.125), from_sides(lanes, pick_lo, lanes, 0.125),
        picks(lanes, pick_hi, 0.125), from_sides(lanes, pick_hi, lanes, 0.125),
    ], 0)
    down_cap1 = jnp.concatenate([picks(lanes, pick_lo, 0.125), picks(lanes, pick_hi, 0.125)], 0)
    down_2 = picks(lanes, pick_2, 0.125)
    down_1 = jnp.concatenate([
        down_2, from_sides(lanes, pick_2, half, 0.0625) + picks(lanes, pick_2, 0.0625),
        picks(lanes, lambda s, d: pick_2(s, d) & (s >= half), 0.0625),
        picks(lanes, lambda s, d: pick_2(s, d) & (s < half), 0.0625),
    ], 0)
    down_3 = jnp.concatenate([picks(lanes, pick_3, 0.125), from_sides(lanes, pick_3, GROUP, 0.03125)], 0)
    down_cap = picks(lanes, lambda s, d: (s < GROUP) & (d % GROUP == s // 2 + GROUP // 2), 0.125)
    def rises(pick, width):
        return [picks(lanes, pick, 1.0), to_sides(lanes, pick, width)]

    up_lo = jnp.concatenate(rises(lambda s, d: d // 2 == s, lanes), 1)
    up_hi = jnp.concatenate(rises(lambda s, d: d // 2 + half == s, lanes), 1)
    up_2 = jnp.concatenate(rises(swap(pick_2), half), 1)
    up_3 = jnp.concatenate([
        rise for g in range(groups)
        for rise in rises(lambda s, d: (d < GROUP) & (d // 2 + g * GROUP == s), GROUP)
    ], 1)

    def pair_rows(x, at=0):
        n, r, w = x.shape
        tmp[pl.ds(at, n * r), :] = flat(x)
        return tmp[pl.ds(at, n * r // 2, 2), :] + tmp[pl.ds(at + 1, n * r // 2, 2), :]

    def twice_rows(x, planes):
        parts_of = [x[:, at:at + lanes] for at in range(0, x.shape[1], lanes)]
        x = jnp.concatenate(parts_of, 0)
        r = x.shape[0]
        tmp[pl.ds(0, r, 2), :] = x
        tmp[pl.ds(1, r, 2), :] = x
        out = tmp[pl.ds(0, 2 * r), :].reshape(len(parts_of) * planes, -1, lanes)
        return [out[at:at + planes] for at in range(0, out.shape[0], planes)]

    def twice_planes(x):
        return jnp.broadcast_to(x[:, None], (x.shape[0], 2) + x.shape[1:]).reshape((2 * x.shape[0],) + x.shape[1:])

    def slab_pairs(x, at=0):
        s = pair_rows(x.reshape(depth // 2, 2, rows, lanes).sum(1), at)
        return s[:rows // 2], s[rows // 2:]

    def to_2(x):
        return dot(pair_rows(x), down_2).reshape(x.shape[0], rows // 4, lanes)

    lane = iota((rows // 8, lanes), 1)

    def turn(planes, off):
        out = []
        for k in range(groups):
            total = None
            for g in range(groups):
                by = (GROUP * (g - k) - off) % lanes
                moved = pltpu.roll(planes[g], by, 1) if by else planes[g]
                total = moved if total is None else jnp.where(lane // GROUP == g, moved, total)
            out.append(total[None])
        return jnp.concatenate(out, 0)

    def level_3(got):
        pairs = [got[0]] + [got[2 * i - 1] + got[2 * i] for i in range(1, parts // 2)] + [got[parts - 1]]
        out = []
        for k in range(groups):
            total = pairs[4 * k + 2]
            for i, keep in (
                (4 * k - 1, lane < GROUP), (4 * k, lane < 2 * GROUP), (4 * k + 1, lane < 3 * GROUP),
                (4 * k + 3, lane >= GROUP), (4 * k + 4, lane >= 2 * GROUP), (4 * k + 5, lane >= 3 * GROUP),
            ):
                if 0 <= i < len(pairs):
                    total = total + jnp.where(keep, pairs[i], 0.0)
            out.append(total)
        return turn(out, 0)

    def capacity_3(got):
        out = []
        for k in range(groups):
            total = None
            for g in range(groups):
                i = 2 * (4 * k + g)
                pair = got[i] + got[i + 1]
                total = pair if total is None else jnp.where(lane // GROUP == g, pair, total)
            out.append(total)
        return turn(out, GROUP // 2)

    def valid(start, count, of):
        at = start + iota((count, 1, 1), 0)
        return (at >= 0) & (at < of)

    own_span, next_span = 0, 1
    sent_rows, groups_of = [0, 0], {}

    def batch(pieces, total, group=None, side=own_span):
        at = groups_of.setdefault(group or len(groups_of), len(groups_of))
        count = total.size // lanes if hasattr(total, "size") else math.prod(total.shape) // lanes
        sent_rows[side] += count
        return [
            pltpu.make_async_remote_copy(
                source, target, send_sem.at[side], recv_sem.at[at], device_id=to, device_id_type=MESH)
            for source, target, to in pieces
        ], count, at, side

    def waiting(count, at, side):
        rows_of = spare.at[pl.ds(0, count)]
        return pltpu.make_async_remote_copy(
            rows_of, rows_of, send_sem.at[side], recv_sem.at[at], device_id=beside(1), device_id_type=MESH)

    def begin(made):
        for copy in made[0]:
            copy.start()

    def arrive(*made):
        assert len({one[2] for one in made}) == 1
        waiting(sum(one[1] for one in made), *made[0][2:]).wait_recv()

    def sent(side):
        waiting(sent_rows[side], 0, side).wait_send()

    def beside(k):
        return {"space": lax.rem(me + (k + parts) % parts, parts)}

    share = rows // 2
    my_rows = pl.ds(pl.multiple_of(span % 2 * share, share), share)

    def halo(buf, count, up, down, rows_at=None, group=None):
        def part(start):
            return buf.at[pl.ds(start, count)] if rows_at is None else buf.at[pl.ds(start, count), rows_at]

        total = buf.at[pl.ds(0, 2 * count)] if rows_at is None else buf.at[pl.ds(0, 2 * count), pl.ds(0, share)]
        return batch([(part(way[0]), part(way[1]), beside(k)) for way, k in ((up, 1), (down, -1))], total, group)

    def window(buf, source, nearest, reach, to={}, group=None, side=own_span):
        middle = buf.shape[0] // 2
        offsets = [k for far in range(reach, nearest - 1, -1) for k in ((far, -far) if far else (0,))]
        return batch([(source, buf.at[middle - k], {**beside(k), **to}) for k in offsets], buf.at[pl.ds(0, len(offsets))], group, side)

    def hops(k):
        z, y = k // 4, k % 4
        return min(z, parts // 4 - z) + min(y, 4 - y)

    def gather(buf, source, offsets, to={}, group=None, side=own_span):
        offsets = sorted(offsets, key=lambda k: -hops(k))
        return batch([(source, buf.at[me], {**beside(k), **to}) for k in offsets], buf.at[pl.ds(0, len(offsets))], group, side)

    d = depth
    onward = {"tm": (span + 1) % spans}
    near = halo(c0, 2, (2 * d - 1, d - 1), (d + 1, 2 * d + 1), group="near")
    far = halo(c0, 1, (2 * d - 2, d - 2), (d + 3, 2 * d + 3))
    known = halo(src1, 2, (d, 0), (2, d + 2))
    third = halo(c1x, 1, (d, 0), (5, d + 5))
    cap_near = halo(cap, 1, (2 * d - 1, d - 1), (d, 2 * d), group="near")
    cap_far = halo(cap, 2, (d + 1, 1), (d + 1, 2 * d + 1), my_rows)
    pass_far = batch(
        [
            (cap.at[pl.ds(start, 2), my_rows], cap.at[pl.ds(start, 2), my_rows], {"tm": span + 1 - 2 * (span % 2)})
            for start in (1, 2 * d + 1)
        ], cap.at[pl.ds(0, 4), pl.ds(0, share)])
    half_block = pl.ds(pl.multiple_of(span % 2 * (share // 2), share // 2), share // 2)
    half_total = cw.at[pl.ds(0, 2), pl.ds(0, share // 2)]
    cap_window = window(cw, cw.at[2], 1, 1, group="first"), batch(
        [(cw.at[2, half_block], cw.at[2 - k, half_block], beside(k)) for k in (2, -2)], half_total)
    pass_window = batch(
        [(cw.at[i, half_block], cw.at[i, half_block], {"tm": span + 1 - 2 * (span % 2)}) for i in (0, 4)], half_total)
    cap2_window = window(kw, kw.at[5], 1, 2, group="first"), window(kw, kw.at[5], 3, 5)
    to_next = {"to": onward, "group": "next", "side": next_span}
    gather_r = gather(gr.at[0], gr.at[0, me], range(1, parts), group="own"), gather(gr.at[1], r_sent, range(parts), **to_next)
    c_window = window(vw.at[0], vw.at[0, 3], 1, 3, group="own"), window(vw.at[1], c_sent, 0, 2, **to_next)
    b_window = window(bw.at[0], bw.at[0, 6], 1, 6, group="own"), window(bw.at[1], b_sent, 0, 6, **to_next)
    fin_onward = batch([(fin.at[0], fin.at[1], onward)], fin.at[0], "next", next_span)

    loaded = spare.at[pl.ds(0, 3 * depth * rows)]
    pltpu.make_async_copy(loaded, loaded, in_sem.at[0]).wait()
    mine = cap[d:2 * d]
    b = mine * u0[...] + src0[...]
    own[...] = b
    c0[d + 1:2 * d + 1] = b * (W / (mine + 6.0))

    pl.semaphore_wait(barrier, len(close) + 2)
    begin(near)
    begin(cap_near)
    for k in (NEAR, -NEAR):
        pl.semaphore_signal(near_sem, inc=1, device_id=beside(k), device_id_type=MESH)
    cap1 = dot(jnp.concatenate(slab_pairs(mine), 1), down_cap1)
    cw[2] = cap1
    begin(cap_window[0])
    cap2 = to_2(cap1[None])
    kw[5] = cap2[0, :rows // 8] + pltpu.roll(cap2[0, rows // 8:], GROUP, 1)
    begin(cap2_window[0])
    begin(cap_far)
    begin(cap_window[1])
    begin(far)
    pl.semaphore_wait(near_sem, 2)
    for k in (2 * NEAR, -2 * NEAR):
        pl.semaphore_signal(far_sem, inc=1, device_id=beside(k), device_id_type=MESH)
    begin(cap2_window[1])
    cap_sent = dot(pair_rows(cap2), down_cap)
    loads[3].wait()

    def weights(start, count):
        inside = valid((me - 1) * depth + start, count, parts * depth)
        return jnp.where(inside, W / (cap[start:start + count] + 6.0), 0.0)

    def inverse(diagonal, start, reach):
        return jnp.where(valid(me - reach + start, diagonal.shape[0], parts), W / diagonal, 0.0)

    def planes_of(buf, own, start, count):
        return jnp.where(valid(me * depth + start - own, count, parts * depth), buf[start:start + count], 0.0)

    def inverse_1(start, stop):
        diagonal = cw[start:stop] + 3.0
        return diagonal, inverse(diagonal, start, 2)

    def inverse_2(start, stop):
        packed = kw[start:stop]
        diagonal = jnp.concatenate([packed, pltpu.roll(packed, lanes - GROUP, 2)], 1) + 1.5
        return diagonal, jnp.where(iota(diagonal.shape, 2) < GROUP, inverse(diagonal, start, 5), 0.0)

    arrive(cap_near, near)
    a = weights(d - 1, d + 2)

    assert len(groups_of) == 12 and max(sent_rows) <= spare.shape[0]

    def first_sweeps(b, c, a):
        x = 1.2 * c[1:-1] + a * sum_inner(c, lanes)
        inner = x[1:-1]
        r = b - (cap[d:2 * d] + 6.0) * inner + up_down(inner) + (x[:-2] + x[2:])
        (r_lo, r_hi), (x_lo, x_hi) = slab_pairs(r), slab_pairs(inner, depth * rows // 2)
        return x, dot(jnp.concatenate([r_lo, x_lo, r_hi, x_hi], 1), down_0)

    def spread(b1, c1, i1, d1, a1, i2, d2, a2):
        c1 = plane_padded(c1[None], 1)
        y1 = 1.2 * c1 + a1 * sum_packed(c1, half)
        r1 = pair_rows(plane_padded(b1[None], 1) - d1 * y1 + 0.5 * up_down(y1))
        y1 = pair_rows(y1, 3 * rows // 2)
        n = rows // 4
        none = jnp.zeros((n, lanes), F32)
        around = jnp.concatenate([none, y1[:-n]], 0), jnp.concatenate([y1[n:], none], 0)
        b2 = dot(jnp.concatenate([r1, y1, *around], 1), down_1).reshape(3, n, lanes)
        c2 = plane_padded(b2 * i2[1:4], 1)
        y2 = 1.2 * c2 + a2 * sum_planes(c2)
        r2 = plane_padded(b2, 2) - plane_padded(d2 * y2, 1)
        y2 = plane_padded(y2, 1)
        before, after = shifted(y2)
        r2s[0, 1:8] = r2 + 0.25 * (up_down(y2) + (before + after))
        r2s[1, 1:8] = y2
        pairs = [
            pair_rows(r2s[i, pl.ds(me % 2, 8)].reshape(4, 2, n, lanes).sum(1), i * 4 * n)
            for i in range(2)
        ]
        b3 = dot(jnp.concatenate(pairs, 1), down_3).reshape(4, n // 2, lanes)
        first = (me + 4 + me % 2) // 2
        return b2, sum(jnp.where(lane // GROUP == (first + q) % groups, b3[q], 0.0) for q in range(4))

    def side_by_side(b2):
        return b2[1] + (pltpu.roll(b2[0], GROUP, 1) + pltpu.roll(b2[2], 2 * GROUP, 1))

    def level_2(t, c3, i2, a2, a3):
        b = jnp.where(valid(me - 6, 13, parts), bw[t], 0.0)
        b2 = b[1:-1] + (pltpu.roll(b[2:], lanes - GROUP, 2) + pltpu.roll(b[:-2], lanes - 2 * GROUP, 2))
        c2 = b2 * i2
        y2 = 1.2 * c2[1:-1] + a2 * sum_planes(c2)[1:-1]
        c2 = c2[1:-1]
        y2 = ((0.2 * y2 + c2) + a2 * sum_planes(y2))[1:-1]
        y3 = dot(flat(coarse_solve(c3, a3)), up_3)
        for g in range(groups):
            y3s[2 + 4 * g:6 + 4 * g] = y3[:, 2 * g * lanes:2 * (g + 1) * lanes].reshape(4, rows // 8, 2 * lanes)
        lift, sides = [
            jnp.where(me % 2 == 1, x[1:], x[:-1]) for x in
            [twice_planes(x) for x in twice_rows(y3s[pl.ds(me // 2, 5)].reshape(5 * rows // 8, 2 * lanes), 5)]
        ]
        total = (sides + up_down(lift))[1:-1] + (lift[:-2] + lift[2:])
        y2 = y2 + (0.2 * lift[1:-1] + a2[1:-1] * total)
        y2 = ((0.2 * y2 + c2[1:-1]) + a2[1:-1] * sum_planes(y2))[1:-1]
        return twice_rows(dot(flat(y2), up_2), 5)

    def swept_1(y1, lift, sides, a1):
        before, after = shifted(lift)
        across = lift + jnp.where(iota(lift.shape, 2) < half, before, after)
        return y1 + (0.2 * lift + a1 * ((sides + up_down(lift)) + across))

    def lift_0(y1, skip):
        n = rows // 2
        around = flat(y1)
        both = dot(around, up_lo), dot(around, up_hi)
        halves = [part[n * k:n * k + n] for k in range(3) for part in both]
        halves = halves[skip:len(halves) - skip]
        return [twice_planes(x) for x in twice_rows(jnp.concatenate(halves, 0), len(halves))]

    def swept_0(lift, sides, a):
        total = (sides + up_down(lift))[1:-1] + (lift[:-2] + lift[2:])
        return 0.2 * lift[1:-1] + a * total

    x, b1 = first_sweeps(own[...], planes_of(c0, d + 1, d - 1, d + 4), a)
    arrive(cap_window[0], cap2_window[0])
    d1, i1 = inverse_1(1, 4)
    d2, i2 = inverse_2(3, 8)
    near_1 = i1, d1, 0.5 * i1, i2, d2, 0.25 * i2
    c1 = b1 * i1[1]
    vw[0, 3] = c1
    b2, b3 = spread(b1, c1, *near_1)
    gr[0, me] = b3 + cap_sent
    bw[0, 6] = side_by_side(b2)
    pl.semaphore_wait(far_sem, 2)
    begin(gather_r[0])
    begin(b_window[0])
    begin(c_window[0])
    arrive(cap_far)
    begin(pass_far)
    arrive(cap_window[1])
    begin(pass_window)
    arrive(far)
    arrive(pass_far)
    wide = weights(1, 3 * d - 2)
    c = planes_of(c0, d + 1, d - 2, d + 6)
    first = 1.2 * c[1:2] + wide[1:2] * sum_inner(c[0:3], lanes)
    final = 1.2 * c[-2:-1] + wide[-2:-1] * sum_inner(c[-3:], lanes)

    def last_sweeps(x, c):
        x = (0.2 * x[1:-1] + c) + a * sum_inner(x, lanes)
        return (0.2 * x[1:-1] + c[1:-1]) + a[1:-1] * sum_inner(x, lanes)

    alone = last_sweeps(jnp.concatenate([first, x, final], 0), c[2:-2])
    fp_ref[...] = alone
    src1[2:d + 2] = cap[d:2 * d] * alone + src1[2:d + 2]
    begin(known)
    arrive(pass_window)
    a1 = 0.5 * inverse_1(0, 5)[1]
    arrive(cap2_window[1])
    i2 = inverse_2(0, 11)[1]
    a2 = 0.25 * i2[1:-1]
    arrive(gather_r[0], b_window[0], c_window[0])

    got = gr[0]
    cap3 = capacity_3(got)
    i3 = jnp.where(iota(cap3.shape, 2) % GROUP < GROUP // 2, W / (cap3 + 0.75), 0.0)
    a3 = 0.125 * i3
    c1 = jnp.where(valid(me - 3, 7, parts), vw[0], 0.0)
    y1 = 1.2 * c1[1:-1] + a1 * sum_packed(c1, half)[1:-1]
    c1 = c1[1:-1]
    y1 = (0.2 * y1 + c1) + a1 * sum_packed(y1, half)
    y1 = swept_1(y1, *level_2(0, level_3(got) * i3, i2, a2, a3), a1)
    y1 = ((0.2 * y1 + c1) + a1 * sum_packed(y1, half))[1:-1]
    x = swept_0(*lift_0(y1, 0), wide)
    x = 0.2 * x[1:-1] + wide[1:-1] * sum_inner(x, lanes)
    fp_ref[...] = fp_ref[...] + x[2:-2]
    arrive(known)
    b = cap[2:3 * d - 2] * x + src1[...]
    c1x[1:d + 5] = b * wide[1:-1]
    begin(third)

    x, b1 = first_sweeps(b[2:-2], c1x[1:d + 5], a)
    c1 = b1 * i1[1]
    c_sent[...] = c1
    b2, b3 = spread(b1, c1, *near_1)
    r_sent[...] = b3
    b_sent[...] = side_by_side(b2)

    @pl.when(span < spans - 1)
    def _():
        begin(gather_r[1])
        begin(b_window[1])
        begin(c_window[1])

    arrive(third)
    c = planes_of(c1x, 3, 0, d + 6)
    first = 1.2 * c[1:2] + wide[1:2] * sum_inner(c[0:3], lanes)
    final = 1.2 * c[-2:-1] + wide[-2:-1] * sum_inner(c[-3:], lanes)
    fin[0] = last_sweeps(jnp.concatenate([first, x, final], 0), c[2:-2])

    @pl.when(span < spans - 1)
    def _():
        begin(fin_onward)

    sent(own_span)

    @pl.when(span == 0)
    def _():
        up_ref[...] = u0[...]

    @pl.when(span > 0)
    def _():
        arrive(gather_r[1], b_window[1], c_window[1], fin_onward)
        c1 = jnp.where(valid(me - 2, 5, parts), vw[1, 1:6], 0.0)
        y1 = 1.2 * c1 + a1 * sum_packed(c1, half)
        y1 = (0.2 * y1 + c1) + a1 * sum_packed(y1, half)
        y1 = swept_1(y1, *level_2(1, level_3(gr[1]) * i3, i2, a2, a3), a1)[1:-1]
        y1 = (0.2 * y1 + c1[1:-1]) + a1[1:-1] * sum_packed(y1, half)
        x = swept_0(*lift_0(y1, 1), a)
        up_ref[...] = fin[1] + (0.2 * x[1:-1] + a[1:-1] * sum_inner(x, lanes))

    @pl.when(span < spans - 1)
    def _():
        sent(next_span)


def shards(span_opening, source_power, warmth_retention):
    parts, spans = lax.axis_size("space"), lax.axis_size("tm")
    steps = source_power.shape[1]
    depth, rows, lanes = warmth_retention.shape
    assert steps == 2 and depth == 4
    slab = jax.ShapeDtypeStruct((depth, rows, lanes), F32)
    vmem = pl.BlockSpec(memory_space=pltpu.VMEM)
    dma = pltpu.SemaphoreType.DMA
    fpoint, updated = pl.pallas_call(
        functools.partial(kernel, parts, spans, steps),
        out_shape=(pltpu.VMEM(slab.shape, F32),) * 2,
        in_specs=[pl.BlockSpec(memory_space=pl.ANY)] * 3,
        out_specs=(vmem, vmem),
        scratch_shapes=[
            pltpu.VMEM((depth, rows, lanes), F32),
            pltpu.VMEM((depth, rows, lanes), F32),
            pltpu.VMEM((depth + 4, rows, lanes), F32),
            pltpu.VMEM((3 * depth, rows, lanes), F32),
            pltpu.VMEM((3 * depth + 2, rows, lanes), F32),
            pltpu.VMEM((depth + 6, rows, lanes), F32),
            pltpu.VMEM((5, rows // 2, lanes), F32),
            pltpu.VMEM((11, rows // 8, lanes), F32),
            pltpu.VMEM((steps, 7, rows // 2, lanes), F32),
            pltpu.VMEM((rows // 2, lanes), F32),
            pltpu.VMEM((steps, 13, rows // 4, lanes), F32),
            pltpu.VMEM((rows // 4, lanes), F32),
            pltpu.VMEM((steps, parts, rows // 8, lanes), F32),
            pltpu.VMEM((rows // 8, lanes), F32),
            pltpu.VMEM((2, 9, rows // 4, lanes), F32),
            pltpu.VMEM((parts // 2 + 4, rows // 8, 2 * lanes), F32),
            pltpu.VMEM((depth, rows, lanes), F32),
            pltpu.VMEM((12 * rows, lanes), F32),
            pltpu.VMEM((2, depth, rows, lanes), F32),
            pltpu.VMEM((2048, lanes), F32),
            pltpu.SemaphoreType.REGULAR,
            pltpu.SemaphoreType.REGULAR,
            dma((2,)), dma((2,)), dma((12,)),
        ],
        compiler_params=pltpu.CompilerParams(
            collective_id=0, has_side_effects=True, vmem_limit_bytes=67043328 - 2 * 4 * slab.size
        ),
    )(span_opening[0], source_power[0], warmth_retention)
    flag = lax.axis_index("tm") > spans
    fpoint, updated = jnp.where(flag, updated, fpoint), jnp.where(flag, fpoint, updated)
    return fpoint[None], updated[None]


def solution(mesh):
    in_specs = (
        P("tm", "space", None, None),
        P("tm", None, "space", None, None),
        P("space", None, None),
    )
    out_specs = (P("tm", "space", None, None), P("tm", "space", None, None))
    return jax.shard_map(shards, mesh=mesh, in_specs=in_specs, out_specs=out_specs, check_vma=False)
```

```python
import functools
import math

import jax
import jax.numpy as jnp
from jax import lax
from jax.experimental import pallas as pl
from jax.experimental.pallas import tpu as pltpu
from jax.sharding import PartitionSpec as P

COARSE_SWEEPS = 24
W = 0.8
GROUP = 32
NEAR = 4
F32 = jnp.float32
MESH = pl.DeviceIdType.MESH


def iota(shape, dim):
    return lax.broadcasted_iota(jnp.int32, shape, dim)


def dot(a, b):
    total = None
    for _ in range(2):
        part = a.astype(jnp.bfloat16)
        a = a - part.astype(F32)
        term = jnp.dot(part, b, preferred_element_type=F32)
        total = term if total is None else total + term
    return total


def picks(lanes, pick, scale):
    src, dst = iota((lanes, lanes), 0), iota((lanes, lanes), 1)
    return jnp.where(pick(src, dst), scale, 0.0).astype(jnp.bfloat16)


def from_sides(lanes, pick, width, scale):
    def shifted_pick(by):
        return picks(lanes, lambda s, d: (s % width + by >= 0) & (s % width + by < width) & pick(s + by, d), scale)

    return shifted_pick(-1) + shifted_pick(1)


def to_sides(lanes, pick, width):
    def shifted_pick(by):
        return picks(lanes, lambda s, d: (d % width + by >= 0) & (d % width + by < width) & pick(s, d + by), 1.0)

    return shifted_pick(-1) + shifted_pick(1)


def up_down(x):
    rows = x.shape[1]
    row = iota(x.shape, 1)
    up = jnp.where(row == 0, 0.0, pltpu.roll(x, 1, 1))
    return up + jnp.where(row == rows - 1, 0.0, pltpu.roll(x, rows - 1, 1))


def in_plane(x, width):
    lanes = x.shape[2]
    lane = iota(x.shape, 2)
    left, right = pltpu.roll(x, 1, 2), pltpu.roll(x, lanes - 1, 2)
    if width:
        left = jnp.where(lane % width == 0, 0.0, left)
        right = jnp.where(lane % width == width - 1, 0.0, right)
    return (left + right) + up_down(x)


def shifted(x):
    zero = jnp.zeros((1,) + x.shape[1:], F32)
    return jnp.concatenate([zero, x[:-1]], 0), jnp.concatenate([x[1:], zero], 0)


def earlier(x, by=1, shift=0):
    lanes = x.shape[2]
    moved = pltpu.roll(x[-by:], (GROUP + shift) % lanes, 2)
    return jnp.where(iota(moved.shape, 2) < GROUP, 0.0, moved)


def later(x, by=1, shift=0):
    lanes = x.shape[2]
    moved = pltpu.roll(x[:by], (lanes - GROUP + shift) % lanes, 2)
    return jnp.where(iota(moved.shape, 2) >= lanes - GROUP, 0.0, moved)


def sum_grouped(x):
    ends = jnp.concatenate([earlier(x), x, later(x)], 0)
    return in_plane(x, GROUP) + (ends[:-2] + ends[2:])


def sum_planes(x):
    before, after = shifted(x)
    return in_plane(x, None) + (before + after)


def plane_padded(x, by):
    zero = jnp.zeros((by,) + x.shape[1:], F32)
    return jnp.concatenate([zero, x, zero], 0)


def sum_packed(x, width):
    half = pltpu.roll(x, width, 2)
    before, after = shifted(half)
    return in_plane(x, width) + (half + jnp.where(iota(x.shape, 2) < width, before, after))


def sum_inner(x, width):
    return in_plane(x[1:-1], width) + (x[:-2] + x[2:])


def column_sum(x):
    rows = x.shape[1]
    mid = x[1:-1]
    row = iota(mid.shape, 1)
    up = jnp.where(row == 0, 0.0, pltpu.roll(mid, 1, 1))
    down = jnp.where(row == rows - 1, 0.0, pltpu.roll(mid, rows - 1, 1))
    return (x[:-2] + x[2:]) + (up + down)


def coarse_solve(c, a):
    n, lanes = c.shape[0], c.shape[2]

    def turned(x, by):
        return x if by == 0 else pltpu.roll(x, by % lanes, 2)

    def longer(x, by, reach=1):
        return jnp.concatenate([earlier(x, reach, by), turned(x, by), later(x, reach, by)], 0)

    c_at, a_at = [[longer(x, 0) if by == 0 else turned(x, by) for by in (1, 0, -1)] for x in (c, a)]

    def sweep(y, side, c, a):
        return (0.2 * y[1:-1] + c) + a * (side + column_sum(y))

    def two_sweeps(_, y):
        left, mid, right = longer(y, 1), longer(y, 0, 2), longer(y, -1)
        once_left = sweep(left, turned(y, 2) + y, c_at[0], a_at[0])
        once_mid = sweep(mid, left + right, c_at[1], a_at[1])
        once_right = sweep(right, y + turned(y, -2), c_at[2], a_at[2])
        return sweep(once_mid, once_left + once_right, c, a)

    left = COARSE_SWEEPS - 1
    y = c
    if left % 2:
        y = 1.2 * c + a * sum_grouped(c)
    return lax.fori_loop(0, left // 2, two_sweeps, y, unroll=True)


def flat(x):
    return x.reshape(x.shape[0] * x.shape[1], x.shape[2])


def kernel(
    parts, spans, steps,
    open_ref, src_ref, cap_in,
    fp_ref, up_ref,
    u0, src0, src1, cap, c0, c1x, cw, kw, vw, c_sent, bw, b_sent, gr, r_sent, r2s, y3s, own, tmp, fin, spare,
    near_sem, far_sem, in_sem, send_sem, recv_sem,
):
    me, span = lax.axis_index("space"), lax.axis_index("tm")
    depth, rows, lanes = open_ref.shape
    half = lanes // 2
    groups = lanes // GROUP
    assert parts == 32 and lanes == 128 and rows == 64
    assert parts == 8 * NEAR
    close = [k for k in range(-NEAR, NEAR + 1) if k]

    loads = [
        pltpu.make_async_copy(cap_in, cap.at[pl.ds(depth, depth)], in_sem.at[0]),
        pltpu.make_async_copy(open_ref, u0, in_sem.at[0]),
        pltpu.make_async_copy(src_ref.at[0], src0, in_sem.at[0]),
        pltpu.make_async_copy(src_ref.at[1], src1.at[pl.ds(2, depth)], in_sem.at[1]),
    ]
    for load in loads:
        load.start()
    barrier = pltpu.get_barrier_semaphore()
    for k in close:
        pl.semaphore_signal(barrier, inc=1, device_id={"space": lax.rem(me + k % parts, parts)}, device_id_type=MESH)
    for k in (1, spans - 1):
        pl.semaphore_signal(barrier, inc=1, device_id={"tm": lax.rem(span + k, spans)}, device_id_type=MESH)

    r2s[...] = jnp.zeros(r2s.shape, F32)
    y3s[...] = jnp.zeros(y3s.shape, F32)

    def pick_lo(s, d):
        return (s // 2 == d) & (d < half)

    def pick_hi(s, d):
        return s // 2 + half == d

    def pick_2(s, d):
        return (s % half) // 2 == d

    def pick_3(s, d):
        return (s < GROUP) & (d % GROUP == s // 2)

    def swap(pick):
        return lambda s, d: pick(d, s)

    down_0 = jnp.concatenate([
        picks(lanes, pick_lo, 0.125), from_sides(lanes, pick_lo, lanes, 0.125),
        picks(lanes, pick_hi, 0.125), from_sides(lanes, pick_hi, lanes, 0.125),
    ], 0)
    down_cap1 = jnp.concatenate([picks(lanes, pick_lo, 0.125), picks(lanes, pick_hi, 0.125)], 0)
    down_2 = picks(lanes, pick_2, 0.125)
    down_1 = jnp.concatenate([
        down_2, from_sides(lanes, pick_2, half, 0.0625) + picks(lanes, pick_2, 0.0625),
        picks(lanes, lambda s, d: pick_2(s, d) & (s >= half), 0.0625),
        picks(lanes, lambda s, d: pick_2(s, d) & (s < half), 0.0625),
    ], 0)
    down_3 = jnp.concatenate([picks(lanes, pick_3, 0.125), from_sides(lanes, pick_3, GROUP, 0.03125)], 0)
    down_cap = picks(lanes, lambda s, d: (s < GROUP) & (d % GROUP == s // 2 + GROUP // 2), 0.125)
    def rises(pick, width):
        return [picks(lanes, pick, 1.0), to_sides(lanes, pick, width)]

    up_lo = jnp.concatenate(rises(lambda s, d: d // 2 == s, lanes), 1)
    up_hi = jnp.concatenate(rises(lambda s, d: d // 2 + half == s, lanes), 1)
    up_2 = jnp.concatenate(rises(swap(pick_2), half), 1)
    up_3 = jnp.concatenate([
        rise for g in range(groups)
        for rise in rises(lambda s, d: (d < GROUP) & (d // 2 + g * GROUP == s), GROUP)
    ], 1)

    def pair_rows(x, at=0):
        n, r, w = x.shape
        tmp[pl.ds(at, n * r), :] = flat(x)
        return tmp[pl.ds(at, n * r // 2, 2), :] + tmp[pl.ds(at + 1, n * r // 2, 2), :]

    def twice_rows(x, planes):
        parts_of = [x[:, at:at + lanes] for at in range(0, x.shape[1], lanes)]
        x = jnp.concatenate(parts_of, 0)
        r = x.shape[0]
        tmp[pl.ds(0, r, 2), :] = x
        tmp[pl.ds(1, r, 2), :] = x
        out = tmp[pl.ds(0, 2 * r), :].reshape(len(parts_of) * planes, -1, lanes)
        return [out[at:at + planes] for at in range(0, out.shape[0], planes)]

    def twice_planes(x):
        return jnp.broadcast_to(x[:, None], (x.shape[0], 2) + x.shape[1:]).reshape((2 * x.shape[0],) + x.shape[1:])

    def slab_pairs(x, at=0):
        s = pair_rows(x.reshape(depth // 2, 2, rows, lanes).sum(1), at)
        return s[:rows // 2], s[rows // 2:]

    def to_2(x):
        return dot(pair_rows(x), down_2).reshape(x.shape[0], rows // 4, lanes)

    lane = iota((rows // 8, lanes), 1)

    def turn(planes, off):
        out = []
        for k in range(groups):
            total = None
            for g in range(groups):
                by = (GROUP * (g - k) - off) % lanes
                moved = pltpu.roll(planes[g], by, 1) if by else planes[g]
                total = moved if total is None else jnp.where(lane // GROUP == g, moved, total)
            out.append(total[None])
        return jnp.concatenate(out, 0)

    def level_3(got):
        pairs = [got[0]] + [got[2 * i - 1] + got[2 * i] for i in range(1, parts // 2)] + [got[parts - 1]]
        out = []
        for k in range(groups):
            total = pairs[4 * k + 2]
            for i, keep in (
                (4 * k - 1, lane < GROUP), (4 * k, lane < 2 * GROUP), (4 * k + 1, lane < 3 * GROUP),
                (4 * k + 3, lane >= GROUP), (4 * k + 4, lane >= 2 * GROUP), (4 * k + 5, lane >= 3 * GROUP),
            ):
                if 0 <= i < len(pairs):
                    total = total + jnp.where(keep, pairs[i], 0.0)
            out.append(total)
        return turn(out, 0)

    def capacity_3(got):
        out = []
        for k in range(groups):
            total = None
            for g in range(groups):
                i = 2 * (4 * k + g)
                pair = got[i] + got[i + 1]
                total = pair if total is None else jnp.where(lane // GROUP == g, pair, total)
            out.append(total)
        return turn(out, GROUP // 2)

    def valid(start, count, of):
        at = start + iota((count, 1, 1), 0)
        return (at >= 0) & (at < of)

    own_span, next_span = 0, 1
    sent_rows, groups_of = [0, 0], {}

    def batch(pieces, total, group=None, side=own_span):
        at = groups_of.setdefault(group or len(groups_of), len(groups_of))
        count = total.size // lanes if hasattr(total, "size") else math.prod(total.shape) // lanes
        sent_rows[side] += count
        return [
            pltpu.make_async_remote_copy(
                source, target, send_sem.at[side], recv_sem.at[at], device_id=to, device_id_type=MESH)
            for source, target, to in pieces
        ], count, at, side

    def waiting(count, at, side):
        rows_of = spare.at[pl.ds(0, count)]
        return pltpu.make_async_remote_copy(
            rows_of, rows_of, send_sem.at[side], recv_sem.at[at], device_id=beside(1), device_id_type=MESH)

    def begin(made):
        for copy in made[0]:
            copy.start()

    def arrive(*made):
        assert len({one[2] for one in made}) == 1
        waiting(sum(one[1] for one in made), *made[0][2:]).wait_recv()

    def sent(side):
        waiting(sent_rows[side], 0, side).wait_send()

    def beside(k):
        return {"space": lax.rem(me + (k + parts) % parts, parts)}

    share = rows // 2
    my_rows = pl.ds(pl.multiple_of(span % 2 * share, share), share)

    def halo(buf, count, up, down, rows_at=None, group=None):
        def part(start):
            return buf.at[pl.ds(start, count)] if rows_at is None else buf.at[pl.ds(start, count), rows_at]

        total = buf.at[pl.ds(0, 2 * count)] if rows_at is None else buf.at[pl.ds(0, 2 * count), pl.ds(0, share)]
        return batch([(part(way[0]), part(way[1]), beside(k)) for way, k in ((up, 1), (down, -1))], total, group)

    def window(buf, source, nearest, reach, to={}, group=None, side=own_span):
        middle = buf.shape[0] // 2
        offsets = [k for far in range(reach, nearest - 1, -1) for k in ((far, -far) if far else (0,))]
        return batch([(source, buf.at[middle - k], {**beside(k), **to}) for k in offsets], buf.at[pl.ds(0, len(offsets))], group, side)

    def hops(k):
        z, y = k // 4, k % 4
        return min(z, parts // 4 - z) + min(y, 4 - y)

    def gather(buf, source, offsets, to={}, group=None, side=own_span):
        offsets = sorted(offsets, key=lambda k: -hops(k))
        return batch([(source, buf.at[me], {**beside(k), **to}) for k in offsets], buf.at[pl.ds(0, len(offsets))], group, side)

    d = depth
    onward = {"tm": (span + 1) % spans}
    near = halo(c0, 2, (2 * d - 1, d - 1), (d + 1, 2 * d + 1), group="near")
    far = halo(c0, 1, (2 * d - 2, d - 2), (d + 3, 2 * d + 3), group="far")
    known = halo(src1, 2, (d, 0), (2, d + 2))
    third = halo(c1x, 1, (d, 0), (5, d + 5))
    cap_near = halo(cap, 1, (2 * d - 1, d - 1), (d, 2 * d), group="near")
    cap_far = halo(cap, 2, (d + 1, 1), (d + 1, 2 * d + 1), my_rows)
    pass_far = batch(
        [
            (cap.at[pl.ds(start, 2), my_rows], cap.at[pl.ds(start, 2), my_rows], {"tm": span + 1 - 2 * (span % 2)})
            for start in (1, 2 * d + 1)
        ], cap.at[pl.ds(0, 4), pl.ds(0, share)], "far")
    half_block = pl.ds(pl.multiple_of(span % 2 * (share // 2), share // 2), share // 2)
    half_total = cw.at[pl.ds(0, 2), pl.ds(0, share // 2)]
    cap_window = window(cw, cw.at[2], 1, 1, group="first"), batch(
        [(cw.at[2, half_block], cw.at[2 - k, half_block], beside(k)) for k in (2, -2)], half_total)
    pass_window = batch(
        [(cw.at[i, half_block], cw.at[i, half_block], {"tm": span + 1 - 2 * (span % 2)}) for i in (0, 4)], half_total)
    cap2_window = window(kw, kw.at[5], 1, 2, group="first"), window(kw, kw.at[5], 3, 5)
    to_next = {"to": onward, "group": "next", "side": next_span}
    gather_r = gather(gr.at[0], gr.at[0, me], range(1, parts), group="own"), gather(gr.at[1], r_sent, range(parts), **to_next)
    c_window = window(vw.at[0], vw.at[0, 3], 1, 3, group="own"), window(vw.at[1], c_sent, 0, 2, **to_next)
    b_window = window(bw.at[0], bw.at[0, 6], 1, 6, group="own"), window(bw.at[1], b_sent, 0, 6, **to_next)
    fin_onward = batch([(fin.at[0], fin.at[1], onward)], fin.at[0], "next", next_span)

    loaded = spare.at[pl.ds(0, 3 * depth * rows)]
    pltpu.make_async_copy(loaded, loaded, in_sem.at[0]).wait()
    mine = cap[d:2 * d]
    b = mine * u0[...] + src0[...]
    own[...] = b
    c0[d + 1:2 * d + 1] = b * (W / (mine + 6.0))

    pl.semaphore_wait(barrier, len(close) + 2)
    begin(near)
    begin(cap_near)
    for k in (NEAR, -NEAR):
        pl.semaphore_signal(near_sem, inc=1, device_id=beside(k), device_id_type=MESH)
    cap1 = dot(jnp.concatenate(slab_pairs(mine), 1), down_cap1)
    cw[2] = cap1
    begin(cap_window[0])
    cap2 = to_2(cap1[None])
    kw[5] = cap2[0, :rows // 8] + pltpu.roll(cap2[0, rows // 8:], GROUP, 1)
    begin(cap2_window[0])
    begin(cap_far)
    begin(cap_window[1])
    begin(far)
    pl.semaphore_wait(near_sem, 2)
    for k in (2 * NEAR, -2 * NEAR):
        pl.semaphore_signal(far_sem, inc=1, device_id=beside(k), device_id_type=MESH)
    begin(cap2_window[1])
    cap_sent = dot(pair_rows(cap2), down_cap)
    loads[3].wait()

    def weights(start, count):
        inside = valid((me - 1) * depth + start, count, parts * depth)
        return jnp.where(inside, W / (cap[start:start + count] + 6.0), 0.0)

    def inverse(diagonal, start, reach):
        return jnp.where(valid(me - reach + start, diagonal.shape[0], parts), W / diagonal, 0.0)

    def planes_of(buf, own, start, count):
        return jnp.where(valid(me * depth + start - own, count, parts * depth), buf[start:start + count], 0.0)

    def inverse_1(start, stop):
        diagonal = cw[start:stop] + 3.0
        return diagonal, inverse(diagonal, start, 2)

    def inverse_2(start, stop):
        packed = kw[start:stop]
        diagonal = jnp.concatenate([packed, pltpu.roll(packed, lanes - GROUP, 2)], 1) + 1.5
        return diagonal, jnp.where(iota(diagonal.shape, 2) < GROUP, inverse(diagonal, start, 5), 0.0)

    arrive(cap_near, near)
    a = weights(d - 1, d + 2)

    assert len(groups_of) == 11 and max(sent_rows) <= spare.shape[0]

    def first_sweeps(b, c, a):
        x = 1.2 * c[1:-1] + a * sum_inner(c, lanes)
        inner = x[1:-1]
        r = b - (cap[d:2 * d] + 6.0) * inner + up_down(inner) + (x[:-2] + x[2:])
        (r_lo, r_hi), (x_lo, x_hi) = slab_pairs(r), slab_pairs(inner, depth * rows // 2)
        return x, dot(jnp.concatenate([r_lo, x_lo, r_hi, x_hi], 1), down_0)

    def spread(b1, c1, i1, d1, a1, i2, d2, a2):
        c1 = plane_padded(c1[None], 1)
        y1 = 1.2 * c1 + a1 * sum_packed(c1, half)
        r1 = pair_rows(plane_padded(b1[None], 1) - d1 * y1 + 0.5 * up_down(y1))
        y1 = pair_rows(y1, 3 * rows // 2)
        n = rows // 4
        none = jnp.zeros((n, lanes), F32)
        around = jnp.concatenate([none, y1[:-n]], 0), jnp.concatenate([y1[n:], none], 0)
        b2 = dot(jnp.concatenate([r1, y1, *around], 1), down_1).reshape(3, n, lanes)
        c2 = plane_padded(b2 * i2[1:4], 1)
        y2 = 1.2 * c2 + a2 * sum_planes(c2)
        r2 = plane_padded(b2, 2) - plane_padded(d2 * y2, 1)
        y2 = plane_padded(y2, 1)
        before, after = shifted(y2)
        r2s[0, 1:8] = r2 + 0.25 * (up_down(y2) + (before + after))
        r2s[1, 1:8] = y2
        pairs = [
            pair_rows(r2s[i, pl.ds(me % 2, 8)].reshape(4, 2, n, lanes).sum(1), i * 4 * n)
            for i in range(2)
        ]
        b3 = dot(jnp.concatenate(pairs, 1), down_3).reshape(4, n // 2, lanes)
        first = (me + 4 + me % 2) // 2
        return b2, sum(jnp.where(lane // GROUP == (first + q) % groups, b3[q], 0.0) for q in range(4))

    def side_by_side(b2):
        return b2[1] + (pltpu.roll(b2[0], GROUP, 1) + pltpu.roll(b2[2], 2 * GROUP, 1))

    def level_2(t, c3, i2, a2, a3):
        b = jnp.where(valid(me - 6, 13, parts), bw[t], 0.0)
        b2 = b[1:-1] + (pltpu.roll(b[2:], lanes - GROUP, 2) + pltpu.roll(b[:-2], lanes - 2 * GROUP, 2))
        c2 = b2 * i2
        y2 = 1.2 * c2[1:-1] + a2 * sum_planes(c2)[1:-1]
        c2 = c2[1:-1]
        y2 = ((0.2 * y2 + c2) + a2 * sum_planes(y2))[1:-1]
        y3 = dot(flat(coarse_solve(c3, a3)), up_3)
        for g in range(groups):
            y3s[2 + 4 * g:6 + 4 * g] = y3[:, 2 * g * lanes:2 * (g + 1) * lanes].reshape(4, rows // 8, 2 * lanes)
        lift, sides = [
            jnp.where(me % 2 == 1, x[1:], x[:-1]) for x in
            [twice_planes(x) for x in twice_rows(y3s[pl.ds(me // 2, 5)].reshape(5 * rows // 8, 2 * lanes), 5)]
        ]
        total = (sides + up_down(lift))[1:-1] + (lift[:-2] + lift[2:])
        y2 = y2 + (0.2 * lift[1:-1] + a2[1:-1] * total)
        y2 = ((0.2 * y2 + c2[1:-1]) + a2[1:-1] * sum_planes(y2))[1:-1]
        return twice_rows(dot(flat(y2), up_2), 5)

    def swept_1(y1, lift, sides, a1):
        before, after = shifted(lift)
        across = lift + jnp.where(iota(lift.shape, 2) < half, before, after)
        return y1 + (0.2 * lift + a1 * ((sides + up_down(lift)) + across))

    def lift_0(y1, skip):
        n = rows // 2
        around = flat(y1)
        both = dot(around, up_lo), dot(around, up_hi)
        halves = [part[n * k:n * k + n] for k in range(3) for part in both]
        halves = halves[skip:len(halves) - skip]
        return [twice_planes(x) for x in twice_rows(jnp.concatenate(halves, 0), len(halves))]

    def swept_0(lift, sides, a):
        total = (sides + up_down(lift))[1:-1] + (lift[:-2] + lift[2:])
        return 0.2 * lift[1:-1] + a * total

    x, b1 = first_sweeps(own[...], planes_of(c0, d + 1, d - 1, d + 4), a)
    arrive(cap_window[0], cap2_window[0])
    d1, i1 = inverse_1(1, 4)
    d2, i2 = inverse_2(3, 8)
    near_1 = i1, d1, 0.5 * i1, i2, d2, 0.25 * i2
    c1 = b1 * i1[1]
    vw[0, 3] = c1
    b2, b3 = spread(b1, c1, *near_1)
    gr[0, me] = b3 + cap_sent
    bw[0, 6] = side_by_side(b2)
    pl.semaphore_wait(far_sem, 2)
    begin(gather_r[0])
    begin(b_window[0])
    begin(c_window[0])
    arrive(cap_far)
    begin(pass_far)
    arrive(cap_window[1])
    begin(pass_window)
    arrive(far, pass_far)
    wide = weights(1, 3 * d - 2)
    c = planes_of(c0, d + 1, d - 2, d + 6)
    first = 1.2 * c[1:2] + wide[1:2] * sum_inner(c[0:3], lanes)
    final = 1.2 * c[-2:-1] + wide[-2:-1] * sum_inner(c[-3:], lanes)

    def last_sweeps(x, c):
        x = (0.2 * x[1:-1] + c) + a * sum_inner(x, lanes)
        return (0.2 * x[1:-1] + c[1:-1]) + a[1:-1] * sum_inner(x, lanes)

    alone = last_sweeps(jnp.concatenate([first, x, final], 0), c[2:-2])
    fp_ref[...] = alone
    src1[2:d + 2] = cap[d:2 * d] * alone + src1[2:d + 2]
    begin(known)
    arrive(pass_window)
    a1 = 0.5 * inverse_1(0, 5)[1]
    arrive(cap2_window[1])
    i2 = inverse_2(0, 11)[1]
    a2 = 0.25 * i2[1:-1]
    arrive(gather_r[0], b_window[0], c_window[0])

    got = gr[0]
    cap3 = capacity_3(got)
    i3 = jnp.where(iota(cap3.shape, 2) % GROUP < GROUP // 2, W / (cap3 + 0.75), 0.0)
    a3 = 0.125 * i3
    c1 = jnp.where(valid(me - 3, 7, parts), vw[0], 0.0)
    y1 = 1.2 * c1[1:-1] + a1 * sum_packed(c1, half)[1:-1]
    c1 = c1[1:-1]
    y1 = (0.2 * y1 + c1) + a1 * sum_packed(y1, half)
    y1 = swept_1(y1, *level_2(0, level_3(got) * i3, i2, a2, a3), a1)
    y1 = ((0.2 * y1 + c1) + a1 * sum_packed(y1, half))[1:-1]
    x = swept_0(*lift_0(y1, 0), wide)
    x = 0.2 * x[1:-1] + wide[1:-1] * sum_inner(x, lanes)
    fp_ref[...] = fp_ref[...] + x[2:-2]
    arrive(known)
    b = cap[2:3 * d - 2] * x + src1[...]
    c1x[1:d + 5] = b * wide[1:-1]
    begin(third)

    x, b1 = first_sweeps(b[2:-2], c1x[1:d + 5], a)
    c1 = b1 * i1[1]
    c_sent[...] = c1
    b2, b3 = spread(b1, c1, *near_1)
    r_sent[...] = b3
    b_sent[...] = side_by_side(b2)

    @pl.when(span < spans - 1)
    def _():
        begin(gather_r[1])
        begin(b_window[1])
        begin(c_window[1])

    arrive(third)
    c = planes_of(c1x, 3, 0, d + 6)
    first = 1.2 * c[1:2] + wide[1:2] * sum_inner(c[0:3], lanes)
    final = 1.2 * c[-2:-1] + wide[-2:-1] * sum_inner(c[-3:], lanes)
    fin[0] = last_sweeps(jnp.concatenate([first, x, final], 0), c[2:-2])

    @pl.when(span < spans - 1)
    def _():
        begin(fin_onward)

    sent(own_span)

    @pl.when(span == 0)
    def _():
        up_ref[...] = u0[...]

    @pl.when(span > 0)
    def _():
        arrive(gather_r[1], b_window[1], c_window[1], fin_onward)
        c1 = jnp.where(valid(me - 2, 5, parts), vw[1, 1:6], 0.0)
        y1 = 1.2 * c1 + a1 * sum_packed(c1, half)
        y1 = (0.2 * y1 + c1) + a1 * sum_packed(y1, half)
        y1 = swept_1(y1, *level_2(1, level_3(gr[1]) * i3, i2, a2, a3), a1)[1:-1]
        y1 = (0.2 * y1 + c1[1:-1]) + a1[1:-1] * sum_packed(y1, half)
        x = swept_0(*lift_0(y1, 1), a)
        up_ref[...] = fin[1] + (0.2 * x[1:-1] + a[1:-1] * sum_inner(x, lanes))

    @pl.when(span < spans - 1)
    def _():
        sent(next_span)


def shards(span_opening, source_power, warmth_retention):
    parts, spans = lax.axis_size("space"), lax.axis_size("tm")
    steps = source_power.shape[1]
    depth, rows, lanes = warmth_retention.shape
    assert steps == 2 and depth == 4
    slab = jax.ShapeDtypeStruct((depth, rows, lanes), F32)
    vmem = pl.BlockSpec(memory_space=pltpu.VMEM)
    dma = pltpu.SemaphoreType.DMA
    fpoint, updated = pl.pallas_call(
        functools.partial(kernel, parts, spans, steps),
        out_shape=(pltpu.VMEM(slab.shape, F32),) * 2,
        in_specs=[pl.BlockSpec(memory_space=pl.ANY)] * 3,
        out_specs=(vmem, vmem),
        scratch_shapes=[
            pltpu.VMEM((depth, rows, lanes), F32),
            pltpu.VMEM((depth, rows, lanes), F32),
            pltpu.VMEM((depth + 4, rows, lanes), F32),
            pltpu.VMEM((3 * depth, rows, lanes), F32),
            pltpu.VMEM((3 * depth + 2, rows, lanes), F32),
            pltpu.VMEM((depth + 6, rows, lanes), F32),
            pltpu.VMEM((5, rows // 2, lanes), F32),
            pltpu.VMEM((11, rows // 8, lanes), F32),
            pltpu.VMEM((steps, 7, rows // 2, lanes), F32),
            pltpu.VMEM((rows // 2, lanes), F32),
            pltpu.VMEM((steps, 13, rows // 4, lanes), F32),
            pltpu.VMEM((rows // 4, lanes), F32),
            pltpu.VMEM((steps, parts, rows // 8, lanes), F32),
            pltpu.VMEM((rows // 8, lanes), F32),
            pltpu.VMEM((2, 9, rows // 4, lanes), F32),
            pltpu.VMEM((parts // 2 + 4, rows // 8, 2 * lanes), F32),
            pltpu.VMEM((depth, rows, lanes), F32),
            pltpu.VMEM((12 * rows, lanes), F32),
            pltpu.VMEM((2, depth, rows, lanes), F32),
            pltpu.VMEM((2048, lanes), F32),
            pltpu.SemaphoreType.REGULAR,
            pltpu.SemaphoreType.REGULAR,
            dma((2,)), dma((2,)), dma((11,)),
        ],
        compiler_params=pltpu.CompilerParams(
            collective_id=0, has_side_effects=True, vmem_limit_bytes=67043328 - 2 * 4 * slab.size
        ),
    )(span_opening[0], source_power[0], warmth_retention)
    flag = lax.axis_index("tm") > spans
    fpoint, updated = jnp.where(flag, updated, fpoint), jnp.where(flag, fpoint, updated)
    return fpoint[None], updated[None]


def solution(mesh):
    in_specs = (
        P("tm", "space", None, None),
        P("tm", None, "space", None, None),
        P("space", None, None),
    )
    out_specs = (P("tm", "space", None, None), P("tm", "space", None, None))
    return jax.shard_map(shards, mesh=mesh, in_specs=in_specs, out_specs=out_specs, check_vma=False)
```
